32 devices in a mesh: dp: 1 (over z), yax: 4 (over y), xax: 8 (over x, core).
Axes of the slice: x: 4, y: 4, z: 1, core: 2. Of those that a mesh axis runs over, the one named last changes fastest.
The devices are a block of a 4x4x8 slice.
Arguments:
- hidden: bfloat16 [1024, 1024], P('dp', 'xax')
- cache_len: int32 [1024], P('dp')
- k_cache: bfloat16 [1024, 4096, 64], P(('dp', 'yax', 'xax'))
- v_cache: bfloat16 [1024, 4096, 64], P(('dp', 'yax', 'xax'))
- g_attn: float32 [1024], P('xax')
- w_query: bfloat16 [1024, 1024], P('xax', 'yax')
- w_key: bfloat16 [1024, 64], P('xax')
- w_value: bfloat16 [1024, 64], P('xax')
- w_gate: bfloat16 [1024, 4096], P('xax', 'yax')
- w_up: bfloat16 [1024, 4096], P('xax', 'yax')
- w_out: bfloat16 [1024, 1024], P('yax', 'xax')
- w_down: bfloat16 [4096, 1024], P('yax', 'xax')
- g_final: float32 [1024], P('xax')
- embedding: bfloat16 [50304, 1024], P('yax', 'xax')
Outputs:
- output 1: bfloat16 [1024, 64], P(('dp', 'yax', 'xax'))
- output 2: bfloat16 [1024, 64], P(('dp', 'yax', 'xax'))
- output 3: float32 [1024, 50304], P('dp', ('yax', 'xax'))
- output 4: float32 [1024], P('dp')
All inputs are finite; a program needn't handle non-finite values.
Results may differ from the reference program's by a relative error of at most 0.00831753.
Values are sent between devices in bfloat16 or wider.
A program may use at most 768 MiB of HBM per device.

```python
import jax
import jax.numpy as jnp
from jax import lax

D = 1024
HEADS = 16
HEAD = 64
FF = 4096
VOCAB = 50304
BATCH = 1024
SEQ = 4096
ROW_BLOCK = 16

EPS = 1e-6
ROPE_BASE = 10000.0


def draw_lengths(key):
    drawn = jax.random.randint(key, (BATCH,), 1, SEQ, dtype=jnp.int32)
    row_ids = jnp.arange(BATCH)
    return jnp.where(row_ids == 0, SEQ - 1, jnp.where(row_ids == 1, 1, drawn)).astype(jnp.int32)


def setup_inputs(seed: int = 0, part: int = 0) -> dict:
    base_key = jax.random.key(seed)
    shared = jax.random.split(base_key, 10)
    own = jax.random.split(jax.random.fold_in(base_key, part), 5)

    def weight(key, shape, fan_in, gain):
        return (gain * fan_in ** -0.5 * jax.random.normal(key, shape, jnp.float32)).astype(jnp.bfloat16)

    col_scale = jnp.exp(0.5 * jax.random.normal(own[0], (D,), jnp.float32))
    hidden = jax.random.normal(own[1], (BATCH, D), jnp.float32) * col_scale
    k_cache = 2.5 * jax.random.normal(own[3], (BATCH, SEQ, HEAD), jnp.float32)
    v_cache = 2.0 * jax.random.normal(own[4], (BATCH, SEQ, HEAD), jnp.float32)
    return {
        "hidden": hidden.astype(jnp.bfloat16),
        "cache_len": draw_lengths(own[2]),
        "k_cache": k_cache.astype(jnp.bfloat16),
        "v_cache": v_cache.astype(jnp.bfloat16),
        "g_attn": 1.0 + 0.3 * jax.random.normal(shared[0], (D,), jnp.float32),
        "w_query": weight(shared[1], (D, HEADS * HEAD), D, 1.0),
        "w_key": weight(shared[2], (D, HEAD), D, 1.0),
        "w_value": weight(shared[3], (D, HEAD), D, 1.0),
        "w_gate": weight(shared[4], (D, FF), D, 1.0),
        "w_up": weight(shared[5], (D, FF), D, 1.0),
        "w_out": weight(shared[6], (HEADS * HEAD, D), HEADS * HEAD, 1.0),
        "w_down": weight(shared[7], (FF, D), FF, 1.0),
        "g_final": 1.0 + 0.3 * jax.random.normal(shared[8], (D,), jnp.float32),
        "embedding": weight(shared[9], (VOCAB, D), D, 2.0),
    }


def layer_norm(values_in, gain):
    row_mean = jnp.mean(values_in, axis=-1, keepdims=True)
    row_var = jnp.mean(jnp.square(values_in - row_mean), axis=-1, keepdims=True)
    return (values_in - row_mean) * lax.rsqrt(row_var + EPS) * gain


def rope_angle(positions):
    half_dim = HEAD // 2
    inv_freq = ROPE_BASE ** (-(jnp.arange(half_dim, dtype=jnp.float32) * 2.0) / HEAD)
    return positions.astype(jnp.float32)[:, None] * inv_freq[None, :]


def rotary(values_in, angles):
    half_dim = values_in.shape[-1] // 2
    cos_a = jnp.cos(angles)
    sin_a = jnp.sin(angles)
    first = values_in[..., :half_dim]
    second = values_in[..., half_dim:]
    return jnp.concatenate([first * cos_a - second * sin_a, second * cos_a + first * sin_a], axis=-1)


def attend_block(block):
    q_blk, kc_blk, vc_blk, kn_blk, vn_blk, len_blk = block
    positions = jnp.arange(SEQ)
    at_slot = positions[None, :, None] == len_blk[:, None, None]
    keys_all = jnp.where(at_slot, kn_blk[:, None, :], kc_blk)
    values_all = jnp.where(at_slot, vn_blk[:, None, :], vc_blk)
    scores = jnp.einsum("rhe,rse->rhs", q_blk.astype(jnp.float32), keys_all.astype(jnp.float32)) * HEAD ** -0.5
    valid = positions[None, None, :] <= len_blk[:, None, None]
    scores = jnp.where(valid, scores, -jnp.inf)
    prob_all = jax.nn.softmax(scores, axis=-1).astype(jnp.bfloat16)
    mixed = jnp.einsum("rhs,rse->rhe", prob_all.astype(jnp.float32), values_all.astype(jnp.float32))
    return mixed.astype(jnp.bfloat16)


def reference(hidden, cache_len, k_cache, v_cache, g_attn, w_query, w_key, w_value,
              w_gate, w_up, w_out, w_down, g_final, embedding):
    residual = hidden.astype(jnp.float32)
    normed = layer_norm(residual, g_attn).astype(jnp.bfloat16)
    query = jnp.dot(normed, w_query, preferred_element_type=jnp.float32).astype(jnp.bfloat16)
    key_new = jnp.dot(normed, w_key, preferred_element_type=jnp.float32).astype(jnp.bfloat16)
    value_new = jnp.dot(normed, w_value, preferred_element_type=jnp.float32).astype(jnp.bfloat16)
    gate = jnp.dot(normed, w_gate, preferred_element_type=jnp.float32).astype(jnp.bfloat16)
    up_val = jnp.dot(normed, w_up, preferred_element_type=jnp.float32).astype(jnp.bfloat16)
    angles = rope_angle(cache_len)
    query = rotary(query.astype(jnp.float32).reshape(BATCH, HEADS, HEAD), angles[:, None, :]).astype(jnp.bfloat16)
    key_new = rotary(key_new.astype(jnp.float32), angles).astype(jnp.bfloat16)
    blocks = BATCH // ROW_BLOCK
    attn_out = lax.map(attend_block, (
        query.reshape(blocks, ROW_BLOCK, HEADS, HEAD),
        k_cache.reshape(blocks, ROW_BLOCK, SEQ, HEAD),
        v_cache.reshape(blocks, ROW_BLOCK, SEQ, HEAD),
        key_new.reshape(blocks, ROW_BLOCK, HEAD),
        value_new.reshape(blocks, ROW_BLOCK, HEAD),
        cache_len.reshape(blocks, ROW_BLOCK)))
    attn_out = attn_out.reshape(BATCH, HEADS * HEAD)
    mlp_act = (jax.nn.silu(gate.astype(jnp.float32)) * up_val.astype(jnp.float32)).astype(jnp.bfloat16)
    branch_sum = (jnp.dot(attn_out, w_out, preferred_element_type=jnp.float32)
                  + jnp.dot(mlp_act, w_down, preferred_element_type=jnp.float32))
    residual_out = residual + branch_sum
    final_norm = layer_norm(residual_out, g_final).astype(jnp.bfloat16)
    logits = jnp.dot(final_norm, embedding.T, preferred_element_type=jnp.float32)
    log_norm = jax.nn.logsumexp(logits, axis=-1)
    return key_new, value_new, logits - log_norm[:, None], log_norm
```

```python
import jax
import jax.numpy as jnp
from jax import lax
from jax.sharding import PartitionSpec as P

EPS = 1e-6
ROPE_BASE = 10000.0


def rope_angle(positions, head_dim):
    half_dim = head_dim // 2
    inv_freq = ROPE_BASE ** (-(jnp.arange(half_dim, dtype=jnp.float32) * 2.0) / head_dim)
    return positions.astype(jnp.float32)[:, None] * inv_freq[None, :]


def rotary(values_in, angles):
    half_dim = values_in.shape[-1] // 2
    cos_a = jnp.cos(angles)
    sin_a = jnp.sin(angles)
    first = values_in[..., :half_dim]
    second = values_in[..., half_dim:]
    return jnp.concatenate([first * cos_a - second * sin_a, second * cos_a + first * sin_a], axis=-1)


def sharded_norm(values_in, gain, width):
    stats = jnp.stack([jnp.sum(values_in, axis=-1), jnp.sum(values_in * values_in, axis=-1)])
    stats = lax.psum(stats, "xax")
    row_mean = stats[0] / width
    row_var = stats[1] / width - row_mean * row_mean
    return (values_in - row_mean[:, None]) * lax.rsqrt(row_var + EPS)[:, None] * gain


def attend_local(query, k_cache, v_cache, key_new, value_new, lengths):
    score_scale = query.shape[-1] ** -0.5
    scores = jnp.einsum("bhe,bse->bhs", query, k_cache, preferred_element_type=jnp.float32) * score_scale
    score_new = jnp.einsum("bhe,be->bh", query, key_new, preferred_element_type=jnp.float32) * score_scale
    valid = jnp.arange(k_cache.shape[1])[None, None, :] < lengths[:, None, None]
    row_max = jnp.maximum(jnp.max(jnp.where(valid, scores, -jnp.inf), axis=-1), score_new)
    weights = jnp.where(valid, jnp.exp(scores - row_max[..., None]), 0.0)
    weight_new = jnp.exp(score_new - row_max)
    denominator = jnp.sum(weights, axis=-1) + weight_new
    prob_all = (weights / denominator[..., None]).astype(jnp.bfloat16)
    prob_new = (weight_new / denominator).astype(jnp.bfloat16)
    attn_out = jnp.einsum("bhs,bse->bhe", prob_all, v_cache, preferred_element_type=jnp.float32)
    attn_out = attn_out + prob_new.astype(jnp.float32)[..., None] * value_new.astype(jnp.float32)[:, None, :]
    return attn_out.astype(jnp.bfloat16)


def solution(mesh):
    y_size = mesh.shape["yax"]
    x_size = mesh.shape["xax"]
    row_spec = P(("dp", "yax", "xax"))

    def local_step(hidden, cache_len, k_cache, v_cache, g_attn, w_query, w_key, w_value,
                   w_gate, w_up, w_out, w_down, g_final, embedding):
        rows = hidden.shape[0]
        width = hidden.shape[1] * x_size
        own_rows = k_cache.shape[0]
        head_dim = k_cache.shape[2]
        q_cols = w_query.shape[1]
        kv_end = q_cols + 2 * head_dim
        ff_end = kv_end + w_gate.shape[1]
        y_idx = lax.axis_index("yax")
        x_idx = lax.axis_index("xax")
        own_start = (y_idx * x_size + x_idx) * own_rows

        embed_full = lax.all_to_all(embedding, "xax", 0, 1, tiled=True)
        residual = hidden.astype(jnp.float32)
        normed = sharded_norm(residual, g_attn, width).astype(jnp.bfloat16)
        proj_part = jnp.concatenate([
            jnp.dot(normed, w_query, preferred_element_type=jnp.float32),
            jnp.dot(normed, w_key, preferred_element_type=jnp.float32),
            jnp.dot(normed, w_value, preferred_element_type=jnp.float32),
            jnp.dot(normed, w_gate, preferred_element_type=jnp.float32),
            jnp.dot(normed, w_up, preferred_element_type=jnp.float32)], axis=1)
        projected = lax.psum(proj_part, "xax").astype(jnp.bfloat16)
        angles = rope_angle(cache_len, head_dim)
        query = projected[:, :q_cols].astype(jnp.float32).reshape(rows, q_cols // head_dim, head_dim)
        query = rotary(query, angles[:, None, :]).astype(jnp.bfloat16)
        key_new = rotary(projected[:, q_cols:q_cols + head_dim].astype(jnp.float32), angles).astype(jnp.bfloat16)
        value_new = projected[:, q_cols + head_dim:kv_end]
        gate = projected[:, kv_end:ff_end]
        up_val = projected[:, ff_end:]

        query_grp = lax.all_to_all(query, "yax", 0, 1, tiled=True)
        query_own = lax.dynamic_slice_in_dim(query_grp, x_idx * own_rows, own_rows, axis=0)
        key_own = lax.dynamic_slice_in_dim(key_new, own_start, own_rows, axis=0)
        value_own = lax.dynamic_slice_in_dim(value_new, own_start, own_rows, axis=0)
        len_own = lax.dynamic_slice_in_dim(cache_len, own_start, own_rows, axis=0)
        attn_own = attend_local(query_own, k_cache, v_cache, key_own, value_own, len_own)
        attn_grp = lax.all_gather(attn_own, "xax", axis=0, tiled=True)
        attn_heads = lax.all_to_all(attn_grp, "yax", 1, 0, tiled=True).reshape(rows, q_cols)

        mlp_act = (jax.nn.silu(gate.astype(jnp.float32)) * up_val.astype(jnp.float32)).astype(jnp.bfloat16)
        branch_sum = (jnp.dot(attn_heads, w_out, preferred_element_type=jnp.float32)
                      + jnp.dot(mlp_act, w_down, preferred_element_type=jnp.float32))
        residual_out = residual + lax.psum(branch_sum, "yax")
        final_norm = sharded_norm(residual_out, g_final, width).astype(jnp.bfloat16)
        final_full = lax.all_gather(final_norm, "xax", axis=1, tiled=True)
        logits = jnp.einsum("bd,vd->bv", final_full, embed_full, preferred_element_type=jnp.float32)
        part_max = jnp.max(logits, axis=1)
        part_sum = jnp.sum(jnp.exp(logits - part_max[:, None]), axis=1)
        parts = lax.all_gather(jnp.stack([part_max, part_sum]), ("yax", "xax"), axis=0)
        row_max = jnp.max(parts[:, 0], axis=0)
        sum_exp = jnp.sum(parts[:, 1] * jnp.exp(parts[:, 0] - row_max), axis=0)
        log_norm = row_max + jnp.log(sum_exp)
        return key_own, value_own, logits - log_norm[:, None], log_norm

    in_specs = (P("dp", "xax"), P("dp"), row_spec, row_spec, P("xax"), P("xax", "yax"),
                P("xax", None), P("xax", None), P("xax", "yax"), P("xax", "yax"),
                P("yax", "xax"), P("yax", "xax"), P("xax"), P("yax", "xax"))
    out_specs = (row_spec, row_spec, P("dp", ("yax", "xax")), P("dp"))
    return jax.shard_map(local_step, mesh=mesh, in_specs=in_specs, out_specs=out_specs, check_vma=False)
```

```python
import functools

import jax
import jax.numpy as jnp
import numpy as np
from jax import lax
from jax.experimental import pallas as pl
from jax.experimental.pallas import tpu as pltpu
from jax.sharding import PartitionSpec as P

EPS = 1e-6
ROPE_BASE = 10000.0
F32 = jnp.float32
BF16 = jnp.bfloat16
NT = (((1,), (1,)), ((), ()))
EMBED_CHUNKS = 8


def layer_norm(values_in, gain):
    mean = jnp.mean(values_in, axis=-1, keepdims=True)
    centred = values_in - mean
    var = jnp.mean(centred * centred, axis=-1, keepdims=True)
    return centred * lax.rsqrt(var + EPS) * gain


def row_chunks(total, count):
    tiles = total // 8
    cuts = [8 * (tiles * i // count) for i in range(count + 1)]
    return [(cuts[i], cuts[i + 1] - cuts[i]) for i in range(count)]


def kernel(cfg, lens, hidden, k_hbm, v_hbm, g_attn, g_final, w_query, w_key, w_value, w_gate, w_up,
           w_out, w_down, embed, freq,
           k_out, v_out, logits_out, norm_out,
           k_buf, v_buf, h_buf, ga_buf, gf_buf, wqt, wq_buf, gu_buf, down_buf, out_buf, kv_buf,
           n_buf, q_scr, qx_buf, q2d, snew, krep, vrep, s_scr, od_scr, o_scr, ox_buf, act, part_scr,
           rs_buf, f_buf, e_buf, e_al, z_scr, st_scr, st_buf,
           kv_sem, own_sem, z_sem, x_send, x_recv, y_send, y_recv, e_send, e_recv,
           f_send, f_recv, p_send, p_recv, s_send, s_recv):
    ys, xs, own, vocab, shift = cfg
    y = lax.axis_index("yax")
    x = lax.axis_index("xax")
    core = lax.rem(x, 2)
    partner = x + 1 - 2 * core
    blk = hidden.shape[1]
    quarter = xs * own
    head_dim = k_hbm.shape[1]
    half = head_dim // 2
    seqs = k_hbm.shape[0]
    slots = k_hbm.shape[2]
    heads = w_query.shape[1] * ys // head_dim
    groups = k_buf.shape[0]
    per = seqs // groups
    window = e_buf.shape[0]

    def lanes(i):
        return pl.ds(pl.multiple_of(i * blk, 128), blk)

    def rows(i, n):
        return pl.ds(pl.multiple_of(i * n, n), n)

    def cache_copy(g, src, dst, s):
        return pltpu.make_async_copy(src.at[pl.ds(g * per, per)], dst.at[g], kv_sem.at[s, g])

    def start_cache(g, carry):
        cache_copy(g, k_hbm, k_buf, 0).start()
        return carry
    lax.fori_loop(0, groups, start_cache, 0)

    wqt[...] = w_query[...].astype(F32).T.astype(BF16)

    barrier = pltpu.get_barrier_semaphore()

    def signal_all(i, carry):
        py = lax.rem(y + i // xs, ys)
        px = lax.rem(x + lax.rem(i, xs), xs)
        pl.semaphore_signal(barrier, inc=1, device_id={"yax": py, "xax": px},
                            device_id_type=pl.DeviceIdType.MESH)
        return carry
    lax.fori_loop(1, ys * xs, signal_all, 0)
    pl.semaphore_wait(barrier, ys * xs - 1)

    cols = wqt.shape[0] // xs
    ff = w_gate.shape[1] // xs
    x_kinds = {
        "hidden": (lambda p: hidden.at[rows(y, quarter), :], lambda s: h_buf.at[:, lanes(s)]),
        "wq": (lambda p: wqt.at[rows(p, cols), :], lambda s: wq_buf.at[y, :, lanes(s)]),
        "ga": (lambda p: g_attn, lambda s: ga_buf.at[:, lanes(s)]),
        "gf": (lambda p: g_final, lambda s: gf_buf.at[:, lanes(s)]),
        "wk": (lambda p: w_key, lambda s: kv_buf.at[pl.ds(0, head_dim), lanes(s)]),
        "wv": (lambda p: w_value, lambda s: kv_buf.at[pl.ds(head_dim, head_dim), lanes(s)]),
        "wo": (lambda p: w_out.at[rows(p, cols), :], lambda s: out_buf.at[y, :, lanes(s)]),
        "gate": (lambda p: w_gate.at[:, lanes(p)], lambda s: gu_buf.at[y, rows(s, blk), pl.ds(0, ff)]),
        "up": (lambda p: w_up.at[:, lanes(p)], lambda s: gu_buf.at[y, rows(s, blk), pl.ds(ff, ff)]),
        "down": (lambda p: w_down.at[rows(p, ff), :], lambda s: down_buf.at[y, :, lanes(s)]),
        "q": (lambda p: q_scr.at[rows(p, own), :], lambda s: qx_buf.at[s]),
        "o": (lambda p: o_scr.at[p], lambda s: ox_buf.at[rows(s, own), :]),
        "rs": (lambda p: part_scr.at[rows(p, own), :], lambda s: rs_buf.at[s]),
    }
    x_index = {name: i for i, name in enumerate(x_kinds)}

    def x_copy(name, dest, sender):
        src, dst = x_kinds[name]
        k = x_index[name]
        return pltpu.make_async_remote_copy(
            src_ref=src(dest), dst_ref=dst(sender), send_sem=x_send.at[k, dest],
            recv_sem=x_recv.at[k, sender], device_id={"xax": dest},
            device_id_type=pl.DeviceIdType.MESH)

    def own_copy(name):
        src, dst = x_kinds[name]
        return pltpu.make_async_copy(src(x), dst(x), own_sem.at[x_index[name]])

    def x_start(name):
        def body(d, carry):
            x_copy(name, lax.rem(x + d, xs), x).start()
            return carry
        lax.fori_loop(1, xs, body, 0)
        own_copy(name).start()

    def x_wait(name):
        def body(d, carry):
            x_copy(name, x, lax.rem(x + xs - d, xs)).wait_recv()
            return carry
        lax.fori_loop(1, xs, body, 0)
        own_copy(name).wait()

    def x_drain(name):
        def body(d, carry):
            x_copy(name, lax.rem(x + d, xs), x).wait_send()
            return carry
        lax.fori_loop(1, xs, body, 0)

    y_kinds = {"wq": wq_buf, "wo": out_buf, "gu": gu_buf, "down": down_buf}
    y_index = {name: i for i, name in enumerate(y_kinds)}

    def y_copy(name, dest, sender):
        buf = y_kinds[name]
        k = y_index[name]
        return pltpu.make_async_remote_copy(
            src_ref=buf.at[sender], dst_ref=buf.at[sender], send_sem=y_send.at[k, dest],
            recv_sem=y_recv.at[k, sender], device_id={"yax": dest},
            device_id_type=pl.DeviceIdType.MESH)

    def y_start(name):
        def body(d, carry):
            y_copy(name, lax.rem(y + d, ys), y).start()
            return carry
        lax.fori_loop(1, ys, body, 0)

    def y_wait(name):
        def body(d, carry):
            y_copy(name, y, lax.rem(y + ys - d, ys)).wait_recv()
            return carry
        lax.fori_loop(1, ys, body, 0)

    def y_drain(name):
        def body(d, carry):
            y_copy(name, lax.rem(y + d, ys), y).wait_send()
            return carry
        lax.fori_loop(1, ys, body, 0)

    e_parts = row_chunks(window, EMBED_CHUNKS)

    def e_first(p):
        return p * vocab - lax.rem(p, 2) * shift

    def e_copy(c, dest, sender):
        r0, n = e_parts[c]
        return pltpu.make_async_remote_copy(
            src_ref=embed.at[pl.ds(pl.multiple_of(e_first(dest) + r0, 8), n), :],
            dst_ref=e_buf.at[pl.ds(r0, n), lanes(sender)],
            send_sem=e_send.at[c, dest], recv_sem=e_recv.at[c, sender],
            device_id={"xax": dest}, device_id_type=pl.DeviceIdType.MESH)

    def e_own():
        return pltpu.make_async_copy(
            embed.at[pl.ds(pl.multiple_of(e_first(x), 8), window), :], e_buf.at[:, lanes(x)],
            own_sem.at[len(x_kinds)])

    def e_start(c):
        def body(d, carry):
            e_copy(c, lax.rem(x + d, xs), x).start()
            return carry
        lax.fori_loop(1, xs, body, 0)

    for name in ("hidden", "wq", "ga", "gf", "wk", "wv", "wo", "gate", "up", "down"):
        x_start(name)
    e_own().start()

    def start_cache_v(g, carry):
        cache_copy(g, v_hbm, v_buf, 1).start()
        return carry
    lax.fori_loop(0, groups, start_cache_v, 0)
    e_start(0)

    x_wait("wq")
    y_start("wq")
    x_wait("hidden")
    x_wait("ga")
    n_buf[...] = layer_norm(h_buf[...].astype(F32), ga_buf[...]).astype(BF16)
    y_wait("wq")
    wq_all = wq_buf[...].reshape(ys * cols, xs * blk)
    q_scr[...] = lax.dot_general(n_buf[...], wq_all, NT, preferred_element_type=F32).astype(BF16)
    x_start("q")
    x_wait("wo")
    y_start("wo")
    x_wait("gate")
    x_wait("up")
    y_start("gu")
    x_wait("down")
    y_start("down")
    e_start(1)

    row_id = lax.broadcasted_iota(jnp.int32, (own, 4 * half), 0)
    first_row = (y * xs + x) * own
    position = jnp.zeros((own, 4 * half), jnp.int32)
    for b in range(own):
        position = jnp.where(row_id == b, lens[first_row + b], position)
    angle = position.astype(F32) * freq[...]
    cos_a = jnp.cos(angle)
    sin_a = jnp.sin(angle)
    x_wait("wk")
    x_wait("wv")
    n_own = n_buf[rows(x, own), :]
    kv = lax.dot_general(n_own, kv_buf[...], NT, preferred_element_type=F32).astype(BF16).astype(F32)
    k1 = kv[:, :half]
    k2 = kv[:, half:head_dim]
    c1 = cos_a[:, :half]
    s1 = sin_a[:, :half]
    key = jnp.concatenate([k1 * c1 - k2 * s1, k2 * c1 + k1 * s1], axis=1).astype(BF16)
    value = kv[:, head_dim:].astype(BF16)
    k_out[...] = key
    v_out[...] = value
    for h in range(heads):
        krep[pl.ds(h, own, stride=heads), :] = key.astype(F32)
        vrep[pl.ds(h, own, stride=heads), :] = value.astype(F32)

    x_wait("q")
    for xc in range(xs // 2):
        qa = qx_buf[2 * xc].astype(F32)
        qb = qx_buf[2 * xc + 1].astype(F32)
        ra = (qa * cos_a - qb * sin_a).astype(BF16).astype(F32)
        rb = (qb * cos_a + qa * sin_a).astype(BF16).astype(F32)
        for yc in range(ys):
            pair = jnp.concatenate([ra[:, yc * half:(yc + 1) * half], rb[:, yc * half:(yc + 1) * half]], axis=1)
            q2d[pl.ds(xc * ys + yc, own, stride=heads), :] = pair
    scale = head_dim ** -0.5
    snew[...] = jnp.sum(q2d[...] * krep[...], axis=1, keepdims=True) * scale

    gr = per * heads
    seg_r = lax.broadcasted_iota(jnp.int32, (gr, per * head_dim), 0) // heads
    seg_c = lax.broadcasted_iota(jnp.int32, (gr, per * head_dim), 1) // head_dim
    diag = (seg_r == seg_c).astype(F32)
    tile = min(512, slots)
    row_g = lax.broadcasted_iota(jnp.int32, (gr, 1), 0) // heads
    lane_g = lax.broadcasted_iota(jnp.int32, (gr, tile), 1)

    def attend(g, carry):
        cache_copy(g, k_hbm, k_buf, 0).wait()
        qg = q2d[rows(g, gr), :]
        qbd = (jnp.concatenate([qg] * per, axis=1) * diag).astype(BF16)
        len_g = jnp.zeros((gr, 1), jnp.int32)
        for s in range(per):
            len_g = jnp.where(row_g == s, lens[first_row + g * per + s], len_g)
        new = snew[rows(g, gr), :]
        top = jnp.full((gr, tile), -jnp.inf, F32)
        kg = k_buf.at[g]
        vg = v_buf.at[g]
        for c in range(slots // tile):
            kc = kg[:, :, pl.ds(c * tile, tile)].reshape(per * head_dim, tile)
            sc = jnp.dot(qbd, kc, preferred_element_type=F32) * scale
            sc = jnp.where(lane_g < len_g - c * tile, sc, -jnp.inf)
            s_scr[:, pl.ds(c * tile, tile)] = sc
            top = jnp.maximum(top, sc)
        row_max = jnp.maximum(jnp.max(top, axis=1, keepdims=True), new)
        total = jnp.zeros((gr, tile), F32)
        for c in range(slots // tile):
            ex = jnp.exp(s_scr[:, pl.ds(c * tile, tile)] - row_max)
            s_scr[:, pl.ds(c * tile, tile)] = ex
            total = total + ex
        w_new = jnp.exp(new - row_max)
        den = jnp.sum(total, axis=1, keepdims=True) + w_new
        inv = 1.0 / den
        cache_copy(g, v_hbm, v_buf, 1).wait()
        mixed = jnp.zeros((gr, per * head_dim), F32)
        for c in range(slots // tile):
            pr = (s_scr[:, pl.ds(c * tile, tile)] * inv).astype(BF16)
            vc = vg[:, :, pl.ds(c * tile, tile)].reshape(per * head_dim, tile)
            mixed = mixed + lax.dot_general(pr, vc, NT, preferred_element_type=F32)
        add = (w_new * inv).astype(BF16).astype(F32) * vrep[rows(g, gr), :]
        for s in range(per):
            od_scr[pl.ds(pl.multiple_of(g * gr + s * heads, heads), heads), :] = (
                mixed[s * heads:(s + 1) * heads, s * head_dim:(s + 1) * head_dim]
                + add[s * heads:(s + 1) * heads, :])
        return carry

    e_done = 2
    steps = 4
    for i in range(steps):
        lax.fori_loop(i * groups // steps, (i + 1) * groups // steps, attend, 0)
        if e_done < EMBED_CHUNKS:
            e_start(e_done)
            e_done += 1
    for xc in range(xs // 2):
        parts = [od_scr[pl.ds(xc * ys + yc, own, stride=heads), :] for yc in range(ys)]
        o_scr[2 * xc] = jnp.concatenate([p[:, :half] for p in parts], axis=1).astype(BF16)
        o_scr[2 * xc + 1] = jnp.concatenate([p[:, half:] for p in parts], axis=1).astype(BF16)
    x_start("o")

    y_wait("gu")
    for j in range(ys):
        gu = jnp.dot(n_buf[...], gu_buf[j], preferred_element_type=F32).astype(BF16).astype(F32)
        gate = gu[:, :ff]
        act[:, pl.ds(j * ff, ff)] = (gate * jax.nn.sigmoid(gate) * gu[:, ff:]).astype(BF16)
    y_wait("down")
    part_scr[...] = jnp.dot(act[...], down_buf[...].reshape(ys * ff, xs * blk), preferred_element_type=F32)
    y_wait("wo")
    x_wait("o")
    part_scr[...] = part_scr[...] + jnp.dot(
        ox_buf[...], out_buf[...].reshape(ys * cols, xs * blk), preferred_element_type=F32)
    x_start("rs")
    while e_done < EMBED_CHUNKS:
        e_start(e_done)
        e_done += 1
    x_wait("gf")
    x_wait("rs")
    res = h_buf[rows(x, own), :].astype(F32) + jnp.sum(rs_buf[...], axis=0)
    mine = y * xs + x
    f_buf[rows(mine, own), :] = layer_norm(res, gf_buf[...]).astype(BF16)

    chips = xs // 2

    def f_copy(dy, dx, src_y, src_x):
        r = rows(src_y * xs + src_x, own)
        return pltpu.make_async_remote_copy(
            src_ref=f_buf.at[r, :], dst_ref=f_buf.at[r, :],
            send_sem=f_send.at[dy * xs + dx], recv_sem=f_recv.at[src_y * xs + src_x],
            device_id={"yax": dy, "xax": dx}, device_id_type=pl.DeviceIdType.MESH)

    def p_copy(src_y, src_x):
        r = rows(src_y * xs + src_x, own)
        return pltpu.make_async_remote_copy(
            src_ref=f_buf.at[r, :], dst_ref=f_buf.at[r, :],
            send_sem=p_send.at[src_y * xs + src_x], recv_sem=p_recv.at[src_y * xs + src_x],
            device_id={"xax": partner}, device_id_type=pl.DeviceIdType.MESH)

    def plane_peer(i, sign):
        py = lax.rem(y + ys + sign * (i // chips), ys)
        px = lax.rem(x + xs + sign * 2 * lax.rem(i, chips), xs)
        return py, px

    def f_start(i, carry):
        py, px = plane_peer(i, 1)
        f_copy(py, px, y, x).start()
        return carry
    lax.fori_loop(1, ys * chips, f_start, 0)
    p_copy(y, x).start()

    e_own().wait()
    for c in range(EMBED_CHUNKS):
        def e_wait(d, carry, c=c):
            e_copy(c, x, lax.rem(x + xs - d, xs)).wait_recv()
            return carry
        lax.fori_loop(1, xs, e_wait, 0)
    if shift:
        @pl.when(core == 1)
        def _():
            for r0 in range(0, vocab, 256):
                n = min(256, vocab - r0)
                e_al[pl.ds(r0, n), :] = e_buf[pl.ds(r0 + shift, n), :]

        @pl.when(core == 0)
        def _():
            for r0 in range(0, vocab, 256):
                n = min(256, vocab - r0)
                e_al[pl.ds(r0, n), :] = e_buf[pl.ds(r0, n), :]
    else:
        e_al[...] = e_buf[...]

    def z_copy(j, slot):
        return pltpu.make_async_copy(z_scr.at[slot], logits_out.at[:, rows(j, quarter)], z_sem.at[slot])

    def head(dy, carry):
        j = lax.rem(y + ys - dy, ys)

        def forward(i, c2):
            sx = lax.rem(x + xs - 2 * i, xs)

            @pl.when(jnp.logical_or(dy > 0, i > 0))
            def _():
                f_copy(y, x, j, sx).wait_recv()
                p_copy(j, sx).start()
            return c2
        lax.fori_loop(0, chips, forward, 0)

        def arrive(i, c2):
            p_copy(j, lax.rem(partner + xs - 2 * i, xs)).wait_recv()
            return c2
        lax.fori_loop(0, chips, arrive, 0)
        slot = lax.rem(dy, 2)

        @pl.when(dy >= 2)
        def _():
            z_copy(j, slot).wait()
        z = lax.dot_general(e_al[...], f_buf[rows(j, quarter), :], NT, preferred_element_type=F32)
        z_scr[slot] = z
        z_copy(j, slot).start()
        top = jnp.max(z, axis=0, keepdims=True)
        tot = jnp.sum(jnp.exp(z - top), axis=0, keepdims=True)
        st_scr[0:1, rows(j, quarter)] = top
        st_scr[1:2, rows(j, quarter)] = tot
        return carry
    lax.fori_loop(0, ys, head, 0)

    def s_copy(dest_y, dest_x, src):
        return pltpu.make_async_remote_copy(
            src_ref=st_scr, dst_ref=st_buf.at[src], send_sem=s_send.at[dest_y * xs + dest_x],
            recv_sem=s_recv.at[src], device_id={"yax": dest_y, "xax": dest_x},
            device_id_type=pl.DeviceIdType.MESH)

    def s_start(i, carry):
        s_copy(lax.rem(y + i // xs, ys), lax.rem(x + lax.rem(i, xs), xs), mine).start()
        return carry
    lax.fori_loop(1, ys * xs, s_start, 0)
    st_buf[mine] = st_scr[...]

    for name in x_kinds:
        x_drain(name)
    for name in y_kinds:
        y_drain(name)
    for c in range(EMBED_CHUNKS):
        def e_drain(d, carry, c=c):
            e_copy(c, lax.rem(x + d, xs), x).wait_send()
            return carry
        lax.fori_loop(1, xs, e_drain, 0)

    def f_drain(i, carry):
        py, px = plane_peer(i, 1)
        f_copy(py, px, y, x).wait_send()
        return carry
    lax.fori_loop(1, ys * chips, f_drain, 0)

    def p_drain(i, carry):
        py, px = plane_peer(i, 1)
        p_copy(py, px).wait_send()
        return carry
    lax.fori_loop(0, ys * chips, p_drain, 0)

    def s_wait(i, carry):
        sy = lax.rem(y + ys - i // xs, ys)
        sx = lax.rem(x + xs - lax.rem(i, xs), xs)
        s_copy(y, x, sy * xs + sx).wait_recv()
        return carry
    lax.fori_loop(1, ys * xs, s_wait, 0)
    tops = st_buf[:, 0, :]
    best = jnp.max(tops, axis=0, keepdims=True)
    whole = jnp.sum(st_buf[:, 1, :] * jnp.exp(tops - best), axis=0, keepdims=True)
    norm_out[...] = best + jnp.log(whole)

    def s_drain(i, carry):
        s_copy(lax.rem(y + i // xs, ys), lax.rem(x + lax.rem(i, xs), xs), mine).wait_send()
        return carry
    lax.fori_loop(1, ys * xs, s_drain, 0)
    for dy in range(max(ys - 2, 0), ys):
        z_copy(lax.rem(y + ys - dy, ys), dy % 2).wait()


def solution(mesh):
    ys = mesh.shape["yax"]
    xs = mesh.shape["xax"]
    row_spec = P(("dp", "yax", "xax"))

    def local_step(hidden, cache_len, k_cache, v_cache, g_attn, w_query, w_key, w_value,
                   w_gate, w_up, w_out, w_down, g_final, embedding):
        batch, blk = hidden.shape
        own, slots, head_dim = k_cache.shape
        width = blk * xs
        vocab = embedding.shape[0] // xs
        shift = vocab % 8
        window = -(-vocab // 8) * 8
        half = head_dim // 2
        quarter = xs * own
        cols = w_query.shape[1] // xs
        ff = w_gate.shape[1] // xs
        heads = w_query.shape[1] * ys // head_dim
        per = 4
        groups = own // per
        freq_row = (ROPE_BASE ** (-(np.arange(half, dtype=np.float32) * 2.0) / head_dim)).astype(np.float32)
        freq = jnp.asarray(np.tile(freq_row, 4)[None, :])
        any_spec = pl.BlockSpec(memory_space=pl.ANY)
        vmem = pl.BlockSpec(memory_space=pltpu.VMEM)
        smem = pl.BlockSpec(memory_space=pltpu.SMEM)
        dma = pltpu.SemaphoreType.DMA
        nx = 13
        all_n = ys * xs
        scratch = [
            pltpu.VMEM((groups, per, head_dim, slots), BF16),
            pltpu.VMEM((groups, per, head_dim, slots), BF16),
            pltpu.VMEM((quarter, width), BF16),
            pltpu.VMEM((1, width), F32),
            pltpu.VMEM((1, width), F32),
            pltpu.VMEM((w_query.shape[1], blk), BF16),
            pltpu.VMEM((ys, cols, width), BF16),
            pltpu.VMEM((ys, width, 2 * ff), BF16),
            pltpu.VMEM((ys, ff, width), BF16),
            pltpu.VMEM((ys, cols, width), BF16),
            pltpu.VMEM((2 * head_dim, width), BF16),
            pltpu.VMEM((quarter, width), BF16),
            pltpu.VMEM((quarter, ys * cols), BF16),
            pltpu.VMEM((xs, own, ys * cols), BF16),
            pltpu.VMEM((own * heads, head_dim), F32),
            pltpu.VMEM((own * heads, 1), F32),
            pltpu.VMEM((own * heads, head_dim), F32),
            pltpu.VMEM((own * heads, head_dim), F32),
            pltpu.VMEM((per * heads, slots), F32),
            pltpu.VMEM((own * heads, head_dim), F32),
            pltpu.VMEM((xs, own, ys * cols), BF16),
            pltpu.VMEM((quarter, ys * cols), BF16),
            pltpu.VMEM((quarter, ys * ff), BF16),
            pltpu.VMEM((quarter, width), F32),
            pltpu.VMEM((xs, own, width), F32),
            pltpu.VMEM((batch, width), BF16),
            pltpu.VMEM((window, width), BF16),
            pltpu.VMEM((vocab, width), BF16),
            pltpu.VMEM((2, vocab, quarter), F32),
            pltpu.VMEM((2, batch), F32),
            pltpu.VMEM((all_n, 2, batch), F32),
            dma((2, groups)), dma((nx + 1,)), dma((2,)),
            dma((nx, xs)), dma((nx, xs)), dma((4, ys)), dma((4, ys)),
            dma((EMBED_CHUNKS, xs)), dma((EMBED_CHUNKS, xs)),
            dma((all_n,)), dma((all_n,)), dma((all_n,)), dma((all_n,)), dma((all_n,)), dma((all_n,)),
        ]
        cfg = (ys, xs, own, vocab, shift)
        key_new, value_new, logits, norm = pl.pallas_call(
            functools.partial(kernel, cfg),
            name="decode_layer",
            out_shape=(
                jax.ShapeDtypeStruct((own, head_dim), BF16),
                jax.ShapeDtypeStruct((own, head_dim), BF16),
                jax.ShapeDtypeStruct((vocab, batch), F32),
                jax.ShapeDtypeStruct((1, batch), F32)),
            in_specs=[smem, any_spec, any_spec, any_spec, any_spec, any_spec, vmem] + [any_spec] * 7 + [vmem],
            out_specs=(vmem, vmem, any_spec, vmem),
            scratch_shapes=scratch,
            compiler_params=pltpu.CompilerParams(
                collective_id=0, has_side_effects=True, vmem_limit_bytes=67043328),
        )(cache_len, hidden, k_cache.transpose(0, 2, 1), v_cache.transpose(0, 2, 1),
          g_attn[None, :], g_final[None, :], w_query, w_key.T, w_value.T, w_gate, w_up, w_out, w_down,
          embedding, freq)
        log_norm = norm[0]
        return key_new, value_new, (logits - norm).T, log_norm

    in_specs = (P("dp", "xax"), P("dp"), row_spec, row_spec, P("xax"), P("xax", "yax"),
                P("xax", None), P("xax", None), P("xax", "yax"), P("xax", "yax"),
                P("yax", "xax"), P("yax", "xax"), P("xax"), P("yax", "xax"))
    out_specs = (row_spec, row_spec, P("dp", ("yax", "xax")), P("dp"))
    return jax.shard_map(local_step, mesh=mesh, in_specs=in_specs, out_specs=out_specs, check_vma=False)
```

```python
import functools

import jax
import jax.numpy as jnp
import numpy as np
from jax import lax
from jax.experimental import pallas as pl
from jax.experimental.pallas import tpu as pltpu
from jax.sharding import PartitionSpec as P

EPS = 1e-6
ROPE_BASE = 10000.0
F32 = jnp.float32
BF16 = jnp.bfloat16
NT = (((1,), (1,)), ((), ()))
EMBED_CHUNKS = 8


def layer_norm(values_in, gain):
    mean = jnp.mean(values_in, axis=-1, keepdims=True)
    centred = values_in - mean
    var = jnp.mean(centred * centred, axis=-1, keepdims=True)
    return centred * lax.rsqrt(var + EPS) * gain


def row_chunks(total, count):
    tiles = total // 8
    cuts = [8 * (tiles * i // count) for i in range(count + 1)]
    return [(cuts[i], cuts[i + 1] - cuts[i]) for i in range(count)]


def kernel(cfg, lens, hidden, k_hbm, v_hbm, g_attn, g_final, w_query, w_key, w_value, w_gate, w_up,
           w_out, w_down, embed, freq,
           k_out, v_out, logits_out, norm_out,
           k_buf, v_buf, h_buf, ga_buf, gf_buf, wqt, wq_buf, gu_buf, down_buf, out_buf, kv_buf,
           n_all, q_scr, qx_buf, q2d, snew, krep, vrep, s_scr, od_scr, o_scr, ox_buf, act_scr, act, part_scr,
           pre_buf, rs_scr, rs_buf, f_buf, e_buf, e_al, z_scr, st_scr, sx_buf, sy_scr, sy_buf,
           kv_sem, own_sem, z_sem, x_send, x_recv, g_send, y_send, y_recv, e_send, e_recv,
           n_recv, n_fwd, pre_sem, f_send, f_recv, fy_send, fp_send, sx_send, sx_recv, sy_send, sy_recv):
    ys, xs, own, vocab, shift = cfg
    y = lax.axis_index("yax")
    x = lax.axis_index("xax")
    core = lax.rem(x, 2)
    partner = x + 1 - 2 * core
    blk = hidden.shape[1]
    quarter = xs * own
    head_dim = k_hbm.shape[1]
    half = head_dim // 2
    seqs = k_hbm.shape[0]
    slots = k_hbm.shape[2]
    heads = w_query.shape[1] * ys // head_dim
    groups = k_buf.shape[0]
    per = seqs // groups
    window = e_buf.shape[0]

    def lanes(i):
        return pl.ds(pl.multiple_of(i * blk, 128), blk)

    def rows(i, n):
        return pl.ds(pl.multiple_of(i * n, n), n)

    def cache_copy(g, src, dst, s):
        return pltpu.make_async_copy(src.at[pl.ds(g * per, per)], dst.at[g], kv_sem.at[s, g])

    def start_cache(g, carry):
        cache_copy(g, k_hbm, k_buf, 0).start()
        return carry
    lax.fori_loop(0, groups, start_cache, 0)

    wqt[...] = w_query[...].astype(F32).T.astype(BF16)

    barrier = pltpu.get_barrier_semaphore()

    def signal_row(d, carry):
        pl.semaphore_signal(barrier, inc=1, device_id={"xax": lax.rem(x + d, xs)},
                            device_id_type=pl.DeviceIdType.MESH)
        return carry
    lax.fori_loop(1, xs, signal_row, 0)

    def signal_column(d, carry):
        pl.semaphore_signal(barrier, inc=1, device_id={"yax": lax.rem(y + d, ys)},
                            device_id_type=pl.DeviceIdType.MESH)
        return carry
    lax.fori_loop(1, ys, signal_column, 0)
    pl.semaphore_wait(barrier, xs + ys - 2)

    cols = wqt.shape[0] // xs
    ff = w_gate.shape[1] // xs
    x_kinds = {
        "hidden": (lambda p: hidden.at[rows(y, quarter), :], lambda s: h_buf.at[:, lanes(s)]),
        "wq": (lambda p: wqt.at[rows(p, cols), :], lambda s: wq_buf.at[y, :, lanes(s)]),
        "ga": (lambda p: g_attn, lambda s: ga_buf.at[:, lanes(s)]),
        "gf": (lambda p: g_final, lambda s: gf_buf.at[:, lanes(s)]),
        "wk": (lambda p: w_key, lambda s: kv_buf.at[pl.ds(0, head_dim), lanes(s)]),
        "wv": (lambda p: w_value, lambda s: kv_buf.at[pl.ds(head_dim, head_dim), lanes(s)]),
        "wo": (lambda p: w_out.at[rows(p, cols), :], lambda s: out_buf.at[y, :, lanes(s)]),
        "gate": (lambda p: w_gate.at[:, lanes(p)], lambda s: gu_buf.at[rows(s, blk), pl.ds(0, ff)]),
        "up": (lambda p: w_up.at[:, lanes(p)], lambda s: gu_buf.at[rows(s, blk), pl.ds(ff, ff)]),
        "down": (lambda p: w_down.at[rows(p, ff), :], lambda s: down_buf.at[y, :, lanes(s)]),
        "q": (lambda p: q_scr.at[rows(p, own), :], lambda s: qx_buf.at[s]),
        "o": (lambda p: o_scr.at[p], lambda s: ox_buf.at[rows(s, own), :]),
    }
    x_index = {name: i for i, name in enumerate(x_kinds)}

    def x_copy(name, dest, sender):
        src, dst = x_kinds[name]
        k = x_index[name]
        return pltpu.make_async_remote_copy(
            src_ref=src(dest), dst_ref=dst(sender), send_sem=x_send.at[k, dest],
            recv_sem=x_recv.at[k, sender], device_id={"xax": dest},
            device_id_type=pl.DeviceIdType.MESH)

    def own_copy(name):
        src, dst = x_kinds[name]
        return pltpu.make_async_copy(src(x), dst(x), own_sem.at[x_index[name]])

    chips = xs // 2
    gathers = {name: i for i, name in enumerate(("hidden", "ga", "gf", "wk", "wv"))}

    def g_copy(name, sender, source):
        src, dst = x_kinds[name]
        return pltpu.make_async_remote_copy(
            src_ref=source, dst_ref=dst(sender), send_sem=g_send.at[gathers[name], sender],
            recv_sem=x_recv.at[x_index[name], sender], device_id={"xax": partner},
            device_id_type=pl.DeviceIdType.MESH)

    def g_start(name):
        def body(i, carry):
            x_copy(name, lax.rem(x + 2 * i, xs), x).start()
            return carry
        lax.fori_loop(1, chips, body, 0)
        g_copy(name, x, x_kinds[name][0](x)).start()
        own_copy(name).start()

    def g_forward(name):
        def body(i, carry):
            sender = lax.rem(x + xs - 2 * i, xs)
            x_copy(name, x, sender).wait_recv()
            g_copy(name, sender, x_kinds[name][1](sender)).start()
            return carry
        lax.fori_loop(1, chips, body, 0)

    def g_wait(name):
        def body(i, carry):
            sender = lax.rem(partner + xs - 2 * i, xs)
            g_copy(name, sender, x_kinds[name][1](sender)).wait_recv()
            return carry
        lax.fori_loop(0, chips, body, 0)
        own_copy(name).wait()

    def g_drain(name):
        def body(i, carry):
            @pl.when(i > 0)
            def _():
                x_copy(name, lax.rem(x + 2 * i, xs), x).wait_send()
            sender = lax.rem(x + xs - 2 * i, xs)
            g_copy(name, sender, x_kinds[name][1](sender)).wait_send()
            return carry
        lax.fori_loop(0, chips, body, 0)

    def x_start(name):
        def body(d, carry):
            x_copy(name, lax.rem(x + d, xs), x).start()
            return carry
        lax.fori_loop(1, xs, body, 0)
        own_copy(name).start()

    def x_wait(name):
        def body(d, carry):
            x_copy(name, x, lax.rem(x + xs - d, xs)).wait_recv()
            return carry
        lax.fori_loop(1, xs, body, 0)
        own_copy(name).wait()

    def x_drain(name):
        def body(d, carry):
            x_copy(name, lax.rem(x + d, xs), x).wait_send()
            return carry
        lax.fori_loop(1, xs, body, 0)

    y_kinds = {"wq": wq_buf, "wo": out_buf, "down": down_buf}
    y_index = {name: i for i, name in enumerate(y_kinds)}

    def y_copy(name, dest, sender):
        buf = y_kinds[name]
        k = y_index[name]
        return pltpu.make_async_remote_copy(
            src_ref=buf.at[sender], dst_ref=buf.at[sender], send_sem=y_send.at[k, dest],
            recv_sem=y_recv.at[k, sender], device_id={"yax": dest},
            device_id_type=pl.DeviceIdType.MESH)

    def y_start(name):
        def body(d, carry):
            y_copy(name, lax.rem(y + d, ys), y).start()
            return carry
        lax.fori_loop(1, ys, body, 0)

    def y_wait(name):
        def body(d, carry):
            y_copy(name, y, lax.rem(y + ys - d, ys)).wait_recv()
            return carry
        lax.fori_loop(1, ys, body, 0)

    def y_drain(name):
        def body(d, carry):
            y_copy(name, lax.rem(y + d, ys), y).wait_send()
            return carry
        lax.fori_loop(1, ys, body, 0)

    e_parts = row_chunks(window, EMBED_CHUNKS)

    def e_first(p):
        return p * vocab - lax.rem(p, 2) * shift

    def e_copy(c, dest, sender):
        r0, n = e_parts[c]
        return pltpu.make_async_remote_copy(
            src_ref=embed.at[pl.ds(pl.multiple_of(e_first(dest) + r0, 8), n), :],
            dst_ref=e_buf.at[pl.ds(r0, n), lanes(sender)],
            send_sem=e_send.at[c, dest], recv_sem=e_recv.at[c, sender],
            device_id={"xax": dest}, device_id_type=pl.DeviceIdType.MESH)

    def e_own():
        return pltpu.make_async_copy(
            embed.at[pl.ds(pl.multiple_of(e_first(x), 8), window), :], e_buf.at[:, lanes(x)],
            own_sem.at[len(x_kinds)])

    def e_start(c):
        def body(d, carry):
            e_copy(c, lax.rem(x + d, xs), x).start()
            return carry
        lax.fori_loop(1, xs, body, 0)

    x_start("wq")
    for name in ("hidden", "ga"):
        g_start(name)
    for name in ("wo", "down"):
        x_start(name)
    for name in ("wk", "wv", "gf"):
        g_start(name)
    e_own().start()

    def start_cache_v(g, carry):
        cache_copy(g, v_hbm, v_buf, 1).start()
        return carry
    lax.fori_loop(0, groups, start_cache_v, 0)

    x_wait("wq")
    y_start("wq")
    for name in ("hidden", "ga"):
        g_forward(name)
    for name in ("hidden", "ga"):
        g_wait(name)
    my_rows = rows(y, quarter)
    n_all[my_rows, :] = layer_norm(h_buf[...].astype(F32), ga_buf[...]).astype(BF16)

    part = quarter // 2

    def n_rows(j, c):
        return pl.ds(pl.multiple_of(j * quarter + c * part, part), part)

    def n_copy(dest, sender):
        r = n_rows(sender, core)
        return pltpu.make_async_remote_copy(
            src_ref=n_all.at[r, :], dst_ref=n_all.at[r, :], send_sem=y_send.at[len(y_kinds), dest],
            recv_sem=n_recv.at[sender, core], device_id={"yax": dest},
            device_id_type=pl.DeviceIdType.MESH)

    def n_pass(sender, c):
        r = n_rows(sender, c)
        return pltpu.make_async_remote_copy(
            src_ref=n_all.at[r, :], dst_ref=n_all.at[r, :], send_sem=n_fwd.at[sender],
            recv_sem=n_recv.at[sender, c], device_id={"xax": partner},
            device_id_type=pl.DeviceIdType.MESH)

    y_wait("wq")
    wq_all = wq_buf[...].reshape(ys * cols, xs * blk)
    q_scr[...] = lax.dot_general(n_all[my_rows, :], wq_all, NT, preferred_element_type=F32).astype(BF16)
    x_start("q")
    x_start("gate")
    x_start("up")

    def n_start(d, carry):
        n_copy(lax.rem(y + d, ys), y).start()
        return carry
    lax.fori_loop(1, ys, n_start, 0)
    x_wait("wo")
    y_start("wo")
    x_wait("down")
    y_start("down")
    e_start(0)

    row_id = lax.broadcasted_iota(jnp.int32, (own, 4 * half), 0)
    first_row = (y * xs + x) * own
    position = jnp.zeros((own, 4 * half), jnp.int32)
    for b in range(own):
        position = jnp.where(row_id == b, lens[first_row + b], position)
    angle = position.astype(F32) * freq[...]
    cos_a = jnp.cos(angle)
    sin_a = jnp.sin(angle)
    for name in ("wk", "wv", "gf"):
        g_forward(name)
    for name in ("wk", "wv", "gf"):
        g_wait(name)
    mine = y * xs + x
    n_own = n_all[rows(mine, own), :]
    kv = lax.dot_general(n_own, kv_buf[...], NT, preferred_element_type=F32).astype(BF16).astype(F32)
    k1 = kv[:, :half]
    k2 = kv[:, half:head_dim]
    c1 = cos_a[:, :half]
    s1 = sin_a[:, :half]
    key = jnp.concatenate([k1 * c1 - k2 * s1, k2 * c1 + k1 * s1], axis=1).astype(BF16)
    value = kv[:, head_dim:].astype(BF16)
    k_out[...] = key
    v_out[...] = value
    for h in range(heads):
        krep[pl.ds(h, own, stride=heads), :] = key.astype(F32)
        vrep[pl.ds(h, own, stride=heads), :] = value.astype(F32)

    x_wait("q")
    for xc in range(xs // 2):
        qa = qx_buf[2 * xc].astype(F32)
        qb = qx_buf[2 * xc + 1].astype(F32)
        ra = (qa * cos_a - qb * sin_a).astype(BF16).astype(F32)
        rb = (qb * cos_a + qa * sin_a).astype(BF16).astype(F32)
        for yc in range(ys):
            pair = jnp.concatenate([ra[:, yc * half:(yc + 1) * half], rb[:, yc * half:(yc + 1) * half]], axis=1)
            q2d[pl.ds(xc * ys + yc, own, stride=heads), :] = pair
    scale = head_dim ** -0.5
    snew[...] = jnp.sum(q2d[...] * krep[...], axis=1, keepdims=True) * scale

    gr = per * heads
    seg_r = lax.broadcasted_iota(jnp.int32, (gr, per * head_dim), 0) // heads
    seg_c = lax.broadcasted_iota(jnp.int32, (gr, per * head_dim), 1) // head_dim
    diag = (seg_r == seg_c).astype(F32)
    tile = min(512, slots)
    row_g = lax.broadcasted_iota(jnp.int32, (gr, 1), 0) // heads
    lane_g = lax.broadcasted_iota(jnp.int32, (gr, tile), 1)

    def attend(g, carry):
        cache_copy(g, k_hbm, k_buf, 0).wait()
        qg = q2d[rows(g, gr), :]
        qbd = (jnp.concatenate([qg] * per, axis=1) * diag).astype(BF16)
        len_g = jnp.zeros((gr, 1), jnp.int32)
        for s in range(per):
            len_g = jnp.where(row_g == s, lens[first_row + g * per + s], len_g)
        new = snew[rows(g, gr), :]
        top = jnp.full((gr, tile), -jnp.inf, F32)
        kg = k_buf.at[g]
        vg = v_buf.at[g]
        for c in range(slots // tile):
            kc = kg[:, :, pl.ds(c * tile, tile)].reshape(per * head_dim, tile)
            sc = jnp.dot(qbd, kc, preferred_element_type=F32) * scale
            sc = jnp.where(lane_g < len_g - c * tile, sc, -jnp.inf)
            s_scr[:, pl.ds(c * tile, tile)] = sc
            top = jnp.maximum(top, sc)
        row_max = jnp.maximum(jnp.max(top, axis=1, keepdims=True), new)
        total = jnp.zeros((gr, tile), F32)
        for c in range(slots // tile):
            ex = jnp.exp(s_scr[:, pl.ds(c * tile, tile)] - row_max)
            s_scr[:, pl.ds(c * tile, tile)] = ex
            total = total + ex
        w_new = jnp.exp(new - row_max)
        den = jnp.sum(total, axis=1, keepdims=True) + w_new
        inv = 1.0 / den
        cache_copy(g, v_hbm, v_buf, 1).wait()
        mixed = jnp.zeros((gr, per * head_dim), F32)
        for c in range(slots // tile):
            pr = (s_scr[:, pl.ds(c * tile, tile)] * inv).astype(BF16)
            vc = vg[:, :, pl.ds(c * tile, tile)].reshape(per * head_dim, tile)
            mixed = mixed + lax.dot_general(pr, vc, NT, preferred_element_type=F32)
        add = (w_new * inv).astype(BF16).astype(F32) * vrep[rows(g, gr), :]
        for s in range(per):
            od_scr[pl.ds(pl.multiple_of(g * gr + s * heads, heads), heads), :] = (
                mixed[s * heads:(s + 1) * heads, s * head_dim:(s + 1) * head_dim]
                + add[s * heads:(s + 1) * heads, :])
        return carry

    e_done = 1
    steps = 4
    for i in range(steps):
        lax.fori_loop(i * groups // steps, (i + 1) * groups // steps, attend, 0)
        if e_done < EMBED_CHUNKS:
            e_start(e_done)
            e_done += 1
    for xc in range(xs // 2):
        parts = [od_scr[pl.ds(xc * ys + yc, own, stride=heads), :] for yc in range(ys)]
        o_scr[2 * xc] = jnp.concatenate([p[:, :half] for p in parts], axis=1).astype(BF16)
        o_scr[2 * xc + 1] = jnp.concatenate([p[:, half:] for p in parts], axis=1).astype(BF16)
    x_start("o")

    def act_copy(dest, sender):
        return pltpu.make_async_remote_copy(
            src_ref=act_scr.at[dest], dst_ref=act.at[:, pl.ds(pl.multiple_of(sender * ff, ff), ff)],
            send_sem=y_send.at[len(y_kinds) + 1, dest], recv_sem=y_recv.at[len(y_kinds), sender],
            device_id={"yax": dest}, device_id_type=pl.DeviceIdType.MESH)

    x_wait("gate")
    x_wait("up")

    def feed(d, carry):
        @pl.when(d < ys - 1)
        def _():
            nxt = lax.rem(y + ys - d - 1, ys)
            n_copy(y, nxt).wait_recv()
            n_pass(nxt, core).start()
        j = lax.rem(y + ys - d, ys)

        @pl.when(d > 0)
        def _():
            n_pass(j, 1 - core).wait_recv()
        gu = jnp.dot(n_all[rows(j, quarter), :], gu_buf[...], preferred_element_type=F32)
        gu = gu.astype(BF16).astype(F32)
        gate = gu[:, :ff]
        act_scr[j] = (gate * jax.nn.sigmoid(gate) * gu[:, ff:]).astype(BF16)

        @pl.when(d > 0)
        def _():
            act_copy(j, y).start()
        return carry
    lax.fori_loop(0, ys, feed, 0)
    act[:, pl.ds(pl.multiple_of(y * ff, ff), ff)] = act_scr[y]
    if e_done < EMBED_CHUNKS:
        e_start(e_done)
        e_done += 1
    y_wait("wo")
    x_wait("o")
    part_scr[...] = jnp.dot(
        ox_buf[...], out_buf[...].reshape(ys * cols, xs * blk), preferred_element_type=F32)
    y_wait("down")

    def act_wait(d, carry):
        act_copy(y, lax.rem(y + ys - d, ys)).wait_recv()
        return carry
    lax.fori_loop(1, ys, act_wait, 0)

    def branch(c):
        for i in range(chips):
            r = pl.ds(pl.multiple_of((2 * i + c) * own, own), own)
            rs_scr[c, i] = part_scr[r, :] + jnp.dot(
                act[r, :], down_buf[...].reshape(ys * ff, xs * blk), preferred_element_type=F32)

    def pre_copy():
        return pltpu.make_async_remote_copy(
            src_ref=rs_scr.at[1 - core], dst_ref=pre_buf, send_sem=pre_sem.at[0], recv_sem=pre_sem.at[1],
            device_id={"xax": partner}, device_id_type=pl.DeviceIdType.MESH)

    def rs_copy(dest, sender):
        return pltpu.make_async_remote_copy(
            src_ref=rs_scr.at[core, dest], dst_ref=rs_buf.at[sender], send_sem=f_send.at[1, dest],
            recv_sem=pre_sem.at[2 + sender], device_id={"xax": 2 * dest + core},
            device_id_type=pl.DeviceIdType.MESH)

    chip = x // 2
    branch(1 - core)
    pre_copy().start()
    branch(core)
    pre_copy().wait_recv()
    rs_scr[core] = rs_scr[core] + pre_buf[...]

    def rs_start(i, carry):
        rs_copy(lax.rem(chip + i, chips), chip).start()
        return carry
    lax.fori_loop(1, chips, rs_start, 0)
    if e_done < EMBED_CHUNKS:
        e_start(e_done)
        e_done += 1

    def rs_wait(i, carry):
        rs_copy(chip, lax.rem(chip + chips - i, chips)).wait_recv()
        return carry
    lax.fori_loop(1, chips, rs_wait, 0)
    rs_buf[chip] = rs_scr[core, chip]
    res = h_buf[rows(x, own), :].astype(F32) + jnp.sum(rs_buf[...], axis=0)
    f_buf[rows(mine, own), :] = layer_norm(res, gf_buf[...]).astype(BF16)

    def f_rows(sy, sx):
        return f_buf.at[rows(sy * xs + sx, own), :]

    def f_recv_of(sy, sx):
        return f_recv.at[sy * xs + sx]

    def fx_copy(dest, sx):
        return pltpu.make_async_remote_copy(
            src_ref=f_rows(y, sx), dst_ref=f_rows(y, sx), send_sem=f_send.at[0, dest // 2],
            recv_sem=f_recv_of(y, sx), device_id={"xax": dest}, device_id_type=pl.DeviceIdType.MESH)

    def fy_copy(dest, sy, sx):
        return pltpu.make_async_remote_copy(
            src_ref=f_rows(sy, sx), dst_ref=f_rows(sy, sx), send_sem=fy_send.at[sx // 2, dest],
            recv_sem=f_recv_of(sy, sx), device_id={"yax": dest}, device_id_type=pl.DeviceIdType.MESH)

    def fp_copy(sy, sx):
        return pltpu.make_async_remote_copy(
            src_ref=f_rows(sy, sx), dst_ref=f_rows(sy, sx), send_sem=fp_send.at[sy, sx // 2],
            recv_sem=f_recv_of(sy, sx), device_id={"xax": partner}, device_id_type=pl.DeviceIdType.MESH)

    def fx_start(i, carry):
        fx_copy(lax.rem(x + 2 * i, xs), x).start()
        return carry
    lax.fori_loop(1, chips, fx_start, 0)

    def f_spread(i, carry):
        sx = lax.rem(x + xs - 2 * i, xs)

        @pl.when(i > 0)
        def _():
            fx_copy(x, sx).wait_recv()

        def over_y(d, c2):
            fy_copy(lax.rem(y + d, ys), y, sx).start()
            return c2
        lax.fori_loop(1, ys, over_y, 0)
        fp_copy(y, sx).start()
        return carry
    lax.fori_loop(0, 1, f_spread, 0)
    while e_done < EMBED_CHUNKS:
        e_start(e_done)
        e_done += 1
    lax.fori_loop(1, chips, f_spread, 0)

    e_own().wait()
    for c in range(EMBED_CHUNKS):
        def e_wait(d, carry, c=c):
            e_copy(c, x, lax.rem(x + xs - d, xs)).wait_recv()
            return carry
        lax.fori_loop(1, xs, e_wait, 0)
    if shift:
        @pl.when(core == 1)
        def _():
            for r0 in range(0, vocab, 256):
                n = min(256, vocab - r0)
                e_al[pl.ds(r0, n), :] = e_buf[pl.ds(r0 + shift, n), :]

        @pl.when(core == 0)
        def _():
            for r0 in range(0, vocab, 256):
                n = min(256, vocab - r0)
                e_al[pl.ds(r0, n), :] = e_buf[pl.ds(r0, n), :]
    else:
        e_al[...] = e_buf[...]

    def z_copy(j, slot):
        return pltpu.make_async_copy(z_scr.at[slot], logits_out.at[:, rows(j, quarter)], z_sem.at[slot])

    def head(dy, carry):
        j = lax.rem(y + ys - dy, ys)

        def forward(i, c2):
            sx = lax.rem(x + xs - 2 * i, xs)
            fy_copy(y, j, sx).wait_recv()
            fp_copy(j, sx).start()
            return c2

        @pl.when(dy > 0)
        def _():
            lax.fori_loop(0, chips, forward, 0)

        def arrive(i, c2):
            fp_copy(j, lax.rem(partner + xs - 2 * i, xs)).wait_recv()
            return c2
        lax.fori_loop(0, chips, arrive, 0)
        slot = lax.rem(dy, 2)

        @pl.when(dy >= 2)
        def _():
            z_copy(j, slot).wait()
        z = lax.dot_general(e_al[...], f_buf[rows(j, quarter), :], NT, preferred_element_type=F32)
        z_scr[slot] = z
        z_copy(j, slot).start()
        top = jnp.max(z, axis=0, keepdims=True)
        tot = jnp.sum(jnp.exp(z - top), axis=0, keepdims=True)
        st_scr[0:1, rows(j, quarter)] = top
        st_scr[1:2, rows(j, quarter)] = tot
        return carry
    lax.fori_loop(0, ys, head, 0)

    def sx_copy(dest, src):
        return pltpu.make_async_remote_copy(
            src_ref=st_scr, dst_ref=sx_buf.at[src], send_sem=sx_send.at[dest], recv_sem=sx_recv.at[src],
            device_id={"xax": dest}, device_id_type=pl.DeviceIdType.MESH)

    def sy_copy(dest, src):
        return pltpu.make_async_remote_copy(
            src_ref=sy_scr, dst_ref=sy_buf.at[src], send_sem=sy_send.at[dest], recv_sem=sy_recv.at[src],
            device_id={"yax": dest}, device_id_type=pl.DeviceIdType.MESH)

    def combine(buf):
        tops = buf[:, 0, :]
        best = jnp.max(tops, axis=0, keepdims=True)
        return best, jnp.sum(buf[:, 1, :] * jnp.exp(tops - best), axis=0, keepdims=True)

    def sx_start(d, carry):
        sx_copy(lax.rem(x + d, xs), x).start()
        return carry
    lax.fori_loop(1, xs, sx_start, 0)
    sx_buf[x] = st_scr[...]

    for name in x_kinds:
        if name in gathers:
            g_drain(name)
        else:
            x_drain(name)
    for name in y_kinds:
        y_drain(name)

    def yn_drain(d, carry):
        dest = lax.rem(y + d, ys)
        n_copy(dest, y).wait_send()
        n_pass(dest, core).wait_send()
        act_copy(dest, y).wait_send()
        return carry
    lax.fori_loop(1, ys, yn_drain, 0)
    pre_copy().wait_send()
    for c in range(EMBED_CHUNKS):
        def e_drain(d, carry, c=c):
            e_copy(c, lax.rem(x + d, xs), x).wait_send()
            return carry
        lax.fori_loop(1, xs, e_drain, 0)

    def f_drain(i, carry):
        @pl.when(i > 0)
        def _():
            rs_copy(lax.rem(chip + i, chips), chip).wait_send()
            fx_copy(lax.rem(x + 2 * i, xs), x).wait_send()
        sx = lax.rem(x + xs - 2 * i, xs)

        def over_y(d, c2):
            other = lax.rem(y + d, ys)

            @pl.when(d > 0)
            def _():
                fy_copy(other, y, sx).wait_send()
            fp_copy(other, sx).wait_send()
            return c2
        lax.fori_loop(0, ys, over_y, 0)
        return carry
    lax.fori_loop(0, chips, f_drain, 0)

    def sx_wait(d, carry):
        sx_copy(x, lax.rem(x + xs - d, xs)).wait_recv()
        return carry
    lax.fori_loop(1, xs, sx_wait, 0)
    best, whole = combine(sx_buf)
    sy_scr[0:1, :] = best
    sy_scr[1:2, :] = whole

    def sy_start(d, carry):
        sy_copy(lax.rem(y + d, ys), y).start()
        return carry
    lax.fori_loop(1, ys, sy_start, 0)
    sy_buf[y] = sy_scr[...]

    def sx_drain(d, carry):
        sx_copy(lax.rem(x + d, xs), x).wait_send()
        return carry
    lax.fori_loop(1, xs, sx_drain, 0)

    def sy_wait(d, carry):
        sy_copy(y, lax.rem(y + ys - d, ys)).wait_recv()
        sy_copy(lax.rem(y + d, ys), y).wait_send()
        return carry
    lax.fori_loop(1, ys, sy_wait, 0)
    best, whole = combine(sy_buf)
    norm_out[...] = best + jnp.log(whole)
    for dy in range(max(ys - 2, 0), ys):
        z_copy(lax.rem(y + ys - dy, ys), dy % 2).wait()


def solution(mesh):
    ys = mesh.shape["yax"]
    xs = mesh.shape["xax"]
    row_spec = P(("dp", "yax", "xax"))

    def local_step(hidden, cache_len, k_cache, v_cache, g_attn, w_query, w_key, w_value,
                   w_gate, w_up, w_out, w_down, g_final, embedding):
        batch, blk = hidden.shape
        own, slots, head_dim = k_cache.shape
        width = blk * xs
        vocab = embedding.shape[0] // xs
        shift = vocab % 8
        window = -(-vocab // 8) * 8
        half = head_dim // 2
        quarter = xs * own
        cols = w_query.shape[1] // xs
        ff = w_gate.shape[1] // xs
        heads = w_query.shape[1] * ys // head_dim
        per = 4
        groups = own // per
        freq_row = (ROPE_BASE ** (-(np.arange(half, dtype=np.float32) * 2.0) / head_dim)).astype(np.float32)
        freq = jnp.asarray(np.tile(freq_row, 4)[None, :])
        any_spec = pl.BlockSpec(memory_space=pl.ANY)
        vmem = pl.BlockSpec(memory_space=pltpu.VMEM)
        smem = pl.BlockSpec(memory_space=pltpu.SMEM)
        dma = pltpu.SemaphoreType.DMA
        nx = 12
        chips = xs // 2
        scratch = [
            pltpu.VMEM((groups, per, head_dim, slots), BF16),
            pltpu.VMEM((groups, per, head_dim, slots), BF16),
            pltpu.VMEM((quarter, width), BF16),
            pltpu.VMEM((1, width), F32),
            pltpu.VMEM((1, width), F32),
            pltpu.VMEM((w_query.shape[1], blk), BF16),
            pltpu.VMEM((ys, cols, width), BF16),
            pltpu.VMEM((width, 2 * ff), BF16),
            pltpu.VMEM((ys, ff, width), BF16),
            pltpu.VMEM((ys, cols, width), BF16),
            pltpu.VMEM((2 * head_dim, width), BF16),
            pltpu.VMEM((batch, width), BF16),
            pltpu.VMEM((quarter, ys * cols), BF16),
            pltpu.VMEM((xs, own, ys * cols), BF16),
            pltpu.VMEM((own * heads, head_dim), F32),
            pltpu.VMEM((own * heads, 1), F32),
            pltpu.VMEM((own * heads, head_dim), F32),
            pltpu.VMEM((own * heads, head_dim), F32),
            pltpu.VMEM((per * heads, slots), F32),
            pltpu.VMEM((own * heads, head_dim), F32),
            pltpu.VMEM((xs, own, ys * cols), BF16),
            pltpu.VMEM((quarter, ys * cols), BF16),
            pltpu.VMEM((ys, quarter, ff), BF16),
            pltpu.VMEM((quarter, ys * ff), BF16),
            pltpu.VMEM((quarter, width), F32),
            pltpu.VMEM((chips, own, width), F32),
            pltpu.VMEM((2, chips, own, width), F32),
            pltpu.VMEM((chips, own, width), F32),
            pltpu.VMEM((batch, width), BF16),
            pltpu.VMEM((window, width), BF16),
            pltpu.VMEM((vocab, width), BF16),
            pltpu.VMEM((2, vocab, quarter), F32),
            pltpu.VMEM((2, batch), F32),
            pltpu.VMEM((xs, 2, batch), F32),
            pltpu.VMEM((2, batch), F32),
            pltpu.VMEM((ys, 2, batch), F32),
            dma((2, groups)), dma((nx + 1,)), dma((2,)),
            dma((nx, xs)), dma((nx, xs)), dma((5, xs)), dma((5, ys)), dma((4, ys)),
            dma((EMBED_CHUNKS, xs)), dma((EMBED_CHUNKS, xs)),
            dma((ys, 2)), dma((ys,)), dma((2 + chips,)), dma((2, chips)), dma((ys * xs,)),
            dma((chips, ys)), dma((ys, chips)), dma((xs,)), dma((xs,)), dma((ys,)), dma((ys,)),
        ]
        cfg = (ys, xs, own, vocab, shift)
        key_new, value_new, logits, norm = pl.pallas_call(
            functools.partial(kernel, cfg),
            name="decode_layer",
            out_shape=(
                jax.ShapeDtypeStruct((own, head_dim), BF16),
                jax.ShapeDtypeStruct((own, head_dim), BF16),
                jax.ShapeDtypeStruct((vocab, batch), F32),
                jax.ShapeDtypeStruct((1, batch), F32)),
            in_specs=[smem, any_spec, any_spec, any_spec, any_spec, any_spec, vmem] + [any_spec] * 7 + [vmem],
            out_specs=(vmem, vmem, any_spec, vmem),
            scratch_shapes=scratch,
            compiler_params=pltpu.CompilerParams(
                collective_id=0, has_side_effects=True, vmem_limit_bytes=67043328),
        )(cache_len, hidden, k_cache.transpose(0, 2, 1), v_cache.transpose(0, 2, 1),
          g_attn[None, :], g_final[None, :], w_query, w_key.T, w_value.T, w_gate, w_up, w_out, w_down,
          embedding, freq)
        log_norm = norm[0]
        return key_new, value_new, (logits - norm).T, log_norm

    in_specs = (P("dp", "xax"), P("dp"), row_spec, row_spec, P("xax"), P("xax", "yax"),
                P("xax", None), P("xax", None), P("xax", "yax"), P("xax", "yax"),
                P("yax", "xax"), P("yax", "xax"), P("xax"), P("yax", "xax"))
    out_specs = (row_spec, row_spec, P("dp", ("yax", "xax")), P("dp"))
    return jax.shard_map(local_step, mesh=mesh, in_specs=in_specs, out_specs=out_specs, check_vma=False)
```

```python
import functools

import jax
import jax.numpy as jnp
import numpy as np
from jax import lax
from jax.experimental import pallas as pl
from jax.experimental.pallas import tpu as pltpu
from jax.sharding import PartitionSpec as P

EPS = 1e-6
ROPE_BASE = 10000.0
F32 = jnp.float32
BF16 = jnp.bfloat16
NT = (((1,), (1,)), ((), ()))
EMBED_CHUNKS = 16
EMBED_GROUPS = 4


def layer_norm(values_in, gain):
    mean = jnp.mean(values_in, axis=-1, keepdims=True)
    centred = values_in - mean
    var = jnp.mean(centred * centred, axis=-1, keepdims=True)
    return centred * lax.rsqrt(var + EPS) * gain


def row_chunks(total, count):
    cuts = [16 * (total // 16 * i // count) for i in range(count)] + [total]
    return [(cuts[i], cuts[i + 1] - cuts[i]) for i in range(count)]


def kernel(cfg, lens, hidden, k_hbm, v_hbm, g_attn, g_final, w_query, w_key, w_value, w_gate, w_up,
           w_out, w_down, embed, freq,
           k_out, v_out, logits_out, norm_out,
           k_buf, v_buf, h_buf, ga_buf, gf_buf, wqt, wq_buf, gu_buf, down_buf, out_buf, kv_buf,
           n_all, q_scr, qx_buf, q2d, snew, krep, vrep, s_scr, od_scr, o_scr, ox_buf, act_scr, act, part_scr,
           pre_buf, rs_scr, rs_buf, f_buf, e_buf, z_scr, st_scr, k_scr, v_scr, norm_scr, sx_buf, sy_scr, sy_buf,
           kv_sem, own_sem, z_sem, x_send, x_recv, g_send, y_send, y_recv, e_send, e_recv,
           n_recv, n_fwd, pre_sem, f_send, f_recv, fy_send, fp_send, sx_send, sx_recv, sy_send, sy_recv):
    ys, xs, own, vocab, shift = cfg
    y = lax.axis_index("yax")
    x = lax.axis_index("xax")
    core = lax.rem(x, 2)
    partner = x + 1 - 2 * core
    blk = hidden.shape[1]
    quarter = xs * own
    head_dim = k_hbm.shape[1]
    half = head_dim // 2
    seqs = k_hbm.shape[0]
    slots = k_hbm.shape[2]
    heads = w_query.shape[1] * ys // head_dim
    groups = k_buf.shape[0]
    per = seqs // groups
    window = e_buf.shape[0]

    def lanes(i):
        return pl.ds(pl.multiple_of(i * blk, 128), blk)

    def rows(i, n):
        return pl.ds(pl.multiple_of(i * n, n), n)

    def cache_copy(g, src, dst, s):
        return pltpu.make_async_copy(src.at[pl.ds(g * per, per)], dst.at[g], kv_sem.at[s, g])

    def start_cache(g, carry):
        cache_copy(g, k_hbm, k_buf, 0).start()
        return carry
    lax.fori_loop(0, groups, start_cache, 0)

    wqt[...] = w_query[...].astype(F32).T.astype(BF16)

    barrier = pltpu.get_barrier_semaphore()

    def signal_row(d, carry):
        pl.semaphore_signal(barrier, inc=1, device_id={"xax": lax.rem(x + d, xs)},
                            device_id_type=pl.DeviceIdType.MESH)
        return carry
    lax.fori_loop(1, xs, signal_row, 0)

    def signal_column(d, carry):
        pl.semaphore_signal(barrier, inc=1, device_id={"yax": lax.rem(y + d, ys)},
                            device_id_type=pl.DeviceIdType.MESH)
        return carry
    lax.fori_loop(1, ys, signal_column, 0)
    pl.semaphore_wait(barrier, xs + ys - 2)

    cols = wqt.shape[0] // xs
    ff = w_gate.shape[1] // xs
    x_kinds = {
        "hidden": (lambda p: hidden.at[rows(y, quarter), :], lambda s: h_buf.at[:, lanes(s)]),
        "wq": (lambda p: wqt.at[rows(p, cols), :], lambda s: wq_buf.at[y, :, lanes(s)]),
        "ga": (lambda p: g_attn, lambda s: ga_buf.at[:, lanes(s)]),
        "gf": (lambda p: g_final, lambda s: gf_buf.at[:, lanes(s)]),
        "wk": (lambda p: w_key, lambda s: kv_buf.at[pl.ds(0, head_dim), lanes(s)]),
        "wv": (lambda p: w_value, lambda s: kv_buf.at[pl.ds(head_dim, head_dim), lanes(s)]),
        "wo": (lambda p: w_out.at[rows(p, cols), :], lambda s: out_buf.at[y, :, lanes(s)]),
        "gate": (lambda p: w_gate.at[:, lanes(p)], lambda s: gu_buf.at[rows(s, blk), pl.ds(0, ff)]),
        "up": (lambda p: w_up.at[:, lanes(p)], lambda s: gu_buf.at[rows(s, blk), pl.ds(ff, ff)]),
        "down": (lambda p: w_down.at[rows(p, ff), :], lambda s: down_buf.at[y, :, lanes(s)]),
        "q": (lambda p: q_scr.at[rows(p, own), :], lambda s: qx_buf.at[s]),
        "o": (lambda p: o_scr.at[p], lambda s: ox_buf.at[rows(s, own), :]),
    }
    x_index = {name: i for i, name in enumerate(x_kinds)}

    def x_copy(name, dest, sender):
        src, dst = x_kinds[name]
        k = x_index[name]
        return pltpu.make_async_remote_copy(
            src_ref=src(dest), dst_ref=dst(sender), send_sem=x_send.at[k, dest],
            recv_sem=x_recv.at[k, sender], device_id={"xax": dest},
            device_id_type=pl.DeviceIdType.MESH)

    def own_copy(name):
        src, dst = x_kinds[name]
        return pltpu.make_async_copy(src(x), dst(x), own_sem.at[x_index[name]])

    chips = xs // 2
    gathers = {name: i for i, name in enumerate(("hidden", "ga", "gf", "wk", "wv"))}

    def g_copy(name, sender, source):
        src, dst = x_kinds[name]
        return pltpu.make_async_remote_copy(
            src_ref=source, dst_ref=dst(sender), send_sem=g_send.at[gathers[name], sender],
            recv_sem=x_recv.at[x_index[name], sender], device_id={"xax": partner},
            device_id_type=pl.DeviceIdType.MESH)

    def g_start(name):
        def body(i, carry):
            x_copy(name, lax.rem(x + 2 * i, xs), x).start()
            return carry
        lax.fori_loop(1, chips, body, 0)
        g_copy(name, x, x_kinds[name][0](x)).start()
        own_copy(name).start()

    def g_forward(name):
        def body(i, carry):
            sender = lax.rem(x + xs - 2 * i, xs)
            x_copy(name, x, sender).wait_recv()
            g_copy(name, sender, x_kinds[name][1](sender)).start()
            return carry
        lax.fori_loop(1, chips, body, 0)

    def g_wait(name):
        def body(i, carry):
            sender = lax.rem(partner + xs - 2 * i, xs)
            g_copy(name, sender, x_kinds[name][1](sender)).wait_recv()
            return carry
        lax.fori_loop(0, chips, body, 0)
        own_copy(name).wait()

    def g_drain(name):
        def body(i, carry):
            @pl.when(i > 0)
            def _():
                x_copy(name, lax.rem(x + 2 * i, xs), x).wait_send()
            sender = lax.rem(x + xs - 2 * i, xs)
            g_copy(name, sender, x_kinds[name][1](sender)).wait_send()
            return carry
        lax.fori_loop(0, chips, body, 0)

    def x_start(name):
        def body(d, carry):
            x_copy(name, lax.rem(x + d, xs), x).start()
            return carry
        lax.fori_loop(1, xs, body, 0)
        own_copy(name).start()

    def x_wait(name):
        def body(d, carry):
            x_copy(name, x, lax.rem(x + xs - d, xs)).wait_recv()
            return carry
        lax.fori_loop(1, xs, body, 0)
        own_copy(name).wait()

    def x_drain(name):
        def body(d, carry):
            x_copy(name, lax.rem(x + d, xs), x).wait_send()
            return carry
        lax.fori_loop(1, xs, body, 0)

    y_kinds = {"wq": wq_buf, "wo": out_buf, "down": down_buf}
    y_index = {name: i for i, name in enumerate(y_kinds)}

    def y_copy(name, dest, sender):
        buf = y_kinds[name]
        k = y_index[name]
        return pltpu.make_async_remote_copy(
            src_ref=buf.at[sender], dst_ref=buf.at[sender], send_sem=y_send.at[k, dest],
            recv_sem=y_recv.at[k, sender], device_id={"yax": dest},
            device_id_type=pl.DeviceIdType.MESH)

    def y_start(name):
        def body(d, carry):
            y_copy(name, lax.rem(y + d, ys), y).start()
            return carry
        lax.fori_loop(1, ys, body, 0)

    def y_wait(name):
        def body(d, carry):
            y_copy(name, y, lax.rem(y + ys - d, ys)).wait_recv()
            return carry
        lax.fori_loop(1, ys, body, 0)

    def y_drain(name):
        def body(d, carry):
            y_copy(name, lax.rem(y + d, ys), y).wait_send()
            return carry
        lax.fori_loop(1, ys, body, 0)

    e_parts = row_chunks(window, EMBED_CHUNKS)

    def e_first(p):
        return p * vocab - lax.rem(p, 2) * shift

    def e_copy(c, dest, sender):
        r0, n = e_parts[c]
        return pltpu.make_async_remote_copy(
            src_ref=embed.at[pl.ds(pl.multiple_of(e_first(dest) + r0, 8), n), :],
            dst_ref=e_buf.at[pl.ds(r0, n), lanes(sender)],
            send_sem=e_send.at[c, dest], recv_sem=e_recv.at[c, sender],
            device_id={"xax": dest}, device_id_type=pl.DeviceIdType.MESH)

    def e_own():
        return pltpu.make_async_copy(
            embed.at[pl.ds(pl.multiple_of(e_first(x), 8), window), :], e_buf.at[:, lanes(x)],
            own_sem.at[len(x_kinds)])

    def e_start(c):
        def body(d, carry):
            e_copy(c, lax.rem(x + d, xs), x).start()
            return carry
        lax.fori_loop(1, xs, body, 0)

    x_start("wq")
    for name in ("hidden", "ga"):
        g_start(name)
    for name in ("wo", "down"):
        x_start(name)
    for name in ("wk", "wv", "gf"):
        g_start(name)
    e_start(0)
    e_own().start()

    def start_cache_v(g, carry):
        cache_copy(g, v_hbm, v_buf, 1).start()
        return carry
    lax.fori_loop(0, groups, start_cache_v, 0)

    x_wait("wq")
    y_start("wq")
    for name in ("hidden", "ga"):
        g_forward(name)
    for name in ("hidden", "ga"):
        g_wait(name)
    my_rows = rows(y, quarter)
    n_all[my_rows, :] = layer_norm(h_buf[...].astype(F32), ga_buf[...]).astype(BF16)

    part = quarter // 2

    def n_rows(j, c):
        return pl.ds(pl.multiple_of(j * quarter + c * part, part), part)

    def n_copy(dest, sender):
        r = n_rows(sender, core)
        return pltpu.make_async_remote_copy(
            src_ref=n_all.at[r, :], dst_ref=n_all.at[r, :], send_sem=y_send.at[len(y_kinds), dest],
            recv_sem=n_recv.at[sender, core], device_id={"yax": dest},
            device_id_type=pl.DeviceIdType.MESH)

    def n_pass(sender, c):
        r = n_rows(sender, c)
        return pltpu.make_async_remote_copy(
            src_ref=n_all.at[r, :], dst_ref=n_all.at[r, :], send_sem=n_fwd.at[sender],
            recv_sem=n_recv.at[sender, c], device_id={"xax": partner},
            device_id_type=pl.DeviceIdType.MESH)

    y_wait("wq")
    wq_all = wq_buf[...].reshape(ys * cols, xs * blk)
    q_scr[...] = lax.dot_general(n_all[my_rows, :], wq_all, NT, preferred_element_type=F32).astype(BF16)
    x_start("q")
    x_start("gate")
    x_start("up")

    def n_start(d, carry):
        n_copy(lax.rem(y + d, ys), y).start()
        return carry
    lax.fori_loop(1, ys, n_start, 0)
    x_wait("wo")
    y_start("wo")
    x_wait("down")
    y_start("down")
    for c in range(1, 6):
        e_start(c)

    row_id = lax.broadcasted_iota(jnp.int32, (own, 4 * half), 0)
    first_row = (y * xs + x) * own
    position = jnp.zeros((own, 4 * half), jnp.int32)
    for b in range(own):
        position = jnp.where(row_id == b, lens[first_row + b], position)
    angle = position.astype(F32) * freq[...]
    cos_a = jnp.cos(angle)
    sin_a = jnp.sin(angle)
    for name in ("wk", "wv", "gf"):
        g_forward(name)
    for name in ("wk", "wv", "gf"):
        g_wait(name)
    mine = y * xs + x
    n_own = n_all[rows(mine, own), :]
    kv = lax.dot_general(n_own, kv_buf[...], NT, preferred_element_type=F32).astype(BF16).astype(F32)
    k1 = kv[:, :half]
    k2 = kv[:, half:head_dim]
    c1 = cos_a[:, :half]
    s1 = sin_a[:, :half]
    key = jnp.concatenate([k1 * c1 - k2 * s1, k2 * c1 + k1 * s1], axis=1).astype(BF16)
    value = kv[:, head_dim:].astype(BF16)
    k_scr[...] = key
    v_scr[...] = value
    small_outs = [pltpu.make_async_copy(k_scr, k_out, z_sem.at[EMBED_GROUPS]),
                  pltpu.make_async_copy(v_scr, v_out, z_sem.at[EMBED_GROUPS + 1])]
    for copy in small_outs:
        copy.start()
    for h in range(heads):
        krep[pl.ds(h, own, stride=heads), :] = key.astype(F32)
        vrep[pl.ds(h, own, stride=heads), :] = value.astype(F32)

    x_wait("q")
    for xc in range(xs // 2):
        qa = qx_buf[2 * xc].astype(F32)
        qb = qx_buf[2 * xc + 1].astype(F32)
        ra = (qa * cos_a - qb * sin_a).astype(BF16).astype(F32)
        rb = (qb * cos_a + qa * sin_a).astype(BF16).astype(F32)
        for yc in range(ys):
            pair = jnp.concatenate([ra[:, yc * half:(yc + 1) * half], rb[:, yc * half:(yc + 1) * half]], axis=1)
            q2d[pl.ds(xc * ys + yc, own, stride=heads), :] = pair
    scale = head_dim ** -0.5
    snew[...] = jnp.sum(q2d[...] * krep[...], axis=1, keepdims=True) * scale

    gr = per * heads
    seg_r = lax.broadcasted_iota(jnp.int32, (gr, per * head_dim), 0) // heads
    seg_c = lax.broadcasted_iota(jnp.int32, (gr, per * head_dim), 1) // head_dim
    diag = (seg_r == seg_c).astype(F32)
    tile = min(512, slots)
    row_g = lax.broadcasted_iota(jnp.int32, (gr, 1), 0) // heads
    lane_g = lax.broadcasted_iota(jnp.int32, (gr, tile), 1)

    def attend(g, carry):
        cache_copy(g, k_hbm, k_buf, 0).wait()
        qg = q2d[rows(g, gr), :]
        qbd = (jnp.concatenate([qg] * per, axis=1) * diag).astype(BF16)
        len_g = jnp.zeros((gr, 1), jnp.int32)
        for s in range(per):
            len_g = jnp.where(row_g == s, lens[first_row + g * per + s], len_g)
        new = snew[rows(g, gr), :]
        top = jnp.full((gr, tile), -jnp.inf, F32)
        kg = k_buf.at[g]
        vg = v_buf.at[g]
        for c in range(slots // tile):
            kc = kg[:, :, pl.ds(c * tile, tile)].reshape(per * head_dim, tile)
            sc = jnp.dot(qbd, kc, preferred_element_type=F32) * scale
            sc = jnp.where(lane_g < len_g - c * tile, sc, -jnp.inf)
            s_scr[:, pl.ds(c * tile, tile)] = sc
            top = jnp.maximum(top, sc)
        row_max = jnp.maximum(jnp.max(top, axis=1, keepdims=True), new)
        total = jnp.zeros((gr, tile), F32)
        for c in range(slots // tile):
            ex = jnp.exp(s_scr[:, pl.ds(c * tile, tile)] - row_max)
            s_scr[:, pl.ds(c * tile, tile)] = ex
            total = total + ex
        w_new = jnp.exp(new - row_max)
        den = jnp.sum(total, axis=1, keepdims=True) + w_new
        inv = 1.0 / den
        cache_copy(g, v_hbm, v_buf, 1).wait()
        mixed = jnp.zeros((gr, per * head_dim), F32)
        for c in range(slots // tile):
            pr = (s_scr[:, pl.ds(c * tile, tile)] * inv).astype(BF16)
            vc = vg[:, :, pl.ds(c * tile, tile)].reshape(per * head_dim, tile)
            mixed = mixed + lax.dot_general(pr, vc, NT, preferred_element_type=F32)
        add = (w_new * inv).astype(BF16).astype(F32) * vrep[rows(g, gr), :]
        for s in range(per):
            od_scr[pl.ds(pl.multiple_of(g * gr + s * heads, heads), heads), :] = (
                mixed[s * heads:(s + 1) * heads, s * head_dim:(s + 1) * head_dim]
                + add[s * heads:(s + 1) * heads, :])
        return carry

    lax.fori_loop(0, groups, attend, 0)
    for xc in range(xs // 2):
        parts = [od_scr[pl.ds(xc * ys + yc, own, stride=heads), :] for yc in range(ys)]
        o_scr[2 * xc] = jnp.concatenate([p[:, :half] for p in parts], axis=1).astype(BF16)
        o_scr[2 * xc + 1] = jnp.concatenate([p[:, half:] for p in parts], axis=1).astype(BF16)
    x_start("o")
    e_start(6)

    def act_copy(dest, sender):
        return pltpu.make_async_remote_copy(
            src_ref=act_scr.at[dest], dst_ref=act.at[:, pl.ds(pl.multiple_of(sender * ff, ff), ff)],
            send_sem=y_send.at[len(y_kinds) + 1, dest], recv_sem=y_recv.at[len(y_kinds), sender],
            device_id={"yax": dest}, device_id_type=pl.DeviceIdType.MESH)

    x_wait("gate")
    x_wait("up")

    def feed(d, carry):
        @pl.when(d < ys - 1)
        def _():
            nxt = lax.rem(y + ys - d - 1, ys)
            n_copy(y, nxt).wait_recv()
            n_pass(nxt, core).start()
        j = lax.rem(y + ys - d, ys)

        @pl.when(d > 0)
        def _():
            n_pass(j, 1 - core).wait_recv()
        gu = jnp.dot(n_all[rows(j, quarter), :], gu_buf[...], preferred_element_type=F32)
        gu = gu.astype(BF16).astype(F32)
        gate = gu[:, :ff]
        act_scr[j] = (gate * jax.nn.sigmoid(gate) * gu[:, ff:]).astype(BF16)

        @pl.when(d > 0)
        def _():
            act_copy(j, y).start()
        return carry
    lax.fori_loop(0, ys, feed, 0)
    act[:, pl.ds(pl.multiple_of(y * ff, ff), ff)] = act_scr[y]
    e_start(7)
    y_wait("wo")
    x_wait("o")
    part_scr[...] = jnp.dot(
        ox_buf[...], out_buf[...].reshape(ys * cols, xs * blk), preferred_element_type=F32)
    y_wait("down")

    def act_wait(d, carry):
        act_copy(y, lax.rem(y + ys - d, ys)).wait_recv()
        return carry
    lax.fori_loop(1, ys, act_wait, 0)

    down_all = down_buf[...].reshape(ys * ff, xs * blk)
    part_scr[...] = part_scr[...] + jnp.dot(act[...], down_all, preferred_element_type=F32)

    def branch(c):
        for i in range(chips):
            rs_scr[c, i] = part_scr[pl.ds(pl.multiple_of((2 * i + c) * own, own), own), :]

    def pre_copy():
        return pltpu.make_async_remote_copy(
            src_ref=rs_scr.at[1 - core], dst_ref=pre_buf, send_sem=pre_sem.at[0], recv_sem=pre_sem.at[1],
            device_id={"xax": partner}, device_id_type=pl.DeviceIdType.MESH)

    def rs_copy(dest, sender):
        return pltpu.make_async_remote_copy(
            src_ref=rs_scr.at[core, dest], dst_ref=rs_buf.at[sender], send_sem=f_send.at[1, dest],
            recv_sem=pre_sem.at[2 + sender], device_id={"xax": 2 * dest + core},
            device_id_type=pl.DeviceIdType.MESH)

    chip = x // 2
    branch(1 - core)
    pre_copy().start()
    branch(core)
    pre_copy().wait_recv()
    rs_scr[core] = rs_scr[core] + pre_buf[...]

    def rs_start(i, carry):
        rs_copy(lax.rem(chip + i, chips), chip).start()
        return carry
    lax.fori_loop(1, chips, rs_start, 0)
    e_start(8)

    def rs_wait(i, carry):
        rs_copy(chip, lax.rem(chip + chips - i, chips)).wait_recv()
        return carry
    lax.fori_loop(1, chips, rs_wait, 0)
    rs_buf[chip] = rs_scr[core, chip]
    res = h_buf[rows(x, own), :].astype(F32) + jnp.sum(rs_buf[...], axis=0)
    f_buf[rows(mine, own), :] = layer_norm(res, gf_buf[...]).astype(BF16)

    def f_rows(sy, sx):
        return f_buf.at[rows(sy * xs + sx, own), :]

    def f_recv_of(sy, sx):
        return f_recv.at[sy * xs + sx]

    def fx_copy(dest, sx):
        return pltpu.make_async_remote_copy(
            src_ref=f_rows(y, sx), dst_ref=f_rows(y, sx), send_sem=f_send.at[0, dest // 2],
            recv_sem=f_recv_of(y, sx), device_id={"xax": dest}, device_id_type=pl.DeviceIdType.MESH)

    def fy_copy(dest, sy, sx):
        return pltpu.make_async_remote_copy(
            src_ref=f_rows(sy, sx), dst_ref=f_rows(sy, sx), send_sem=fy_send.at[sx // 2, dest],
            recv_sem=f_recv_of(sy, sx), device_id={"yax": dest}, device_id_type=pl.DeviceIdType.MESH)

    def fp_copy(sy, sx):
        return pltpu.make_async_remote_copy(
            src_ref=f_rows(sy, sx), dst_ref=f_rows(sy, sx), send_sem=fp_send.at[sy, sx // 2],
            recv_sem=f_recv_of(sy, sx), device_id={"xax": partner}, device_id_type=pl.DeviceIdType.MESH)

    def fx_start(i, carry):
        fx_copy(lax.rem(x + 2 * i, xs), x).start()
        return carry
    lax.fori_loop(1, chips, fx_start, 0)

    def f_spread(i, carry):
        sx = lax.rem(x + xs - 2 * i, xs)

        @pl.when(i > 0)
        def _():
            fx_copy(x, sx).wait_recv()

        def over_y(d, c2):
            fy_copy(lax.rem(y + d, ys), y, sx).start()
            return c2
        lax.fori_loop(1, ys, over_y, 0)
        fp_copy(y, sx).start()
        return carry
    lax.fori_loop(0, 1, f_spread, 0)
    for c in range(9, EMBED_CHUNKS):
        e_start(c)
    lax.fori_loop(1, chips, f_spread, 0)

    for name in x_kinds:
        if name in gathers:
            g_drain(name)
        else:
            x_drain(name)
    for name in y_kinds:
        y_drain(name)

    def yn_drain(d, carry):
        dest = lax.rem(y + d, ys)
        n_copy(dest, y).wait_send()
        n_pass(dest, core).wait_send()
        act_copy(dest, y).wait_send()
        return carry
    lax.fori_loop(1, ys, yn_drain, 0)
    pre_copy().wait_send()
    for copy in small_outs:
        copy.wait()

    def f_from_y(d, carry):
        sy = lax.rem(y + ys - d, ys)

        def one(i, c2):
            sx = lax.rem(x + xs - 2 * i, xs)
            fy_copy(y, sy, sx).wait_recv()
            fp_copy(sy, sx).start()
            return c2
        lax.fori_loop(0, chips, one, 0)
        return carry
    lax.fori_loop(1, ys, f_from_y, 0)

    def f_from_core(d, carry):
        sy = lax.rem(y + ys - d, ys)

        def one(i, c2):
            fp_copy(sy, lax.rem(partner + xs - 2 * i, xs)).wait_recv()
            return c2
        lax.fori_loop(0, chips, one, 0)
        return carry
    lax.fori_loop(0, ys, f_from_core, 0)

    each = EMBED_CHUNKS // EMBED_GROUPS

    def group_rows(g):
        r0 = e_parts[g * each][0]
        last = e_parts[(g + 1) * each - 1]
        return r0, last[0] + last[1] - r0

    def z_copy(g):
        r0, n = group_rows(g)
        return pltpu.make_async_copy(z_scr.at[pl.ds(r0, n), :], logits_out.at[pl.ds(r0, n), :], z_sem.at[g])

    skip = core * shift
    top = jnp.full((1, f_buf.shape[0]), -jnp.inf, F32)
    total = jnp.zeros((1, f_buf.shape[0]), F32)
    e_own().wait()
    for g in range(EMBED_GROUPS):
        for c in range(g * each, (g + 1) * each):
            def e_wait(d, carry, c=c):
                e_copy(c, x, lax.rem(x + xs - d, xs)).wait_recv()
                return carry
            lax.fori_loop(1, xs, e_wait, 0)
        r0, n = group_rows(g)
        z = lax.dot_general(e_buf[pl.ds(r0, n), :], f_buf[...], NT, preferred_element_type=F32)
        z_scr[pl.ds(r0, n), :] = z
        z_copy(g).start()
        z = z_scr[pl.ds(r0, n), :]
        if shift and g in (0, EMBED_GROUPS - 1):
            index = lax.broadcasted_iota(jnp.int32, (n, 1), 0) + r0
            z = jnp.where(jnp.logical_and(index >= skip, index < skip + vocab), z, -jnp.inf)
        top_g = jnp.maximum(top, jnp.max(z, axis=0, keepdims=True))
        total = total * jnp.exp(top - top_g) + jnp.sum(jnp.exp(z - top_g), axis=0, keepdims=True)
        top = top_g
    st_scr[0:1, :] = top
    st_scr[1:2, :] = total

    def sx_copy(dest, src):
        return pltpu.make_async_remote_copy(
            src_ref=st_scr, dst_ref=sx_buf.at[src], send_sem=sx_send.at[dest], recv_sem=sx_recv.at[src],
            device_id={"xax": dest}, device_id_type=pl.DeviceIdType.MESH)

    def sy_copy(dest, src):
        return pltpu.make_async_remote_copy(
            src_ref=sy_scr, dst_ref=sy_buf.at[src], send_sem=sy_send.at[dest], recv_sem=sy_recv.at[src],
            device_id={"yax": dest}, device_id_type=pl.DeviceIdType.MESH)

    def combine(buf):
        tops = buf[:, 0, :]
        best = jnp.max(tops, axis=0, keepdims=True)
        return best, jnp.sum(buf[:, 1, :] * jnp.exp(tops - best), axis=0, keepdims=True)

    def sx_start(d, carry):
        sx_copy(lax.rem(x + d, xs), x).start()
        return carry
    lax.fori_loop(1, xs, sx_start, 0)
    sx_buf[x] = st_scr[...]

    for c in range(EMBED_CHUNKS):
        def e_drain(d, carry, c=c):
            e_copy(c, lax.rem(x + d, xs), x).wait_send()
            return carry
        lax.fori_loop(1, xs, e_drain, 0)

    def f_drain(i, carry):
        @pl.when(i > 0)
        def _():
            rs_copy(lax.rem(chip + i, chips), chip).wait_send()
            fx_copy(lax.rem(x + 2 * i, xs), x).wait_send()
        sx = lax.rem(x + xs - 2 * i, xs)

        def over_y(d, c2):
            other = lax.rem(y + d, ys)

            @pl.when(d > 0)
            def _():
                fy_copy(other, y, sx).wait_send()
            fp_copy(other, sx).wait_send()
            return c2
        lax.fori_loop(0, ys, over_y, 0)
        return carry
    lax.fori_loop(0, chips, f_drain, 0)

    def sx_wait(d, carry):
        sx_copy(x, lax.rem(x + xs - d, xs)).wait_recv()
        return carry
    lax.fori_loop(1, xs, sx_wait, 0)
    best, whole = combine(sx_buf)
    sy_scr[0:1, :] = best
    sy_scr[1:2, :] = whole

    def sy_start(d, carry):
        sy_copy(lax.rem(y + d, ys), y).start()
        return carry
    lax.fori_loop(1, ys, sy_start, 0)
    sy_buf[y] = sy_scr[...]

    def sx_drain(d, carry):
        sx_copy(lax.rem(x + d, xs), x).wait_send()
        return carry
    lax.fori_loop(1, xs, sx_drain, 0)

    def sy_wait(d, carry):
        sy_copy(y, lax.rem(y + ys - d, ys)).wait_recv()
        sy_copy(lax.rem(y + d, ys), y).wait_send()
        return carry
    lax.fori_loop(1, ys, sy_wait, 0)
    best, whole = combine(sy_buf)
    norm_scr[...] = best + jnp.log(whole)
    norm_copy = pltpu.make_async_copy(norm_scr, norm_out, z_sem.at[EMBED_GROUPS + 2])
    norm_copy.start()
    for g in range(EMBED_GROUPS):
        z_copy(g).wait()
    norm_copy.wait()


def finish_kernel(shift, z_ref, next_ref, norm, key, value, out_ref, k_out, v_out, norm_out):
    n = z_ref.shape[0]
    if shift:
        odd = lax.rem(lax.axis_index("xax"), 2) == 1

        @pl.when(odd)
        def _():
            out_ref[pl.ds(0, n - shift), :] = z_ref[pl.ds(shift, n - shift), :] - norm[...]
            out_ref[pl.ds(n - shift, shift), :] = next_ref[pl.ds(0, shift), :] - norm[...]

        @pl.when(jnp.logical_not(odd))
        def _():
            out_ref[...] = z_ref[...] - norm[...]
    else:
        out_ref[...] = z_ref[...] - norm[...]
    k_out[...] = key[...]
    v_out[...] = value[...]
    norm_out[...] = norm[...]


def solution(mesh):
    ys = mesh.shape["yax"]
    xs = mesh.shape["xax"]
    row_spec = P(("dp", "yax", "xax"))

    def local_step(hidden, cache_len, k_cache, v_cache, g_attn, w_query, w_key, w_value,
                   w_gate, w_up, w_out, w_down, g_final, embedding):
        batch, blk = hidden.shape
        own, slots, head_dim = k_cache.shape
        width = blk * xs
        vocab = embedding.shape[0] // xs
        shift = vocab % 8
        window = -(-vocab // 8) * 8
        half = head_dim // 2
        quarter = xs * own
        cols = w_query.shape[1] // xs
        ff = w_gate.shape[1] // xs
        heads = w_query.shape[1] * ys // head_dim
        per = 4
        groups = own // per
        freq_row = (ROPE_BASE ** (-(np.arange(half, dtype=np.float32) * 2.0) / head_dim)).astype(np.float32)
        freq = jnp.asarray(np.tile(freq_row, 4)[None, :])
        any_spec = pl.BlockSpec(memory_space=pl.ANY)
        vmem = pl.BlockSpec(memory_space=pltpu.VMEM)
        smem = pl.BlockSpec(memory_space=pltpu.SMEM)
        dma = pltpu.SemaphoreType.DMA
        nx = 12
        chips = xs // 2
        scratch = [
            pltpu.VMEM((groups, per, head_dim, slots), BF16),
            pltpu.VMEM((groups, per, head_dim, slots), BF16),
            pltpu.VMEM((quarter, width), BF16),
            pltpu.VMEM((1, width), F32),
            pltpu.VMEM((1, width), F32),
            pltpu.VMEM((w_query.shape[1], blk), BF16),
            pltpu.VMEM((ys, cols, width), BF16),
            pltpu.VMEM((width, 2 * ff), BF16),
            pltpu.VMEM((ys, ff, width), BF16),
            pltpu.VMEM((ys, cols, width), BF16),
            pltpu.VMEM((2 * head_dim, width), BF16),
            pltpu.VMEM((batch, width), BF16),
            pltpu.VMEM((quarter, ys * cols), BF16),
            pltpu.VMEM((xs, own, ys * cols), BF16),
            pltpu.VMEM((own * heads, head_dim), F32),
            pltpu.VMEM((own * heads, 1), F32),
            pltpu.VMEM((own * heads, head_dim), F32),
            pltpu.VMEM((own * heads, head_dim), F32),
            pltpu.VMEM((per * heads, slots), F32),
            pltpu.VMEM((own * heads, head_dim), F32),
            pltpu.VMEM((xs, own, ys * cols), BF16),
            pltpu.VMEM((quarter, ys * cols), BF16),
            pltpu.VMEM((ys, quarter, ff), BF16),
            pltpu.VMEM((quarter, ys * ff), BF16),
            pltpu.VMEM((quarter, width), F32),
            pltpu.VMEM((chips, own, width), F32),
            pltpu.VMEM((2, chips, own, width), F32),
            pltpu.VMEM((chips, own, width), F32),
            pltpu.VMEM((batch, width), BF16),
            pltpu.VMEM((window, width), BF16),
            pltpu.VMEM((window, batch), F32),
            pltpu.VMEM((2, batch), F32),
            pltpu.VMEM((own, head_dim), BF16),
            pltpu.VMEM((own, head_dim), BF16),
            pltpu.VMEM((1, batch), F32),
            pltpu.VMEM((xs, 2, batch), F32),
            pltpu.VMEM((2, batch), F32),
            pltpu.VMEM((ys, 2, batch), F32),
            dma((2, groups)), dma((nx + 1,)), dma((EMBED_GROUPS + 3,)),
            dma((nx, xs)), dma((nx, xs)), dma((5, xs)), dma((5, ys)), dma((4, ys)),
            dma((EMBED_CHUNKS, xs)), dma((EMBED_CHUNKS, xs)),
            dma((ys, 2)), dma((ys,)), dma((2 + chips,)), dma((2, chips)), dma((ys * xs,)),
            dma((chips, ys)), dma((ys, chips)), dma((xs,)), dma((xs,)), dma((ys,)), dma((ys,)),
        ]
        cfg = (ys, xs, own, vocab, shift)
        key_new, value_new, logits, norm = pl.pallas_call(
            functools.partial(kernel, cfg),
            name="decode_layer",
            out_shape=(
                jax.ShapeDtypeStruct((own, head_dim), BF16),
                jax.ShapeDtypeStruct((own, head_dim), BF16),
                jax.ShapeDtypeStruct((window, batch), F32),
                jax.ShapeDtypeStruct((1, batch), F32)),
            in_specs=[smem, any_spec, any_spec, any_spec, any_spec, any_spec, vmem] + [any_spec] * 7 + [vmem],
            out_specs=(any_spec, any_spec, any_spec, any_spec),
            scratch_shapes=scratch,
            compiler_params=pltpu.CompilerParams(
                collective_id=0, has_side_effects=True, vmem_limit_bytes=67043328),
        )(cache_len, hidden, k_cache.transpose(0, 2, 1), v_cache.transpose(0, 2, 1),
          g_attn[None, :], g_final[None, :], w_query, w_key.T, w_value.T, w_gate, w_up, w_out, w_down,
          embedding, freq)
        step = min(320, window)
        steps = -(-window // step)

        def fixed(shape):
            return pl.BlockSpec(shape, lambda i: (0, 0))
        log_probs, key_new, value_new, norm = pl.pallas_call(
            functools.partial(finish_kernel, shift),
            name="finish",
            grid=(steps,),
            out_shape=(
                jax.ShapeDtypeStruct((vocab, batch), F32),
                jax.ShapeDtypeStruct((own, head_dim), BF16),
                jax.ShapeDtypeStruct((own, head_dim), BF16),
                jax.ShapeDtypeStruct((1, batch), F32)),
            in_specs=[
                pl.BlockSpec((step, batch), lambda i: (i, 0)),
                pl.BlockSpec((8, batch), lambda i: (jnp.minimum((i + 1) * (step // 8), window // 8 - 1), 0)),
                fixed((1, batch)), fixed((own, head_dim)), fixed((own, head_dim))],
            out_specs=(
                pl.BlockSpec((step, batch), lambda i: (i, 0)),
                fixed((own, head_dim)), fixed((own, head_dim)), fixed((1, batch))),
        )(logits, logits, norm, key_new, value_new)
        return key_new, value_new, log_probs.T, norm[0]

    in_specs = (P("dp", "xax"), P("dp"), row_spec, row_spec, P("xax"), P("xax", "yax"),
                P("xax", None), P("xax", None), P("xax", "yax"), P("xax", "yax"),
                P("yax", "xax"), P("yax", "xax"), P("xax"), P("yax", "xax"))
    out_specs = (row_spec, row_spec, P("dp", ("yax", "xax")), P("dp"))
    return jax.shard_map(local_step, mesh=mesh, in_specs=in_specs, out_specs=out_specs, check_vma=False)
```

```python
import functools

import jax
import jax.numpy as jnp
import numpy as np
from jax import lax
from jax.experimental import pallas as pl
from jax.experimental.pallas import tpu as pltpu
from jax.sharding import PartitionSpec as P

EPS = 1e-6
ROPE_BASE = 10000.0
F32 = jnp.float32
BF16 = jnp.bfloat16
NT = (((1,), (1,)), ((), ()))
EMBED_CHUNKS = 16


def layer_norm(values_in, gain):
    mean = jnp.mean(values_in, axis=-1, keepdims=True)
    centred = values_in - mean
    var = jnp.mean(centred * centred, axis=-1, keepdims=True)
    return centred * lax.rsqrt(var + EPS) * gain


def row_chunks(total, count):
    cuts = [16 * (total // 16 * i // count) for i in range(count)] + [total]
    return [(cuts[i], cuts[i + 1] - cuts[i]) for i in range(count)]


class Marker:
    def __init__(self):
        self.scope = None

    def __call__(self, name):
        if self.scope is not None:
            self.scope.__exit__(None, None, None)
        self.scope = None
        if name:
            self.scope = jax.named_scope(name)
            self.scope.__enter__()


def kernel(cfg, lens, hidden, k_hbm, v_hbm, g_attn, g_final, w_query, w_key, w_value, w_gate, w_up,
           w_out, w_down, embed, freq,
           k_out, v_out, logits_out, norm_out,
           k_buf, v_buf, h_buf, ga_buf, gf_buf, wqt, wq_buf, gu_buf, down_buf, out_buf, kv_buf,
           n_all, q_scr, qx_buf, q2d, snew, krep, vrep, s_scr, od_scr, o_scr, ox_buf, act_scr, act, part_scr,
           pre_buf, rs_scr, rs_buf, f_buf, e_buf, z_scr, st_scr, k_scr, v_scr, norm_scr, sx_buf, sy_scr, sy_buf,
           kv_sem, e_own_sem, z_sem, x_send, x_recv, g_send, g_recv, g_last, y_send, y_recv, e_send, e_recv,
           n_recv, n_last, n_send, pre_sem, rs_sem, fx_recv, fy_recv, f_sem, s_sem):
    ys, xs, own, vocab, shift = cfg
    mark = Marker()
    y = lax.axis_index("yax")
    x = lax.axis_index("xax")
    core = lax.rem(x, 2)
    partner = x + 1 - 2 * core
    blk = hidden.shape[1]
    quarter = xs * own
    head_dim = k_hbm.shape[1]
    half = head_dim // 2
    seqs = k_hbm.shape[0]
    slots = k_hbm.shape[2]
    heads = w_query.shape[1] * ys // head_dim
    groups = k_buf.shape[0]
    per = seqs // groups
    window = e_buf.shape[0]

    def lanes(i):
        return pl.ds(pl.multiple_of(i * blk, 128), blk)

    def rows(i, n):
        return pl.ds(pl.multiple_of(i * n, n), n)

    def cache_copy(g, src, dst, s):
        return pltpu.make_async_copy(src.at[pl.ds(g * per, per)], dst.at[g], kv_sem.at[s, g])

    def start_cache(g, carry):
        cache_copy(g, k_hbm, k_buf, 0).start()
        return carry
    lax.fori_loop(0, groups, start_cache, 0)

    wqt[...] = w_query[...].astype(F32).T.astype(BF16)

    mark("a0barrier")
    barrier = pltpu.get_barrier_semaphore()

    def signal_row(d, carry):
        pl.semaphore_signal(barrier, inc=1, device_id={"xax": lax.rem(x + d, xs)},
                            device_id_type=pl.DeviceIdType.MESH)
        return carry
    lax.fori_loop(1, xs, signal_row, 0)

    def signal_column(d, carry):
        pl.semaphore_signal(barrier, inc=1, device_id={"yax": lax.rem(y + d, ys)},
                            device_id_type=pl.DeviceIdType.MESH)
        return carry
    lax.fori_loop(1, ys, signal_column, 0)
    pl.semaphore_wait(barrier, xs + ys - 2)

    def arrived(ref, sem):
        pltpu.make_async_copy(ref, ref, sem).wait()

    cols = wqt.shape[0] // xs
    ff = w_gate.shape[1] // xs
    most = pl.ds(0, (xs - 1) * blk)
    x_kinds = {
        "wq": (lambda p: wqt.at[rows(p, cols), :], lambda s: wq_buf.at[y, :, lanes(s)],
               wq_buf.at[y], wq_buf.at[y, :, most]),
        "wo": (lambda p: w_out.at[rows(p, cols), :], lambda s: out_buf.at[y, :, lanes(s)],
               out_buf.at[y], out_buf.at[y, :, most]),
        "down": (lambda p: w_down.at[rows(p, ff), :], lambda s: down_buf.at[y, :, lanes(s)],
                 down_buf.at[y], down_buf.at[y, :, most]),
        "gate": (lambda p: w_gate.at[:, lanes(p)], lambda s: gu_buf.at[rows(s, blk), pl.ds(0, ff)],
                 gu_buf.at[:, pl.ds(0, ff)], gu_buf.at[most, pl.ds(0, ff)]),
        "up": (lambda p: w_up.at[:, lanes(p)], lambda s: gu_buf.at[rows(s, blk), pl.ds(ff, ff)],
               gu_buf.at[:, pl.ds(ff, ff)], gu_buf.at[most, pl.ds(ff, ff)]),
        "q": (lambda p: q_scr.at[rows(p, own), :], lambda s: qx_buf.at[s],
              qx_buf, qx_buf.at[pl.ds(0, xs - 1)]),
        "o": (lambda p: o_scr.at[p], lambda s: ox_buf.at[rows(s, own), :],
              ox_buf, ox_buf.at[pl.ds(0, (xs - 1) * own), :]),
    }
    x_index = {name: i for i, name in enumerate(x_kinds)}

    def x_start(name):
        src, dst = x_kinds[name][:2]
        k = x_index[name]

        def body(d, carry):
            p = lax.rem(x + d, xs)
            pltpu.make_async_remote_copy(
                src_ref=src(p), dst_ref=dst(x), send_sem=x_send.at[k], recv_sem=x_recv.at[k],
                device_id={"xax": p}, device_id_type=pl.DeviceIdType.MESH).start()
            return carry
        lax.fori_loop(1, xs, body, 0)
        pltpu.make_async_copy(src(x), dst(x), x_recv.at[k]).start()

    def x_wait(name):
        arrived(x_kinds[name][2], x_recv.at[x_index[name]])

    def x_drain(name):
        arrived(x_kinds[name][3], x_send.at[x_index[name]])

    chips = xs // 2
    g_kinds = {
        "hidden": (hidden.at[rows(y, quarter), :], lambda s: h_buf.at[:, lanes(s)], h_buf),
        "ga": (g_attn, lambda s: ga_buf.at[:, lanes(s)], ga_buf),
        "gf": (g_final, lambda s: gf_buf.at[:, lanes(s)], gf_buf),
        "wk": (w_key, lambda s: kv_buf.at[pl.ds(0, head_dim), lanes(s)], kv_buf.at[pl.ds(0, head_dim), :]),
        "wv": (w_value, lambda s: kv_buf.at[pl.ds(head_dim, head_dim), lanes(s)],
               kv_buf.at[pl.ds(head_dim, head_dim), :]),
    }
    g_index = {name: i for i, name in enumerate(g_kinds)}

    def g_copy(name, i, sender):
        src, dst, _ = g_kinds[name]
        k = g_index[name]
        return pltpu.make_async_remote_copy(
            src_ref=src, dst_ref=dst(sender), send_sem=g_send.at[k], recv_sem=g_recv.at[k, i],
            device_id={"xax": lax.rem(x + 2 * i, xs)}, device_id_type=pl.DeviceIdType.MESH)

    def g_pass(name, sender, source):
        k = g_index[name]
        return pltpu.make_async_remote_copy(
            src_ref=source, dst_ref=g_kinds[name][1](sender), send_sem=g_send.at[k], recv_sem=g_last.at[k],
            device_id={"xax": partner}, device_id_type=pl.DeviceIdType.MESH)

    def g_start(name):
        def body(i, carry):
            g_copy(name, i, x).start()
            return carry
        lax.fori_loop(1, chips, body, 0)
        src, dst, _ = g_kinds[name]
        g_pass(name, x, src).start()
        pltpu.make_async_copy(src, dst(x), g_last.at[g_index[name]]).start()

    def g_forward(name):
        def body(i, carry):
            sender = lax.rem(x + xs - 2 * i, xs)
            g_copy(name, i, sender).wait_recv()
            g_pass(name, sender, g_kinds[name][1](sender)).start()
            return carry
        lax.fori_loop(1, chips, body, 0)

    def g_wait(name):
        whole = g_kinds[name][2]
        arrived(whole.at[:, pl.ds(0, (chips + 1) * blk)], g_last.at[g_index[name]])

    def g_drain(name):
        arrived(g_kinds[name][2].at[:, most], g_send.at[g_index[name]])

    y_kinds = {"wq": wq_buf, "wo": out_buf, "down": down_buf}
    y_index = {name: i for i, name in enumerate(y_kinds)}
    others = pl.ds(0, ys - 1)

    def y_start(name):
        buf = y_kinds[name]
        k = y_index[name]

        def body(d, carry):
            pltpu.make_async_remote_copy(
                src_ref=buf.at[y], dst_ref=buf.at[y], send_sem=y_send.at[k], recv_sem=y_recv.at[k],
                device_id={"yax": lax.rem(y + d, ys)}, device_id_type=pl.DeviceIdType.MESH).start()
            return carry
        lax.fori_loop(1, ys, body, 0)

    def y_wait(name):
        arrived(y_kinds[name].at[others], y_recv.at[y_index[name]])

    def y_drain(name):
        arrived(y_kinds[name].at[others], y_send.at[y_index[name]])

    e_parts = row_chunks(window, EMBED_CHUNKS)

    def e_first(p):
        return p * vocab - lax.rem(p, 2) * shift

    def e_own():
        return pltpu.make_async_copy(
            embed.at[pl.ds(pl.multiple_of(e_first(x), 8), window), :], e_buf.at[:, lanes(x)], e_own_sem)

    def e_start(c):
        r0, n = e_parts[c]

        def body(d, carry):
            p = lax.rem(x + d, xs)
            pltpu.make_async_remote_copy(
                src_ref=embed.at[pl.ds(pl.multiple_of(e_first(p) + r0, 8), n), :],
                dst_ref=e_buf.at[pl.ds(r0, n), lanes(x)], send_sem=e_send, recv_sem=e_recv,
                device_id={"xax": p}, device_id_type=pl.DeviceIdType.MESH).start()
            return carry
        lax.fori_loop(1, xs, body, 0)

    mark("a1send")
    x_start("wq")
    for name in ("hidden", "ga"):
        g_start(name)
    for name in ("wo", "down"):
        x_start(name)
    for name in ("wk", "wv", "gf"):
        g_start(name)
    e_start(0)
    e_own().start()

    def start_cache_v(g, carry):
        cache_copy(g, v_hbm, v_buf, 1).start()
        return carry
    lax.fori_loop(0, groups, start_cache_v, 0)

    mark("a2wqx")
    x_wait("wq")
    y_start("wq")
    mark("a3hfwd")
    for name in ("hidden", "ga"):
        g_forward(name)
    mark("a4hwait")
    for name in ("hidden", "ga"):
        g_wait(name)
    mark("a5ln")
    my_rows = rows(y, quarter)
    n_all[my_rows, :] = layer_norm(h_buf[...].astype(F32), ga_buf[...]).astype(BF16)

    part = quarter // 2

    def n_rows(j, c):
        return pl.ds(pl.multiple_of(j * quarter + c * part, part), part)

    def n_copy(d, sender):
        r = n_rows(sender, core)
        return pltpu.make_async_remote_copy(
            src_ref=n_all.at[r, :], dst_ref=n_all.at[r, :], send_sem=n_send.at[0],
            recv_sem=n_recv.at[d], device_id={"yax": lax.rem(y + d, ys)},
            device_id_type=pl.DeviceIdType.MESH)

    def n_pass(d, c):
        r = n_rows(lax.rem(y + ys - d, ys), c)
        return pltpu.make_async_remote_copy(
            src_ref=n_all.at[r, :], dst_ref=n_all.at[r, :], send_sem=n_send.at[1],
            recv_sem=n_last.at[d], device_id={"xax": partner},
            device_id_type=pl.DeviceIdType.MESH)

    mark("a6wqy")
    y_wait("wq")
    mark("a7q")
    wq_all = wq_buf[...].reshape(ys * cols, xs * blk)
    q_scr[...] = lax.dot_general(n_all[my_rows, :], wq_all, NT, preferred_element_type=F32).astype(BF16)
    mark("a8send")
    x_start("q")
    x_start("gate")
    x_start("up")

    def n_start(d, carry):
        n_copy(d, y).start()
        return carry
    lax.fori_loop(1, ys, n_start, 0)
    mark("a9wo")
    x_wait("wo")
    y_start("wo")
    mark("b0down")
    x_wait("down")
    y_start("down")
    for c in range(1, 7):
        e_start(c)

    mark("b1kv")
    row_id = lax.broadcasted_iota(jnp.int32, (own, 4 * half), 0)
    first_row = (y * xs + x) * own
    position = jnp.zeros((own, 4 * half), jnp.int32)
    for b in range(own):
        position = jnp.where(row_id == b, lens[first_row + b], position)
    angle = position.astype(F32) * freq[...]
    cos_a = jnp.cos(angle)
    sin_a = jnp.sin(angle)
    for name in ("wk", "wv", "gf"):
        g_forward(name)
    for name in ("wk", "wv", "gf"):
        g_wait(name)
    mine = y * xs + x
    n_own = n_all[rows(mine, own), :]
    kv = lax.dot_general(n_own, kv_buf[...], NT, preferred_element_type=F32).astype(BF16).astype(F32)
    k1 = kv[:, :half]
    k2 = kv[:, half:head_dim]
    c1 = cos_a[:, :half]
    s1 = sin_a[:, :half]
    key = jnp.concatenate([k1 * c1 - k2 * s1, k2 * c1 + k1 * s1], axis=1).astype(BF16)
    value = kv[:, head_dim:].astype(BF16)
    k_scr[...] = key
    v_scr[...] = value
    small_outs = [pltpu.make_async_copy(k_scr, k_out, z_sem.at[0]),
                  pltpu.make_async_copy(v_scr, v_out, z_sem.at[1])]
    for copy in small_outs:
        copy.start()
    for h in range(heads):
        krep[pl.ds(h, own, stride=heads), :] = key.astype(F32)
        vrep[pl.ds(h, own, stride=heads), :] = value.astype(F32)

    mark("b2q")
    x_wait("q")
    mark("b3rot")
    for xc in range(xs // 2):
        qa = qx_buf[2 * xc].astype(F32)
        qb = qx_buf[2 * xc + 1].astype(F32)
        ra = (qa * cos_a - qb * sin_a).astype(BF16).astype(F32)
        rb = (qb * cos_a + qa * sin_a).astype(BF16).astype(F32)
        for yc in range(ys):
            pair = jnp.concatenate([ra[:, yc * half:(yc + 1) * half], rb[:, yc * half:(yc + 1) * half]], axis=1)
            q2d[pl.ds(xc * ys + yc, own, stride=heads), :] = pair
    scale = head_dim ** -0.5
    snew[...] = jnp.sum(q2d[...] * krep[...], axis=1, keepdims=True) * scale

    mark("b4attn")
    gr = per * heads
    seg_r = lax.broadcasted_iota(jnp.int32, (gr, per * head_dim), 0) // heads
    seg_c = lax.broadcasted_iota(jnp.int32, (gr, per * head_dim), 1) // head_dim
    diag = (seg_r == seg_c).astype(F32)
    tile = min(512, slots)
    row_g = lax.broadcasted_iota(jnp.int32, (gr, 1), 0) // heads
    lane_g = lax.broadcasted_iota(jnp.int32, (gr, tile), 1)

    def attend(g, carry):
        cache_copy(g, k_hbm, k_buf, 0).wait()
        qg = q2d[rows(g, gr), :]
        qbd = (jnp.concatenate([qg] * per, axis=1) * diag).astype(BF16)
        len_g = jnp.zeros((gr, 1), jnp.int32)
        for s in range(per):
            len_g = jnp.where(row_g == s, lens[first_row + g * per + s], len_g)
        new = snew[rows(g, gr), :]
        top = jnp.full((gr, tile), -jnp.inf, F32)
        kg = k_buf.at[g]
        vg = v_buf.at[g]
        for c in range(slots // tile):
            kc = kg[:, :, pl.ds(c * tile, tile)].reshape(per * head_dim, tile)
            sc = jnp.dot(qbd, kc, preferred_element_type=F32) * scale
            sc = jnp.where(lane_g < len_g - c * tile, sc, -jnp.inf)
            s_scr[:, pl.ds(c * tile, tile)] = sc
            top = jnp.maximum(top, sc)
        row_max = jnp.maximum(jnp.max(top, axis=1, keepdims=True), new)
        total = jnp.zeros((gr, tile), F32)
        for c in range(slots // tile):
            ex = jnp.exp(s_scr[:, pl.ds(c * tile, tile)] - row_max)
            s_scr[:, pl.ds(c * tile, tile)] = ex
            total = total + ex
        w_new = jnp.exp(new - row_max)
        den = jnp.sum(total, axis=1, keepdims=True) + w_new
        inv = 1.0 / den
        cache_copy(g, v_hbm, v_buf, 1).wait()
        mixed = jnp.zeros((gr, per * head_dim), F32)
        for c in range(slots // tile):
            pr = (s_scr[:, pl.ds(c * tile, tile)] * inv).astype(BF16)
            vc = vg[:, :, pl.ds(c * tile, tile)].reshape(per * head_dim, tile)
            mixed = mixed + lax.dot_general(pr, vc, NT, preferred_element_type=F32)
        add = (w_new * inv).astype(BF16).astype(F32) * vrep[rows(g, gr), :]
        for s in range(per):
            od_scr[pl.ds(pl.multiple_of(g * gr + s * heads, heads), heads), :] = (
                mixed[s * heads:(s + 1) * heads, s * head_dim:(s + 1) * head_dim]
                + add[s * heads:(s + 1) * heads, :])
        return carry

    lax.fori_loop(0, groups, attend, 0)
    mark("b5o")
    for xc in range(xs // 2):
        parts = [od_scr[pl.ds(xc * ys + yc, own, stride=heads), :] for yc in range(ys)]
        o_scr[2 * xc] = jnp.concatenate([p[:, :half] for p in parts], axis=1).astype(BF16)
        o_scr[2 * xc + 1] = jnp.concatenate([p[:, half:] for p in parts], axis=1).astype(BF16)
    x_start("o")
    for c in range(7, 11):
        e_start(c)

    def act_copy(dest):
        return pltpu.make_async_remote_copy(
            src_ref=act_scr.at[dest], dst_ref=act.at[:, pl.ds(pl.multiple_of(y * ff, ff), ff)],
            send_sem=y_send.at[len(y_kinds)], recv_sem=y_recv.at[len(y_kinds)],
            device_id={"yax": dest}, device_id_type=pl.DeviceIdType.MESH)

    mark("b6gu")
    x_wait("gate")
    x_wait("up")

    mark("b7feed")
    def feed(d, carry):
        @pl.when(d < ys - 1)
        def _():
            n_copy(d + 1, lax.rem(y + ys - d - 1, ys)).wait_recv()
            n_pass(d + 1, core).start()
        j = lax.rem(y + ys - d, ys)

        @pl.when(d > 0)
        def _():
            n_pass(d, 1 - core).wait_recv()
        gu = jnp.dot(n_all[rows(j, quarter), :], gu_buf[...], preferred_element_type=F32)
        gu = gu.astype(BF16).astype(F32)
        gate = gu[:, :ff]
        act_scr[j] = (gate * jax.nn.sigmoid(gate) * gu[:, ff:]).astype(BF16)

        @pl.when(d > 0)
        def _():
            act_copy(j).start()
        return carry
    lax.fori_loop(0, ys, feed, 0)
    act[:, pl.ds(pl.multiple_of(y * ff, ff), ff)] = act_scr[y]
    mark("b8wo")
    y_wait("wo")
    mark("b9o")
    x_wait("o")
    mark("c0op")
    part_scr[...] = jnp.dot(
        ox_buf[...], out_buf[...].reshape(ys * cols, xs * blk), preferred_element_type=F32)
    mark("c1down")
    y_wait("down")

    mark("c2act")
    arrived(act_scr.at[others], y_recv.at[len(y_kinds)])

    mark("c3branch")
    down_all = down_buf[...].reshape(ys * ff, xs * blk)
    part_scr[...] = part_scr[...] + jnp.dot(act[...], down_all, preferred_element_type=F32)

    def branch(c):
        for i in range(chips):
            rs_scr[c, i] = part_scr[pl.ds(pl.multiple_of((2 * i + c) * own, own), own), :]

    def pre_copy():
        return pltpu.make_async_remote_copy(
            src_ref=rs_scr.at[1 - core], dst_ref=pre_buf, send_sem=pre_sem.at[0], recv_sem=pre_sem.at[1],
            device_id={"xax": partner}, device_id_type=pl.DeviceIdType.MESH)

    def rs_copy(dest):
        return pltpu.make_async_remote_copy(
            src_ref=rs_scr.at[core, dest], dst_ref=rs_buf.at[chip], send_sem=rs_sem.at[0],
            recv_sem=rs_sem.at[1], device_id={"xax": 2 * dest + core},
            device_id_type=pl.DeviceIdType.MESH)

    chip = x // 2
    branch(1 - core)
    pre_copy().start()
    branch(core)
    mark("c4pre")
    pre_copy().wait_recv()
    rs_scr[core] = rs_scr[core] + pre_buf[...]

    mark("c5rs")
    def rs_start(i, carry):
        rs_copy(lax.rem(chip + i, chips)).start()
        return carry
    lax.fori_loop(1, chips, rs_start, 0)
    mark("c6rsw")
    arrived(rs_buf.at[pl.ds(0, chips - 1)], rs_sem.at[1])
    mark("c7ln")
    rs_buf[chip] = rs_scr[core, chip]
    res = h_buf[rows(x, own), :].astype(F32) + jnp.sum(rs_buf[...], axis=0)
    f_buf[rows(mine, own), :] = layer_norm(res, gf_buf[...]).astype(BF16)

    def f_rows(sy, sx):
        return f_buf.at[rows(sy * xs + sx, own), :]

    def fx_copy(i, sx):
        return pltpu.make_async_remote_copy(
            src_ref=f_rows(y, sx), dst_ref=f_rows(y, sx), send_sem=f_sem.at[0],
            recv_sem=fx_recv.at[i], device_id={"xax": lax.rem(x + 2 * i, xs)},
            device_id_type=pl.DeviceIdType.MESH)

    def fy_copy(d, i, sy, sx):
        return pltpu.make_async_remote_copy(
            src_ref=f_rows(sy, sx), dst_ref=f_rows(sy, sx), send_sem=f_sem.at[1],
            recv_sem=fy_recv.at[d, i], device_id={"yax": lax.rem(y + d, ys)},
            device_id_type=pl.DeviceIdType.MESH)

    def fp_copy(d, sy, sx):
        return pltpu.make_async_remote_copy(
            src_ref=f_rows(sy, sx), dst_ref=f_rows(sy, sx), send_sem=f_sem.at[2],
            recv_sem=f_sem.at[3 + d], device_id={"xax": partner}, device_id_type=pl.DeviceIdType.MESH)

    mark("c8fx")
    def fx_start(i, carry):
        fx_copy(i, x).start()
        return carry
    lax.fori_loop(1, chips, fx_start, 0)

    def f_spread(i, carry):
        sx = lax.rem(x + xs - 2 * i, xs)

        @pl.when(i > 0)
        def _():
            fx_copy(i, sx).wait_recv()

        def over_y(d, c2):
            fy_copy(d, i, y, sx).start()
            return c2
        lax.fori_loop(1, ys, over_y, 0)
        fp_copy(0, y, sx).start()
        return carry
    lax.fori_loop(0, 1, f_spread, 0)
    for c in range(11, EMBED_CHUNKS):
        e_start(c)
    mark("c9sp")
    lax.fori_loop(1, chips, f_spread, 0)

    mark("d0drain")
    for name in x_kinds:
        x_drain(name)
    for name in g_kinds:
        g_drain(name)
    for name in y_kinds:
        y_drain(name)
    arrived(act_scr.at[others], y_send.at[len(y_kinds)])
    for i in range(2):
        arrived(n_all.at[pl.ds(0, (ys - 1) * part), :], n_send.at[i])
    pre_copy().wait_send()
    arrived(rs_buf.at[pl.ds(0, chips - 1)], rs_sem.at[0])
    for copy in small_outs:
        copy.wait()

    mark("d1e")
    e_own().wait()
    arrived(e_buf.at[:, most], e_recv)

    mark("d3head")
    def z_copy(j):
        return pltpu.make_async_copy(z_scr.at[j], logits_out.at[:, rows(j, quarter)], z_sem.at[2])

    skip = core * shift
    index = lax.broadcasted_iota(jnp.int32, (window, 1), 0)
    inside = jnp.logical_and(index >= skip, index < skip + vocab)
    half_block = pl.ds(0, chips * own)

    def head(d, carry):
        j = lax.rem(y + ys - d, ys)

        def forward(i, c2):
            sx = lax.rem(x + xs - 2 * i, xs)
            fy_copy(d, i, j, sx).wait_recv()
            fp_copy(d, j, sx).start()
            return c2

        with jax.named_scope("hfwd"):
            @pl.when(d > 0)
            def _():
                lax.fori_loop(0, chips, forward, 0)
        with jax.named_scope("hpart"):
            arrived(f_buf.at[half_block, :], f_sem.at[3 + d])
        z = lax.dot_general(e_buf[...], f_buf[rows(j, quarter), :], NT, preferred_element_type=F32)
        z_scr[j] = z
        z_copy(j).start()
        if shift:
            z = jnp.where(inside, z, -jnp.inf)
        top = jnp.max(z, axis=0, keepdims=True)
        st_scr[0:1, rows(j, quarter)] = top
        st_scr[1:2, rows(j, quarter)] = jnp.sum(jnp.exp(z - top), axis=0, keepdims=True)
        return carry
    lax.fori_loop(0, ys, head, 0)

    mark("d4stat")
    def combine(buf):
        tops = buf[:, 0, :]
        best = jnp.max(tops, axis=0, keepdims=True)
        return best, jnp.sum(buf[:, 1, :] * jnp.exp(tops - best), axis=0, keepdims=True)

    def sx_start(d, carry):
        pltpu.make_async_remote_copy(
            src_ref=st_scr, dst_ref=sx_buf.at[x], send_sem=s_sem.at[0], recv_sem=s_sem.at[1],
            device_id={"xax": lax.rem(x + d, xs)}, device_id_type=pl.DeviceIdType.MESH).start()
        return carry
    lax.fori_loop(1, xs, sx_start, 0)
    sx_buf[x] = st_scr[...]

    mark("d5sx")
    arrived(e_buf.at[:, most], e_send)
    arrived(f_buf.at[pl.ds(0, (chips - 1) * own), :], f_sem.at[0])
    arrived(f_buf.at[pl.ds(0, (ys - 1) * chips * own), :], f_sem.at[1])
    arrived(f_buf.at[pl.ds(0, ys * chips * own), :], f_sem.at[2])
    arrived(z_scr, z_sem.at[2])

    mark("d6sxw")
    arrived(sx_buf.at[pl.ds(0, xs - 1)], s_sem.at[1])
    best, whole = combine(sx_buf)
    sy_scr[0:1, :] = best
    sy_scr[1:2, :] = whole

    mark("d7sy")
    def sy_start(d, carry):
        pltpu.make_async_remote_copy(
            src_ref=sy_scr, dst_ref=sy_buf.at[y], send_sem=s_sem.at[2], recv_sem=s_sem.at[3],
            device_id={"yax": lax.rem(y + d, ys)}, device_id_type=pl.DeviceIdType.MESH).start()
        return carry
    lax.fori_loop(1, ys, sy_start, 0)
    sy_buf[y] = sy_scr[...]
    arrived(sx_buf.at[pl.ds(0, xs - 1)], s_sem.at[0])
    mark("d8syw")
    arrived(sy_buf.at[others], s_sem.at[3])
    best, whole = combine(sy_buf)
    mark("d9n")
    norm_scr[...] = best + jnp.log(whole)
    norm_copy = pltpu.make_async_copy(norm_scr, norm_out, z_sem.at[0])
    norm_copy.start()
    arrived(sy_buf.at[others], s_sem.at[2])
    norm_copy.wait()
    mark(None)


def finish_kernel(shift, z_ref, next_ref, norm, key, value, out_ref, k_out, v_out, norm_out):
    n = z_ref.shape[0]
    if shift:
        odd = lax.rem(lax.axis_index("xax"), 2) == 1

        @pl.when(odd)
        def _():
            out_ref[pl.ds(0, n - shift), :] = z_ref[pl.ds(shift, n - shift), :] - norm[...]
            out_ref[pl.ds(n - shift, shift), :] = next_ref[pl.ds(0, shift), :] - norm[...]

        @pl.when(jnp.logical_not(odd))
        def _():
            out_ref[...] = z_ref[...] - norm[...]
    else:
        out_ref[...] = z_ref[...] - norm[...]
    k_out[...] = key[...]
    v_out[...] = value[...]
    norm_out[...] = norm[...]


def solution(mesh):
    ys = mesh.shape["yax"]
    xs = mesh.shape["xax"]
    row_spec = P(("dp", "yax", "xax"))

    def local_step(hidden, cache_len, k_cache, v_cache, g_attn, w_query, w_key, w_value,
                   w_gate, w_up, w_out, w_down, g_final, embedding):
        batch, blk = hidden.shape
        own, slots, head_dim = k_cache.shape
        width = blk * xs
        vocab = embedding.shape[0] // xs
        shift = vocab % 8
        window = -(-vocab // 8) * 8
        half = head_dim // 2
        quarter = xs * own
        cols = w_query.shape[1] // xs
        ff = w_gate.shape[1] // xs
        heads = w_query.shape[1] * ys // head_dim
        per = 4
        groups = own // per
        freq_row = (ROPE_BASE ** (-(np.arange(half, dtype=np.float32) * 2.0) / head_dim)).astype(np.float32)
        freq = jnp.asarray(np.tile(freq_row, 4)[None, :])
        any_spec = pl.BlockSpec(memory_space=pl.ANY)
        vmem = pl.BlockSpec(memory_space=pltpu.VMEM)
        smem = pl.BlockSpec(memory_space=pltpu.SMEM)
        dma = pltpu.SemaphoreType.DMA
        chips = xs // 2
        scratch = [
            pltpu.VMEM((groups, per, head_dim, slots), BF16),
            pltpu.VMEM((groups, per, head_dim, slots), BF16),
            pltpu.VMEM((quarter, width), BF16),
            pltpu.VMEM((1, width), F32),
            pltpu.VMEM((1, width), F32),
            pltpu.VMEM((w_query.shape[1], blk), BF16),
            pltpu.VMEM((ys, cols, width), BF16),
            pltpu.VMEM((width, 2 * ff), BF16),
            pltpu.VMEM((ys, ff, width), BF16),
            pltpu.VMEM((ys, cols, width), BF16),
            pltpu.VMEM((2 * head_dim, width), BF16),
            pltpu.VMEM((batch, width), BF16),
            pltpu.VMEM((quarter, ys * cols), BF16),
            pltpu.VMEM((xs, own, ys * cols), BF16),
            pltpu.VMEM((own * heads, head_dim), F32),
            pltpu.VMEM((own * heads, 1), F32),
            pltpu.VMEM((own * heads, head_dim), F32),
            pltpu.VMEM((own * heads, head_dim), F32),
            pltpu.VMEM((per * heads, slots), F32),
            pltpu.VMEM((own * heads, head_dim), F32),
            pltpu.VMEM((xs, own, ys * cols), BF16),
            pltpu.VMEM((quarter, ys * cols), BF16),
            pltpu.VMEM((ys, quarter, ff), BF16),
            pltpu.VMEM((quarter, ys * ff), BF16),
            pltpu.VMEM((quarter, width), F32),
            pltpu.VMEM((chips, own, width), F32),
            pltpu.VMEM((2, chips, own, width), F32),
            pltpu.VMEM((chips, own, width), F32),
            pltpu.VMEM((batch, width), BF16),
            pltpu.VMEM((window, width), BF16),
            pltpu.VMEM((ys, window, quarter), F32),
            pltpu.VMEM((2, batch), F32),
            pltpu.VMEM((own, head_dim), BF16),
            pltpu.VMEM((own, head_dim), BF16),
            pltpu.VMEM((1, batch), F32),
            pltpu.VMEM((xs, 2, batch), F32),
            pltpu.VMEM((2, batch), F32),
            pltpu.VMEM((ys, 2, batch), F32),
            dma((2, groups)), dma, dma((3,)), dma((7,)), dma((7,)),
            dma((5,)), dma((5, chips)), dma((5,)), dma((4,)), dma((4,)), dma, dma,
            dma((ys,)), dma((ys,)), dma((2,)), dma((2,)), dma((2,)),
            dma((chips,)), dma((ys, chips)), dma((3 + ys,)), dma((4,)),
        ]
        cfg = (ys, xs, own, vocab, shift)
        key_new, value_new, logits, norm = pl.pallas_call(
            functools.partial(kernel, cfg),
            name="decode_layer",
            out_shape=(
                jax.ShapeDtypeStruct((own, head_dim), BF16),
                jax.ShapeDtypeStruct((own, head_dim), BF16),
                jax.ShapeDtypeStruct((window, batch), F32),
                jax.ShapeDtypeStruct((1, batch), F32)),
            in_specs=[smem, any_spec, any_spec, any_spec, any_spec, any_spec, vmem] + [any_spec] * 7 + [vmem],
            out_specs=(any_spec, any_spec, any_spec, any_spec),
            scratch_shapes=scratch,
            compiler_params=pltpu.CompilerParams(
                collective_id=0, has_side_effects=True, vmem_limit_bytes=67043328),
        )(cache_len, hidden, k_cache.transpose(0, 2, 1), v_cache.transpose(0, 2, 1),
          g_attn[None, :], g_final[None, :], w_query, w_key.T, w_value.T, w_gate, w_up, w_out, w_down,
          embedding, freq)
        step = min(320, window)
        steps = -(-window // step)

        def fixed(shape):
            return pl.BlockSpec(shape, lambda i: (0, 0))
        log_probs, key_new, value_new, norm = pl.pallas_call(
            functools.partial(finish_kernel, shift),
            name="finish",
            grid=(steps,),
            out_shape=(
                jax.ShapeDtypeStruct((vocab, batch), F32),
                jax.ShapeDtypeStruct((own, head_dim), BF16),
                jax.ShapeDtypeStruct((own, head_dim), BF16),
                jax.ShapeDtypeStruct((1, batch), F32)),
            in_specs=[
                pl.BlockSpec((step, batch), lambda i: (i, 0)),
                pl.BlockSpec((8, batch), lambda i: (jnp.minimum((i + 1) * (step // 8), window // 8 - 1), 0)),
                fixed((1, batch)), fixed((own, head_dim)), fixed((own, head_dim))],
            out_specs=(
                pl.BlockSpec((step, batch), lambda i: (i, 0)),
                fixed((own, head_dim)), fixed((own, head_dim)), fixed((1, batch))),
        )(logits, logits, norm, key_new, value_new)
        return key_new, value_new, log_probs.T, norm[0]

    in_specs = (P("dp", "xax"), P("dp"), row_spec, row_spec, P("xax"), P("xax", "yax"),
                P("xax", None), P("xax", None), P("xax", "yax"), P("xax", "yax"),
                P("yax", "xax"), P("yax", "xax"), P("xax"), P("yax", "xax"))
    out_specs = (row_spec, row_spec, P("dp", ("yax", "xax")), P("dp"))
    return jax.shard_map(local_step, mesh=mesh, in_specs=in_specs, out_specs=out_specs, check_vma=False)
```

```python
import functools

import jax
import jax.numpy as jnp
import numpy as np
from jax import lax
from jax.experimental import pallas as pl
from jax.experimental.pallas import tpu as pltpu
from jax.sharding import PartitionSpec as P

EPS = 1e-6
ROPE_BASE = 10000.0
F32 = jnp.float32
BF16 = jnp.bfloat16
NT = (((1,), (1,)), ((), ()))
EMBED_CHUNKS = 16


def layer_norm(values_in, gain):
    mean = jnp.mean(values_in, axis=-1, keepdims=True)
    centred = values_in - mean
    var = jnp.mean(centred * centred, axis=-1, keepdims=True)
    return centred * lax.rsqrt(var + EPS) * gain


def row_chunks(total, count):
    cuts = [16 * (total // 16 * i // count) for i in range(count)] + [total]
    return [(cuts[i], cuts[i + 1] - cuts[i]) for i in range(count)]


class Marker:
    def __init__(self):
        self.scope = None

    def __call__(self, name):
        if self.scope is not None:
            self.scope.__exit__(None, None, None)
        self.scope = None
        if name:
            self.scope = jax.named_scope(name)
            self.scope.__enter__()


def kernel(cfg, lens, hidden, k_hbm, v_hbm, g_attn, g_final, w_query, w_key, w_value, w_gate, w_up,
           w_out, w_down, embed, freq,
           k_out, v_out, logits_out, norm_out,
           k_buf, v_buf, h_buf, ga_buf, gf_buf, wqt, wq_buf, gu_buf, down_buf, out_buf, kv_buf,
           n_all, q_scr, qx_buf, q2d, snew, krep, vrep, s_scr, od_scr, o_scr, ox_buf, act_scr, act, part_scr,
           pre_buf, rs_scr, rs_buf, f_buf, e_buf, z_scr, st_scr, k_scr, v_scr, norm_scr, s_buf,
           kv_sem, e_own_sem, z_sem, x_send, x_recv, g_send, g_recv, g_last, y_send, y_recv, e_send, e_recv,
           n_recv, n_last, n_send, pre_sem, rs_sem, fxa, fyb, fya, fxb, f_sem, s_sem):
    ys, xs, own, vocab, shift = cfg
    mark = Marker()
    y = lax.axis_index("yax")
    x = lax.axis_index("xax")
    core = lax.rem(x, 2)
    partner = x + 1 - 2 * core
    blk = hidden.shape[1]
    quarter = xs * own
    head_dim = k_hbm.shape[1]
    half = head_dim // 2
    seqs = k_hbm.shape[0]
    slots = k_hbm.shape[2]
    heads = w_query.shape[1] * ys // head_dim
    groups = k_buf.shape[0]
    per = seqs // groups
    window = e_buf.shape[0]

    def lanes(i):
        return pl.ds(pl.multiple_of(i * blk, 128), blk)

    def rows(i, n):
        return pl.ds(pl.multiple_of(i * n, n), n)

    def cache_copy(g, src, dst, s):
        return pltpu.make_async_copy(src.at[pl.ds(g * per, per)], dst.at[g], kv_sem.at[s, g])

    def start_cache(g, carry):
        cache_copy(g, k_hbm, k_buf, 0).start()
        return carry
    lax.fori_loop(0, groups, start_cache, 0)

    wqt[...] = w_query[...].astype(F32).T.astype(BF16)

    mark("a0barrier")
    barrier = pltpu.get_barrier_semaphore()

    def signal_row(d, carry):
        pl.semaphore_signal(barrier, inc=1, device_id={"xax": lax.rem(x + d, xs)},
                            device_id_type=pl.DeviceIdType.MESH)
        return carry
    lax.fori_loop(1, xs, signal_row, 0)

    def signal_column(d, carry):
        pl.semaphore_signal(barrier, inc=1, device_id={"yax": lax.rem(y + d, ys)},
                            device_id_type=pl.DeviceIdType.MESH)
        return carry
    lax.fori_loop(1, ys, signal_column, 0)
    pl.semaphore_wait(barrier, xs + ys - 2)

    def arrived(ref, sem):
        pltpu.make_async_copy(ref, ref, sem).wait()

    cols = wqt.shape[0] // xs
    ff = w_gate.shape[1] // xs
    most = pl.ds(0, (xs - 1) * blk)
    x_kinds = {
        "wq": (lambda p: wqt.at[rows(p, cols), :], lambda s: wq_buf.at[y, :, lanes(s)],
               wq_buf.at[y], wq_buf.at[y, :, most]),
        "wo": (lambda p: w_out.at[rows(p, cols), :], lambda s: out_buf.at[y, :, lanes(s)],
               out_buf.at[y], out_buf.at[y, :, most]),
        "down": (lambda p: w_down.at[rows(p, ff), :], lambda s: down_buf.at[y, :, lanes(s)],
                 down_buf.at[y], down_buf.at[y, :, most]),
        "gate": (lambda p: w_gate.at[:, lanes(p)], lambda s: gu_buf.at[rows(s, blk), pl.ds(0, ff)],
                 gu_buf.at[:, pl.ds(0, ff)], gu_buf.at[most, pl.ds(0, ff)]),
        "up": (lambda p: w_up.at[:, lanes(p)], lambda s: gu_buf.at[rows(s, blk), pl.ds(ff, ff)],
               gu_buf.at[:, pl.ds(ff, ff)], gu_buf.at[most, pl.ds(ff, ff)]),
        "q": (lambda p: q_scr.at[rows(p, own), :], lambda s: qx_buf.at[s],
              qx_buf, qx_buf.at[pl.ds(0, xs - 1)]),
        "o": (lambda p: o_scr.at[p], lambda s: ox_buf.at[rows(s, own), :],
              ox_buf, ox_buf.at[pl.ds(0, (xs - 1) * own), :]),
    }
    x_index = {name: i for i, name in enumerate(x_kinds)}

    def x_start(name):
        src, dst = x_kinds[name][:2]
        k = x_index[name]

        def body(d, carry):
            p = lax.rem(x + d, xs)
            pltpu.make_async_remote_copy(
                src_ref=src(p), dst_ref=dst(x), send_sem=x_send.at[k], recv_sem=x_recv.at[k],
                device_id={"xax": p}, device_id_type=pl.DeviceIdType.MESH).start()
            return carry
        lax.fori_loop(1, xs, body, 0)
        pltpu.make_async_copy(src(x), dst(x), x_recv.at[k]).start()

    def x_wait(name):
        arrived(x_kinds[name][2], x_recv.at[x_index[name]])

    def x_drain(name):
        arrived(x_kinds[name][3], x_send.at[x_index[name]])

    chips = xs // 2
    g_kinds = {
        "hidden": (hidden.at[rows(y, quarter), :], lambda s: h_buf.at[:, lanes(s)], h_buf),
        "ga": (g_attn, lambda s: ga_buf.at[:, lanes(s)], ga_buf),
        "gf": (g_final, lambda s: gf_buf.at[:, lanes(s)], gf_buf),
        "wk": (w_key, lambda s: kv_buf.at[pl.ds(0, head_dim), lanes(s)], kv_buf.at[pl.ds(0, head_dim), :]),
        "wv": (w_value, lambda s: kv_buf.at[pl.ds(head_dim, head_dim), lanes(s)],
               kv_buf.at[pl.ds(head_dim, head_dim), :]),
    }
    g_index = {name: i for i, name in enumerate(g_kinds)}

    def g_copy(name, i, sender):
        src, dst, _ = g_kinds[name]
        k = g_index[name]
        return pltpu.make_async_remote_copy(
            src_ref=src, dst_ref=dst(sender), send_sem=g_send.at[k], recv_sem=g_recv.at[k, i],
            device_id={"xax": lax.rem(x + 2 * i, xs)}, device_id_type=pl.DeviceIdType.MESH)

    def g_pass(name, sender, source):
        k = g_index[name]
        return pltpu.make_async_remote_copy(
            src_ref=source, dst_ref=g_kinds[name][1](sender), send_sem=g_send.at[k], recv_sem=g_last.at[k],
            device_id={"xax": partner}, device_id_type=pl.DeviceIdType.MESH)

    def g_start(name):
        def body(i, carry):
            g_copy(name, i, x).start()
            return carry
        lax.fori_loop(1, chips, body, 0)
        src, dst, _ = g_kinds[name]
        g_pass(name, x, src).start()
        pltpu.make_async_copy(src, dst(x), g_last.at[g_index[name]]).start()

    def g_forward(name):
        def body(i, carry):
            sender = lax.rem(x + xs - 2 * i, xs)
            g_copy(name, i, sender).wait_recv()
            g_pass(name, sender, g_kinds[name][1](sender)).start()
            return carry
        lax.fori_loop(1, chips, body, 0)

    def g_wait(name):
        whole = g_kinds[name][2]
        arrived(whole.at[:, pl.ds(0, (chips + 1) * blk)], g_last.at[g_index[name]])

    def g_drain(name):
        arrived(g_kinds[name][2].at[:, most], g_send.at[g_index[name]])

    y_kinds = {"wq": wq_buf, "wo": out_buf, "down": down_buf}
    y_index = {name: i for i, name in enumerate(y_kinds)}
    others = pl.ds(0, ys - 1)

    def y_start(name):
        buf = y_kinds[name]
        k = y_index[name]

        def body(d, carry):
            pltpu.make_async_remote_copy(
                src_ref=buf.at[y], dst_ref=buf.at[y], send_sem=y_send.at[k], recv_sem=y_recv.at[k],
                device_id={"yax": lax.rem(y + d, ys)}, device_id_type=pl.DeviceIdType.MESH).start()
            return carry
        lax.fori_loop(1, ys, body, 0)

    def y_wait(name):
        arrived(y_kinds[name].at[others], y_recv.at[y_index[name]])

    def y_drain(name):
        arrived(y_kinds[name].at[others], y_send.at[y_index[name]])

    e_parts = row_chunks(window, EMBED_CHUNKS)

    def e_first(p):
        return p * vocab - lax.rem(p, 2) * shift

    def e_own():
        return pltpu.make_async_copy(
            embed.at[pl.ds(pl.multiple_of(e_first(x), 8), window), :], e_buf.at[:, lanes(x)], e_own_sem)

    def e_start(c):
        r0, n = e_parts[c]

        def body(d, carry):
            p = lax.rem(x + d, xs)
            pltpu.make_async_remote_copy(
                src_ref=embed.at[pl.ds(pl.multiple_of(e_first(p) + r0, 8), n), :],
                dst_ref=e_buf.at[pl.ds(r0, n), lanes(x)], send_sem=e_send, recv_sem=e_recv,
                device_id={"xax": p}, device_id_type=pl.DeviceIdType.MESH).start()
            return carry
        lax.fori_loop(1, xs, body, 0)

    mark("a1send")
    x_start("wq")
    for name in ("hidden", "ga"):
        g_start(name)
    for name in ("wo", "down"):
        x_start(name)
    for name in ("wk", "wv", "gf"):
        g_start(name)
    e_start(0)
    e_own().start()

    def start_cache_v(g, carry):
        cache_copy(g, v_hbm, v_buf, 1).start()
        return carry
    lax.fori_loop(0, groups, start_cache_v, 0)

    mark("a2wqx")
    x_wait("wq")
    y_start("wq")
    mark("a3hfwd")
    for name in ("hidden", "ga"):
        g_forward(name)
    mark("a4hwait")
    for name in ("hidden", "ga"):
        g_wait(name)
    mark("a5ln")
    my_rows = rows(y, quarter)
    n_all[my_rows, :] = layer_norm(h_buf[...].astype(F32), ga_buf[...]).astype(BF16)

    part = quarter // 2

    def n_rows(j, c):
        return pl.ds(pl.multiple_of(j * quarter + c * part, part), part)

    def n_copy(d, sender):
        r = n_rows(sender, core)
        return pltpu.make_async_remote_copy(
            src_ref=n_all.at[r, :], dst_ref=n_all.at[r, :], send_sem=n_send.at[0],
            recv_sem=n_recv.at[d], device_id={"yax": lax.rem(y + d, ys)},
            device_id_type=pl.DeviceIdType.MESH)

    def n_pass(d, c):
        r = n_rows(lax.rem(y + ys - d, ys), c)
        return pltpu.make_async_remote_copy(
            src_ref=n_all.at[r, :], dst_ref=n_all.at[r, :], send_sem=n_send.at[1],
            recv_sem=n_last.at[d], device_id={"xax": partner},
            device_id_type=pl.DeviceIdType.MESH)

    mark("a6wo")
    x_wait("wo")
    y_start("wo")
    mark("a6wqy")
    y_wait("wq")
    mark("a7q")
    wq_all = wq_buf[...].reshape(ys * cols, xs * blk)
    q_scr[...] = lax.dot_general(n_all[my_rows, :], wq_all, NT, preferred_element_type=F32).astype(BF16)
    mark("a8send")
    x_start("q")
    x_start("gate")
    x_start("up")

    def n_start(d, carry):
        n_copy(d, y).start()
        return carry
    lax.fori_loop(1, ys, n_start, 0)
    mark("b0down")
    x_wait("down")
    y_start("down")
    for c in range(1, 7):
        e_start(c)

    mark("b1kv")
    row_id = lax.broadcasted_iota(jnp.int32, (own, 4 * half), 0)
    first_row = (y * xs + x) * own
    position = jnp.zeros((own, 4 * half), jnp.int32)
    for b in range(own):
        position = jnp.where(row_id == b, lens[first_row + b], position)
    angle = position.astype(F32) * freq[...]
    cos_a = jnp.cos(angle)
    sin_a = jnp.sin(angle)
    for name in ("wk", "wv", "gf"):
        g_forward(name)
    for name in ("wk", "wv", "gf"):
        g_wait(name)
    mine = y * xs + x
    n_own = n_all[rows(mine, own), :]
    kv = lax.dot_general(n_own, kv_buf[...], NT, preferred_element_type=F32).astype(BF16).astype(F32)
    k1 = kv[:, :half]
    k2 = kv[:, half:head_dim]
    c1 = cos_a[:, :half]
    s1 = sin_a[:, :half]
    key = jnp.concatenate([k1 * c1 - k2 * s1, k2 * c1 + k1 * s1], axis=1).astype(BF16)
    value = kv[:, head_dim:].astype(BF16)
    k_scr[...] = key
    v_scr[...] = value
    small_outs = [pltpu.make_async_copy(k_scr, k_out, z_sem.at[0]),
                  pltpu.make_async_copy(v_scr, v_out, z_sem.at[1])]
    for copy in small_outs:
        copy.start()
    for h in range(heads):
        krep[pl.ds(h, own, stride=heads), :] = key.astype(F32)
        vrep[pl.ds(h, own, stride=heads), :] = value.astype(F32)

    mark("b2q")
    x_wait("q")
    mark("b3rot")
    for xc in range(xs // 2):
        qa = qx_buf[2 * xc].astype(F32)
        qb = qx_buf[2 * xc + 1].astype(F32)
        ra = (qa * cos_a - qb * sin_a).astype(BF16).astype(F32)
        rb = (qb * cos_a + qa * sin_a).astype(BF16).astype(F32)
        for yc in range(ys):
            pair = jnp.concatenate([ra[:, yc * half:(yc + 1) * half], rb[:, yc * half:(yc + 1) * half]], axis=1)
            q2d[pl.ds(xc * ys + yc, own, stride=heads), :] = pair
    scale = head_dim ** -0.5
    snew[...] = jnp.sum(q2d[...] * krep[...], axis=1, keepdims=True) * scale

    mark("b4attn")
    gr = per * heads
    seg_r = lax.broadcasted_iota(jnp.int32, (gr, per * head_dim), 0) // heads
    seg_c = lax.broadcasted_iota(jnp.int32, (gr, per * head_dim), 1) // head_dim
    diag = (seg_r == seg_c).astype(F32)
    tile = min(512, slots)
    row_g = lax.broadcasted_iota(jnp.int32, (gr, 1), 0) // heads
    lane_g = lax.broadcasted_iota(jnp.int32, (gr, tile), 1)

    def attend(g, carry):
        cache_copy(g, k_hbm, k_buf, 0).wait()
        qg = q2d[rows(g, gr), :]
        qbd = (jnp.concatenate([qg] * per, axis=1) * diag).astype(BF16)
        len_g = jnp.zeros((gr, 1), jnp.int32)
        for s in range(per):
            len_g = jnp.where(row_g == s, lens[first_row + g * per + s], len_g)
        new = snew[rows(g, gr), :]
        top = jnp.full((gr, tile), -jnp.inf, F32)
        kg = k_buf.at[g]
        vg = v_buf.at[g]
        for c in range(slots // tile):
            kc = kg[:, :, pl.ds(c * tile, tile)].reshape(per * head_dim, tile)
            sc = jnp.dot(qbd, kc, preferred_element_type=F32) * scale
            sc = jnp.where(lane_g < len_g - c * tile, sc, -jnp.inf)
            s_scr[:, pl.ds(c * tile, tile)] = sc
            top = jnp.maximum(top, sc)
        row_max = jnp.maximum(jnp.max(top, axis=1, keepdims=True), new)
        total = jnp.zeros((gr, tile), F32)
        for c in range(slots // tile):
            ex = jnp.exp(s_scr[:, pl.ds(c * tile, tile)] - row_max)
            s_scr[:, pl.ds(c * tile, tile)] = ex
            total = total + ex
        w_new = jnp.exp(new - row_max)
        den = jnp.sum(total, axis=1, keepdims=True) + w_new
        inv = 1.0 / den
        cache_copy(g, v_hbm, v_buf, 1).wait()
        mixed = jnp.zeros((gr, per * head_dim), F32)
        for c in range(slots // tile):
            pr = (s_scr[:, pl.ds(c * tile, tile)] * inv).astype(BF16)
            vc = vg[:, :, pl.ds(c * tile, tile)].reshape(per * head_dim, tile)
            mixed = mixed + lax.dot_general(pr, vc, NT, preferred_element_type=F32)
        add = (w_new * inv).astype(BF16).astype(F32) * vrep[rows(g, gr), :]
        for s in range(per):
            od_scr[pl.ds(pl.multiple_of(g * gr + s * heads, heads), heads), :] = (
                mixed[s * heads:(s + 1) * heads, s * head_dim:(s + 1) * head_dim]
                + add[s * heads:(s + 1) * heads, :])
        return carry

    lax.fori_loop(0, groups, attend, 0)
    mark("b5o")
    for xc in range(xs // 2):
        parts = [od_scr[pl.ds(xc * ys + yc, own, stride=heads), :] for yc in range(ys)]
        o_scr[2 * xc] = jnp.concatenate([p[:, :half] for p in parts], axis=1).astype(BF16)
        o_scr[2 * xc + 1] = jnp.concatenate([p[:, half:] for p in parts], axis=1).astype(BF16)
    x_start("o")
    for c in range(7, 13):
        e_start(c)

    def act_copy(dest):
        return pltpu.make_async_remote_copy(
            src_ref=act_scr.at[dest], dst_ref=act.at[:, pl.ds(pl.multiple_of(y * ff, ff), ff)],
            send_sem=y_send.at[len(y_kinds)], recv_sem=y_recv.at[len(y_kinds)],
            device_id={"yax": dest}, device_id_type=pl.DeviceIdType.MESH)

    mark("b6gu")
    x_wait("gate")
    x_wait("up")

    mark("b7feed")
    def feed(d, carry):
        @pl.when(d < ys - 1)
        def _():
            n_copy(d + 1, lax.rem(y + ys - d - 1, ys)).wait_recv()
            n_pass(d + 1, core).start()
        j = lax.rem(y + ys - d, ys)

        @pl.when(d > 0)
        def _():
            n_pass(d, 1 - core).wait_recv()
        gu = jnp.dot(n_all[rows(j, quarter), :], gu_buf[...], preferred_element_type=F32)
        gu = gu.astype(BF16).astype(F32)
        gate = gu[:, :ff]
        act_scr[j] = (gate * jax.nn.sigmoid(gate) * gu[:, ff:]).astype(BF16)

        @pl.when(d > 0)
        def _():
            act_copy(j).start()
        return carry
    lax.fori_loop(0, ys, feed, 0)
    act[:, pl.ds(pl.multiple_of(y * ff, ff), ff)] = act_scr[y]
    mark("b8wo")
    y_wait("wo")
    mark("b9o")
    x_wait("o")
    mark("c0op")
    part_scr[...] = jnp.dot(
        ox_buf[...], out_buf[...].reshape(ys * cols, xs * blk), preferred_element_type=F32)
    mark("c1down")
    y_wait("down")

    mark("c2act")
    arrived(act_scr.at[others], y_recv.at[len(y_kinds)])

    mark("c3branch")
    down_all = down_buf[...].reshape(ys * ff, xs * blk)
    part_scr[...] = part_scr[...] + jnp.dot(act[...], down_all, preferred_element_type=F32)

    def branch(c):
        for i in range(chips):
            rs_scr[c, i] = part_scr[pl.ds(pl.multiple_of((2 * i + c) * own, own), own), :]

    def pre_copy():
        return pltpu.make_async_remote_copy(
            src_ref=rs_scr.at[1 - core], dst_ref=pre_buf, send_sem=pre_sem.at[0], recv_sem=pre_sem.at[1],
            device_id={"xax": partner}, device_id_type=pl.DeviceIdType.MESH)

    def rs_copy(dest):
        return pltpu.make_async_remote_copy(
            src_ref=rs_scr.at[core, dest], dst_ref=rs_buf.at[chip], send_sem=rs_sem.at[0],
            recv_sem=rs_sem.at[1], device_id={"xax": 2 * dest + core},
            device_id_type=pl.DeviceIdType.MESH)

    chip = x // 2
    branch(1 - core)
    pre_copy().start()
    branch(core)
    mark("c4pre")
    pre_copy().wait_recv()
    rs_scr[core] = rs_scr[core] + pre_buf[...]

    mark("c5rs")
    def rs_start(i, carry):
        rs_copy(lax.rem(chip + i, chips)).start()
        return carry
    lax.fori_loop(1, chips, rs_start, 0)
    mark("c6rsw")
    arrived(rs_buf.at[pl.ds(0, chips - 1)], rs_sem.at[1])
    mark("c7ln")
    rs_buf[chip] = rs_scr[core, chip]
    res = h_buf[rows(x, own), :].astype(F32) + jnp.sum(rs_buf[...], axis=0)
    f_buf[rows(mine, own), :] = layer_norm(res, gf_buf[...]).astype(BF16)

    piece = own // 2

    def f_half(sy, sx, h):
        return f_buf.at[pl.ds(pl.multiple_of((sy * xs + sx) * own + h * piece, piece), piece), :]

    def f_over_x(i, h, sy, sx, sem):
        return pltpu.make_async_remote_copy(
            src_ref=f_half(sy, sx, h), dst_ref=f_half(sy, sx, h), send_sem=f_sem.at[0], recv_sem=sem,
            device_id={"xax": lax.rem(x + 2 * i, xs)}, device_id_type=pl.DeviceIdType.MESH)

    def f_over_y(d, h, sy, sx, sem):
        return pltpu.make_async_remote_copy(
            src_ref=f_half(sy, sx, h), dst_ref=f_half(sy, sx, h), send_sem=f_sem.at[0], recv_sem=sem,
            device_id={"yax": lax.rem(y + d, ys)}, device_id_type=pl.DeviceIdType.MESH)

    def f_pass(d, h, sy, sx):
        pltpu.make_async_remote_copy(
            src_ref=f_half(sy, sx, h), dst_ref=f_half(sy, sx, h), send_sem=f_sem.at[1],
            recv_sem=f_sem.at[2 + d], device_id={"xax": partner},
            device_id_type=pl.DeviceIdType.MESH).start()

    def from_y(d):
        return lax.rem(y + ys - d, ys)

    def from_x(i):
        return lax.rem(x + xs - 2 * i, xs)

    def spread_y(i):
        def body(d, carry):
            f_over_y(d, 0, y, from_x(i), fya.at[d, i]).start()
            return carry
        lax.fori_loop(1, ys, body, 0)

    def spread_x(d):
        def body(i, carry):
            f_over_x(i, 1, from_y(d), x, fxb.at[d, i]).start()
            return carry
        lax.fori_loop(1, chips, body, 0)

    mark("c8fx")
    def first_x(i, carry):
        f_over_x(i, 0, y, x, fxa.at[i]).start()
        return carry
    lax.fori_loop(1, chips, first_x, 0)

    def first_y(d, carry):
        f_over_y(d, 1, y, x, fyb.at[d]).start()
        return carry
    lax.fori_loop(1, ys, first_y, 0)
    spread_y(0)
    spread_x(0)
    f_pass(0, 0, y, x)
    f_pass(0, 1, y, x)
    for c in range(13, EMBED_CHUNKS):
        e_start(c)
    mark("c9sp")
    for i in range(1, max(chips, ys)):
        if i < chips:
            f_over_x(i, 0, y, from_x(i), fxa.at[i]).wait_recv()
            spread_y(i)
            f_pass(0, 0, y, from_x(i))
        if i < ys:
            f_over_y(i, 1, from_y(i), x, fyb.at[i]).wait_recv()
            spread_x(i)
            f_pass(i, 1, from_y(i), x)

    def collect(d):
        def body(i, carry):
            if d > 0:
                f_over_y(d, 0, from_y(d), from_x(i), fya.at[d, i]).wait_recv()
                f_pass(d, 0, from_y(d), from_x(i))

            @pl.when(i > 0)
            def _():
                f_over_x(i, 1, from_y(d), from_x(i), fxb.at[d, i]).wait_recv()
                f_pass(d, 1, from_y(d), from_x(i))
            return carry
        lax.fori_loop(0, chips, body, 0)

    mark("d0drain")
    for name in x_kinds:
        x_drain(name)
    for name in g_kinds:
        g_drain(name)
    for name in y_kinds:
        y_drain(name)
    arrived(act_scr.at[others], y_send.at[len(y_kinds)])
    for i in range(2):
        arrived(n_all.at[pl.ds(0, (ys - 1) * part), :], n_send.at[i])
    pre_copy().wait_send()
    arrived(rs_buf.at[pl.ds(0, chips - 1)], rs_sem.at[0])
    for copy in small_outs:
        copy.wait()

    def z_copy(j):
        return pltpu.make_async_copy(z_scr.at[j], logits_out.at[:, rows(j, quarter)], z_sem.at[2])

    skip = core * shift
    index = lax.broadcasted_iota(jnp.int32, (window, 1), 0)
    inside = jnp.logical_and(index >= skip, index < skip + vocab)
    half_block = pl.ds(0, chips * own)

    def head(d):
        mark(f'hw{d}')
        j = from_y(d)
        arrived(f_buf.at[half_block, :], f_sem.at[2 + d])
        mark(f'hz{d}')
        z = lax.dot_general(e_buf[...], f_buf[rows(j, quarter), :], NT, preferred_element_type=F32)
        z_scr[j] = z
        z_copy(j).start()
        if shift:
            z = jnp.where(inside, z, -jnp.inf)
        top = jnp.max(z, axis=0, keepdims=True)
        st_scr[0:1, rows(j, quarter)] = top
        st_scr[1:2, rows(j, quarter)] = jnp.sum(jnp.exp(z - top), axis=0, keepdims=True)

    mark("d1coll")
    order = sorted(range(ys), key=lambda d: (min(d, ys - d), d))
    for d in order[:2]:
        collect(d)
    mark("d1e")
    e_own().wait()
    arrived(e_buf.at[:, most], e_recv)

    mark("d3head")
    for k, d in enumerate(order):
        mark(f'h{k}')
        head(d)
        mark(f'hc{k}')
        if k + 2 < ys:
            collect(order[k + 2])

    mark("d4stat")
    def s_start(i, carry):
        pltpu.make_async_remote_copy(
            src_ref=st_scr, dst_ref=s_buf.at[mine], send_sem=s_sem.at[0], recv_sem=s_sem.at[1],
            device_id={"yax": lax.rem(y + i // xs, ys), "xax": lax.rem(x + lax.rem(i, xs), xs)},
            device_id_type=pl.DeviceIdType.MESH).start()
        return carry
    lax.fori_loop(1, ys * xs, s_start, 0)
    s_buf[mine] = st_scr[...]

    mark("d5sx")
    arrived(e_buf.at[:, most], e_send)
    arrived(f_buf.at[pl.ds(0, 2 * (ys * chips - 1) * piece), :], f_sem.at[0])
    arrived(f_buf.at[pl.ds(0, ys * chips * own), :], f_sem.at[1])
    arrived(z_scr, z_sem.at[2])
    everyone = s_buf.at[pl.ds(0, ys * xs - 1)]
    mark("d6sw")
    arrived(everyone, s_sem.at[1])
    tops = s_buf[:, 0, :]
    best = jnp.max(tops, axis=0, keepdims=True)
    whole = jnp.sum(s_buf[:, 1, :] * jnp.exp(tops - best), axis=0, keepdims=True)
    mark("d9n")
    norm_scr[...] = best + jnp.log(whole)
    norm_copy = pltpu.make_async_copy(norm_scr, norm_out, z_sem.at[0])
    norm_copy.start()
    arrived(everyone, s_sem.at[0])
    norm_copy.wait()
    mark(None)


def finish_kernel(shift, z_ref, next_ref, norm, key, value, out_ref, k_out, v_out, norm_out):
    n = z_ref.shape[0]
    if shift:
        odd = lax.rem(lax.axis_index("xax"), 2) == 1

        @pl.when(odd)
        def _():
            out_ref[pl.ds(0, n - shift), :] = z_ref[pl.ds(shift, n - shift), :] - norm[...]
            out_ref[pl.ds(n - shift, shift), :] = next_ref[pl.ds(0, shift), :] - norm[...]

        @pl.when(jnp.logical_not(odd))
        def _():
            out_ref[...] = z_ref[...] - norm[...]
    else:
        out_ref[...] = z_ref[...] - norm[...]
    k_out[...] = key[...]
    v_out[...] = value[...]
    norm_out[...] = norm[...]


def solution(mesh):
    ys = mesh.shape["yax"]
    xs = mesh.shape["xax"]
    row_spec = P(("dp", "yax", "xax"))

    def local_step(hidden, cache_len, k_cache, v_cache, g_attn, w_query, w_key, w_value,
                   w_gate, w_up, w_out, w_down, g_final, embedding):
        batch, blk = hidden.shape
        own, slots, head_dim = k_cache.shape
        width = blk * xs
        vocab = embedding.shape[0] // xs
        shift = vocab % 8
        window = -(-vocab // 8) * 8
        half = head_dim // 2
        quarter = xs * own
        cols = w_query.shape[1] // xs
        ff = w_gate.shape[1] // xs
        heads = w_query.shape[1] * ys // head_dim
        per = 4
        groups = own // per
        freq_row = (ROPE_BASE ** (-(np.arange(half, dtype=np.float32) * 2.0) / head_dim)).astype(np.float32)
        freq = jnp.asarray(np.tile(freq_row, 4)[None, :])
        any_spec = pl.BlockSpec(memory_space=pl.ANY)
        vmem = pl.BlockSpec(memory_space=pltpu.VMEM)
        smem = pl.BlockSpec(memory_space=pltpu.SMEM)
        dma = pltpu.SemaphoreType.DMA
        chips = xs // 2
        scratch = [
            pltpu.VMEM((groups, per, head_dim, slots), BF16),
            pltpu.VMEM((groups, per, head_dim, slots), BF16),
            pltpu.VMEM((quarter, width), BF16),
            pltpu.VMEM((1, width), F32),
            pltpu.VMEM((1, width), F32),
            pltpu.VMEM((w_query.shape[1], blk), BF16),
            pltpu.VMEM((ys, cols, width), BF16),
            pltpu.VMEM((width, 2 * ff), BF16),
            pltpu.VMEM((ys, ff, width), BF16),
            pltpu.VMEM((ys, cols, width), BF16),
            pltpu.VMEM((2 * head_dim, width), BF16),
            pltpu.VMEM((batch, width), BF16),
            pltpu.VMEM((quarter, ys * cols), BF16),
            pltpu.VMEM((xs, own, ys * cols), BF16),
            pltpu.VMEM((own * heads, head_dim), F32),
            pltpu.VMEM((own * heads, 1), F32),
            pltpu.VMEM((own * heads, head_dim), F32),
            pltpu.VMEM((own * heads, head_dim), F32),
            pltpu.VMEM((per * heads, slots), F32),
            pltpu.VMEM((own * heads, head_dim), F32),
            pltpu.VMEM((xs, own, ys * cols), BF16),
            pltpu.VMEM((quarter, ys * cols), BF16),
            pltpu.VMEM((ys, quarter, ff), BF16),
            pltpu.VMEM((quarter, ys * ff), BF16),
            pltpu.VMEM((quarter, width), F32),
            pltpu.VMEM((chips, own, width), F32),
            pltpu.VMEM((2, chips, own, width), F32),
            pltpu.VMEM((chips, own, width), F32),
            pltpu.VMEM((batch, width), BF16),
            pltpu.VMEM((window, width), BF16),
            pltpu.VMEM((ys, window, quarter), F32),
            pltpu.VMEM((2, batch), F32),
            pltpu.VMEM((own, head_dim), BF16),
            pltpu.VMEM((own, head_dim), BF16),
            pltpu.VMEM((1, batch), F32),
            pltpu.VMEM((ys * xs, 2, batch), F32),
            dma((2, groups)), dma, dma((3,)), dma((7,)), dma((7,)),
            dma((5,)), dma((5, chips)), dma((5,)), dma((4,)), dma((4,)), dma, dma,
            dma((ys,)), dma((ys,)), dma((2,)), dma((2,)), dma((2,)),
            dma((chips,)), dma((ys,)), dma((ys, chips)), dma((ys, chips)), dma((2 + ys,)), dma((2,)),
        ]
        cfg = (ys, xs, own, vocab, shift)
        key_new, value_new, logits, norm = pl.pallas_call(
            functools.partial(kernel, cfg),
            name="decode_layer",
            out_shape=(
                jax.ShapeDtypeStruct((own, head_dim), BF16),
                jax.ShapeDtypeStruct((own, head_dim), BF16),
                jax.ShapeDtypeStruct((window, batch), F32),
                jax.ShapeDtypeStruct((1, batch), F32)),
            in_specs=[smem, any_spec, any_spec, any_spec, any_spec, any_spec, vmem] + [any_spec] * 7 + [vmem],
            out_specs=(any_spec, any_spec, any_spec, any_spec),
            scratch_shapes=scratch,
            compiler_params=pltpu.CompilerParams(
                collective_id=0, has_side_effects=True, vmem_limit_bytes=67043328),
        )(cache_len, hidden, k_cache.transpose(0, 2, 1), v_cache.transpose(0, 2, 1),
          g_attn[None, :], g_final[None, :], w_query, w_key.T, w_value.T, w_gate, w_up, w_out, w_down,
          embedding, freq)
        step = min(200, window)
        steps = -(-window // step)

        def fixed(shape):
            return pl.BlockSpec(shape, lambda i: (0, 0))
        log_probs, key_new, value_new, norm = pl.pallas_call(
            functools.partial(finish_kernel, shift),
            name="finish",
            grid=(steps,),
            out_shape=(
                jax.ShapeDtypeStruct((vocab, batch), F32),
                jax.ShapeDtypeStruct((own, head_dim), BF16),
                jax.ShapeDtypeStruct((own, head_dim), BF16),
                jax.ShapeDtypeStruct((1, batch), F32)),
            in_specs=[
                pl.BlockSpec((step, batch), lambda i: (i, 0)),
                pl.BlockSpec((8, batch), lambda i: (jnp.minimum((i + 1) * (step // 8), window // 8 - 1), 0)),
                fixed((1, batch)), fixed((own, head_dim)), fixed((own, head_dim))],
            out_specs=(
                pl.BlockSpec((step, batch), lambda i: (i, 0)),
                fixed((own, head_dim)), fixed((own, head_dim)), fixed((1, batch))),
        )(logits, logits, norm, key_new, value_new)
        return key_new, value_new, log_probs.T, norm[0]

    in_specs = (P("dp", "xax"), P("dp"), row_spec, row_spec, P("xax"), P("xax", "yax"),
                P("xax", None), P("xax", None), P("xax", "yax"), P("xax", "yax"),
                P("yax", "xax"), P("yax", "xax"), P("xax"), P("yax", "xax"))
    out_specs = (row_spec, row_spec, P("dp", ("yax", "xax")), P("dp"))
    return jax.shard_map(local_step, mesh=mesh, in_specs=in_specs, out_specs=out_specs, check_vma=False)
```

```python
import functools

import jax
import jax.numpy as jnp
import numpy as np
from jax import lax
from jax.experimental import pallas as pl
from jax.experimental.pallas import tpu as pltpu
from jax.sharding import PartitionSpec as P

EPS = 1e-6
ROPE_BASE = 10000.0
F32 = jnp.float32
BF16 = jnp.bfloat16
NT = (((1,), (1,)), ((), ()))
EMBED_CHUNKS = 16


def layer_norm(values_in, gain):
    mean = jnp.mean(values_in, axis=-1, keepdims=True)
    centred = values_in - mean
    var = jnp.mean(centred * centred, axis=-1, keepdims=True)
    return centred * lax.rsqrt(var + EPS) * gain


def row_chunks(total, count):
    cuts = [16 * (total // 16 * i // count) for i in range(count)] + [total]
    return [(cuts[i], cuts[i + 1] - cuts[i]) for i in range(count)]


class Marker:
    def __init__(self):
        self.scope = None

    def __call__(self, name):
        if self.scope is not None:
            self.scope.__exit__(None, None, None)
        self.scope = None
        if name:
            self.scope = jax.named_scope(name)
            self.scope.__enter__()


def kernel(cfg, lens, hidden, k_hbm, v_hbm, g_attn, g_final, w_query, w_key, w_value, w_gate, w_up,
           w_out, w_down, embed, freq,
           k_out, v_out, logits_out, norm_out,
           k_buf, v_buf, h_buf, ga_buf, gf_buf, wqt, wq_buf, gu_buf, down_buf, out_buf, kv_buf,
           n_all, q_scr, qx_buf, q2d, snew, krep, vrep, s_scr, od_scr, o_scr, ox_buf, act_scr, act, part_scr,
           pre_buf, rs_scr, rs_buf, f_buf, e_buf, z_scr, st_scr, k_scr, v_scr, norm_scr, s_buf,
           kv_sem, e_own_sem, z_sem, x_send, x_recv, g_send, g_recv, g_last, y_send, y_recv, e_send, e_recv,
           n_recv, n_last, n_send, pre_sem, rs_sem, fxa, fyb, fya, fxb, f_sem, s_sem):
    ys, xs, own, vocab, shift = cfg
    mark = Marker()
    y = lax.axis_index("yax")
    x = lax.axis_index("xax")
    core = lax.rem(x, 2)
    partner = x + 1 - 2 * core
    blk = hidden.shape[1]
    quarter = xs * own
    head_dim = k_hbm.shape[1]
    half = head_dim // 2
    seqs = k_hbm.shape[0]
    slots = k_hbm.shape[2]
    heads = w_query.shape[1] * ys // head_dim
    groups = k_buf.shape[0]
    per = seqs // groups
    window = e_buf.shape[0]

    def lanes(i):
        return pl.ds(pl.multiple_of(i * blk, 128), blk)

    def rows(i, n):
        return pl.ds(pl.multiple_of(i * n, n), n)

    def cache_copy(g, src, dst, s):
        return pltpu.make_async_copy(src.at[pl.ds(g * per, per)], dst.at[g], kv_sem.at[s, g])

    def start_cache(g, carry):
        cache_copy(g, k_hbm, k_buf, 0).start()
        return carry
    lax.fori_loop(0, groups, start_cache, 0)

    wqt[...] = w_query[...].astype(F32).T.astype(BF16)

    mark("a0barrier")
    barrier = pltpu.get_barrier_semaphore()

    def signal_row(d, carry):
        pl.semaphore_signal(barrier, inc=1, device_id={"xax": lax.rem(x + d, xs)},
                            device_id_type=pl.DeviceIdType.MESH)
        return carry
    lax.fori_loop(1, xs, signal_row, 0)

    def signal_column(d, carry):
        pl.semaphore_signal(barrier, inc=1, device_id={"yax": lax.rem(y + d, ys)},
                            device_id_type=pl.DeviceIdType.MESH)
        return carry
    lax.fori_loop(1, ys, signal_column, 0)
    pl.semaphore_wait(barrier, xs + ys - 2)

    def arrived(ref, sem):
        pltpu.make_async_copy(ref, ref, sem).wait()

    cols = wqt.shape[0] // xs
    ff = w_gate.shape[1] // xs
    most = pl.ds(0, (xs - 1) * blk)
    x_kinds = {
        "wq": (lambda p: wqt.at[rows(p, cols), :], lambda s: wq_buf.at[y, :, lanes(s)],
               wq_buf.at[y], wq_buf.at[y, :, most]),
        "wo": (lambda p: w_out.at[rows(p, cols), :], lambda s: out_buf.at[y, :, lanes(s)],
               out_buf.at[y], out_buf.at[y, :, most]),
        "down": (lambda p: w_down.at[rows(p, ff), :], lambda s: down_buf.at[y, :, lanes(s)],
                 down_buf.at[y], down_buf.at[y, :, most]),
        "gate": (lambda p: w_gate.at[:, lanes(p)], lambda s: gu_buf.at[rows(s, blk), pl.ds(0, ff)],
                 gu_buf.at[:, pl.ds(0, ff)], gu_buf.at[most, pl.ds(0, ff)]),
        "up": (lambda p: w_up.at[:, lanes(p)], lambda s: gu_buf.at[rows(s, blk), pl.ds(ff, ff)],
               gu_buf.at[:, pl.ds(ff, ff)], gu_buf.at[most, pl.ds(ff, ff)]),
        "q": (lambda p: q_scr.at[rows(p, own), :], lambda s: qx_buf.at[s],
              qx_buf, qx_buf.at[pl.ds(0, xs - 1)]),
        "o": (lambda p: o_scr.at[p], lambda s: ox_buf.at[rows(s, own), :],
              ox_buf, ox_buf.at[pl.ds(0, (xs - 1) * own), :]),
    }
    x_index = {name: i for i, name in enumerate(x_kinds)}

    def x_start(name):
        src, dst = x_kinds[name][:2]
        k = x_index[name]

        def body(d, carry):
            p = lax.rem(x + d, xs)
            pltpu.make_async_remote_copy(
                src_ref=src(p), dst_ref=dst(x), send_sem=x_send.at[k], recv_sem=x_recv.at[k],
                device_id={"xax": p}, device_id_type=pl.DeviceIdType.MESH).start()
            return carry
        lax.fori_loop(1, xs, body, 0)
        pltpu.make_async_copy(src(x), dst(x), x_recv.at[k]).start()

    def x_wait(name):
        arrived(x_kinds[name][2], x_recv.at[x_index[name]])

    def x_drain(name):
        arrived(x_kinds[name][3], x_send.at[x_index[name]])

    chips = xs // 2
    g_kinds = {
        "hidden": (hidden.at[rows(y, quarter), :], lambda s: h_buf.at[:, lanes(s)], h_buf),
        "ga": (g_attn, lambda s: ga_buf.at[:, lanes(s)], ga_buf),
        "gf": (g_final, lambda s: gf_buf.at[:, lanes(s)], gf_buf),
        "wk": (w_key, lambda s: kv_buf.at[pl.ds(0, head_dim), lanes(s)], kv_buf.at[pl.ds(0, head_dim), :]),
        "wv": (w_value, lambda s: kv_buf.at[pl.ds(head_dim, head_dim), lanes(s)],
               kv_buf.at[pl.ds(head_dim, head_dim), :]),
    }
    g_index = {name: i for i, name in enumerate(g_kinds)}

    def g_copy(name, i, sender):
        src, dst, _ = g_kinds[name]
        k = g_index[name]
        return pltpu.make_async_remote_copy(
            src_ref=src, dst_ref=dst(sender), send_sem=g_send.at[k], recv_sem=g_recv.at[k, i],
            device_id={"xax": lax.rem(x + 2 * i, xs)}, device_id_type=pl.DeviceIdType.MESH)

    def g_pass(name, sender, source):
        k = g_index[name]
        return pltpu.make_async_remote_copy(
            src_ref=source, dst_ref=g_kinds[name][1](sender), send_sem=g_send.at[k], recv_sem=g_last.at[k],
            device_id={"xax": partner}, device_id_type=pl.DeviceIdType.MESH)

    def g_start(name):
        def body(i, carry):
            g_copy(name, i, x).start()
            return carry
        lax.fori_loop(1, chips, body, 0)
        src, dst, _ = g_kinds[name]
        g_pass(name, x, src).start()
        pltpu.make_async_copy(src, dst(x), g_last.at[g_index[name]]).start()

    def g_forward(name):
        def body(i, carry):
            sender = lax.rem(x + xs - 2 * i, xs)
            g_copy(name, i, sender).wait_recv()
            g_pass(name, sender, g_kinds[name][1](sender)).start()
            return carry
        lax.fori_loop(1, chips, body, 0)

    def g_wait(name):
        whole = g_kinds[name][2]
        arrived(whole.at[:, pl.ds(0, (chips + 1) * blk)], g_last.at[g_index[name]])

    def g_drain(name):
        arrived(g_kinds[name][2].at[:, most], g_send.at[g_index[name]])

    y_kinds = {"wq": wq_buf, "wo": out_buf, "down": down_buf}
    y_index = {name: i for i, name in enumerate(y_kinds)}
    others = pl.ds(0, ys - 1)

    def y_start(name):
        buf = y_kinds[name]
        k = y_index[name]

        def body(d, carry):
            pltpu.make_async_remote_copy(
                src_ref=buf.at[y], dst_ref=buf.at[y], send_sem=y_send.at[k], recv_sem=y_recv.at[k],
                device_id={"yax": lax.rem(y + d, ys)}, device_id_type=pl.DeviceIdType.MESH).start()
            return carry
        lax.fori_loop(1, ys, body, 0)

    def y_wait(name):
        arrived(y_kinds[name].at[others], y_recv.at[y_index[name]])

    def y_drain(name):
        arrived(y_kinds[name].at[others], y_send.at[y_index[name]])

    e_parts = row_chunks(window, EMBED_CHUNKS)

    def e_first(p):
        return p * vocab - lax.rem(p, 2) * shift

    def e_own():
        return pltpu.make_async_copy(
            embed.at[pl.ds(pl.multiple_of(e_first(x), 8), window), :], e_buf.at[:, lanes(x)], e_own_sem)

    def e_start(c):
        r0, n = e_parts[c]

        def body(d, carry):
            p = lax.rem(x + d, xs)
            pltpu.make_async_remote_copy(
                src_ref=embed.at[pl.ds(pl.multiple_of(e_first(p) + r0, 8), n), :],
                dst_ref=e_buf.at[pl.ds(r0, n), lanes(x)], send_sem=e_send, recv_sem=e_recv,
                device_id={"xax": p}, device_id_type=pl.DeviceIdType.MESH).start()
            return carry
        lax.fori_loop(1, xs, body, 0)

    mark("a1send")
    x_start("wq")
    for name in ("hidden", "ga"):
        g_start(name)
    for name in ("wo", "down"):
        x_start(name)
    for name in ("wk", "wv", "gf"):
        g_start(name)
    e_start(0)
    e_own().start()

    def start_cache_v(g, carry):
        cache_copy(g, v_hbm, v_buf, 1).start()
        return carry
    lax.fori_loop(0, groups, start_cache_v, 0)

    mark("a2wqx")
    x_wait("wq")
    y_start("wq")
    mark("a3hfwd")
    for name in ("hidden", "ga"):
        g_forward(name)
    mark("a4hwait")
    for name in ("hidden", "ga"):
        g_wait(name)
    mark("a5ln")
    my_rows = rows(y, quarter)
    n_all[my_rows, :] = layer_norm(h_buf[...].astype(F32), ga_buf[...]).astype(BF16)

    part = quarter // 2

    def n_rows(j, c):
        return pl.ds(pl.multiple_of(j * quarter + c * part, part), part)

    def n_copy(d, sender):
        r = n_rows(sender, core)
        return pltpu.make_async_remote_copy(
            src_ref=n_all.at[r, :], dst_ref=n_all.at[r, :], send_sem=n_send.at[0],
            recv_sem=n_recv.at[d], device_id={"yax": lax.rem(y + d, ys)},
            device_id_type=pl.DeviceIdType.MESH)

    def n_pass(d, c):
        r = n_rows(lax.rem(y + ys - d, ys), c)
        return pltpu.make_async_remote_copy(
            src_ref=n_all.at[r, :], dst_ref=n_all.at[r, :], send_sem=n_send.at[1],
            recv_sem=n_last.at[d], device_id={"xax": partner},
            device_id_type=pl.DeviceIdType.MESH)

    mark("a6wo")
    x_wait("wo")
    y_start("wo")
    mark("a6wqy")
    y_wait("wq")
    mark("a7q")
    wq_all = wq_buf[...].reshape(ys * cols, xs * blk)
    q_scr[...] = lax.dot_general(n_all[my_rows, :], wq_all, NT, preferred_element_type=F32).astype(BF16)
    mark("a8send")
    x_start("q")
    x_start("gate")
    x_start("up")

    def n_start(d, carry):
        n_copy(d, y).start()
        return carry
    lax.fori_loop(1, ys, n_start, 0)
    mark("b0down")
    x_wait("down")
    y_start("down")
    for c in range(1, 7):
        e_start(c)

    mark("b1kv")
    row_id = lax.broadcasted_iota(jnp.int32, (own, 4 * half), 0)
    first_row = (y * xs + x) * own
    position = jnp.zeros((own, 4 * half), jnp.int32)
    for b in range(own):
        position = jnp.where(row_id == b, lens[first_row + b], position)
    angle = position.astype(F32) * freq[...]
    cos_a = jnp.cos(angle)
    sin_a = jnp.sin(angle)
    for name in ("wk", "wv", "gf"):
        g_forward(name)
    for name in ("wk", "wv", "gf"):
        g_wait(name)
    mine = y * xs + x
    n_own = n_all[rows(mine, own), :]
    kv = lax.dot_general(n_own, kv_buf[...], NT, preferred_element_type=F32).astype(BF16).astype(F32)
    k1 = kv[:, :half]
    k2 = kv[:, half:head_dim]
    c1 = cos_a[:, :half]
    s1 = sin_a[:, :half]
    key = jnp.concatenate([k1 * c1 - k2 * s1, k2 * c1 + k1 * s1], axis=1).astype(BF16)
    value = kv[:, head_dim:].astype(BF16)
    k_scr[...] = key
    v_scr[...] = value
    small_outs = [pltpu.make_async_copy(k_scr, k_out, z_sem.at[0]),
                  pltpu.make_async_copy(v_scr, v_out, z_sem.at[1])]
    for copy in small_outs:
        copy.start()
    for h in range(heads):
        krep[pl.ds(h, own, stride=heads), :] = key.astype(F32)
        vrep[pl.ds(h, own, stride=heads), :] = value.astype(F32)

    mark("b2q")
    x_wait("q")
    mark("b3rot")
    for xc in range(xs // 2):
        qa = qx_buf[2 * xc].astype(F32)
        qb = qx_buf[2 * xc + 1].astype(F32)
        ra = (qa * cos_a - qb * sin_a).astype(BF16).astype(F32)
        rb = (qb * cos_a + qa * sin_a).astype(BF16).astype(F32)
        for yc in range(ys):
            pair = jnp.concatenate([ra[:, yc * half:(yc + 1) * half], rb[:, yc * half:(yc + 1) * half]], axis=1)
            q2d[pl.ds(xc * ys + yc, own, stride=heads), :] = pair
    scale = head_dim ** -0.5
    snew[...] = jnp.sum(q2d[...] * krep[...], axis=1, keepdims=True) * scale

    mark("b4attn")
    gr = per * heads
    seg_r = lax.broadcasted_iota(jnp.int32, (gr, per * head_dim), 0) // heads
    seg_c = lax.broadcasted_iota(jnp.int32, (gr, per * head_dim), 1) // head_dim
    diag = (seg_r == seg_c).astype(F32)
    tile = min(512, slots)
    row_g = lax.broadcasted_iota(jnp.int32, (gr, 1), 0) // heads
    lane_g = lax.broadcasted_iota(jnp.int32, (gr, tile), 1)

    def attend(g, carry):
        cache_copy(g, k_hbm, k_buf, 0).wait()
        qg = q2d[rows(g, gr), :]
        qbd = (jnp.concatenate([qg] * per, axis=1) * diag).astype(BF16)
        len_g = jnp.zeros((gr, 1), jnp.int32)
        for s in range(per):
            len_g = jnp.where(row_g == s, lens[first_row + g * per + s], len_g)
        new = snew[rows(g, gr), :]
        top = jnp.full((gr, tile), -jnp.inf, F32)
        kg = k_buf.at[g]
        vg = v_buf.at[g]
        for c in range(slots // tile):
            kc = kg[:, :, pl.ds(c * tile, tile)].reshape(per * head_dim, tile)
            sc = jnp.dot(qbd, kc, preferred_element_type=F32) * scale
            sc = jnp.where(lane_g < len_g - c * tile, sc, -jnp.inf)
            s_scr[:, pl.ds(c * tile, tile)] = sc
            top = jnp.maximum(top, sc)
        row_max = jnp.maximum(jnp.max(top, axis=1, keepdims=True), new)
        total = jnp.zeros((gr, tile), F32)
        for c in range(slots // tile):
            ex = jnp.exp(s_scr[:, pl.ds(c * tile, tile)] - row_max)
            s_scr[:, pl.ds(c * tile, tile)] = ex
            total = total + ex
        w_new = jnp.exp(new - row_max)
        den = jnp.sum(total, axis=1, keepdims=True) + w_new
        inv = 1.0 / den
        cache_copy(g, v_hbm, v_buf, 1).wait()
        mixed = jnp.zeros((gr, per * head_dim), F32)
        for c in range(slots // tile):
            pr = (s_scr[:, pl.ds(c * tile, tile)] * inv).astype(BF16)
            vc = vg[:, :, pl.ds(c * tile, tile)].reshape(per * head_dim, tile)
            mixed = mixed + lax.dot_general(pr, vc, NT, preferred_element_type=F32)
        add = (w_new * inv).astype(BF16).astype(F32) * vrep[rows(g, gr), :]
        for s in range(per):
            od_scr[pl.ds(pl.multiple_of(g * gr + s * heads, heads), heads), :] = (
                mixed[s * heads:(s + 1) * heads, s * head_dim:(s + 1) * head_dim]
                + add[s * heads:(s + 1) * heads, :])
        return carry

    lax.fori_loop(0, groups, attend, 0)
    mark("b5o")
    for xc in range(xs // 2):
        parts = [od_scr[pl.ds(xc * ys + yc, own, stride=heads), :] for yc in range(ys)]
        o_scr[2 * xc] = jnp.concatenate([p[:, :half] for p in parts], axis=1).astype(BF16)
        o_scr[2 * xc + 1] = jnp.concatenate([p[:, half:] for p in parts], axis=1).astype(BF16)
    x_start("o")
    for c in range(7, 12):
        e_start(c)

    def act_copy(dest):
        return pltpu.make_async_remote_copy(
            src_ref=act_scr.at[dest], dst_ref=act.at[:, pl.ds(pl.multiple_of(y * ff, ff), ff)],
            send_sem=y_send.at[len(y_kinds)], recv_sem=y_recv.at[len(y_kinds)],
            device_id={"yax": dest}, device_id_type=pl.DeviceIdType.MESH)

    mark("b6gu")
    x_wait("gate")
    x_wait("up")

    mark("b7feed")
    def feed(d, carry):
        @pl.when(d < ys - 1)
        def _():
            n_copy(d + 1, lax.rem(y + ys - d - 1, ys)).wait_recv()
            n_pass(d + 1, core).start()
        j = lax.rem(y + ys - d, ys)

        @pl.when(d > 0)
        def _():
            n_pass(d, 1 - core).wait_recv()
        gu = jnp.dot(n_all[rows(j, quarter), :], gu_buf[...], preferred_element_type=F32)
        gu = gu.astype(BF16).astype(F32)
        gate = gu[:, :ff]
        act_scr[j] = (gate * jax.nn.sigmoid(gate) * gu[:, ff:]).astype(BF16)

        @pl.when(d > 0)
        def _():
            act_copy(j).start()
        return carry
    lax.fori_loop(0, ys, feed, 0)
    act[:, pl.ds(pl.multiple_of(y * ff, ff), ff)] = act_scr[y]
    mark("b8wo")
    y_wait("wo")
    mark("b9o")
    x_wait("o")
    mark("c0op")
    part_scr[...] = jnp.dot(
        ox_buf[...], out_buf[...].reshape(ys * cols, xs * blk), preferred_element_type=F32)
    mark("c1down")
    y_wait("down")

    mark("c2act")
    arrived(act_scr.at[others], y_recv.at[len(y_kinds)])

    mark("c3branch")
    down_all = down_buf[...].reshape(ys * ff, xs * blk)
    part_scr[...] = part_scr[...] + jnp.dot(act[...], down_all, preferred_element_type=F32)

    def branch(c):
        for i in range(chips):
            rs_scr[c, i] = part_scr[pl.ds(pl.multiple_of((2 * i + c) * own, own), own), :]

    def pre_copy():
        return pltpu.make_async_remote_copy(
            src_ref=rs_scr.at[1 - core], dst_ref=pre_buf, send_sem=pre_sem.at[0], recv_sem=pre_sem.at[1],
            device_id={"xax": partner}, device_id_type=pl.DeviceIdType.MESH)

    def rs_copy(dest):
        return pltpu.make_async_remote_copy(
            src_ref=rs_scr.at[core, dest], dst_ref=rs_buf.at[chip], send_sem=rs_sem.at[0],
            recv_sem=rs_sem.at[1], device_id={"xax": 2 * dest + core},
            device_id_type=pl.DeviceIdType.MESH)

    chip = x // 2
    branch(1 - core)
    pre_copy().start()
    branch(core)
    mark("c4pre")
    pre_copy().wait_recv()
    rs_scr[core] = rs_scr[core] + pre_buf[...]

    mark("c5rs")
    def rs_start(i, carry):
        rs_copy(lax.rem(chip + i, chips)).start()
        return carry
    lax.fori_loop(1, chips, rs_start, 0)
    mark("c6rsw")
    arrived(rs_buf.at[pl.ds(0, chips - 1)], rs_sem.at[1])
    mark("c7ln")
    rs_buf[chip] = rs_scr[core, chip]
    res = h_buf[rows(x, own), :].astype(F32) + jnp.sum(rs_buf[...], axis=0)
    f_buf[rows(mine, own), :] = layer_norm(res, gf_buf[...]).astype(BF16)

    piece = own // 2

    def f_half(sy, sx, h):
        return f_buf.at[pl.ds(pl.multiple_of((sy * xs + sx) * own + h * piece, piece), piece), :]

    def f_over_x(i, h, sy, sx, sem):
        return pltpu.make_async_remote_copy(
            src_ref=f_half(sy, sx, h), dst_ref=f_half(sy, sx, h), send_sem=f_sem.at[0], recv_sem=sem,
            device_id={"xax": lax.rem(x + 2 * i, xs)}, device_id_type=pl.DeviceIdType.MESH)

    def f_over_y(d, h, sy, sx, sem):
        return pltpu.make_async_remote_copy(
            src_ref=f_half(sy, sx, h), dst_ref=f_half(sy, sx, h), send_sem=f_sem.at[0], recv_sem=sem,
            device_id={"yax": lax.rem(y + d, ys)}, device_id_type=pl.DeviceIdType.MESH)

    def f_pass(d, h, sy, sx):
        pltpu.make_async_remote_copy(
            src_ref=f_half(sy, sx, h), dst_ref=f_half(sy, sx, h), send_sem=f_sem.at[1],
            recv_sem=f_sem.at[2 + d], device_id={"xax": partner},
            device_id_type=pl.DeviceIdType.MESH).start()

    def from_y(d):
        return lax.rem(y + ys - d, ys)

    def from_x(i):
        return lax.rem(x + xs - 2 * i, xs)

    def spread_y(i):
        def body(d, carry):
            f_over_y(d, 0, y, from_x(i), fya.at[d, i]).start()
            return carry
        lax.fori_loop(1, ys, body, 0)

    def spread_x(d):
        def body(i, carry):
            f_over_x(i, 1, from_y(d), x, fxb.at[d, i]).start()
            return carry
        lax.fori_loop(1, chips, body, 0)

    mark("c8fx")
    def first_x(i, carry):
        f_over_x(i, 0, y, x, fxa.at[i]).start()
        return carry
    lax.fori_loop(1, chips, first_x, 0)

    def first_y(d, carry):
        f_over_y(d, 1, y, x, fyb.at[d]).start()
        return carry
    lax.fori_loop(1, ys, first_y, 0)
    spread_y(0)
    spread_x(0)
    f_pass(0, 0, y, x)
    f_pass(0, 1, y, x)
    for c in range(12, EMBED_CHUNKS):
        e_start(c)
    mark("c9sp")
    for i in range(1, max(chips, ys)):
        if i < chips:
            f_over_x(i, 0, y, from_x(i), fxa.at[i]).wait_recv()
            spread_y(i)
            f_pass(0, 0, y, from_x(i))
        if i < ys:
            f_over_y(i, 1, from_y(i), x, fyb.at[i]).wait_recv()
            spread_x(i)
            f_pass(i, 1, from_y(i), x)

    def collect(d):
        def body(i, carry):
            @pl.when(d > 0)
            def _():
                f_over_y(d, 0, from_y(d), from_x(i), fya.at[d, i]).wait_recv()
                f_pass(d, 0, from_y(d), from_x(i))

            @pl.when(i > 0)
            def _():
                f_over_x(i, 1, from_y(d), from_x(i), fxb.at[d, i]).wait_recv()
                f_pass(d, 1, from_y(d), from_x(i))
            return carry
        lax.fori_loop(0, chips, body, 0)

    mark("d0drain")
    for name in x_kinds:
        x_drain(name)
    for name in g_kinds:
        g_drain(name)
    for name in y_kinds:
        y_drain(name)
    arrived(act_scr.at[others], y_send.at[len(y_kinds)])
    for i in range(2):
        arrived(n_all.at[pl.ds(0, (ys - 1) * part), :], n_send.at[i])
    pre_copy().wait_send()
    arrived(rs_buf.at[pl.ds(0, chips - 1)], rs_sem.at[0])
    for copy in small_outs:
        copy.wait()

    def z_copy(j):
        return pltpu.make_async_copy(z_scr.at[j], logits_out.at[:, rows(j, quarter)], z_sem.at[2])

    skip = core * shift
    half_block = pl.ds(0, chips * own)
    z_parts = row_chunks(window, 4)

    def nearest(k):
        return k + k // 2 * (1 - 2 * lax.rem(k, 2))

    def head(k, carry):
        d = nearest(k)
        j = from_y(d)
        with jax.named_scope('hw'):
            arrived(f_buf.at[half_block, :], f_sem.at[2 + d])
        z_scr[j] = lax.dot_general(e_buf[...], f_buf[rows(j, quarter), :], NT, preferred_element_type=F32)
        z_copy(j).start()
        stats = []
        for p, (r0, n) in enumerate(z_parts):
            z = z_scr[j, pl.ds(r0, n), :]
            if shift and p in (0, len(z_parts) - 1):
                index = lax.broadcasted_iota(jnp.int32, z.shape, 0) + r0
                z = jnp.where(jnp.logical_and(index >= skip, index < skip + vocab), z, -jnp.inf)
            top = jnp.max(z, axis=0, keepdims=True)
            stats.append((top, jnp.sum(jnp.exp(z - top), axis=0, keepdims=True)))
        top = functools.reduce(jnp.maximum, [t for t, _ in stats])
        st_scr[0:1, rows(j, quarter)] = top
        st_scr[1:2, rows(j, quarter)] = sum(t * jnp.exp(m - top) for m, t in stats)

        @pl.when(k < ys - 2)
        def _():
            collect(nearest(k + 2))
        return carry

    mark("d1coll")
    for k in range(min(2, ys)):
        collect(nearest(k))
    mark("d1e")
    e_own().wait()
    arrived(e_buf.at[:, most], e_recv)

    mark("d3head")
    lax.fori_loop(0, ys, head, 0)

    mark("d4stat")
    def s_start(i, carry):
        pltpu.make_async_remote_copy(
            src_ref=st_scr, dst_ref=s_buf.at[mine], send_sem=s_sem.at[0], recv_sem=s_sem.at[1],
            device_id={"yax": lax.rem(y + i // xs, ys), "xax": lax.rem(x + lax.rem(i, xs), xs)},
            device_id_type=pl.DeviceIdType.MESH).start()
        return carry
    lax.fori_loop(1, ys * xs, s_start, 0)
    s_buf[mine] = st_scr[...]

    mark("d5sx")
    arrived(e_buf.at[:, most], e_send)
    arrived(f_buf.at[pl.ds(0, 2 * (ys * chips - 1) * piece), :], f_sem.at[0])
    arrived(f_buf.at[pl.ds(0, ys * chips * own), :], f_sem.at[1])
    arrived(z_scr, z_sem.at[2])
    everyone = s_buf.at[pl.ds(0, ys * xs - 1)]
    mark("d6sw")
    arrived(everyone, s_sem.at[1])
    tops = s_buf[:, 0, :]
    best = jnp.max(tops, axis=0, keepdims=True)
    whole = jnp.sum(s_buf[:, 1, :] * jnp.exp(tops - best), axis=0, keepdims=True)
    mark("d9n")
    norm_scr[...] = best + jnp.log(whole)
    norm_copy = pltpu.make_async_copy(norm_scr, norm_out, z_sem.at[0])
    norm_copy.start()
    arrived(everyone, s_sem.at[0])
    norm_copy.wait()
    mark(None)


def finish_kernel(shift, z_hbm, norm, key, value, out_hbm, k_out, v_out, norm_out,
                  z_buf, o_buf, in_sem, out_sem):
    count, n, width = o_buf.shape

    def load(i):
        return pltpu.make_async_copy(z_hbm.at[:, pl.ds(i * width, width)], z_buf.at[i], in_sem.at[i])

    def save(i):
        return pltpu.make_async_copy(o_buf.at[i], out_hbm.at[:, pl.ds(i * width, width)], out_sem.at[i])

    for i in range(count):
        load(i).start()
    k_out[...] = key[...]
    v_out[...] = value[...]
    norm_out[...] = norm[...]
    odd = lax.rem(lax.axis_index("xax"), 2) == 1
    for i in range(count):
        row = norm[:, pl.ds(i * width, width)]
        load(i).wait()
        if shift:
            @pl.when(odd)
            def _():
                o_buf[i] = z_buf[i, pl.ds(shift, n), :] - row

            @pl.when(jnp.logical_not(odd))
            def _():
                o_buf[i] = z_buf[i, pl.ds(0, n), :] - row
        else:
            o_buf[i] = z_buf[i] - row
        save(i).start()
    for i in range(count):
        save(i).wait()


def solution(mesh):
    ys = mesh.shape["yax"]
    xs = mesh.shape["xax"]
    row_spec = P(("dp", "yax", "xax"))

    def local_step(hidden, cache_len, k_cache, v_cache, g_attn, w_query, w_key, w_value,
                   w_gate, w_up, w_out, w_down, g_final, embedding):
        batch, blk = hidden.shape
        own, slots, head_dim = k_cache.shape
        width = blk * xs
        vocab = embedding.shape[0] // xs
        shift = vocab % 8
        window = -(-vocab // 8) * 8
        half = head_dim // 2
        quarter = xs * own
        cols = w_query.shape[1] // xs
        ff = w_gate.shape[1] // xs
        heads = w_query.shape[1] * ys // head_dim
        per = 4
        groups = own // per
        freq_row = (ROPE_BASE ** (-(np.arange(half, dtype=np.float32) * 2.0) / head_dim)).astype(np.float32)
        freq = jnp.asarray(np.tile(freq_row, 4)[None, :])
        any_spec = pl.BlockSpec(memory_space=pl.ANY)
        vmem = pl.BlockSpec(memory_space=pltpu.VMEM)
        smem = pl.BlockSpec(memory_space=pltpu.SMEM)
        dma = pltpu.SemaphoreType.DMA
        chips = xs // 2
        scratch = [
            pltpu.VMEM((groups, per, head_dim, slots), BF16),
            pltpu.VMEM((groups, per, head_dim, slots), BF16),
            pltpu.VMEM((quarter, width), BF16),
            pltpu.VMEM((1, width), F32),
            pltpu.VMEM((1, width), F32),
            pltpu.VMEM((w_query.shape[1], blk), BF16),
            pltpu.VMEM((ys, cols, width), BF16),
            pltpu.VMEM((width, 2 * ff), BF16),
            pltpu.VMEM((ys, ff, width), BF16),
            pltpu.VMEM((ys, cols, width), BF16),
            pltpu.VMEM((2 * head_dim, width), BF16),
            pltpu.VMEM((batch, width), BF16),
            pltpu.VMEM((quarter, ys * cols), BF16),
            pltpu.VMEM((xs, own, ys * cols), BF16),
            pltpu.VMEM((own * heads, head_dim), F32),
            pltpu.VMEM((own * heads, 1), F32),
            pltpu.VMEM((own * heads, head_dim), F32),
            pltpu.VMEM((own * heads, head_dim), F32),
            pltpu.VMEM((per * heads, slots), F32),
            pltpu.VMEM((own * heads, head_dim), F32),
            pltpu.VMEM((xs, own, ys * cols), BF16),
            pltpu.VMEM((quarter, ys * cols), BF16),
            pltpu.VMEM((ys, quarter, ff), BF16),
            pltpu.VMEM((quarter, ys * ff), BF16),
            pltpu.VMEM((quarter, width), F32),
            pltpu.VMEM((chips, own, width), F32),
            pltpu.VMEM((2, chips, own, width), F32),
            pltpu.VMEM((chips, own, width), F32),
            pltpu.VMEM((batch, width), BF16),
            pltpu.VMEM((window, width), BF16),
            pltpu.VMEM((ys, window, quarter), F32),
            pltpu.VMEM((2, batch), F32),
            pltpu.VMEM((own, head_dim), BF16),
            pltpu.VMEM((own, head_dim), BF16),
            pltpu.VMEM((1, batch), F32),
            pltpu.VMEM((ys * xs, 2, batch), F32),
            dma((2, groups)), dma, dma((3,)), dma((7,)), dma((7,)),
            dma((5,)), dma((5, chips)), dma((5,)), dma((4,)), dma((4,)), dma, dma,
            dma((ys,)), dma((ys,)), dma((2,)), dma((2,)), dma((2,)),
            dma((chips,)), dma((ys,)), dma((ys, chips)), dma((ys, chips)), dma((2 + ys,)), dma((2,)),
        ]
        cfg = (ys, xs, own, vocab, shift)
        key_new, value_new, logits, norm = pl.pallas_call(
            functools.partial(kernel, cfg),
            name="decode_layer",
            out_shape=(
                jax.ShapeDtypeStruct((own, head_dim), BF16),
                jax.ShapeDtypeStruct((own, head_dim), BF16),
                jax.ShapeDtypeStruct((window, batch), F32),
                jax.ShapeDtypeStruct((1, batch), F32)),
            in_specs=[smem, any_spec, any_spec, any_spec, any_spec, any_spec, vmem] + [any_spec] * 7 + [vmem],
            out_specs=(any_spec, any_spec, any_spec, any_spec),
            scratch_shapes=scratch,
            compiler_params=pltpu.CompilerParams(
                collective_id=0, has_side_effects=True, vmem_limit_bytes=67043328),
        )(cache_len, hidden, k_cache.transpose(0, 2, 1), v_cache.transpose(0, 2, 1),
          g_attn[None, :], g_final[None, :], w_query, w_key.T, w_value.T, w_gate, w_up, w_out, w_down,
          embedding, freq)
        count = 8
        log_probs, key_new, value_new, norm = pl.pallas_call(
            functools.partial(finish_kernel, shift),
            name="finish",
            out_shape=(
                jax.ShapeDtypeStruct((vocab, batch), F32),
                jax.ShapeDtypeStruct((own, head_dim), BF16),
                jax.ShapeDtypeStruct((own, head_dim), BF16),
                jax.ShapeDtypeStruct((1, batch), F32)),
            in_specs=[any_spec, vmem, vmem, vmem],
            out_specs=(any_spec, vmem, vmem, vmem),
            scratch_shapes=[
                pltpu.VMEM((count, window, batch // count), F32),
                pltpu.VMEM((count, vocab, batch // count), F32),
                dma((count,)), dma((count,))],
        )(logits, norm, key_new, value_new)
        return key_new, value_new, log_probs.T, norm[0]

    in_specs = (P("dp", "xax"), P("dp"), row_spec, row_spec, P("xax"), P("xax", "yax"),
                P("xax", None), P("xax", None), P("xax", "yax"), P("xax", "yax"),
                P("yax", "xax"), P("yax", "xax"), P("xax"), P("yax", "xax"))
    out_specs = (row_spec, row_spec, P("dp", ("yax", "xax")), P("dp"))
    return jax.shard_map(local_step, mesh=mesh, in_specs=in_specs, out_specs=out_specs, check_vma=False)
```

```python
import functools

import jax
import jax.numpy as jnp
import numpy as np
from jax import lax
from jax.experimental import pallas as pl
from jax.experimental.pallas import tpu as pltpu
from jax.sharding import PartitionSpec as P

EPS = 1e-6
ROPE_BASE = 10000.0
F32 = jnp.float32
BF16 = jnp.bfloat16
NT = (((1,), (1,)), ((), ()))
EMBED_CHUNKS = 16
EMBED_FIRST = 13


def layer_norm(values_in, gain):
    mean = jnp.mean(values_in, axis=-1, keepdims=True)
    centred = values_in - mean
    var = jnp.mean(centred * centred, axis=-1, keepdims=True)
    return centred * lax.rsqrt(var + EPS) * gain


def row_chunks(total, count):
    cuts = [16 * (total // 16 * i // count) for i in range(count)] + [total]
    return [(cuts[i], cuts[i + 1] - cuts[i]) for i in range(count)]


class Marker:
    def __init__(self):
        self.scope = None

    def __call__(self, name):
        if self.scope is not None:
            self.scope.__exit__(None, None, None)
        self.scope = None
        if name:
            self.scope = jax.named_scope(name)
            self.scope.__enter__()


def kernel(cfg, lens, hidden, k_hbm, v_hbm, g_attn, g_final, w_query, w_key, w_value, w_gate, w_up,
           w_out, w_down, embed, freq,
           k_out, v_out, logits_out, norm_out,
           k_buf, v_buf, h_buf, ga_buf, gf_buf, wqt, wq_buf, gu_buf, down_buf, out_buf, kv_buf,
           n_all, q_scr, qx_buf, q2d, snew, krep, vrep, s_scr, od_scr, o_scr, ox_buf, act_scr, act, part_scr,
           pre_buf, rs_scr, rs_buf, f_buf, e_buf, z_scr, st_scr, k_scr, v_scr, norm_scr, s_buf,
           kv_sem, e_own_sem, z_sem, x_send, x_recv, g_send, g_recv, g_last, y_send, y_recv, e_send, e_recv,
           n_recv, n_last, n_send, pre_sem, rs_sem, fxa, fyb, fya, fxb, f_sem, s_sem):
    ys, xs, own, vocab, shift = cfg
    mark = Marker()
    y = lax.axis_index("yax")
    x = lax.axis_index("xax")
    core = lax.rem(x, 2)
    partner = x + 1 - 2 * core
    blk = hidden.shape[1]
    quarter = xs * own
    head_dim = k_hbm.shape[1]
    half = head_dim // 2
    seqs = k_hbm.shape[0]
    slots = k_hbm.shape[2]
    heads = w_query.shape[1] * ys // head_dim
    groups = k_buf.shape[0]
    per = seqs // groups
    window = e_buf.shape[0]

    def lanes(i):
        return pl.ds(pl.multiple_of(i * blk, 128), blk)

    def rows(i, n):
        return pl.ds(pl.multiple_of(i * n, n), n)

    mark("a0start")
    barrier = pltpu.get_barrier_semaphore()

    def signal_row(d, carry):
        pl.semaphore_signal(barrier, inc=1, device_id={"xax": lax.rem(x + d, xs)},
                            device_id_type=pl.DeviceIdType.MESH)
        return carry
    lax.fori_loop(1, xs, signal_row, 0)

    def signal_column(d, carry):
        pl.semaphore_signal(barrier, inc=1, device_id={"yax": lax.rem(y + d, ys)},
                            device_id_type=pl.DeviceIdType.MESH)
        return carry
    lax.fori_loop(1, ys, signal_column, 0)
    def cache_copy(g, src, dst, s):
        return pltpu.make_async_copy(src.at[pl.ds(g * per, per)], dst.at[g], kv_sem.at[s, g])

    def start_cache(g, carry):
        cache_copy(g, k_hbm, k_buf, 0).start()
        return carry
    lax.fori_loop(0, groups, start_cache, 0)

    wqt[...] = w_query[...].astype(F32).T.astype(BF16)

    mark("a0wait")
    pl.semaphore_wait(barrier, xs + ys - 2)

    def arrived(ref, sem):
        pltpu.make_async_copy(ref, ref, sem).wait()

    cols = wqt.shape[0] // xs
    ff = w_gate.shape[1] // xs
    most = pl.ds(0, (xs - 1) * blk)
    x_kinds = {
        "wq": (lambda p: wqt.at[rows(p, cols), :], lambda s: wq_buf.at[y, :, lanes(s)],
               wq_buf.at[y], wq_buf.at[y, :, most]),
        "wo": (lambda p: w_out.at[rows(p, cols), :], lambda s: out_buf.at[y, :, lanes(s)],
               out_buf.at[y], out_buf.at[y, :, most]),
        "down": (lambda p: w_down.at[rows(p, ff), :], lambda s: down_buf.at[y, :, lanes(s)],
                 down_buf.at[y], down_buf.at[y, :, most]),
        "gate": (lambda p: w_gate.at[:, lanes(p)], lambda s: gu_buf.at[rows(s, blk), pl.ds(0, ff)],
                 gu_buf.at[:, pl.ds(0, ff)], gu_buf.at[most, pl.ds(0, ff)]),
        "up": (lambda p: w_up.at[:, lanes(p)], lambda s: gu_buf.at[rows(s, blk), pl.ds(ff, ff)],
               gu_buf.at[:, pl.ds(ff, ff)], gu_buf.at[most, pl.ds(ff, ff)]),
        "q": (lambda p: q_scr.at[rows(p, own), :], lambda s: qx_buf.at[s],
              qx_buf, qx_buf.at[pl.ds(0, xs - 1)]),
        "o": (lambda p: o_scr.at[p], lambda s: ox_buf.at[rows(s, own), :],
              ox_buf, ox_buf.at[pl.ds(0, (xs - 1) * own), :]),
    }
    x_index = {name: i for i, name in enumerate(x_kinds)}

    def x_start(name):
        src, dst = x_kinds[name][:2]
        k = x_index[name]

        def body(d, carry):
            p = lax.rem(x + d, xs)
            pltpu.make_async_remote_copy(
                src_ref=src(p), dst_ref=dst(x), send_sem=x_send.at[k], recv_sem=x_recv.at[k],
                device_id={"xax": p}, device_id_type=pl.DeviceIdType.MESH).start()
            return carry
        lax.fori_loop(1, xs, body, 0)
        pltpu.make_async_copy(src(x), dst(x), x_recv.at[k]).start()

    def x_wait(name):
        arrived(x_kinds[name][2], x_recv.at[x_index[name]])

    def x_drain(name):
        arrived(x_kinds[name][3], x_send.at[x_index[name]])

    chips = xs // 2
    g_kinds = {
        "hidden": (hidden.at[rows(y, quarter), :], lambda s: h_buf.at[:, lanes(s)], h_buf),
        "ga": (g_attn, lambda s: ga_buf.at[:, lanes(s)], ga_buf),
        "gf": (g_final, lambda s: gf_buf.at[:, lanes(s)], gf_buf),
        "wk": (w_key, lambda s: kv_buf.at[pl.ds(0, head_dim), lanes(s)], kv_buf.at[pl.ds(0, head_dim), :]),
        "wv": (w_value, lambda s: kv_buf.at[pl.ds(head_dim, head_dim), lanes(s)],
               kv_buf.at[pl.ds(head_dim, head_dim), :]),
    }
    g_index = {name: i for i, name in enumerate(g_kinds)}

    def g_copy(name, i, sender):
        src, dst, _ = g_kinds[name]
        k = g_index[name]
        return pltpu.make_async_remote_copy(
            src_ref=src, dst_ref=dst(sender), send_sem=g_send.at[k], recv_sem=g_recv.at[k, i],
            device_id={"xax": lax.rem(x + 2 * i, xs)}, device_id_type=pl.DeviceIdType.MESH)

    def g_pass(name, sender, source):
        k = g_index[name]
        return pltpu.make_async_remote_copy(
            src_ref=source, dst_ref=g_kinds[name][1](sender), send_sem=g_send.at[k], recv_sem=g_last.at[k],
            device_id={"xax": partner}, device_id_type=pl.DeviceIdType.MESH)

    def g_start(name):
        def body(i, carry):
            g_copy(name, i, x).start()
            return carry
        lax.fori_loop(1, chips, body, 0)
        src, dst, _ = g_kinds[name]
        g_pass(name, x, src).start()
        pltpu.make_async_copy(src, dst(x), g_last.at[g_index[name]]).start()

    def g_forward(name):
        def body(i, carry):
            sender = lax.rem(x + xs - 2 * i, xs)
            g_copy(name, i, sender).wait_recv()
            g_pass(name, sender, g_kinds[name][1](sender)).start()
            return carry
        lax.fori_loop(1, chips, body, 0)

    def g_wait(name):
        whole = g_kinds[name][2]
        arrived(whole.at[:, pl.ds(0, (chips + 1) * blk)], g_last.at[g_index[name]])

    def g_drain(name):
        arrived(g_kinds[name][2].at[:, most], g_send.at[g_index[name]])

    y_kinds = {"wq": wq_buf, "wo": out_buf, "down": down_buf}
    y_index = {name: i for i, name in enumerate(y_kinds)}
    others = pl.ds(0, ys - 1)

    def y_start(name):
        buf = y_kinds[name]
        k = y_index[name]

        def body(d, carry):
            pltpu.make_async_remote_copy(
                src_ref=buf.at[y], dst_ref=buf.at[y], send_sem=y_send.at[k], recv_sem=y_recv.at[k],
                device_id={"yax": lax.rem(y + d, ys)}, device_id_type=pl.DeviceIdType.MESH).start()
            return carry
        lax.fori_loop(1, ys, body, 0)

    def y_wait(name):
        arrived(y_kinds[name].at[others], y_recv.at[y_index[name]])

    def y_drain(name):
        arrived(y_kinds[name].at[others], y_send.at[y_index[name]])

    e_parts = row_chunks(window, EMBED_CHUNKS)

    def e_first(p):
        return p * vocab - lax.rem(p, 2) * shift

    def e_own():
        return pltpu.make_async_copy(
            embed.at[pl.ds(pl.multiple_of(e_first(x), 8), window), :], e_buf.at[:, lanes(x)], e_own_sem)

    def e_start(c):
        r0, n = e_parts[c]

        def body(d, carry):
            p = lax.rem(x + d, xs)
            pltpu.make_async_remote_copy(
                src_ref=embed.at[pl.ds(pl.multiple_of(e_first(p) + r0, 8), n), :],
                dst_ref=e_buf.at[pl.ds(r0, n), lanes(x)], send_sem=e_send,
                recv_sem=e_recv.at[int(c >= EMBED_FIRST)],
                device_id={"xax": p}, device_id_type=pl.DeviceIdType.MESH).start()
            return carry
        lax.fori_loop(1, xs, body, 0)

    mark("a1send")
    x_start("wq")
    for name in ("hidden", "ga"):
        g_start(name)
    for name in ("wo", "down"):
        x_start(name)
    for name in ("wk", "wv", "gf"):
        g_start(name)
    e_start(0)
    e_own().start()

    def start_cache_v(g, carry):
        cache_copy(g, v_hbm, v_buf, 1).start()
        return carry
    lax.fori_loop(0, groups, start_cache_v, 0)

    mark("a2wqx")
    x_wait("wq")
    y_start("wq")
    mark("a3hfwd")
    for name in ("hidden", "ga"):
        g_forward(name)
    mark("a4hwait")
    for name in ("hidden", "ga"):
        g_wait(name)
    mark("a5ln")
    my_rows = rows(y, quarter)
    n_all[my_rows, :] = layer_norm(h_buf[...].astype(F32), ga_buf[...]).astype(BF16)

    part = quarter // 2

    def n_rows(j, c):
        return pl.ds(pl.multiple_of(j * quarter + c * part, part), part)

    def n_copy(d, sender):
        r = n_rows(sender, core)
        return pltpu.make_async_remote_copy(
            src_ref=n_all.at[r, :], dst_ref=n_all.at[r, :], send_sem=n_send.at[0],
            recv_sem=n_recv.at[d], device_id={"yax": lax.rem(y + d, ys)},
            device_id_type=pl.DeviceIdType.MESH)

    def n_pass(d, c):
        r = n_rows(lax.rem(y + ys - d, ys), c)
        return pltpu.make_async_remote_copy(
            src_ref=n_all.at[r, :], dst_ref=n_all.at[r, :], send_sem=n_send.at[1],
            recv_sem=n_last.at[d], device_id={"xax": partner},
            device_id_type=pl.DeviceIdType.MESH)

    mark("a6wo")
    x_wait("wo")
    y_start("wo")
    mark("a6wqy")
    y_wait("wq")
    mark("a7q")
    wq_all = wq_buf[...].reshape(ys * cols, xs * blk)
    q_scr[...] = lax.dot_general(n_all[my_rows, :], wq_all, NT, preferred_element_type=F32).astype(BF16)
    mark("a8send")
    x_start("q")
    x_start("gate")
    x_start("up")

    def n_start(d, carry):
        n_copy(d, y).start()
        return carry
    lax.fori_loop(1, ys, n_start, 0)
    mark("b0down")
    x_wait("down")
    y_start("down")
    for c in range(1, 7):
        e_start(c)

    mark("b1kv")
    row_id = lax.broadcasted_iota(jnp.int32, (own, 4 * half), 0)
    first_row = (y * xs + x) * own
    position = jnp.zeros((own, 4 * half), jnp.int32)
    for b in range(own):
        position = jnp.where(row_id == b, lens[first_row + b], position)
    angle = position.astype(F32) * freq[...]
    cos_a = jnp.cos(angle)
    sin_a = jnp.sin(angle)
    for name in ("wk", "wv", "gf"):
        g_forward(name)
    for name in ("wk", "wv", "gf"):
        g_wait(name)
    mine = y * xs + x
    n_own = n_all[rows(mine, own), :]
    kv = lax.dot_general(n_own, kv_buf[...], NT, preferred_element_type=F32).astype(BF16).astype(F32)
    k1 = kv[:, :half]
    k2 = kv[:, half:head_dim]
    c1 = cos_a[:, :half]
    s1 = sin_a[:, :half]
    key = jnp.concatenate([k1 * c1 - k2 * s1, k2 * c1 + k1 * s1], axis=1).astype(BF16)
    value = kv[:, head_dim:].astype(BF16)
    k_scr[...] = key
    v_scr[...] = value
    small_outs = [pltpu.make_async_copy(k_scr, k_out, z_sem.at[0]),
                  pltpu.make_async_copy(v_scr, v_out, z_sem.at[1])]
    for copy in small_outs:
        copy.start()
    for h in range(heads):
        krep[pl.ds(h, own, stride=heads), :] = key.astype(F32)
        vrep[pl.ds(h, own, stride=heads), :] = value.astype(F32)

    mark("b2q")
    x_wait("q")
    mark("b3rot")
    for xc in range(xs // 2):
        qa = qx_buf[2 * xc].astype(F32)
        qb = qx_buf[2 * xc + 1].astype(F32)
        ra = (qa * cos_a - qb * sin_a).astype(BF16).astype(F32)
        rb = (qb * cos_a + qa * sin_a).astype(BF16).astype(F32)
        for yc in range(ys):
            pair = jnp.concatenate([ra[:, yc * half:(yc + 1) * half], rb[:, yc * half:(yc + 1) * half]], axis=1)
            q2d[pl.ds(xc * ys + yc, own, stride=heads), :] = pair
    scale = head_dim ** -0.5
    snew[...] = jnp.sum(q2d[...] * krep[...], axis=1, keepdims=True) * scale

    mark("b4attn")
    gr = per * heads
    seg_r = lax.broadcasted_iota(jnp.int32, (gr, per * head_dim), 0) // heads
    seg_c = lax.broadcasted_iota(jnp.int32, (gr, per * head_dim), 1) // head_dim
    diag = (seg_r == seg_c).astype(F32)
    tile = min(512, slots)
    row_g = lax.broadcasted_iota(jnp.int32, (gr, 1), 0) // heads
    lane_g = lax.broadcasted_iota(jnp.int32, (gr, tile), 1)

    def attend(g, carry):
        cache_copy(g, k_hbm, k_buf, 0).wait()
        qg = q2d[rows(g, gr), :]
        qbd = (jnp.concatenate([qg] * per, axis=1) * diag).astype(BF16)
        len_g = jnp.zeros((gr, 1), jnp.int32)
        for s in range(per):
            len_g = jnp.where(row_g == s, lens[first_row + g * per + s], len_g)
        new = snew[rows(g, gr), :]
        top = jnp.full((gr, tile), -jnp.inf, F32)
        kg = k_buf.at[g]
        vg = v_buf.at[g]
        for c in range(slots // tile):
            kc = kg[:, :, pl.ds(c * tile, tile)].reshape(per * head_dim, tile)
            sc = jnp.dot(qbd, kc, preferred_element_type=F32) * scale
            sc = jnp.where(lane_g < len_g - c * tile, sc, -jnp.inf)
            s_scr[:, pl.ds(c * tile, tile)] = sc
            top = jnp.maximum(top, sc)
        row_max = jnp.maximum(jnp.max(top, axis=1, keepdims=True), new)
        total = jnp.zeros((gr, tile), F32)
        for c in range(slots // tile):
            ex = jnp.exp(s_scr[:, pl.ds(c * tile, tile)] - row_max)
            s_scr[:, pl.ds(c * tile, tile)] = ex
            total = total + ex
        w_new = jnp.exp(new - row_max)
        den = jnp.sum(total, axis=1, keepdims=True) + w_new
        inv = 1.0 / den
        cache_copy(g, v_hbm, v_buf, 1).wait()
        mixed = jnp.zeros((gr, per * head_dim), F32)
        for c in range(slots // tile):
            pr = (s_scr[:, pl.ds(c * tile, tile)] * inv).astype(BF16)
            vc = vg[:, :, pl.ds(c * tile, tile)].reshape(per * head_dim, tile)
            mixed = mixed + lax.dot_general(pr, vc, NT, preferred_element_type=F32)
        add = (w_new * inv).astype(BF16).astype(F32) * vrep[rows(g, gr), :]
        for s in range(per):
            od_scr[pl.ds(pl.multiple_of(g * gr + s * heads, heads), heads), :] = (
                mixed[s * heads:(s + 1) * heads, s * head_dim:(s + 1) * head_dim]
                + add[s * heads:(s + 1) * heads, :])
        return carry

    lax.fori_loop(0, groups, attend, 0)
    mark("b5o")
    for xc in range(xs // 2):
        parts = [od_scr[pl.ds(xc * ys + yc, own, stride=heads), :] for yc in range(ys)]
        o_scr[2 * xc] = jnp.concatenate([p[:, :half] for p in parts], axis=1).astype(BF16)
        o_scr[2 * xc + 1] = jnp.concatenate([p[:, half:] for p in parts], axis=1).astype(BF16)
    x_start("o")
    for c in range(7, 12):
        e_start(c)

    def act_copy(dest):
        return pltpu.make_async_remote_copy(
            src_ref=act_scr.at[dest], dst_ref=act.at[:, pl.ds(pl.multiple_of(y * ff, ff), ff)],
            send_sem=y_send.at[len(y_kinds)], recv_sem=y_recv.at[len(y_kinds)],
            device_id={"yax": dest}, device_id_type=pl.DeviceIdType.MESH)

    mark("b6gu")
    x_wait("gate")
    x_wait("up")

    mark("b7feed")
    def feed(d, carry):
        @pl.when(d < ys - 1)
        def _():
            n_copy(d + 1, lax.rem(y + ys - d - 1, ys)).wait_recv()
            n_pass(d + 1, core).start()
        j = lax.rem(y + ys - d, ys)

        @pl.when(d > 0)
        def _():
            n_pass(d, 1 - core).wait_recv()
        gu = jnp.dot(n_all[rows(j, quarter), :], gu_buf[...], preferred_element_type=F32)
        gu = gu.astype(BF16).astype(F32)
        gate = gu[:, :ff]
        act_scr[j] = (gate * jax.nn.sigmoid(gate) * gu[:, ff:]).astype(BF16)

        @pl.when(d > 0)
        def _():
            act_copy(j).start()
        return carry
    lax.fori_loop(0, ys, feed, 0)
    act[:, pl.ds(pl.multiple_of(y * ff, ff), ff)] = act_scr[y]
    mark("b8wo")
    y_wait("wo")
    mark("b9o")
    x_wait("o")
    mark("c0op")
    part_scr[...] = jnp.dot(
        ox_buf[...], out_buf[...].reshape(ys * cols, xs * blk), preferred_element_type=F32)
    mark("c1down")
    y_wait("down")

    mark("c2act")
    arrived(act_scr.at[others], y_recv.at[len(y_kinds)])

    mark("c3branch")
    down_all = down_buf[...].reshape(ys * ff, xs * blk)
    part_scr[...] = part_scr[...] + jnp.dot(act[...], down_all, preferred_element_type=F32)

    def branch(c):
        for i in range(chips):
            rs_scr[c, i] = part_scr[pl.ds(pl.multiple_of((2 * i + c) * own, own), own), :]

    def pre_copy():
        return pltpu.make_async_remote_copy(
            src_ref=rs_scr.at[1 - core], dst_ref=pre_buf, send_sem=pre_sem.at[0], recv_sem=pre_sem.at[1],
            device_id={"xax": partner}, device_id_type=pl.DeviceIdType.MESH)

    def rs_copy(dest):
        return pltpu.make_async_remote_copy(
            src_ref=rs_scr.at[core, dest], dst_ref=rs_buf.at[chip], send_sem=rs_sem.at[0],
            recv_sem=rs_sem.at[1], device_id={"xax": 2 * dest + core},
            device_id_type=pl.DeviceIdType.MESH)

    chip = x // 2
    branch(1 - core)
    pre_copy().start()
    branch(core)
    mark("c4pre")
    pre_copy().wait_recv()
    rs_scr[core] = rs_scr[core] + pre_buf[...]

    mark("c5rs")
    def rs_start(i, carry):
        rs_copy(lax.rem(chip + i, chips)).start()
        return carry
    lax.fori_loop(1, chips, rs_start, 0)
    mark("c6rsw")
    arrived(rs_buf.at[pl.ds(0, chips - 1)], rs_sem.at[1])
    mark("c7ln")
    rs_buf[chip] = rs_scr[core, chip]
    res = h_buf[rows(x, own), :].astype(F32) + jnp.sum(rs_buf[...], axis=0)
    f_buf[rows(mine, own), :] = layer_norm(res, gf_buf[...]).astype(BF16)

    piece = own // 2

    def f_half(sy, sx, h):
        return f_buf.at[pl.ds(pl.multiple_of((sy * xs + sx) * own + h * piece, piece), piece), :]

    def f_over_x(i, h, sy, sx, sem):
        return pltpu.make_async_remote_copy(
            src_ref=f_half(sy, sx, h), dst_ref=f_half(sy, sx, h), send_sem=f_sem.at[0], recv_sem=sem,
            device_id={"xax": lax.rem(x + 2 * i, xs)}, device_id_type=pl.DeviceIdType.MESH)

    def f_over_y(d, h, sy, sx, sem):
        return pltpu.make_async_remote_copy(
            src_ref=f_half(sy, sx, h), dst_ref=f_half(sy, sx, h), send_sem=f_sem.at[0], recv_sem=sem,
            device_id={"yax": lax.rem(y + d, ys)}, device_id_type=pl.DeviceIdType.MESH)

    def f_pass(d, h, sy, sx):
        pltpu.make_async_remote_copy(
            src_ref=f_half(sy, sx, h), dst_ref=f_half(sy, sx, h), send_sem=f_sem.at[1],
            recv_sem=f_sem.at[2 + d], device_id={"xax": partner},
            device_id_type=pl.DeviceIdType.MESH).start()

    def from_y(d):
        return lax.rem(y + ys - d, ys)

    def from_x(i):
        return lax.rem(x + xs - 2 * i, xs)

    def spread_y(i):
        def body(d, carry):
            f_over_y(d, 0, y, from_x(i), fya.at[d, i]).start()
            return carry
        lax.fori_loop(1, ys, body, 0)

    def spread_x(d):
        def body(i, carry):
            f_over_x(i, 1, from_y(d), x, fxb.at[d, i]).start()
            return carry
        lax.fori_loop(1, chips, body, 0)

    mark("c8fx")
    def first_x(i, carry):
        f_over_x(i, 0, y, x, fxa.at[i]).start()
        return carry
    lax.fori_loop(1, chips, first_x, 0)

    def first_y(d, carry):
        f_over_y(d, 1, y, x, fyb.at[d]).start()
        return carry
    lax.fori_loop(1, ys, first_y, 0)
    spread_y(0)
    spread_x(0)
    f_pass(0, 0, y, x)
    f_pass(0, 1, y, x)
    e_start(12)
    mark("c9sp")
    for i in range(1, max(chips, ys)):
        if i < chips:
            f_over_x(i, 0, y, from_x(i), fxa.at[i]).wait_recv()
            spread_y(i)
            f_pass(0, 0, y, from_x(i))
        if i < ys:
            f_over_y(i, 1, from_y(i), x, fyb.at[i]).wait_recv()
            spread_x(i)
            f_pass(i, 1, from_y(i), x)
    for c in range(13, EMBED_CHUNKS):
        e_start(c)

    def collect(d):
        def body(i, carry):
            @pl.when(d > 0)
            def _():
                f_over_y(d, 0, from_y(d), from_x(i), fya.at[d, i]).wait_recv()
                f_pass(d, 0, from_y(d), from_x(i))

            @pl.when(i > 0)
            def _():
                f_over_x(i, 1, from_y(d), from_x(i), fxb.at[d, i]).wait_recv()
                f_pass(d, 1, from_y(d), from_x(i))
            return carry
        lax.fori_loop(0, chips, body, 0)

    mark("d0drain")
    for name in x_kinds:
        x_drain(name)
    for name in g_kinds:
        g_drain(name)
    for name in y_kinds:
        y_drain(name)
    arrived(act_scr.at[others], y_send.at[len(y_kinds)])
    for i in range(2):
        arrived(n_all.at[pl.ds(0, (ys - 1) * part), :], n_send.at[i])
    pre_copy().wait_send()
    arrived(rs_buf.at[pl.ds(0, chips - 1)], rs_sem.at[0])
    for copy in small_outs:
        copy.wait()

    cut = e_parts[EMBED_FIRST][0]
    skip = core * shift
    half_block = pl.ds(0, chips * own)

    def nearest(k):
        return k + k // 2 * (1 - 2 * lax.rem(k, 2))

    def z_copy(j, r0, n):
        return pltpu.make_async_copy(
            z_scr.at[j, pl.ds(r0, n), :], logits_out.at[pl.ds(r0, n), rows(j, quarter)], z_sem.at[2])

    def block(j, r0, n, pieces):
        r = pl.ds(r0, n)
        z_scr[j, r, :] = lax.dot_general(e_buf[r, :], f_buf[rows(j, quarter), :], NT, preferred_element_type=F32)
        z_copy(j, r0, n).start()
        stats = []
        for q0, m in row_chunks(n, pieces):
            z = z_scr[j, pl.ds(r0 + q0, m), :]
            if shift and (r0 + q0 == 0 or r0 + q0 + m == window):
                index = lax.broadcasted_iota(jnp.int32, z.shape, 0) + (r0 + q0)
                z = jnp.where(jnp.logical_and(index >= skip, index < skip + vocab), z, -jnp.inf)
            top = jnp.max(z, axis=0, keepdims=True)
            stats.append((top, jnp.sum(jnp.exp(z - top), axis=0, keepdims=True)))
        return stats

    def put(j, stats):
        top = functools.reduce(jnp.maximum, [t for t, _ in stats])
        st_scr[0:1, rows(j, quarter)] = top
        st_scr[1:2, rows(j, quarter)] = sum(t * jnp.exp(m - top) for m, t in stats)

    def head(k, carry):
        d = nearest(k)
        j = from_y(d)
        with jax.named_scope('hw'):
            arrived(f_buf.at[half_block, :], f_sem.at[2 + d])
        put(j, block(j, 0, cut, 4))

        @pl.when(k < ys - 2)
        def _():
            collect(nearest(k + 2))
        return carry

    def head_rest(j, carry):
        before = (st_scr[0:1, rows(j, quarter)], st_scr[1:2, rows(j, quarter)])
        put(j, [before] + block(j, cut, window - cut, 1))
        return carry

    mark("d1coll")
    for k in range(min(2, ys)):
        collect(nearest(k))
    mark("d1e")
    e_own().wait()
    arrived(e_buf.at[pl.ds(0, cut), most], e_recv.at[0])

    mark("d3head")
    lax.fori_loop(0, ys, head, 0)
    mark("d3rest")
    arrived(e_buf.at[pl.ds(cut, window - cut), most], e_recv.at[1])
    mark("d3hr")
    lax.fori_loop(0, ys, head_rest, 0)

    mark("d4stat")
    def s_start(i, carry):
        pltpu.make_async_remote_copy(
            src_ref=st_scr, dst_ref=s_buf.at[mine], send_sem=s_sem.at[0], recv_sem=s_sem.at[1],
            device_id={"yax": lax.rem(y + i // xs, ys), "xax": lax.rem(x + lax.rem(i, xs), xs)},
            device_id_type=pl.DeviceIdType.MESH).start()
        return carry
    lax.fori_loop(1, ys * xs, s_start, 0)
    s_buf[mine] = st_scr[...]

    mark("d5sx")
    arrived(e_buf.at[:, most], e_send)
    arrived(f_buf.at[pl.ds(0, 2 * (ys * chips - 1) * piece), :], f_sem.at[0])
    arrived(f_buf.at[pl.ds(0, ys * chips * own), :], f_sem.at[1])
    arrived(z_scr, z_sem.at[2])
    everyone = s_buf.at[pl.ds(0, ys * xs - 1)]
    mark("d6sw")
    arrived(everyone, s_sem.at[1])
    tops = s_buf[:, 0, :]
    best = jnp.max(tops, axis=0, keepdims=True)
    whole = jnp.sum(s_buf[:, 1, :] * jnp.exp(tops - best), axis=0, keepdims=True)
    mark("d9n")
    norm_scr[...] = best + jnp.log(whole)
    norm_copy = pltpu.make_async_copy(norm_scr, norm_out, z_sem.at[0])
    norm_copy.start()
    arrived(everyone, s_sem.at[0])
    norm_copy.wait()
    mark(None)


def finish_kernel(shift, z_hbm, norm_hbm, key, value, out_hbm, k_out, v_out, norm_out,
                  z_buf, o_buf, norm, k_scr, v_scr, in_sem, out_sem):
    count, n, width = o_buf.shape

    def load(i):
        return pltpu.make_async_copy(z_hbm.at[:, pl.ds(i * width, width)], z_buf.at[i], in_sem.at[i])

    def save(i):
        return pltpu.make_async_copy(o_buf.at[i], out_hbm.at[:, pl.ds(i * width, width)], out_sem.at[i])

    small = ((norm_hbm, norm, norm_out), (key, k_scr, k_out), (value, v_scr, v_out))
    small_in = [pltpu.make_async_copy(a, b, in_sem.at[count + i]) for i, (a, b, _) in enumerate(small)]
    small_out = [pltpu.make_async_copy(b, c, out_sem.at[count + i]) for i, (_, b, c) in enumerate(small)]
    small_in[0].start()
    for i in range(count):
        load(i).start()
    for copy in small_in[1:]:
        copy.start()
    small_in[0].wait()
    small_out[0].start()
    odd = lax.rem(lax.axis_index("xax"), 2) == 1
    for i in range(count):
        row = norm[:, pl.ds(i * width, width)]
        load(i).wait()
        if shift:
            @pl.when(odd)
            def _():
                o_buf[i] = z_buf[i, pl.ds(shift, n), :] - row

            @pl.when(jnp.logical_not(odd))
            def _():
                o_buf[i] = z_buf[i, pl.ds(0, n), :] - row
        else:
            o_buf[i] = z_buf[i] - row
        save(i).start()
    for i in (1, 2):
        small_in[i].wait()
        small_out[i].start()
    for copy in small_out:
        copy.wait()
    for i in range(count):
        save(i).wait()


def solution(mesh):
    ys = mesh.shape["yax"]
    xs = mesh.shape["xax"]
    row_spec = P(("dp", "yax", "xax"))

    def local_step(hidden, cache_len, k_cache, v_cache, g_attn, w_query, w_key, w_value,
                   w_gate, w_up, w_out, w_down, g_final, embedding):
        batch, blk = hidden.shape
        own, slots, head_dim = k_cache.shape
        width = blk * xs
        vocab = embedding.shape[0] // xs
        shift = vocab % 8
        window = -(-vocab // 8) * 8
        half = head_dim // 2
        quarter = xs * own
        cols = w_query.shape[1] // xs
        ff = w_gate.shape[1] // xs
        heads = w_query.shape[1] * ys // head_dim
        per = 4
        groups = own // per
        freq_row = (ROPE_BASE ** (-(np.arange(half, dtype=np.float32) * 2.0) / head_dim)).astype(np.float32)
        freq = jnp.asarray(np.tile(freq_row, 4)[None, :])
        any_spec = pl.BlockSpec(memory_space=pl.ANY)
        vmem = pl.BlockSpec(memory_space=pltpu.VMEM)
        smem = pl.BlockSpec(memory_space=pltpu.SMEM)
        dma = pltpu.SemaphoreType.DMA
        chips = xs // 2
        scratch = [
            pltpu.VMEM((groups, per, head_dim, slots), BF16),
            pltpu.VMEM((groups, per, head_dim, slots), BF16),
            pltpu.VMEM((quarter, width), BF16),
            pltpu.VMEM((1, width), F32),
            pltpu.VMEM((1, width), F32),
            pltpu.VMEM((w_query.shape[1], blk), BF16),
            pltpu.VMEM((ys, cols, width), BF16),
            pltpu.VMEM((width, 2 * ff), BF16),
            pltpu.VMEM((ys, ff, width), BF16),
            pltpu.VMEM((ys, cols, width), BF16),
            pltpu.VMEM((2 * head_dim, width), BF16),
            pltpu.VMEM((batch, width), BF16),
            pltpu.VMEM((quarter, ys * cols), BF16),
            pltpu.VMEM((xs, own, ys * cols), BF16),
            pltpu.VMEM((own * heads, head_dim), F32),
            pltpu.VMEM((own * heads, 1), F32),
            pltpu.VMEM((own * heads, head_dim), F32),
            pltpu.VMEM((own * heads, head_dim), F32),
            pltpu.VMEM((per * heads, slots), F32),
            pltpu.VMEM((own * heads, head_dim), F32),
            pltpu.VMEM((xs, own, ys * cols), BF16),
            pltpu.VMEM((quarter, ys * cols), BF16),
            pltpu.VMEM((ys, quarter, ff), BF16),
            pltpu.VMEM((quarter, ys * ff), BF16),
            pltpu.VMEM((quarter, width), F32),
            pltpu.VMEM((chips, own, width), F32),
            pltpu.VMEM((2, chips, own, width), F32),
            pltpu.VMEM((chips, own, width), F32),
            pltpu.VMEM((batch, width), BF16),
            pltpu.VMEM((window, width), BF16),
            pltpu.VMEM((ys, window, quarter), F32),
            pltpu.VMEM((2, batch), F32),
            pltpu.VMEM((own, head_dim), BF16),
            pltpu.VMEM((own, head_dim), BF16),
            pltpu.VMEM((1, batch), F32),
            pltpu.VMEM((ys * xs, 2, batch), F32),
            dma((2, groups)), dma, dma((3,)), dma((7,)), dma((7,)),
            dma((5,)), dma((5, chips)), dma((5,)), dma((4,)), dma((4,)), dma, dma((2,)),
            dma((ys,)), dma((ys,)), dma((2,)), dma((2,)), dma((2,)),
            dma((chips,)), dma((ys,)), dma((ys, chips)), dma((ys, chips)), dma((2 + ys,)), dma((2,)),
        ]
        cfg = (ys, xs, own, vocab, shift)
        key_new, value_new, logits, norm = pl.pallas_call(
            functools.partial(kernel, cfg),
            name="decode_layer",
            out_shape=(
                jax.ShapeDtypeStruct((own, head_dim), BF16),
                jax.ShapeDtypeStruct((own, head_dim), BF16),
                jax.ShapeDtypeStruct((window, batch), F32),
                jax.ShapeDtypeStruct((1, batch), F32)),
            in_specs=[smem, any_spec, any_spec, any_spec, any_spec, any_spec, vmem] + [any_spec] * 7 + [vmem],
            out_specs=(any_spec, any_spec, any_spec, any_spec),
            scratch_shapes=scratch,
            compiler_params=pltpu.CompilerParams(
                collective_id=0, has_side_effects=True, vmem_limit_bytes=67043328),
        )(cache_len, hidden, k_cache.transpose(0, 2, 1), v_cache.transpose(0, 2, 1),
          g_attn[None, :], g_final[None, :], w_query, w_key.T, w_value.T, w_gate, w_up, w_out, w_down,
          embedding, freq)
        count = 8
        log_probs, key_new, value_new, norm = pl.pallas_call(
            functools.partial(finish_kernel, shift),
            name="finish",
            out_shape=(
                jax.ShapeDtypeStruct((vocab, batch), F32),
                jax.ShapeDtypeStruct((own, head_dim), BF16),
                jax.ShapeDtypeStruct((own, head_dim), BF16),
                jax.ShapeDtypeStruct((1, batch), F32)),
            in_specs=[any_spec] * 4,
            out_specs=(any_spec,) * 4,
            scratch_shapes=[
                pltpu.VMEM((count, window, batch // count), F32),
                pltpu.VMEM((count, vocab, batch // count), F32),
                pltpu.VMEM((1, batch), F32), pltpu.VMEM((own, head_dim), BF16), pltpu.VMEM((own, head_dim), BF16),
                dma((count + 3,)), dma((count + 3,))],
        )(logits, norm, key_new, value_new)
        return key_new, value_new, log_probs.T, norm[0]

    in_specs = (P("dp", "xax"), P("dp"), row_spec, row_spec, P("xax"), P("xax", "yax"),
                P("xax", None), P("xax", None), P("xax", "yax"), P("xax", "yax"),
                P("yax", "xax"), P("yax", "xax"), P("xax"), P("yax", "xax"))
    out_specs = (row_spec, row_spec, P("dp", ("yax", "xax")), P("dp"))
    return jax.shard_map(local_step, mesh=mesh, in_specs=in_specs, out_specs=out_specs, check_vma=False)
```

```python
import functools

import jax
import jax.numpy as jnp
import numpy as np
from jax import lax
from jax.experimental import pallas as pl
from jax.experimental.pallas import tpu as pltpu
from jax.sharding import PartitionSpec as P

EPS = 1e-6
ROPE_BASE = 10000.0
F32 = jnp.float32
BF16 = jnp.bfloat16
NT = (((1,), (1,)), ((), ()))
EMBED_CHUNKS = 16
EMBED_FIRST = 14


def layer_norm(values_in, gain):
    mean = jnp.mean(values_in, axis=-1, keepdims=True)
    centred = values_in - mean
    var = jnp.mean(centred * centred, axis=-1, keepdims=True)
    return centred * lax.rsqrt(var + EPS) * gain


def row_chunks(total, count):
    cuts = [16 * (total // 16 * i // count) for i in range(count)] + [total]
    return [(cuts[i], cuts[i + 1] - cuts[i]) for i in range(count)]


class Marker:
    def __init__(self):
        self.scope = None

    def __call__(self, name):
        if self.scope is not None:
            self.scope.__exit__(None, None, None)
        self.scope = None
        if name:
            self.scope = jax.named_scope(name)
            self.scope.__enter__()


def kernel(cfg, lens_hbm, hidden, k_hbm, v_hbm, g_attn, g_final, wq_hbm, w_key, w_value, w_gate, w_up,
           w_out, w_down, embed, freq_hbm,
           k_out, v_out, logits_out, norm_out,
           k_buf, v_buf, h_buf, ga_buf, gf_buf, wqt, wq_buf, gu_buf, down_buf, out_buf, kv_buf,
           n_all, q_scr, qx_buf, q2d, snew, krep, vrep, s_scr, od_scr, o_scr, ox_buf, act_scr, act, part_scr,
           pre_buf, rs_scr, rs_buf, f_buf, e_buf, z_scr, st_scr, k_scr, v_scr, norm_scr, s_buf,
           lens, w_query, freq,
           kv_sem, e_own_sem, z_sem, x_send, x_recv, g_send, g_recv, g_last, y_send, y_recv, e_send, e_recv,
           n_recv, n_last, n_send, pre_sem, rs_sem, fxa, fyb, fya, fxb, f_sem, s_sem):
    ys, xs, own, vocab, shift = cfg
    mark = Marker()
    y = lax.axis_index("yax")
    x = lax.axis_index("xax")
    core = lax.rem(x, 2)
    partner = x + 1 - 2 * core
    blk = hidden.shape[1]
    quarter = xs * own
    head_dim = k_hbm.shape[1]
    half = head_dim // 2
    seqs = k_hbm.shape[0]
    slots = k_hbm.shape[2]
    heads = w_query.shape[1] * ys // head_dim
    groups = k_buf.shape[0]
    per = seqs // groups
    window = e_buf.shape[0]

    def lanes(i):
        return pl.ds(pl.multiple_of(i * blk, 128), blk)

    def rows(i, n):
        return pl.ds(pl.multiple_of(i * n, n), n)

    mark("a0start")
    barrier = pltpu.get_barrier_semaphore()

    def signal_row(d, carry):
        pl.semaphore_signal(barrier, inc=1, device_id={"xax": lax.rem(x + d, xs)},
                            device_id_type=pl.DeviceIdType.MESH)
        return carry
    lax.fori_loop(1, xs, signal_row, 0)

    def signal_column(d, carry):
        pl.semaphore_signal(barrier, inc=1, device_id={"yax": lax.rem(y + d, ys)},
                            device_id_type=pl.DeviceIdType.MESH)
        return carry
    lax.fori_loop(1, ys, signal_column, 0)
    small_ins = [pltpu.make_async_copy(a, b, z_sem.at[i])
                 for i, (a, b) in enumerate(((wq_hbm, w_query), (freq_hbm, freq), (lens_hbm, lens)))]
    for copy in small_ins:
        copy.start()
    def cache_copy(g, src, dst, s):
        return pltpu.make_async_copy(src.at[pl.ds(g * per, per)], dst.at[g], kv_sem.at[s, g])

    def start_cache(g, carry):
        cache_copy(g, k_hbm, k_buf, 0).start()
        return carry
    lax.fori_loop(0, groups, start_cache, 0)

    for copy in small_ins:
        copy.wait()
    wqt[...] = w_query[...].astype(F32).T.astype(BF16)

    mark("a0wait")
    pl.semaphore_wait(barrier, xs + ys - 2)

    def arrived(ref, sem):
        pltpu.make_async_copy(ref, ref, sem).wait()

    cols = wqt.shape[0] // xs
    ff = w_gate.shape[1] // xs
    most = pl.ds(0, (xs - 1) * blk)
    x_kinds = {
        "wq": (lambda p: wqt.at[rows(p, cols), :], lambda s: wq_buf.at[y, :, lanes(s)],
               wq_buf.at[y], wq_buf.at[y, :, most]),
        "wo": (lambda p: w_out.at[rows(p, cols), :], lambda s: out_buf.at[y, :, lanes(s)],
               out_buf.at[y], out_buf.at[y, :, most]),
        "down": (lambda p: w_down.at[rows(p, ff), :], lambda s: down_buf.at[y, :, lanes(s)],
                 down_buf.at[y], down_buf.at[y, :, most]),
        "gate": (lambda p: w_gate.at[:, lanes(p)], lambda s: gu_buf.at[rows(s, blk), pl.ds(0, ff)],
                 gu_buf.at[:, pl.ds(0, ff)], gu_buf.at[most, pl.ds(0, ff)]),
        "up": (lambda p: w_up.at[:, lanes(p)], lambda s: gu_buf.at[rows(s, blk), pl.ds(ff, ff)],
               gu_buf.at[:, pl.ds(ff, ff)], gu_buf.at[most, pl.ds(ff, ff)]),
        "q": (lambda p: q_scr.at[rows(p, own), :], lambda s: qx_buf.at[s],
              qx_buf, qx_buf.at[pl.ds(0, xs - 1)]),
        "o": (lambda p: o_scr.at[p], lambda s: ox_buf.at[rows(s, own), :],
              ox_buf, ox_buf.at[pl.ds(0, (xs - 1) * own), :]),
    }
    x_index = {name: i for i, name in enumerate(x_kinds)}

    def x_start(name):
        src, dst = x_kinds[name][:2]
        k = x_index[name]

        def body(d, carry):
            p = lax.rem(x + d, xs)
            pltpu.make_async_remote_copy(
                src_ref=src(p), dst_ref=dst(x), send_sem=x_send.at[k], recv_sem=x_recv.at[k],
                device_id={"xax": p}, device_id_type=pl.DeviceIdType.MESH).start()
            return carry
        lax.fori_loop(1, xs, body, 0)
        pltpu.make_async_copy(src(x), dst(x), x_recv.at[k]).start()

    def x_wait(name):
        arrived(x_kinds[name][2], x_recv.at[x_index[name]])

    def x_drain(name):
        arrived(x_kinds[name][3], x_send.at[x_index[name]])

    chips = xs // 2
    g_kinds = {
        "hidden": (hidden.at[rows(y, quarter), :], lambda s: h_buf.at[:, lanes(s)], h_buf),
        "ga": (g_attn, lambda s: ga_buf.at[:, lanes(s)], ga_buf),
        "gf": (g_final, lambda s: gf_buf.at[:, lanes(s)], gf_buf),
        "wk": (w_key, lambda s: kv_buf.at[pl.ds(0, head_dim), lanes(s)], kv_buf.at[pl.ds(0, head_dim), :]),
        "wv": (w_value, lambda s: kv_buf.at[pl.ds(head_dim, head_dim), lanes(s)],
               kv_buf.at[pl.ds(head_dim, head_dim), :]),
    }
    g_index = {name: i for i, name in enumerate(g_kinds)}

    def g_copy(name, i, sender):
        src, dst, _ = g_kinds[name]
        k = g_index[name]
        return pltpu.make_async_remote_copy(
            src_ref=src, dst_ref=dst(sender), send_sem=g_send.at[k], recv_sem=g_recv.at[k, i],
            device_id={"xax": lax.rem(x + 2 * i, xs)}, device_id_type=pl.DeviceIdType.MESH)

    def g_pass(name, sender, source):
        k = g_index[name]
        return pltpu.make_async_remote_copy(
            src_ref=source, dst_ref=g_kinds[name][1](sender), send_sem=g_send.at[k], recv_sem=g_last.at[k],
            device_id={"xax": partner}, device_id_type=pl.DeviceIdType.MESH)

    def g_start(name):
        def body(i, carry):
            g_copy(name, i, x).start()
            return carry
        lax.fori_loop(1, chips, body, 0)
        src, dst, _ = g_kinds[name]
        g_pass(name, x, src).start()
        pltpu.make_async_copy(src, dst(x), g_last.at[g_index[name]]).start()

    def g_forward(name):
        def body(i, carry):
            sender = lax.rem(x + xs - 2 * i, xs)
            g_copy(name, i, sender).wait_recv()
            g_pass(name, sender, g_kinds[name][1](sender)).start()
            return carry
        lax.fori_loop(1, chips, body, 0)

    def g_wait(name):
        whole = g_kinds[name][2]
        arrived(whole.at[:, pl.ds(0, (chips + 1) * blk)], g_last.at[g_index[name]])

    def g_drain(name):
        arrived(g_kinds[name][2].at[:, most], g_send.at[g_index[name]])

    y_kinds = {"wq": wq_buf, "wo": out_buf, "down": down_buf}
    y_index = {name: i for i, name in enumerate(y_kinds)}
    others = pl.ds(0, ys - 1)

    def y_start(name):
        buf = y_kinds[name]
        k = y_index[name]

        def body(d, carry):
            pltpu.make_async_remote_copy(
                src_ref=buf.at[y], dst_ref=buf.at[y], send_sem=y_send.at[k], recv_sem=y_recv.at[k],
                device_id={"yax": lax.rem(y + d, ys)}, device_id_type=pl.DeviceIdType.MESH).start()
            return carry
        lax.fori_loop(1, ys, body, 0)

    def y_wait(name):
        arrived(y_kinds[name].at[others], y_recv.at[y_index[name]])

    def y_drain(name):
        arrived(y_kinds[name].at[others], y_send.at[y_index[name]])

    e_parts = row_chunks(window, EMBED_CHUNKS)

    def e_first(p):
        return p * vocab - lax.rem(p, 2) * shift

    def e_own():
        return pltpu.make_async_copy(
            embed.at[pl.ds(pl.multiple_of(e_first(x), 8), window), :], e_buf.at[:, lanes(x)], e_own_sem)

    def e_start(c):
        r0, n = e_parts[c]

        def body(d, carry):
            p = lax.rem(x + d, xs)
            pltpu.make_async_remote_copy(
                src_ref=embed.at[pl.ds(pl.multiple_of(e_first(p) + r0, 8), n), :],
                dst_ref=e_buf.at[pl.ds(r0, n), lanes(x)], send_sem=e_send,
                recv_sem=e_recv.at[int(c >= EMBED_FIRST)],
                device_id={"xax": p}, device_id_type=pl.DeviceIdType.MESH).start()
            return carry
        lax.fori_loop(1, xs, body, 0)

    mark("a1send")
    x_start("wq")
    for name in ("hidden", "ga"):
        g_start(name)
    for name in ("wo", "down"):
        x_start(name)
    for name in ("wk", "wv", "gf"):
        g_start(name)
    e_start(0)
    e_own().start()

    def start_cache_v(g, carry):
        cache_copy(g, v_hbm, v_buf, 1).start()
        return carry
    lax.fori_loop(0, groups, start_cache_v, 0)

    mark("a2wqx")
    x_wait("wq")
    y_start("wq")
    mark("a3hfwd")
    for name in ("hidden", "ga"):
        g_forward(name)
    mark("a4hwait")
    for name in ("hidden", "ga"):
        g_wait(name)
    mark("a5ln")
    my_rows = rows(y, quarter)
    n_all[my_rows, :] = layer_norm(h_buf[...].astype(F32), ga_buf[...]).astype(BF16)

    part = quarter // 2

    def n_rows(j, c):
        return pl.ds(pl.multiple_of(j * quarter + c * part, part), part)

    def n_copy(d, sender):
        r = n_rows(sender, core)
        return pltpu.make_async_remote_copy(
            src_ref=n_all.at[r, :], dst_ref=n_all.at[r, :], send_sem=n_send.at[0],
            recv_sem=n_recv.at[d], device_id={"yax": lax.rem(y + d, ys)},
            device_id_type=pl.DeviceIdType.MESH)

    def n_pass(d, c):
        r = n_rows(lax.rem(y + ys - d, ys), c)
        return pltpu.make_async_remote_copy(
            src_ref=n_all.at[r, :], dst_ref=n_all.at[r, :], send_sem=n_send.at[1],
            recv_sem=n_last.at[d], device_id={"xax": partner},
            device_id_type=pl.DeviceIdType.MESH)

    mark("a6wo")
    x_wait("wo")
    y_start("wo")
    mark("a6wqy")
    y_wait("wq")
    mark("a7q")
    wq_all = wq_buf[...].reshape(ys * cols, xs * blk)
    q_scr[...] = lax.dot_general(n_all[my_rows, :], wq_all, NT, preferred_element_type=F32).astype(BF16)
    mark("a8send")
    x_start("q")
    x_start("gate")
    x_start("up")

    def n_start(d, carry):
        n_copy(d, y).start()
        return carry
    lax.fori_loop(1, ys, n_start, 0)
    mark("b0down")
    x_wait("down")
    y_start("down")
    for c in range(1, 7):
        e_start(c)

    mark("b1kv")
    row_id = lax.broadcasted_iota(jnp.int32, (own, 4 * half), 0)
    first_row = (y * xs + x) * own
    position = jnp.zeros((own, 4 * half), jnp.int32)
    for b in range(own):
        position = jnp.where(row_id == b, lens[first_row + b], position)
    angle = position.astype(F32) * freq[...]
    cos_a = jnp.cos(angle)
    sin_a = jnp.sin(angle)
    for name in ("wk", "wv", "gf"):
        g_forward(name)
    for name in ("wk", "wv", "gf"):
        g_wait(name)
    mine = y * xs + x
    n_own = n_all[rows(mine, own), :]
    kv = lax.dot_general(n_own, kv_buf[...], NT, preferred_element_type=F32).astype(BF16).astype(F32)
    k1 = kv[:, :half]
    k2 = kv[:, half:head_dim]
    c1 = cos_a[:, :half]
    s1 = sin_a[:, :half]
    key = jnp.concatenate([k1 * c1 - k2 * s1, k2 * c1 + k1 * s1], axis=1).astype(BF16)
    value = kv[:, head_dim:].astype(BF16)
    k_scr[...] = key
    v_scr[...] = value
    small_outs = [pltpu.make_async_copy(k_scr, k_out, z_sem.at[0]),
                  pltpu.make_async_copy(v_scr, v_out, z_sem.at[1])]
    for copy in small_outs:
        copy.start()
    for h in range(heads):
        krep[pl.ds(h, own, stride=heads), :] = key.astype(F32)
        vrep[pl.ds(h, own, stride=heads), :] = value.astype(F32)

    mark("b2q")
    x_wait("q")
    mark("b3rot")
    for xc in range(xs // 2):
        qa = qx_buf[2 * xc].astype(F32)
        qb = qx_buf[2 * xc + 1].astype(F32)
        ra = (qa * cos_a - qb * sin_a).astype(BF16).astype(F32)
        rb = (qb * cos_a + qa * sin_a).astype(BF16).astype(F32)
        for yc in range(ys):
            pair = jnp.concatenate([ra[:, yc * half:(yc + 1) * half], rb[:, yc * half:(yc + 1) * half]], axis=1)
            q2d[pl.ds(xc * ys + yc, own, stride=heads), :] = pair
    scale = head_dim ** -0.5
    snew[...] = jnp.sum(q2d[...] * krep[...], axis=1, keepdims=True) * scale

    mark("b4attn")
    gr = per * heads
    seg_r = lax.broadcasted_iota(jnp.int32, (gr, per * head_dim), 0) // heads
    seg_c = lax.broadcasted_iota(jnp.int32, (gr, per * head_dim), 1) // head_dim
    diag = (seg_r == seg_c).astype(F32)
    tile = min(512, slots)
    row_g = lax.broadcasted_iota(jnp.int32, (gr, 1), 0) // heads
    lane_g = lax.broadcasted_iota(jnp.int32, (gr, tile), 1)

    def attend(g, carry):
        cache_copy(g, k_hbm, k_buf, 0).wait()
        qg = q2d[rows(g, gr), :]
        qbd = (jnp.concatenate([qg] * per, axis=1) * diag).astype(BF16)
        len_g = jnp.zeros((gr, 1), jnp.int32)
        for s in range(per):
            len_g = jnp.where(row_g == s, lens[first_row + g * per + s], len_g)
        new = snew[rows(g, gr), :]
        top = jnp.full((gr, tile), -jnp.inf, F32)
        kg = k_buf.at[g]
        vg = v_buf.at[g]
        for c in range(slots // tile):
            kc = kg[:, :, pl.ds(c * tile, tile)].reshape(per * head_dim, tile)
            sc = jnp.dot(qbd, kc, preferred_element_type=F32) * scale
            sc = jnp.where(lane_g < len_g - c * tile, sc, -jnp.inf)
            s_scr[:, pl.ds(c * tile, tile)] = sc
            top = jnp.maximum(top, sc)
        row_max = jnp.maximum(jnp.max(top, axis=1, keepdims=True), new)
        total = jnp.zeros((gr, tile), F32)
        for c in range(slots // tile):
            ex = jnp.exp(s_scr[:, pl.ds(c * tile, tile)] - row_max)
            s_scr[:, pl.ds(c * tile, tile)] = ex
            total = total + ex
        w_new = jnp.exp(new - row_max)
        den = jnp.sum(total, axis=1, keepdims=True) + w_new
        inv = 1.0 / den
        cache_copy(g, v_hbm, v_buf, 1).wait()
        mixed = jnp.zeros((gr, per * head_dim), F32)
        for c in range(slots // tile):
            pr = (s_scr[:, pl.ds(c * tile, tile)] * inv).astype(BF16)
            vc = vg[:, :, pl.ds(c * tile, tile)].reshape(per * head_dim, tile)
            mixed = mixed + lax.dot_general(pr, vc, NT, preferred_element_type=F32)
        add = (w_new * inv).astype(BF16).astype(F32) * vrep[rows(g, gr), :]
        for s in range(per):
            od_scr[pl.ds(pl.multiple_of(g * gr + s * heads, heads), heads), :] = (
                mixed[s * heads:(s + 1) * heads, s * head_dim:(s + 1) * head_dim]
                + add[s * heads:(s + 1) * heads, :])
        return carry

    lax.fori_loop(0, groups, attend, 0)
    mark("b5o")
    for xc in range(xs // 2):
        parts = [od_scr[pl.ds(xc * ys + yc, own, stride=heads), :] for yc in range(ys)]
        o_scr[2 * xc] = jnp.concatenate([p[:, :half] for p in parts], axis=1).astype(BF16)
        o_scr[2 * xc + 1] = jnp.concatenate([p[:, half:] for p in parts], axis=1).astype(BF16)
    x_start("o")
    for c in range(7, 12):
        e_start(c)

    def act_copy(dest):
        return pltpu.make_async_remote_copy(
            src_ref=act_scr.at[dest], dst_ref=act.at[:, pl.ds(pl.multiple_of(y * ff, ff), ff)],
            send_sem=y_send.at[len(y_kinds)], recv_sem=y_recv.at[len(y_kinds)],
            device_id={"yax": dest}, device_id_type=pl.DeviceIdType.MESH)

    mark("b6gu")
    x_wait("gate")
    x_wait("up")

    mark("b7feed")
    def feed(d, carry):
        @pl.when(d < ys - 1)
        def _():
            n_copy(d + 1, lax.rem(y + ys - d - 1, ys)).wait_recv()
            n_pass(d + 1, core).start()
        j = lax.rem(y + ys - d, ys)

        @pl.when(d > 0)
        def _():
            n_pass(d, 1 - core).wait_recv()
        gu = jnp.dot(n_all[rows(j, quarter), :], gu_buf[...], preferred_element_type=F32)
        gu = gu.astype(BF16).astype(F32)
        gate = gu[:, :ff]
        act_scr[j] = (gate * jax.nn.sigmoid(gate) * gu[:, ff:]).astype(BF16)

        @pl.when(d > 0)
        def _():
            act_copy(j).start()
        return carry
    lax.fori_loop(0, ys, feed, 0)
    act[:, pl.ds(pl.multiple_of(y * ff, ff), ff)] = act_scr[y]
    mark("b8wo")
    y_wait("wo")
    mark("b9o")
    x_wait("o")
    mark("c0op")
    part_scr[...] = jnp.dot(
        ox_buf[...], out_buf[...].reshape(ys * cols, xs * blk), preferred_element_type=F32)
    mark("c1down")
    y_wait("down")

    mark("c2act")
    arrived(act_scr.at[others], y_recv.at[len(y_kinds)])

    mark("c3branch")
    down_all = down_buf[...].reshape(ys * ff, xs * blk)
    part_scr[...] = part_scr[...] + jnp.dot(act[...], down_all, preferred_element_type=F32)

    def branch(c):
        for i in range(chips):
            rs_scr[c, i] = part_scr[pl.ds(pl.multiple_of((2 * i + c) * own, own), own), :]

    def pre_copy():
        return pltpu.make_async_remote_copy(
            src_ref=rs_scr.at[1 - core], dst_ref=pre_buf, send_sem=pre_sem.at[0], recv_sem=pre_sem.at[1],
            device_id={"xax": partner}, device_id_type=pl.DeviceIdType.MESH)

    def rs_copy(dest):
        return pltpu.make_async_remote_copy(
            src_ref=rs_scr.at[core, dest], dst_ref=rs_buf.at[chip], send_sem=rs_sem.at[0],
            recv_sem=rs_sem.at[1], device_id={"xax": 2 * dest + core},
            device_id_type=pl.DeviceIdType.MESH)

    chip = x // 2
    branch(1 - core)
    pre_copy().start()
    branch(core)
    mark("c4pre")
    pre_copy().wait_recv()
    rs_scr[core] = rs_scr[core] + pre_buf[...]

    mark("c5rs")
    def rs_start(i, carry):
        rs_copy(lax.rem(chip + i, chips)).start()
        return carry
    lax.fori_loop(1, chips, rs_start, 0)
    e_start(12)
    mark("c6rsw")
    arrived(rs_buf.at[pl.ds(0, chips - 1)], rs_sem.at[1])
    mark("c7ln")
    rs_buf[chip] = rs_scr[core, chip]
    res = h_buf[rows(x, own), :].astype(F32) + jnp.sum(rs_buf[...], axis=0)
    f_buf[rows(mine, own), :] = layer_norm(res, gf_buf[...]).astype(BF16)

    piece = own // 2

    def f_half(sy, sx, h):
        return f_buf.at[pl.ds(pl.multiple_of((sy * xs + sx) * own + h * piece, piece), piece), :]

    def f_over_x(i, h, sy, sx, sem):
        return pltpu.make_async_remote_copy(
            src_ref=f_half(sy, sx, h), dst_ref=f_half(sy, sx, h), send_sem=f_sem.at[0], recv_sem=sem,
            device_id={"xax": lax.rem(x + 2 * i, xs)}, device_id_type=pl.DeviceIdType.MESH)

    def f_over_y(d, h, sy, sx, sem):
        return pltpu.make_async_remote_copy(
            src_ref=f_half(sy, sx, h), dst_ref=f_half(sy, sx, h), send_sem=f_sem.at[0], recv_sem=sem,
            device_id={"yax": lax.rem(y + d, ys)}, device_id_type=pl.DeviceIdType.MESH)

    def f_pass(d, h, sy, sx):
        pltpu.make_async_remote_copy(
            src_ref=f_half(sy, sx, h), dst_ref=f_half(sy, sx, h), send_sem=f_sem.at[1],
            recv_sem=f_sem.at[2 + d], device_id={"xax": partner},
            device_id_type=pl.DeviceIdType.MESH).start()

    def from_y(d):
        return lax.rem(y + ys - d, ys)

    def from_x(i):
        return lax.rem(x + xs - 2 * i, xs)

    def spread_y(i):
        def body(d, carry):
            f_over_y(d, 0, y, from_x(i), fya.at[d, i]).start()
            return carry
        lax.fori_loop(1, ys, body, 0)

    def spread_x(d):
        def body(i, carry):
            f_over_x(i, 1, from_y(d), x, fxb.at[d, i]).start()
            return carry
        lax.fori_loop(1, chips, body, 0)

    mark("c8fx")
    def first_x(i, carry):
        f_over_x(i, 0, y, x, fxa.at[i]).start()
        return carry
    lax.fori_loop(1, chips, first_x, 0)

    def first_y(d, carry):
        f_over_y(d, 1, y, x, fyb.at[d]).start()
        return carry
    lax.fori_loop(1, ys, first_y, 0)
    spread_y(0)
    spread_x(0)
    f_pass(0, 0, y, x)
    f_pass(0, 1, y, x)
    mark("c9sp")
    for i in range(1, max(chips, ys)):
        if i < chips:
            f_over_x(i, 0, y, from_x(i), fxa.at[i]).wait_recv()
            spread_y(i)
            f_pass(0, 0, y, from_x(i))
        if i < ys:
            f_over_y(i, 1, from_y(i), x, fyb.at[i]).wait_recv()
            spread_x(i)
            f_pass(i, 1, from_y(i), x)
    for c in range(13, EMBED_CHUNKS):
        e_start(c)

    def collect(d):
        def body(i, carry):
            @pl.when(d > 0)
            def _():
                f_over_y(d, 0, from_y(d), from_x(i), fya.at[d, i]).wait_recv()
                f_pass(d, 0, from_y(d), from_x(i))

            @pl.when(i > 0)
            def _():
                f_over_x(i, 1, from_y(d), from_x(i), fxb.at[d, i]).wait_recv()
                f_pass(d, 1, from_y(d), from_x(i))
            return carry
        lax.fori_loop(0, chips, body, 0)

    mark("d0drain")
    for name in x_kinds:
        x_drain(name)
    for name in g_kinds:
        g_drain(name)
    for name in y_kinds:
        y_drain(name)
    arrived(act_scr.at[others], y_send.at[len(y_kinds)])
    for i in range(2):
        arrived(n_all.at[pl.ds(0, (ys - 1) * part), :], n_send.at[i])
    pre_copy().wait_send()
    arrived(rs_buf.at[pl.ds(0, chips - 1)], rs_sem.at[0])
    for copy in small_outs:
        copy.wait()

    cut = e_parts[EMBED_FIRST][0]
    skip = core * shift
    half_block = pl.ds(0, chips * own)

    def nearest(k):
        return k + k // 2 * (1 - 2 * lax.rem(k, 2))

    def z_copy(j, r0, n):
        return pltpu.make_async_copy(
            z_scr.at[j, pl.ds(r0, n), :], logits_out.at[pl.ds(r0, n), rows(j, quarter)], z_sem.at[2])

    def block(j, r0, n, pieces):
        r = pl.ds(r0, n)
        z_scr[j, r, :] = lax.dot_general(e_buf[r, :], f_buf[rows(j, quarter), :], NT, preferred_element_type=F32)
        z_copy(j, r0, n).start()
        stats = []
        for q0, m in row_chunks(n, pieces):
            z = z_scr[j, pl.ds(r0 + q0, m), :]
            if shift and (r0 + q0 == 0 or r0 + q0 + m == window):
                index = lax.broadcasted_iota(jnp.int32, z.shape, 0) + (r0 + q0)
                z = jnp.where(jnp.logical_and(index >= skip, index < skip + vocab), z, -jnp.inf)
            top = jnp.max(z, axis=0, keepdims=True)
            stats.append((top, jnp.sum(jnp.exp(z - top), axis=0, keepdims=True)))
        return stats

    def put(j, stats):
        top = functools.reduce(jnp.maximum, [t for t, _ in stats])
        st_scr[0:1, rows(j, quarter)] = top
        st_scr[1:2, rows(j, quarter)] = sum(t * jnp.exp(m - top) for m, t in stats)

    def head(k, carry):
        d = nearest(k)
        j = from_y(d)
        with jax.named_scope('hw'):
            arrived(f_buf.at[half_block, :], f_sem.at[2 + d])
        put(j, block(j, 0, cut, 4))

        @pl.when(k < ys - 2)
        def _():
            collect(nearest(k + 2))
        return carry

    def head_rest(j, carry):
        before = (st_scr[0:1, rows(j, quarter)], st_scr[1:2, rows(j, quarter)])
        put(j, [before] + block(j, cut, window - cut, 1))
        return carry

    mark("d1coll")
    for k in range(min(2, ys)):
        collect(nearest(k))
    mark("d1e")
    e_own().wait()
    arrived(e_buf.at[pl.ds(0, cut), most], e_recv.at[0])

    mark("d3head")
    lax.fori_loop(0, ys, head, 0)
    mark("d3rest")
    arrived(e_buf.at[pl.ds(cut, window - cut), most], e_recv.at[1])
    mark("d3hr")
    lax.fori_loop(0, ys, head_rest, 0)

    mark("d4stat")
    def s_start(k, carry):
        dy = lax.rem(ys // 2 + k, ys)

        def body(dx, c2):
            @pl.when(dy + dx > 0)
            def _():
                pltpu.make_async_remote_copy(
                    src_ref=st_scr, dst_ref=s_buf.at[mine], send_sem=s_sem.at[0], recv_sem=s_sem.at[1],
                    device_id={"yax": lax.rem(y + dy, ys), "xax": lax.rem(x + dx, xs)},
                    device_id_type=pl.DeviceIdType.MESH).start()
            return c2
        lax.fori_loop(0, xs, body, 0)
        return carry
    lax.fori_loop(0, ys, s_start, 0)
    s_buf[mine] = st_scr[...]

    mark("d5sx")
    arrived(e_buf.at[:, most], e_send)
    arrived(f_buf.at[pl.ds(0, 2 * (ys * chips - 1) * piece), :], f_sem.at[0])
    arrived(f_buf.at[pl.ds(0, ys * chips * own), :], f_sem.at[1])
    arrived(z_scr, z_sem.at[2])
    everyone = s_buf.at[pl.ds(0, ys * xs - 1)]
    mark("d6sw")
    arrived(everyone, s_sem.at[1])
    tops = s_buf[:, 0, :]
    best = jnp.max(tops, axis=0, keepdims=True)
    whole = jnp.sum(s_buf[:, 1, :] * jnp.exp(tops - best), axis=0, keepdims=True)
    mark("d9n")
    norm_scr[...] = best + jnp.log(whole)
    norm_copy = pltpu.make_async_copy(norm_scr, norm_out, z_sem.at[0])
    norm_copy.start()
    arrived(everyone, s_sem.at[0])
    norm_copy.wait()
    mark(None)


def finish_kernel(shift, z_hbm, norm_hbm, key, value, out_hbm, k_out, v_out, norm_out,
                  z_buf, o_buf, norm, k_scr, v_scr, in_sem, out_sem):
    count, n, width = o_buf.shape

    def load(i):
        return pltpu.make_async_copy(z_hbm.at[:, pl.ds(i * width, width)], z_buf.at[i], in_sem.at[i])

    def save(i):
        return pltpu.make_async_copy(o_buf.at[i], out_hbm.at[:, pl.ds(i * width, width)], out_sem.at[i])

    small = ((norm_hbm, norm, norm_out), (key, k_scr, k_out), (value, v_scr, v_out))
    small_in = [pltpu.make_async_copy(a, b, in_sem.at[count + i]) for i, (a, b, _) in enumerate(small)]
    small_out = [pltpu.make_async_copy(b, c, out_sem.at[count + i]) for i, (_, b, c) in enumerate(small)]
    small_in[0].start()
    for i in range(count):
        load(i).start()
    for copy in small_in[1:]:
        copy.start()
    small_in[0].wait()
    small_out[0].start()
    odd = lax.rem(lax.axis_index("xax"), 2) == 1
    for i in range(count):
        row = norm[:, pl.ds(i * width, width)]
        load(i).wait()
        if shift:
            @pl.when(odd)
            def _():
                o_buf[i] = z_buf[i, pl.ds(shift, n), :] - row

            @pl.when(jnp.logical_not(odd))
            def _():
                o_buf[i] = z_buf[i, pl.ds(0, n), :] - row
        else:
            o_buf[i] = z_buf[i] - row
        save(i).start()
    for i in (1, 2):
        small_in[i].wait()
        small_out[i].start()
    for copy in small_out:
        copy.wait()
    for i in range(count):
        save(i).wait()


def solution(mesh):
    ys = mesh.shape["yax"]
    xs = mesh.shape["xax"]
    row_spec = P(("dp", "yax", "xax"))

    def local_step(hidden, cache_len, k_cache, v_cache, g_attn, w_query, w_key, w_value,
                   w_gate, w_up, w_out, w_down, g_final, embedding):
        batch, blk = hidden.shape
        own, slots, head_dim = k_cache.shape
        width = blk * xs
        vocab = embedding.shape[0] // xs
        shift = vocab % 8
        window = -(-vocab // 8) * 8
        half = head_dim // 2
        quarter = xs * own
        cols = w_query.shape[1] // xs
        ff = w_gate.shape[1] // xs
        heads = w_query.shape[1] * ys // head_dim
        per = 4
        groups = own // per
        freq_row = (ROPE_BASE ** (-(np.arange(half, dtype=np.float32) * 2.0) / head_dim)).astype(np.float32)
        freq = jnp.asarray(np.tile(freq_row, 4)[None, :])
        any_spec = pl.BlockSpec(memory_space=pl.ANY)
        dma = pltpu.SemaphoreType.DMA
        chips = xs // 2
        scratch = [
            pltpu.VMEM((groups, per, head_dim, slots), BF16),
            pltpu.VMEM((groups, per, head_dim, slots), BF16),
            pltpu.VMEM((quarter, width), BF16),
            pltpu.VMEM((1, width), F32),
            pltpu.VMEM((1, width), F32),
            pltpu.VMEM((w_query.shape[1], blk), BF16),
            pltpu.VMEM((ys, cols, width), BF16),
            pltpu.VMEM((width, 2 * ff), BF16),
            pltpu.VMEM((ys, ff, width), BF16),
            pltpu.VMEM((ys, cols, width), BF16),
            pltpu.VMEM((2 * head_dim, width), BF16),
            pltpu.VMEM((batch, width), BF16),
            pltpu.VMEM((quarter, ys * cols), BF16),
            pltpu.VMEM((xs, own, ys * cols), BF16),
            pltpu.VMEM((own * heads, head_dim), F32),
            pltpu.VMEM((own * heads, 1), F32),
            pltpu.VMEM((own * heads, head_dim), F32),
            pltpu.VMEM((own * heads, head_dim), F32),
            pltpu.VMEM((per * heads, slots), F32),
            pltpu.VMEM((own * heads, head_dim), F32),
            pltpu.VMEM((xs, own, ys * cols), BF16),
            pltpu.VMEM((quarter, ys * cols), BF16),
            pltpu.VMEM((ys, quarter, ff), BF16),
            pltpu.VMEM((quarter, ys * ff), BF16),
            pltpu.VMEM((quarter, width), F32),
            pltpu.VMEM((chips, own, width), F32),
            pltpu.VMEM((2, chips, own, width), F32),
            pltpu.VMEM((chips, own, width), F32),
            pltpu.VMEM((batch, width), BF16),
            pltpu.VMEM((window, width), BF16),
            pltpu.VMEM((ys, window, quarter), F32),
            pltpu.VMEM((2, batch), F32),
            pltpu.VMEM((own, head_dim), BF16),
            pltpu.VMEM((own, head_dim), BF16),
            pltpu.VMEM((1, batch), F32),
            pltpu.VMEM((ys * xs, 2, batch), F32),
            pltpu.SMEM(cache_len.shape, jnp.int32),
            pltpu.VMEM(w_query.shape, BF16),
            pltpu.VMEM((1, 4 * half), F32),
            dma((2, groups)), dma, dma((3,)), dma((7,)), dma((7,)),
            dma((5,)), dma((5, chips)), dma((5,)), dma((4,)), dma((4,)), dma, dma((2,)),
            dma((ys,)), dma((ys,)), dma((2,)), dma((2,)), dma((2,)),
            dma((chips,)), dma((ys,)), dma((ys, chips)), dma((ys, chips)), dma((2 + ys,)), dma((2,)),
        ]
        cfg = (ys, xs, own, vocab, shift)
        key_new, value_new, logits, norm = pl.pallas_call(
            functools.partial(kernel, cfg),
            name="decode_layer",
            out_shape=(
                jax.ShapeDtypeStruct((own, head_dim), BF16),
                jax.ShapeDtypeStruct((own, head_dim), BF16),
                jax.ShapeDtypeStruct((window, batch), F32),
                jax.ShapeDtypeStruct((1, batch), F32)),
            in_specs=[any_spec] * 15,
            out_specs=(any_spec, any_spec, any_spec, any_spec),
            scratch_shapes=scratch,
            compiler_params=pltpu.CompilerParams(
                collective_id=0, has_side_effects=True, vmem_limit_bytes=67043328),
        )(cache_len, hidden, k_cache.transpose(0, 2, 1), v_cache.transpose(0, 2, 1),
          g_attn[None, :], g_final[None, :], w_query, w_key.T, w_value.T, w_gate, w_up, w_out, w_down,
          embedding, freq)
        count = 8
        log_probs, key_new, value_new, norm = pl.pallas_call(
            functools.partial(finish_kernel, shift),
            name="finish",
            out_shape=(
                jax.ShapeDtypeStruct((vocab, batch), F32),
                jax.ShapeDtypeStruct((own, head_dim), BF16),
                jax.ShapeDtypeStruct((own, head_dim), BF16),
                jax.ShapeDtypeStruct((1, batch), F32)),
            in_specs=[any_spec] * 4,
            out_specs=(any_spec,) * 4,
            scratch_shapes=[
                pltpu.VMEM((count, window, batch // count), F32),
                pltpu.VMEM((count, vocab, batch // count), F32),
                pltpu.VMEM((1, batch), F32), pltpu.VMEM((own, head_dim), BF16), pltpu.VMEM((own, head_dim), BF16),
                dma((count + 3,)), dma((count + 3,))],
        )(logits, norm, key_new, value_new)
        return key_new, value_new, log_probs.T, norm[0]

    in_specs = (P("dp", "xax"), P("dp"), row_spec, row_spec, P("xax"), P("xax", "yax"),
                P("xax", None), P("xax", None), P("xax", "yax"), P("xax", "yax"),
                P("yax", "xax"), P("yax", "xax"), P("xax"), P("yax", "xax"))
    out_specs = (row_spec, row_spec, P("dp", ("yax", "xax")), P("dp"))
    return jax.shard_map(local_step, mesh=mesh, in_specs=in_specs, out_specs=out_specs, check_vma=False)
```

```python
import functools

import jax
import jax.numpy as jnp
import numpy as np
from jax import lax
from jax.experimental import pallas as pl
from jax.experimental.pallas import tpu as pltpu
from jax.sharding import PartitionSpec as P

EPS = 1e-6
ROPE_BASE = 10000.0
F32 = jnp.float32
BF16 = jnp.bfloat16
NT = (((1,), (1,)), ((), ()))
EMBED_CHUNKS = 16
EMBED_FIRST = 14


def layer_norm(values_in, gain):
    mean = jnp.mean(values_in, axis=-1, keepdims=True)
    centred = values_in - mean
    var = jnp.mean(centred * centred, axis=-1, keepdims=True)
    return centred * lax.rsqrt(var + EPS) * gain


def row_chunks(total, count):
    cuts = [16 * (total // 16 * i // count) for i in range(count)] + [total]
    return [(cuts[i], cuts[i + 1] - cuts[i]) for i in range(count)]


class Marker:
    def __init__(self):
        self.scope = None

    def __call__(self, name):
        if self.scope is not None:
            self.scope.__exit__(None, None, None)
        self.scope = None
        if name:
            self.scope = jax.named_scope(name)
            self.scope.__enter__()


def kernel(cfg, lens_hbm, hidden, k_hbm, v_hbm, g_attn, g_final, wq_hbm, w_key, w_value, w_gate, w_up,
           w_out, w_down, embed, freq_hbm,
           k_out, v_out, logits_out, norm_out,
           k_buf, v_buf, h_buf, ga_buf, gf_buf, wqt, wq_buf, gu_buf, down_buf, out_buf, kv_buf,
           n_all, q_scr, qx_buf, q2d, snew, krep, vrep, s_scr, od_scr, o_scr, ox_buf, act_scr, act, part_scr,
           pre_buf, rs_scr, rs_buf, f_buf, e_buf, z_scr, st_scr, k_scr, v_scr, norm_scr, s_buf,
           lens, w_query, freq,
           kv_sem, e_own_sem, z_sem, x_send, x_recv, g_send, g_recv, g_last, y_send, y_recv, e_send, e_recv,
           n_recv, n_last, n_send, pre_sem, rs_sem, fxa, fyb, fya, fxb, f_sem, s_sem):
    ys, xs, own, vocab, shift = cfg
    mark = Marker()
    y = lax.axis_index("yax")
    x = lax.axis_index("xax")
    core = lax.rem(x, 2)
    partner = x + 1 - 2 * core
    blk = hidden.shape[1]
    quarter = xs * own
    head_dim = k_hbm.shape[1]
    half = head_dim // 2
    seqs = k_hbm.shape[0]
    slots = k_hbm.shape[2]
    heads = w_query.shape[1] * ys // head_dim
    groups = k_buf.shape[0]
    per = seqs // groups
    window = e_buf.shape[0]

    def lanes(i):
        return pl.ds(pl.multiple_of(i * blk, 128), blk)

    def rows(i, n):
        return pl.ds(pl.multiple_of(i * n, n), n)

    mark("a0start")
    barrier = pltpu.get_barrier_semaphore()

    def signal_row(d, carry):
        pl.semaphore_signal(barrier, inc=1, device_id={"xax": lax.rem(x + d, xs)},
                            device_id_type=pl.DeviceIdType.MESH)
        return carry
    lax.fori_loop(1, xs, signal_row, 0)

    def signal_column(d, carry):
        pl.semaphore_signal(barrier, inc=1, device_id={"yax": lax.rem(y + d, ys)},
                            device_id_type=pl.DeviceIdType.MESH)
        return carry
    lax.fori_loop(1, ys, signal_column, 0)
    small_ins = [pltpu.make_async_copy(a, b, z_sem.at[i])
                 for i, (a, b) in enumerate(((wq_hbm, w_query), (freq_hbm, freq), (lens_hbm, lens)))]
    for copy in small_ins:
        copy.start()
    def cache_copy(g, src, dst, s):
        return pltpu.make_async_copy(src.at[pl.ds(g * per, per)], dst.at[g], kv_sem.at[s, g])

    def start_cache(g, carry):
        cache_copy(g, k_hbm, k_buf, 0).start()
        return carry
    lax.fori_loop(0, groups, start_cache, 0)

    for copy in small_ins:
        copy.wait()
    wqt[...] = w_query[...].astype(F32).T.astype(BF16)

    mark("a0wait")
    pl.semaphore_wait(barrier, xs + ys - 2)

    def arrived(ref, sem):
        pltpu.make_async_copy(ref, ref, sem).wait()

    cols = wqt.shape[0] // xs
    ff = w_gate.shape[1] // xs
    most = pl.ds(0, (xs - 1) * blk)
    x_kinds = {
        "wq": (lambda p: wqt.at[rows(p, cols), :], lambda s: wq_buf.at[y, :, lanes(s)],
               wq_buf.at[y], wq_buf.at[y, :, most]),
        "wo": (lambda p: w_out.at[rows(p, cols), :], lambda s: out_buf.at[y, :, lanes(s)],
               out_buf.at[y], out_buf.at[y, :, most]),
        "down": (lambda p: w_down.at[rows(p, ff), :], lambda s: down_buf.at[y, :, lanes(s)],
                 down_buf.at[y], down_buf.at[y, :, most]),
        "gate": (lambda p: w_gate.at[:, lanes(p)], lambda s: gu_buf.at[rows(s, blk), pl.ds(0, ff)],
                 gu_buf.at[:, pl.ds(0, ff)], gu_buf.at[most, pl.ds(0, ff)]),
        "up": (lambda p: w_up.at[:, lanes(p)], lambda s: gu_buf.at[rows(s, blk), pl.ds(ff, ff)],
               gu_buf.at[:, pl.ds(ff, ff)], gu_buf.at[most, pl.ds(ff, ff)]),
        "q": (lambda p: q_scr.at[rows(p, own), :], lambda s: qx_buf.at[s],
              qx_buf, qx_buf.at[pl.ds(0, xs - 1)]),
        "o": (lambda p: o_scr.at[p], lambda s: ox_buf.at[rows(s, own), :],
              ox_buf, ox_buf.at[pl.ds(0, (xs - 1) * own), :]),
    }
    x_index = {name: i for i, name in enumerate(x_kinds)}

    def x_start(name):
        src, dst = x_kinds[name][:2]
        k = x_index[name]

        def body(d, carry):
            p = lax.rem(x + d, xs)
            pltpu.make_async_remote_copy(
                src_ref=src(p), dst_ref=dst(x), send_sem=x_send.at[k], recv_sem=x_recv.at[k],
                device_id={"xax": p}, device_id_type=pl.DeviceIdType.MESH).start()
            return carry
        lax.fori_loop(1, xs, body, 0)
        pltpu.make_async_copy(src(x), dst(x), x_recv.at[k]).start()

    def x_wait(name):
        arrived(x_kinds[name][2], x_recv.at[x_index[name]])

    def x_drain(name):
        arrived(x_kinds[name][3], x_send.at[x_index[name]])

    chips = xs // 2
    g_kinds = {
        "hidden": (hidden.at[rows(y, quarter), :], lambda s: h_buf.at[:, lanes(s)], h_buf),
        "ga": (g_attn, lambda s: ga_buf.at[:, lanes(s)], ga_buf),
        "gf": (g_final, lambda s: gf_buf.at[:, lanes(s)], gf_buf),
        "wk": (w_key, lambda s: kv_buf.at[pl.ds(0, head_dim), lanes(s)], kv_buf.at[pl.ds(0, head_dim), :]),
        "wv": (w_value, lambda s: kv_buf.at[pl.ds(head_dim, head_dim), lanes(s)],
               kv_buf.at[pl.ds(head_dim, head_dim), :]),
    }
    g_index = {name: i for i, name in enumerate(g_kinds)}

    def g_copy(name, i, sender):
        src, dst, _ = g_kinds[name]
        k = g_index[name]
        return pltpu.make_async_remote_copy(
            src_ref=src, dst_ref=dst(sender), send_sem=g_send.at[k], recv_sem=g_recv.at[k, i],
            device_id={"xax": lax.rem(x + 2 * i, xs)}, device_id_type=pl.DeviceIdType.MESH)

    def g_pass(name, sender, source):
        k = g_index[name]
        return pltpu.make_async_remote_copy(
            src_ref=source, dst_ref=g_kinds[name][1](sender), send_sem=g_send.at[k], recv_sem=g_last.at[k],
            device_id={"xax": partner}, device_id_type=pl.DeviceIdType.MESH)

    def g_start(name):
        def body(i, carry):
            g_copy(name, i, x).start()
            return carry
        lax.fori_loop(1, chips, body, 0)
        src, dst, _ = g_kinds[name]
        g_pass(name, x, src).start()
        pltpu.make_async_copy(src, dst(x), g_last.at[g_index[name]]).start()

    def g_forward(name):
        def body(i, carry):
            sender = lax.rem(x + xs - 2 * i, xs)
            g_copy(name, i, sender).wait_recv()
            g_pass(name, sender, g_kinds[name][1](sender)).start()
            return carry
        lax.fori_loop(1, chips, body, 0)

    def g_wait(name):
        whole = g_kinds[name][2]
        arrived(whole.at[:, pl.ds(0, (chips + 1) * blk)], g_last.at[g_index[name]])

    def g_drain(name):
        arrived(g_kinds[name][2].at[:, most], g_send.at[g_index[name]])

    y_kinds = {"wq": wq_buf, "wo": out_buf, "down": down_buf}
    y_index = {name: i for i, name in enumerate(y_kinds)}
    others = pl.ds(0, ys - 1)

    def y_start(name):
        buf = y_kinds[name]
        k = y_index[name]

        def body(d, carry):
            pltpu.make_async_remote_copy(
                src_ref=buf.at[y], dst_ref=buf.at[y], send_sem=y_send.at[k], recv_sem=y_recv.at[k],
                device_id={"yax": lax.rem(y + d, ys)}, device_id_type=pl.DeviceIdType.MESH).start()
            return carry
        lax.fori_loop(1, ys, body, 0)

    def y_wait(name):
        arrived(y_kinds[name].at[others], y_recv.at[y_index[name]])

    def y_drain(name):
        arrived(y_kinds[name].at[others], y_send.at[y_index[name]])

    e_parts = row_chunks(window, EMBED_CHUNKS)

    def e_first(p):
        return p * vocab - lax.rem(p, 2) * shift

    def e_own():
        return pltpu.make_async_copy(
            embed.at[pl.ds(pl.multiple_of(e_first(x), 8), window), :], e_buf.at[:, lanes(x)], e_own_sem)

    def e_start(c):
        r0, n = e_parts[c]

        def body(d, carry):
            p = lax.rem(x + d, xs)
            pltpu.make_async_remote_copy(
                src_ref=embed.at[pl.ds(pl.multiple_of(e_first(p) + r0, 8), n), :],
                dst_ref=e_buf.at[pl.ds(r0, n), lanes(x)], send_sem=e_send,
                recv_sem=e_recv.at[int(c >= EMBED_FIRST)],
                device_id={"xax": p}, device_id_type=pl.DeviceIdType.MESH).start()
            return carry
        lax.fori_loop(1, xs, body, 0)

    mark("a1send")
    x_start("wq")
    for name in ("hidden", "ga"):
        g_start(name)
    for name in ("wo", "down"):
        x_start(name)
    for name in ("wk", "wv", "gf"):
        g_start(name)
    e_start(0)
    e_own().start()

    def start_cache_v(g, carry):
        cache_copy(g, v_hbm, v_buf, 1).start()
        return carry
    lax.fori_loop(0, groups, start_cache_v, 0)

    mark("a2wqx")
    x_wait("wq")
    y_start("wq")
    mark("a3hfwd")
    for name in ("hidden", "ga"):
        g_forward(name)
    mark("a4hwait")
    for name in ("hidden", "ga"):
        g_wait(name)
    mark("a5ln")
    my_rows = rows(y, quarter)
    n_all[my_rows, :] = layer_norm(h_buf[...].astype(F32), ga_buf[...]).astype(BF16)

    part = quarter // 2

    def n_rows(j, c):
        return pl.ds(pl.multiple_of(j * quarter + c * part, part), part)

    def n_copy(d, sender):
        r = n_rows(sender, core)
        return pltpu.make_async_remote_copy(
            src_ref=n_all.at[r, :], dst_ref=n_all.at[r, :], send_sem=n_send.at[0],
            recv_sem=n_recv.at[d], device_id={"yax": lax.rem(y + d, ys)},
            device_id_type=pl.DeviceIdType.MESH)

    def n_pass(d, c):
        r = n_rows(lax.rem(y + ys - d, ys), c)
        return pltpu.make_async_remote_copy(
            src_ref=n_all.at[r, :], dst_ref=n_all.at[r, :], send_sem=n_send.at[1],
            recv_sem=n_last.at[d], device_id={"xax": partner},
            device_id_type=pl.DeviceIdType.MESH)

    mark("a6wo")
    x_wait("wo")
    y_start("wo")
    mark("a6wqy")
    y_wait("wq")
    mark("a7q")
    wq_all = wq_buf[...].reshape(ys * cols, xs * blk)
    q_scr[...] = lax.dot_general(n_all[my_rows, :], wq_all, NT, preferred_element_type=F32).astype(BF16)
    mark("a8send")
    x_start("q")
    x_start("gate")
    x_start("up")

    def n_start(d, carry):
        n_copy(d, y).start()
        return carry
    lax.fori_loop(1, ys, n_start, 0)
    mark("b0down")
    x_wait("down")
    y_start("down")
    for c in range(1, 7):
        e_start(c)

    mark("b1kv")
    row_id = lax.broadcasted_iota(jnp.int32, (own, 4 * half), 0)
    first_row = (y * xs + x) * own
    position = jnp.zeros((own, 4 * half), jnp.int32)
    for b in range(own):
        position = jnp.where(row_id == b, lens[first_row + b], position)
    angle = position.astype(F32) * freq[...]
    cos_a = jnp.cos(angle)
    sin_a = jnp.sin(angle)
    for name in ("wk", "wv", "gf"):
        g_forward(name)
    for name in ("wk", "wv", "gf"):
        g_wait(name)
    mine = y * xs + x
    n_own = n_all[rows(mine, own), :]
    kv = lax.dot_general(n_own, kv_buf[...], NT, preferred_element_type=F32).astype(BF16).astype(F32)
    k1 = kv[:, :half]
    k2 = kv[:, half:head_dim]
    c1 = cos_a[:, :half]
    s1 = sin_a[:, :half]
    key = jnp.concatenate([k1 * c1 - k2 * s1, k2 * c1 + k1 * s1], axis=1).astype(BF16)
    value = kv[:, head_dim:].astype(BF16)
    k_scr[...] = key
    v_scr[...] = value
    small_outs = [pltpu.make_async_copy(k_scr, k_out, z_sem.at[0]),
                  pltpu.make_async_copy(v_scr, v_out, z_sem.at[1])]
    for copy in small_outs:
        copy.start()
    for h in range(heads):
        krep[pl.ds(h, own, stride=heads), :] = key.astype(F32)
        vrep[pl.ds(h, own, stride=heads), :] = value.astype(F32)

    mark("b2q")
    x_wait("q")
    mark("b3rot")
    for xc in range(xs // 2):
        qa = qx_buf[2 * xc].astype(F32)
        qb = qx_buf[2 * xc + 1].astype(F32)
        ra = (qa * cos_a - qb * sin_a).astype(BF16).astype(F32)
        rb = (qb * cos_a + qa * sin_a).astype(BF16).astype(F32)
        for yc in range(ys):
            pair = jnp.concatenate([ra[:, yc * half:(yc + 1) * half], rb[:, yc * half:(yc + 1) * half]], axis=1)
            q2d[pl.ds(xc * ys + yc, own, stride=heads), :] = pair
    scale = head_dim ** -0.5
    snew[...] = jnp.sum(q2d[...] * krep[...], axis=1, keepdims=True) * scale

    mark("b4attn")
    gr = per * heads
    seg_r = lax.broadcasted_iota(jnp.int32, (gr, per * head_dim), 0) // heads
    seg_c = lax.broadcasted_iota(jnp.int32, (gr, per * head_dim), 1) // head_dim
    diag = (seg_r == seg_c).astype(F32)
    tile = min(512, slots)
    row_g = lax.broadcasted_iota(jnp.int32, (gr, 1), 0) // heads
    lane_g = lax.broadcasted_iota(jnp.int32, (gr, tile), 1)

    def attend(g, carry):
        cache_copy(g, k_hbm, k_buf, 0).wait()
        qg = q2d[rows(g, gr), :]
        qbd = (jnp.concatenate([qg] * per, axis=1) * diag).astype(BF16)
        len_g = jnp.zeros((gr, 1), jnp.int32)
        for s in range(per):
            len_g = jnp.where(row_g == s, lens[first_row + g * per + s], len_g)
        new = snew[rows(g, gr), :]
        top = jnp.full((gr, tile), -jnp.inf, F32)
        kg = k_buf.at[g]
        vg = v_buf.at[g]
        for c in range(slots // tile):
            kc = kg[:, :, pl.ds(c * tile, tile)].reshape(per * head_dim, tile)
            sc = jnp.dot(qbd, kc, preferred_element_type=F32) * scale
            sc = jnp.where(lane_g < len_g - c * tile, sc, -jnp.inf)
            s_scr[:, pl.ds(c * tile, tile)] = sc
            top = jnp.maximum(top, sc)
        row_max = jnp.maximum(jnp.max(top, axis=1, keepdims=True), new)
        total = jnp.zeros((gr, tile), F32)
        for c in range(slots // tile):
            ex = jnp.exp(s_scr[:, pl.ds(c * tile, tile)] - row_max)
            s_scr[:, pl.ds(c * tile, tile)] = ex
            total = total + ex
        w_new = jnp.exp(new - row_max)
        den = jnp.sum(total, axis=1, keepdims=True) + w_new
        inv = 1.0 / den
        cache_copy(g, v_hbm, v_buf, 1).wait()
        mixed = jnp.zeros((gr, per * head_dim), F32)
        for c in range(slots // tile):
            pr = (s_scr[:, pl.ds(c * tile, tile)] * inv).astype(BF16)
            vc = vg[:, :, pl.ds(c * tile, tile)].reshape(per * head_dim, tile)
            mixed = mixed + lax.dot_general(pr, vc, NT, preferred_element_type=F32)
        add = (w_new * inv).astype(BF16).astype(F32) * vrep[rows(g, gr), :]
        for s in range(per):
            od_scr[pl.ds(pl.multiple_of(g * gr + s * heads, heads), heads), :] = (
                mixed[s * heads:(s + 1) * heads, s * head_dim:(s + 1) * head_dim]
                + add[s * heads:(s + 1) * heads, :])
        return carry

    lax.fori_loop(0, groups, attend, 0)
    mark("b5o")
    for xc in range(xs // 2):
        parts = [od_scr[pl.ds(xc * ys + yc, own, stride=heads), :] for yc in range(ys)]
        o_scr[2 * xc] = jnp.concatenate([p[:, :half] for p in parts], axis=1).astype(BF16)
        o_scr[2 * xc + 1] = jnp.concatenate([p[:, half:] for p in parts], axis=1).astype(BF16)
    x_start("o")
    for c in range(7, 12):
        e_start(c)

    def act_copy(dest):
        return pltpu.make_async_remote_copy(
            src_ref=act_scr.at[dest], dst_ref=act.at[:, pl.ds(pl.multiple_of(y * ff, ff), ff)],
            send_sem=y_send.at[len(y_kinds)], recv_sem=y_recv.at[len(y_kinds)],
            device_id={"yax": dest}, device_id_type=pl.DeviceIdType.MESH)

    mark("b6gu")
    x_wait("gate")
    x_wait("up")

    mark("b7feed")
    def feed(d, carry):
        @pl.when(d < ys - 1)
        def _():
            n_copy(d + 1, lax.rem(y + ys - d - 1, ys)).wait_recv()
            n_pass(d + 1, core).start()
        j = lax.rem(y + ys - d, ys)

        @pl.when(d > 0)
        def _():
            n_pass(d, 1 - core).wait_recv()
        gu = jnp.dot(n_all[rows(j, quarter), :], gu_buf[...], preferred_element_type=F32)
        gu = gu.astype(BF16).astype(F32)
        gate = gu[:, :ff]
        act_scr[j] = (gate * jax.nn.sigmoid(gate) * gu[:, ff:]).astype(BF16)

        @pl.when(d > 0)
        def _():
            act_copy(j).start()
        return carry
    lax.fori_loop(0, ys, feed, 0)
    act[:, pl.ds(pl.multiple_of(y * ff, ff), ff)] = act_scr[y]
    mark("b8wo")
    y_wait("wo")
    mark("b9o")
    x_wait("o")
    mark("c0op")
    part_scr[...] = jnp.dot(
        ox_buf[...], out_buf[...].reshape(ys * cols, xs * blk), preferred_element_type=F32)
    mark("c1down")
    y_wait("down")

    mark("c2act")
    arrived(act_scr.at[others], y_recv.at[len(y_kinds)])

    mark("c3branch")
    down_all = down_buf[...].reshape(ys * ff, xs * blk)
    part_scr[...] = part_scr[...] + jnp.dot(act[...], down_all, preferred_element_type=F32)

    def branch(c):
        for i in range(chips):
            rs_scr[c, i] = part_scr[pl.ds(pl.multiple_of((2 * i + c) * own, own), own), :]

    def pre_copy():
        return pltpu.make_async_remote_copy(
            src_ref=rs_scr.at[1 - core], dst_ref=pre_buf, send_sem=pre_sem.at[0], recv_sem=pre_sem.at[1],
            device_id={"xax": partner}, device_id_type=pl.DeviceIdType.MESH)

    def rs_copy(dest):
        return pltpu.make_async_remote_copy(
            src_ref=rs_scr.at[core, dest], dst_ref=rs_buf.at[chip], send_sem=rs_sem.at[0],
            recv_sem=rs_sem.at[1], device_id={"xax": 2 * dest + core},
            device_id_type=pl.DeviceIdType.MESH)

    chip = x // 2
    branch(1 - core)
    pre_copy().start()
    branch(core)
    mark("c4pre")
    pre_copy().wait_recv()
    rs_scr[core] = rs_scr[core] + pre_buf[...]

    mark("c5rs")
    def rs_start(i, carry):
        rs_copy(lax.rem(chip + i, chips)).start()
        return carry
    lax.fori_loop(1, chips, rs_start, 0)
    e_start(12)
    mark("c6rsw")
    arrived(rs_buf.at[pl.ds(0, chips - 1)], rs_sem.at[1])
    mark("c7ln")
    rs_buf[chip] = rs_scr[core, chip]
    res = h_buf[rows(x, own), :].astype(F32) + jnp.sum(rs_buf[...], axis=0)
    f_buf[rows(mine, own), :] = layer_norm(res, gf_buf[...]).astype(BF16)

    piece = own // 2

    def f_half(sy, sx, h):
        return f_buf.at[pl.ds(pl.multiple_of((sy * xs + sx) * own + h * piece, piece), piece), :]

    def f_over_x(i, h, sy, sx, sem):
        return pltpu.make_async_remote_copy(
            src_ref=f_half(sy, sx, h), dst_ref=f_half(sy, sx, h), send_sem=f_sem.at[0], recv_sem=sem,
            device_id={"xax": lax.rem(x + 2 * i, xs)}, device_id_type=pl.DeviceIdType.MESH)

    def f_over_y(d, h, sy, sx, sem):
        return pltpu.make_async_remote_copy(
            src_ref=f_half(sy, sx, h), dst_ref=f_half(sy, sx, h), send_sem=f_sem.at[0], recv_sem=sem,
            device_id={"yax": lax.rem(y + d, ys)}, device_id_type=pl.DeviceIdType.MESH)

    def f_pass(d, h, sy, sx):
        pltpu.make_async_remote_copy(
            src_ref=f_half(sy, sx, h), dst_ref=f_half(sy, sx, h), send_sem=f_sem.at[1],
            recv_sem=f_sem.at[2 + d], device_id={"xax": partner},
            device_id_type=pl.DeviceIdType.MESH).start()

    def from_y(d):
        return lax.rem(y + ys - d, ys)

    def from_x(i):
        return lax.rem(x + xs - 2 * i, xs)

    def spread_y(i):
        def body(d, carry):
            f_over_y(d, 0, y, from_x(i), fya.at[d, i]).start()
            return carry
        lax.fori_loop(1, ys, body, 0)

    def spread_x(d):
        def body(i, carry):
            f_over_x(i, 1, from_y(d), x, fxb.at[d, i]).start()
            return carry
        lax.fori_loop(1, chips, body, 0)

    mark("c8fx")
    def first_x(i, carry):
        f_over_x(i, 0, y, x, fxa.at[i]).start()
        return carry
    lax.fori_loop(1, chips, first_x, 0)

    def first_y(d, carry):
        f_over_y(d, 1, y, x, fyb.at[d]).start()
        return carry
    lax.fori_loop(1, ys, first_y, 0)
    spread_y(0)
    spread_x(0)
    f_pass(0, 0, y, x)
    f_pass(0, 1, y, x)
    e_start(13)
    mark("c9sp")
    for i in range(1, max(chips, ys)):
        if i < chips:
            f_over_x(i, 0, y, from_x(i), fxa.at[i]).wait_recv()
            spread_y(i)
            f_pass(0, 0, y, from_x(i))
        if i < ys:
            f_over_y(i, 1, from_y(i), x, fyb.at[i]).wait_recv()
            spread_x(i)
            f_pass(i, 1, from_y(i), x)
    for c in range(14, EMBED_CHUNKS):
        e_start(c)

    def collect(d):
        def body(i, carry):
            @pl.when(d > 0)
            def _():
                f_over_y(d, 0, from_y(d), from_x(i), fya.at[d, i]).wait_recv()
                f_pass(d, 0, from_y(d), from_x(i))

            @pl.when(i > 0)
            def _():
                f_over_x(i, 1, from_y(d), from_x(i), fxb.at[d, i]).wait_recv()
                f_pass(d, 1, from_y(d), from_x(i))
            return carry
        lax.fori_loop(0, chips, body, 0)

    mark("d0drain")
    for name in x_kinds:
        x_drain(name)
    for name in g_kinds:
        g_drain(name)
    for name in y_kinds:
        y_drain(name)
    arrived(act_scr.at[others], y_send.at[len(y_kinds)])
    for i in range(2):
        arrived(n_all.at[pl.ds(0, (ys - 1) * part), :], n_send.at[i])
    pre_copy().wait_send()
    arrived(rs_buf.at[pl.ds(0, chips - 1)], rs_sem.at[0])
    for copy in small_outs:
        copy.wait()

    cut = e_parts[EMBED_FIRST][0]
    skip = core * shift
    half_block = pl.ds(0, chips * own)

    def nearest(k):
        return k + k // 2 * (1 - 2 * lax.rem(k, 2))

    def z_copy(j, r0, n):
        return pltpu.make_async_copy(
            z_scr.at[j, pl.ds(r0, n), :], logits_out.at[pl.ds(r0, n), rows(j, quarter)], z_sem.at[2])

    def block(j, r0, n, pieces):
        r = pl.ds(r0, n)
        z_scr[j, r, :] = lax.dot_general(e_buf[r, :], f_buf[rows(j, quarter), :], NT, preferred_element_type=F32)
        z_copy(j, r0, n).start()
        stats = []
        for q0, m in row_chunks(n, pieces):
            z = z_scr[j, pl.ds(r0 + q0, m), :]
            if shift and (r0 + q0 == 0 or r0 + q0 + m == window):
                index = lax.broadcasted_iota(jnp.int32, z.shape, 0) + (r0 + q0)
                z = jnp.where(jnp.logical_and(index >= skip, index < skip + vocab), z, -jnp.inf)
            top = jnp.max(z, axis=0, keepdims=True)
            stats.append((top, jnp.sum(jnp.exp(z - top), axis=0, keepdims=True)))
        return stats

    def put(j, stats):
        top = functools.reduce(jnp.maximum, [t for t, _ in stats])
        st_scr[0:1, rows(j, quarter)] = top
        st_scr[1:2, rows(j, quarter)] = sum(t * jnp.exp(m - top) for m, t in stats)

    def head(k, carry):
        d = nearest(k)
        j = from_y(d)
        with jax.named_scope('hw'):
            arrived(f_buf.at[half_block, :], f_sem.at[2 + d])
        put(j, block(j, 0, cut, 4))

        @pl.when(k < ys - 2)
        def _():
            collect(nearest(k + 2))
        return carry

    def head_rest(j, carry):
        before = (st_scr[0:1, rows(j, quarter)], st_scr[1:2, rows(j, quarter)])
        put(j, [before] + block(j, cut, window - cut, 1))
        return carry

    mark("d1coll")
    for k in range(min(2, ys)):
        collect(nearest(k))
    mark("d1e")
    e_own().wait()
    arrived(e_buf.at[pl.ds(0, cut), most], e_recv.at[0])

    mark("d3head")
    lax.fori_loop(0, ys, head, 0)
    mark("d3rest")
    arrived(e_buf.at[pl.ds(cut, window - cut), most], e_recv.at[1])
    mark("d3hr")
    lax.fori_loop(0, ys, head_rest, 0)

    mark("d4stat")
    for k in range(ys):
        dy = (ys // 2 + k) % ys
        for dx in range(xs):
            if dy + dx > 0:
                pltpu.make_async_remote_copy(
                    src_ref=st_scr, dst_ref=s_buf.at[mine], send_sem=s_sem.at[0], recv_sem=s_sem.at[1],
                    device_id={"yax": lax.rem(y + dy, ys), "xax": lax.rem(x + dx, xs)},
                    device_id_type=pl.DeviceIdType.MESH).start()
    s_buf[mine] = st_scr[...]

    mark("d5sx")
    arrived(e_buf.at[:, most], e_send)
    arrived(f_buf.at[pl.ds(0, 2 * (ys * chips - 1) * piece), :], f_sem.at[0])
    arrived(f_buf.at[pl.ds(0, ys * chips * own), :], f_sem.at[1])
    arrived(z_scr, z_sem.at[2])
    everyone = s_buf.at[pl.ds(0, ys * xs - 1)]
    mark("d6sw")
    arrived(everyone, s_sem.at[1])
    tops = s_buf[:, 0, :]
    best = jnp.max(tops, axis=0, keepdims=True)
    whole = jnp.sum(s_buf[:, 1, :] * jnp.exp(tops - best), axis=0, keepdims=True)
    mark("d9n")
    norm_scr[...] = best + jnp.log(whole)
    norm_copy = pltpu.make_async_copy(norm_scr, norm_out, z_sem.at[0])
    norm_copy.start()
    arrived(everyone, s_sem.at[0])
    norm_copy.wait()
    mark(None)


def finish_kernel(shift, z_hbm, norm_hbm, key, value, out_hbm, k_out, v_out, norm_out,
                  z_buf, o_buf, norm, k_scr, v_scr, in_sem, out_sem):
    count, n, width = o_buf.shape

    def load(i):
        return pltpu.make_async_copy(z_hbm.at[:, pl.ds(i * width, width)], z_buf.at[i], in_sem.at[i])

    def save(i):
        return pltpu.make_async_copy(o_buf.at[i], out_hbm.at[:, pl.ds(i * width, width)], out_sem.at[i])

    small = ((norm_hbm, norm, norm_out), (key, k_scr, k_out), (value, v_scr, v_out))
    small_in = [pltpu.make_async_copy(a, b, in_sem.at[count + i]) for i, (a, b, _) in enumerate(small)]
    small_out = [pltpu.make_async_copy(b, c, out_sem.at[count + i]) for i, (_, b, c) in enumerate(small)]
    small_in[0].start()
    for i in range(count):
        load(i).start()
    for copy in small_in[1:]:
        copy.start()
    small_in[0].wait()
    small_out[0].start()
    odd = lax.rem(lax.axis_index("xax"), 2) == 1
    for i in range(count):
        row = norm[:, pl.ds(i * width, width)]
        load(i).wait()
        if shift:
            @pl.when(odd)
            def _():
                o_buf[i] = z_buf[i, pl.ds(shift, n), :] - row

            @pl.when(jnp.logical_not(odd))
            def _():
                o_buf[i] = z_buf[i, pl.ds(0, n), :] - row
        else:
            o_buf[i] = z_buf[i] - row
        save(i).start()
    for i in (1, 2):
        small_in[i].wait()
        small_out[i].start()
    for copy in small_out:
        copy.wait()
    for i in range(count):
        save(i).wait()


def solution(mesh):
    ys = mesh.shape["yax"]
    xs = mesh.shape["xax"]
    row_spec = P(("dp", "yax", "xax"))

    def local_step(hidden, cache_len, k_cache, v_cache, g_attn, w_query, w_key, w_value,
                   w_gate, w_up, w_out, w_down, g_final, embedding):
        batch, blk = hidden.shape
        own, slots, head_dim = k_cache.shape
        width = blk * xs
        vocab = embedding.shape[0] // xs
        shift = vocab % 8
        window = -(-vocab // 8) * 8
        half = head_dim // 2
        quarter = xs * own
        cols = w_query.shape[1] // xs
        ff = w_gate.shape[1] // xs
        heads = w_query.shape[1] * ys // head_dim
        per = 4
        groups = own // per
        freq_row = (ROPE_BASE ** (-(np.arange(half, dtype=np.float32) * 2.0) / head_dim)).astype(np.float32)
        freq = jnp.asarray(np.tile(freq_row, 4)[None, :])
        any_spec = pl.BlockSpec(memory_space=pl.ANY)
        dma = pltpu.SemaphoreType.DMA
        chips = xs // 2
        scratch = [
            pltpu.VMEM((groups, per, head_dim, slots), BF16),
            pltpu.VMEM((groups, per, head_dim, slots), BF16),
            pltpu.VMEM((quarter, width), BF16),
            pltpu.VMEM((1, width), F32),
            pltpu.VMEM((1, width), F32),
            pltpu.VMEM((w_query.shape[1], blk), BF16),
            pltpu.VMEM((ys, cols, width), BF16),
            pltpu.VMEM((width, 2 * ff), BF16),
            pltpu.VMEM((ys, ff, width), BF16),
            pltpu.VMEM((ys, cols, width), BF16),
            pltpu.VMEM((2 * head_dim, width), BF16),
            pltpu.VMEM((batch, width), BF16),
            pltpu.VMEM((quarter, ys * cols), BF16),
            pltpu.VMEM((xs, own, ys * cols), BF16),
            pltpu.VMEM((own * heads, head_dim), F32),
            pltpu.VMEM((own * heads, 1), F32),
            pltpu.VMEM((own * heads, head_dim), F32),
            pltpu.VMEM((own * heads, head_dim), F32),
            pltpu.VMEM((per * heads, slots), F32),
            pltpu.VMEM((own * heads, head_dim), F32),
            pltpu.VMEM((xs, own, ys * cols), BF16),
            pltpu.VMEM((quarter, ys * cols), BF16),
            pltpu.VMEM((ys, quarter, ff), BF16),
            pltpu.VMEM((quarter, ys * ff), BF16),
            pltpu.VMEM((quarter, width), F32),
            pltpu.VMEM((chips, own, width), F32),
            pltpu.VMEM((2, chips, own, width), F32),
            pltpu.VMEM((chips, own, width), F32),
            pltpu.VMEM((batch, width), BF16),
            pltpu.VMEM((window, width), BF16),
            pltpu.VMEM((ys, window, quarter), F32),
            pltpu.VMEM((2, batch), F32),
            pltpu.VMEM((own, head_dim), BF16),
            pltpu.VMEM((own, head_dim), BF16),
            pltpu.VMEM((1, batch), F32),
            pltpu.VMEM((ys * xs, 2, batch), F32),
            pltpu.SMEM(cache_len.shape, jnp.int32),
            pltpu.VMEM(w_query.shape, BF16),
            pltpu.VMEM((1, 4 * half), F32),
            dma((2, groups)), dma, dma((3,)), dma((7,)), dma((7,)),
            dma((5,)), dma((5, chips)), dma((5,)), dma((4,)), dma((4,)), dma, dma((2,)),
            dma((ys,)), dma((ys,)), dma((2,)), dma((2,)), dma((2,)),
            dma((chips,)), dma((ys,)), dma((ys, chips)), dma((ys, chips)), dma((2 + ys,)), dma((2,)),
        ]
        cfg = (ys, xs, own, vocab, shift)
        key_new, value_new, logits, norm = pl.pallas_call(
            functools.partial(kernel, cfg),
            name="decode_layer",
            out_shape=(
                jax.ShapeDtypeStruct((own, head_dim), BF16),
                jax.ShapeDtypeStruct((own, head_dim), BF16),
                jax.ShapeDtypeStruct((window, batch), F32),
                jax.ShapeDtypeStruct((1, batch), F32)),
            in_specs=[any_spec] * 15,
            out_specs=(any_spec, any_spec, any_spec, any_spec),
            scratch_shapes=scratch,
            compiler_params=pltpu.CompilerParams(
                collective_id=0, has_side_effects=True, vmem_limit_bytes=67043328),
        )(cache_len, hidden, k_cache.transpose(0, 2, 1), v_cache.transpose(0, 2, 1),
          g_attn[None, :], g_final[None, :], w_query, w_key.T, w_value.T, w_gate, w_up, w_out, w_down,
          embedding, freq)
        count = 8
        log_probs, key_new, value_new, norm = pl.pallas_call(
            functools.partial(finish_kernel, shift),
            name="finish",
            out_shape=(
                jax.ShapeDtypeStruct((vocab, batch), F32),
                jax.ShapeDtypeStruct((own, head_dim), BF16),
                jax.ShapeDtypeStruct((own, head_dim), BF16),
                jax.ShapeDtypeStruct((1, batch), F32)),
            in_specs=[any_spec] * 4,
            out_specs=(any_spec,) * 4,
            scratch_shapes=[
                pltpu.VMEM((count, window, batch // count), F32),
                pltpu.VMEM((count, vocab, batch // count), F32),
                pltpu.VMEM((1, batch), F32), pltpu.VMEM((own, head_dim), BF16), pltpu.VMEM((own, head_dim), BF16),
                dma((count + 3,)), dma((count + 3,))],
        )(logits, norm, key_new, value_new)
        return key_new, value_new, log_probs.T, norm[0]

    in_specs = (P("dp", "xax"), P("dp"), row_spec, row_spec, P("xax"), P("xax", "yax"),
                P("xax", None), P("xax", None), P("xax", "yax"), P("xax", "yax"),
                P("yax", "xax"), P("yax", "xax"), P("xax"), P("yax", "xax"))
    out_specs = (row_spec, row_spec, P("dp", ("yax", "xax")), P("dp"))
    return jax.shard_map(local_step, mesh=mesh, in_specs=in_specs, out_specs=out_specs, check_vma=False)
```

```python
import functools

import jax
import jax.numpy as jnp
import numpy as np
from jax import lax
from jax.experimental import pallas as pl
from jax.experimental.pallas import tpu as pltpu
from jax.sharding import PartitionSpec as P

EPS = 1e-6
ROPE_BASE = 10000.0
F32 = jnp.float32
BF16 = jnp.bfloat16
NT = (((1,), (1,)), ((), ()))
EMBED_CHUNKS = 16
EMBED_FIRST = 14


def layer_norm(values_in, gain):
    mean = jnp.mean(values_in, axis=-1, keepdims=True)
    centred = values_in - mean
    var = jnp.mean(centred * centred, axis=-1, keepdims=True)
    return centred * lax.rsqrt(var + EPS) * gain


def row_chunks(total, count):
    cuts = [16 * (total // 16 * i // count) for i in range(count)] + [total]
    return [(cuts[i], cuts[i + 1] - cuts[i]) for i in range(count)]


def kernel(cfg, lens_hbm, hidden, k_hbm, v_hbm, g_attn, g_final, wq_hbm, w_key, w_value, w_gate, w_up,
           w_out, w_down, embed, freq_hbm,
           k_out, v_out, logits_out, norm_out,
           k_buf, v_buf, h_buf, ga_buf, gf_buf, wqt, wq_buf, gu_buf, down_buf, out_buf, kv_buf,
           n_all, q_scr, qx_buf, q2d, snew, krep, vrep, s_scr, od_scr, o_scr, ox_buf, act_scr, act, part_scr,
           pre_buf, rs_scr, rs_buf, f_buf, e_buf, z_scr, st_scr, k_scr, v_scr, norm_scr, s_buf,
           lens, w_query, freq,
           kv_sem, e_own_sem, z_sem, x_send, x_recv, g_send, g_recv, g_last, y_send, y_recv, e_send, e_recv,
           n_recv, n_last, n_send, pre_sem, rs_sem, fxa, fyb, fya, fxb, f_sem, s_sem):
    ys, xs, own, vocab, shift = cfg
    y = lax.axis_index("yax")
    x = lax.axis_index("xax")
    core = lax.rem(x, 2)
    partner = x + 1 - 2 * core
    blk = hidden.shape[1]
    quarter = xs * own
    head_dim = k_hbm.shape[1]
    half = head_dim // 2
    seqs = k_hbm.shape[0]
    slots = k_hbm.shape[2]
    heads = w_query.shape[1] * ys // head_dim
    groups = k_buf.shape[0]
    per = seqs // groups
    window = e_buf.shape[0]

    def lanes(i):
        return pl.ds(pl.multiple_of(i * blk, 128), blk)

    def rows(i, n):
        return pl.ds(pl.multiple_of(i * n, n), n)

    barrier = pltpu.get_barrier_semaphore()

    def signal_row(d, carry):
        pl.semaphore_signal(barrier, inc=1, device_id={"xax": lax.rem(x + d, xs)},
                            device_id_type=pl.DeviceIdType.MESH)
        return carry
    lax.fori_loop(1, xs, signal_row, 0)

    def signal_column(d, carry):
        pl.semaphore_signal(barrier, inc=1, device_id={"yax": lax.rem(y + d, ys)},
                            device_id_type=pl.DeviceIdType.MESH)
        return carry
    lax.fori_loop(1, ys, signal_column, 0)
    small_ins = [pltpu.make_async_copy(a, b, z_sem.at[i])
                 for i, (a, b) in enumerate(((wq_hbm, w_query), (freq_hbm, freq), (lens_hbm, lens)))]
    for copy in small_ins:
        copy.start()
    def cache_copy(g, src, dst, s):
        return pltpu.make_async_copy(src.at[pl.ds(g * per, per)], dst.at[g], kv_sem.at[s, g])

    def start_cache(g, carry):
        cache_copy(g, k_hbm, k_buf, 0).start()
        return carry
    lax.fori_loop(0, groups, start_cache, 0)

    for copy in small_ins:
        copy.wait()
    wqt[...] = w_query[...].astype(F32).T.astype(BF16)

    pl.semaphore_wait(barrier, xs + ys - 2)

    def far(k, n):
        return n // 2 + k // 2 * (2 * lax.rem(k, 2) - 1)

    def arrived(ref, sem):
        pltpu.make_async_copy(ref, ref, sem).wait()

    cols = wqt.shape[0] // xs
    ff = w_gate.shape[1] // xs
    most = pl.ds(0, (xs - 1) * blk)
    x_kinds = {
        "wq": (lambda p: wqt.at[rows(p, cols), :], lambda s: wq_buf.at[y, :, lanes(s)],
               wq_buf.at[y], wq_buf.at[y, :, most]),
        "wo": (lambda p: w_out.at[rows(p, cols), :], lambda s: out_buf.at[y, :, lanes(s)],
               out_buf.at[y], out_buf.at[y, :, most]),
        "down": (lambda p: w_down.at[rows(p, ff), :], lambda s: down_buf.at[y, :, lanes(s)],
                 down_buf.at[y], down_buf.at[y, :, most]),
        "gate": (lambda p: w_gate.at[:, lanes(p)], lambda s: gu_buf.at[rows(s, blk), pl.ds(0, ff)],
                 gu_buf.at[:, pl.ds(0, ff)], gu_buf.at[most, pl.ds(0, ff)]),
        "up": (lambda p: w_up.at[:, lanes(p)], lambda s: gu_buf.at[rows(s, blk), pl.ds(ff, ff)],
               gu_buf.at[:, pl.ds(ff, ff)], gu_buf.at[most, pl.ds(ff, ff)]),
        "q": (lambda p: q_scr.at[rows(p, own), :], lambda s: qx_buf.at[s],
              qx_buf, qx_buf.at[pl.ds(0, xs - 1)]),
        "o": (lambda p: o_scr.at[p], lambda s: ox_buf.at[rows(s, own), :],
              ox_buf, ox_buf.at[pl.ds(0, (xs - 1) * own), :]),
    }
    x_index = {name: i for i, name in enumerate(x_kinds)}

    def x_start(name):
        src, dst = x_kinds[name][:2]
        k = x_index[name]

        def body(k1, carry):
            p = lax.rem(x + far(k1, xs), xs)
            pltpu.make_async_remote_copy(
                src_ref=src(p), dst_ref=dst(x), send_sem=x_send.at[k], recv_sem=x_recv.at[k],
                device_id={"xax": p}, device_id_type=pl.DeviceIdType.MESH).start()
            return carry
        lax.fori_loop(1, xs, body, 0)
        pltpu.make_async_copy(src(x), dst(x), x_recv.at[k]).start()

    def x_wait(name):
        arrived(x_kinds[name][2], x_recv.at[x_index[name]])

    def x_drain(name):
        arrived(x_kinds[name][3], x_send.at[x_index[name]])

    chips = xs // 2
    g_kinds = {
        "hidden": (hidden.at[rows(y, quarter), :], lambda s: h_buf.at[:, lanes(s)], h_buf),
        "ga": (g_attn, lambda s: ga_buf.at[:, lanes(s)], ga_buf),
        "gf": (g_final, lambda s: gf_buf.at[:, lanes(s)], gf_buf),
        "wk": (w_key, lambda s: kv_buf.at[pl.ds(0, head_dim), lanes(s)], kv_buf.at[pl.ds(0, head_dim), :]),
        "wv": (w_value, lambda s: kv_buf.at[pl.ds(head_dim, head_dim), lanes(s)],
               kv_buf.at[pl.ds(head_dim, head_dim), :]),
    }
    g_index = {name: i for i, name in enumerate(g_kinds)}

    def g_copy(name, i, sender):
        src, dst, _ = g_kinds[name]
        k = g_index[name]
        return pltpu.make_async_remote_copy(
            src_ref=src, dst_ref=dst(sender), send_sem=g_send.at[k], recv_sem=g_recv.at[k, i],
            device_id={"xax": lax.rem(x + 2 * i, xs)}, device_id_type=pl.DeviceIdType.MESH)

    def g_pass(name, sender, source):
        k = g_index[name]
        return pltpu.make_async_remote_copy(
            src_ref=source, dst_ref=g_kinds[name][1](sender), send_sem=g_send.at[k], recv_sem=g_last.at[k],
            device_id={"xax": partner}, device_id_type=pl.DeviceIdType.MESH)

    def g_start(name):
        def body(i, carry):
            g_copy(name, far(i, chips), x).start()
            return carry
        lax.fori_loop(1, chips, body, 0)
        src, dst, _ = g_kinds[name]
        g_pass(name, x, src).start()
        pltpu.make_async_copy(src, dst(x), g_last.at[g_index[name]]).start()

    def g_forward(name):
        def body(i, carry):
            sender = lax.rem(x + xs - 2 * i, xs)
            g_copy(name, i, sender).wait_recv()
            g_pass(name, sender, g_kinds[name][1](sender)).start()
            return carry
        lax.fori_loop(1, chips, body, 0)

    def g_wait(name):
        whole = g_kinds[name][2]
        arrived(whole.at[:, pl.ds(0, (chips + 1) * blk)], g_last.at[g_index[name]])

    def g_drain(name):
        arrived(g_kinds[name][2].at[:, most], g_send.at[g_index[name]])

    y_kinds = {"wq": wq_buf, "wo": out_buf, "down": down_buf}
    y_index = {name: i for i, name in enumerate(y_kinds)}
    others = pl.ds(0, ys - 1)

    def y_start(name):
        buf = y_kinds[name]
        k = y_index[name]

        def body(d, carry):
            pltpu.make_async_remote_copy(
                src_ref=buf.at[y], dst_ref=buf.at[y], send_sem=y_send.at[k], recv_sem=y_recv.at[k],
                device_id={"yax": lax.rem(y + far(d, ys), ys)}, device_id_type=pl.DeviceIdType.MESH).start()
            return carry
        lax.fori_loop(1, ys, body, 0)

    def y_wait(name):
        arrived(y_kinds[name].at[others], y_recv.at[y_index[name]])

    def y_drain(name):
        arrived(y_kinds[name].at[others], y_send.at[y_index[name]])

    e_parts = row_chunks(window, EMBED_CHUNKS)

    def e_first(p):
        return p * vocab - lax.rem(p, 2) * shift

    def e_own():
        return pltpu.make_async_copy(
            embed.at[pl.ds(pl.multiple_of(e_first(x), 8), window), :], e_buf.at[:, lanes(x)], e_own_sem)

    def e_start(c):
        r0, n = e_parts[c]

        def body(d, carry):
            p = lax.rem(x + d, xs)
            pltpu.make_async_remote_copy(
                src_ref=embed.at[pl.ds(pl.multiple_of(e_first(p) + r0, 8), n), :],
                dst_ref=e_buf.at[pl.ds(r0, n), lanes(x)], send_sem=e_send,
                recv_sem=e_recv.at[int(c >= EMBED_FIRST)],
                device_id={"xax": p}, device_id_type=pl.DeviceIdType.MESH).start()
            return carry
        lax.fori_loop(1, xs, body, 0)

    x_start("wq")
    for name in ("hidden", "ga"):
        g_start(name)
    for name in ("wo", "down"):
        x_start(name)
    for name in ("wk", "wv", "gf"):
        g_start(name)
    e_start(0)
    e_own().start()

    def start_cache_v(g, carry):
        cache_copy(g, v_hbm, v_buf, 1).start()
        return carry
    lax.fori_loop(0, groups, start_cache_v, 0)

    x_wait("wq")
    y_start("wq")
    for name in ("hidden", "ga"):
        g_forward(name)
    for name in ("hidden", "ga"):
        g_wait(name)
    my_rows = rows(y, quarter)
    n_all[my_rows, :] = layer_norm(h_buf[...].astype(F32), ga_buf[...]).astype(BF16)

    part = quarter // 2

    def n_rows(j, c):
        return pl.ds(pl.multiple_of(j * quarter + c * part, part), part)

    def n_copy(d, sender):
        r = n_rows(sender, core)
        return pltpu.make_async_remote_copy(
            src_ref=n_all.at[r, :], dst_ref=n_all.at[r, :], send_sem=n_send.at[0],
            recv_sem=n_recv.at[d], device_id={"yax": lax.rem(y + d, ys)},
            device_id_type=pl.DeviceIdType.MESH)

    def n_pass(d, c):
        r = n_rows(lax.rem(y + ys - d, ys), c)
        return pltpu.make_async_remote_copy(
            src_ref=n_all.at[r, :], dst_ref=n_all.at[r, :], send_sem=n_send.at[1],
            recv_sem=n_last.at[d], device_id={"xax": partner},
            device_id_type=pl.DeviceIdType.MESH)

    x_wait("wo")
    y_start("wo")
    y_wait("wq")
    wq_all = wq_buf[...].reshape(ys * cols, xs * blk)
    q_scr[...] = lax.dot_general(n_all[my_rows, :], wq_all, NT, preferred_element_type=F32).astype(BF16)
    x_start("q")
    x_start("gate")
    x_start("up")

    def n_start(d, carry):
        n_copy(far(d, ys), y).start()
        return carry
    lax.fori_loop(1, ys, n_start, 0)
    x_wait("down")
    y_start("down")
    for c in range(1, 7):
        e_start(c)

    row_id = lax.broadcasted_iota(jnp.int32, (own, 4 * half), 0)
    first_row = (y * xs + x) * own
    position = jnp.zeros((own, 4 * half), jnp.int32)
    for b in range(own):
        position = jnp.where(row_id == b, lens[first_row + b], position)
    angle = position.astype(F32) * freq[...]
    cos_a = jnp.cos(angle)
    sin_a = jnp.sin(angle)
    for name in ("wk", "wv", "gf"):
        g_forward(name)
    for name in ("wk", "wv", "gf"):
        g_wait(name)
    mine = y * xs + x
    n_own = n_all[rows(mine, own), :]
    kv = lax.dot_general(n_own, kv_buf[...], NT, preferred_element_type=F32).astype(BF16).astype(F32)
    k1 = kv[:, :half]
    k2 = kv[:, half:head_dim]
    c1 = cos_a[:, :half]
    s1 = sin_a[:, :half]
    key = jnp.concatenate([k1 * c1 - k2 * s1, k2 * c1 + k1 * s1], axis=1).astype(BF16)
    value = kv[:, head_dim:].astype(BF16)
    k_scr[...] = key
    v_scr[...] = value
    small_outs = [pltpu.make_async_copy(k_scr, k_out, z_sem.at[0]),
                  pltpu.make_async_copy(v_scr, v_out, z_sem.at[1])]
    for copy in small_outs:
        copy.start()
    for h in range(heads):
        krep[pl.ds(h, own, stride=heads), :] = key.astype(F32)
        vrep[pl.ds(h, own, stride=heads), :] = value.astype(F32)

    x_wait("q")
    for xc in range(xs // 2):
        qa = qx_buf[2 * xc].astype(F32)
        qb = qx_buf[2 * xc + 1].astype(F32)
        ra = (qa * cos_a - qb * sin_a).astype(BF16).astype(F32)
        rb = (qb * cos_a + qa * sin_a).astype(BF16).astype(F32)
        for yc in range(ys):
            pair = jnp.concatenate([ra[:, yc * half:(yc + 1) * half], rb[:, yc * half:(yc + 1) * half]], axis=1)
            q2d[pl.ds(xc * ys + yc, own, stride=heads), :] = pair
    scale = head_dim ** -0.5
    snew[...] = jnp.sum(q2d[...] * krep[...], axis=1, keepdims=True) * scale

    gr = per * heads
    seg_r = lax.broadcasted_iota(jnp.int32, (gr, per * head_dim), 0) // heads
    seg_c = lax.broadcasted_iota(jnp.int32, (gr, per * head_dim), 1) // head_dim
    diag = (seg_r == seg_c).astype(F32)
    tile = min(512, slots)
    row_g = lax.broadcasted_iota(jnp.int32, (gr, 1), 0) // heads
    lane_g = lax.broadcasted_iota(jnp.int32, (gr, tile), 1)

    def attend(g, carry):
        cache_copy(g, k_hbm, k_buf, 0).wait()
        qg = q2d[rows(g, gr), :]
        qbd = (jnp.concatenate([qg] * per, axis=1) * diag).astype(BF16)
        len_g = jnp.zeros((gr, 1), jnp.int32)
        for s in range(per):
            len_g = jnp.where(row_g == s, lens[first_row + g * per + s], len_g)
        new = snew[rows(g, gr), :]
        top = jnp.full((gr, tile), -jnp.inf, F32)
        kg = k_buf.at[g]
        vg = v_buf.at[g]
        for c in range(slots // tile):
            kc = kg[:, :, pl.ds(c * tile, tile)].reshape(per * head_dim, tile)
            sc = jnp.dot(qbd, kc, preferred_element_type=F32) * scale
            sc = jnp.where(lane_g < len_g - c * tile, sc, -jnp.inf)
            s_scr[:, pl.ds(c * tile, tile)] = sc
            top = jnp.maximum(top, sc)
        row_max = jnp.maximum(jnp.max(top, axis=1, keepdims=True), new)
        total = jnp.zeros((gr, tile), F32)
        for c in range(slots // tile):
            ex = jnp.exp(s_scr[:, pl.ds(c * tile, tile)] - row_max)
            s_scr[:, pl.ds(c * tile, tile)] = ex
            total = total + ex
        w_new = jnp.exp(new - row_max)
        den = jnp.sum(total, axis=1, keepdims=True) + w_new
        inv = 1.0 / den
        cache_copy(g, v_hbm, v_buf, 1).wait()
        mixed = jnp.zeros((gr, per * head_dim), F32)
        for c in range(slots // tile):
            pr = (s_scr[:, pl.ds(c * tile, tile)] * inv).astype(BF16)
            vc = vg[:, :, pl.ds(c * tile, tile)].reshape(per * head_dim, tile)
            mixed = mixed + lax.dot_general(pr, vc, NT, preferred_element_type=F32)
        add = (w_new * inv).astype(BF16).astype(F32) * vrep[rows(g, gr), :]
        for s in range(per):
            od_scr[pl.ds(pl.multiple_of(g * gr + s * heads, heads), heads), :] = (
                mixed[s * heads:(s + 1) * heads, s * head_dim:(s + 1) * head_dim]
                + add[s * heads:(s + 1) * heads, :])
        return carry

    lax.fori_loop(0, groups, attend, 0)
    for xc in range(xs // 2):
        parts = [od_scr[pl.ds(xc * ys + yc, own, stride=heads), :] for yc in range(ys)]
        o_scr[2 * xc] = jnp.concatenate([p[:, :half] for p in parts], axis=1).astype(BF16)
        o_scr[2 * xc + 1] = jnp.concatenate([p[:, half:] for p in parts], axis=1).astype(BF16)
    x_start("o")
    for c in range(7, 12):
        e_start(c)

    def act_copy(dest):
        return pltpu.make_async_remote_copy(
            src_ref=act_scr.at[dest], dst_ref=act.at[:, pl.ds(pl.multiple_of(y * ff, ff), ff)],
            send_sem=y_send.at[len(y_kinds)], recv_sem=y_recv.at[len(y_kinds)],
            device_id={"yax": dest}, device_id_type=pl.DeviceIdType.MESH)

    x_wait("gate")
    x_wait("up")

    def feed(d, carry):
        @pl.when(d < ys - 1)
        def _():
            n_copy(d + 1, lax.rem(y + ys - d - 1, ys)).wait_recv()
            n_pass(d + 1, core).start()
        j = lax.rem(y + ys - d, ys)

        @pl.when(d > 0)
        def _():
            n_pass(d, 1 - core).wait_recv()
        gu = jnp.dot(n_all[rows(j, quarter), :], gu_buf[...], preferred_element_type=F32)
        gu = gu.astype(BF16).astype(F32)
        gate = gu[:, :ff]
        act_scr[j] = (gate * jax.nn.sigmoid(gate) * gu[:, ff:]).astype(BF16)

        @pl.when(d > 0)
        def _():
            act_copy(j).start()
        return carry
    lax.fori_loop(0, ys, feed, 0)
    act[:, pl.ds(pl.multiple_of(y * ff, ff), ff)] = act_scr[y]
    y_wait("wo")
    x_wait("o")
    part_scr[...] = jnp.dot(
        ox_buf[...], out_buf[...].reshape(ys * cols, xs * blk), preferred_element_type=F32)
    y_wait("down")

    arrived(act_scr.at[others], y_recv.at[len(y_kinds)])

    down_all = down_buf[...].reshape(ys * ff, xs * blk)
    part_scr[...] = part_scr[...] + jnp.dot(act[...], down_all, preferred_element_type=F32)

    def branch(c):
        for i in range(chips):
            rs_scr[c, i] = part_scr[pl.ds(pl.multiple_of((2 * i + c) * own, own), own), :]

    def pre_copy():
        return pltpu.make_async_remote_copy(
            src_ref=rs_scr.at[1 - core], dst_ref=pre_buf, send_sem=pre_sem.at[0], recv_sem=pre_sem.at[1],
            device_id={"xax": partner}, device_id_type=pl.DeviceIdType.MESH)

    def rs_copy(dest):
        return pltpu.make_async_remote_copy(
            src_ref=rs_scr.at[core, dest], dst_ref=rs_buf.at[chip], send_sem=rs_sem.at[0],
            recv_sem=rs_sem.at[1], device_id={"xax": 2 * dest + core},
            device_id_type=pl.DeviceIdType.MESH)

    chip = x // 2
    branch(1 - core)
    pre_copy().start()
    branch(core)
    pre_copy().wait_recv()
    rs_scr[core] = rs_scr[core] + pre_buf[...]

    def rs_start(i, carry):
        rs_copy(lax.rem(chip + far(i, chips), chips)).start()
        return carry
    lax.fori_loop(1, chips, rs_start, 0)
    e_start(12)
    arrived(rs_buf.at[pl.ds(0, chips - 1)], rs_sem.at[1])
    rs_buf[chip] = rs_scr[core, chip]
    res = h_buf[rows(x, own), :].astype(F32) + jnp.sum(rs_buf[...], axis=0)
    f_buf[rows(mine, own), :] = layer_norm(res, gf_buf[...]).astype(BF16)

    piece = own // 2

    def f_half(sy, sx, h):
        return f_buf.at[pl.ds(pl.multiple_of((sy * xs + sx) * own + h * piece, piece), piece), :]

    def f_over_x(i, h, sy, sx, sem):
        return pltpu.make_async_remote_copy(
            src_ref=f_half(sy, sx, h), dst_ref=f_half(sy, sx, h), send_sem=f_sem.at[0], recv_sem=sem,
            device_id={"xax": lax.rem(x + 2 * i, xs)}, device_id_type=pl.DeviceIdType.MESH)

    def f_over_y(d, h, sy, sx, sem):
        return pltpu.make_async_remote_copy(
            src_ref=f_half(sy, sx, h), dst_ref=f_half(sy, sx, h), send_sem=f_sem.at[0], recv_sem=sem,
            device_id={"yax": lax.rem(y + d, ys)}, device_id_type=pl.DeviceIdType.MESH)

    def f_pass(d, h, sy, sx):
        pltpu.make_async_remote_copy(
            src_ref=f_half(sy, sx, h), dst_ref=f_half(sy, sx, h), send_sem=f_sem.at[1],
            recv_sem=f_sem.at[2 + d], device_id={"xax": partner},
            device_id_type=pl.DeviceIdType.MESH).start()

    def from_y(d):
        return lax.rem(y + ys - d, ys)

    def from_x(i):
        return lax.rem(x + xs - 2 * i, xs)

    def spread_y(i):
        def body(d, carry):
            f_over_y(far(d, ys), 0, y, from_x(i), fya.at[far(d, ys), i]).start()
            return carry
        lax.fori_loop(1, ys, body, 0)

    def spread_x(d):
        def body(i, carry):
            f_over_x(far(i, chips), 1, from_y(d), x, fxb.at[d, far(i, chips)]).start()
            return carry
        lax.fori_loop(1, chips, body, 0)

    def first_x(i, carry):
        f_over_x(far(i, chips), 0, y, x, fxa.at[far(i, chips)]).start()
        return carry
    lax.fori_loop(1, chips, first_x, 0)

    def first_y(d, carry):
        f_over_y(far(d, ys), 1, y, x, fyb.at[far(d, ys)]).start()
        return carry
    lax.fori_loop(1, ys, first_y, 0)
    spread_y(0)
    spread_x(0)
    f_pass(0, 0, y, x)
    f_pass(0, 1, y, x)
    e_start(13)
    for i in sorted(range(1, max(chips, ys)), key=lambda d: (min(d, max(chips, ys) - d), d)):
        if i < chips:
            f_over_x(i, 0, y, from_x(i), fxa.at[i]).wait_recv()
            spread_y(i)
            f_pass(0, 0, y, from_x(i))
        if i < ys:
            f_over_y(i, 1, from_y(i), x, fyb.at[i]).wait_recv()
            spread_x(i)
            f_pass(i, 1, from_y(i), x)
    for c in range(14, EMBED_CHUNKS):
        e_start(c)

    def collect(d):
        def body(i, carry):
            @pl.when(d > 0)
            def _():
                f_over_y(d, 0, from_y(d), from_x(i), fya.at[d, i]).wait_recv()
                f_pass(d, 0, from_y(d), from_x(i))

            @pl.when(i > 0)
            def _():
                f_over_x(i, 1, from_y(d), from_x(i), fxb.at[d, i]).wait_recv()
                f_pass(d, 1, from_y(d), from_x(i))
            return carry
        lax.fori_loop(0, chips, body, 0)

    for name in x_kinds:
        x_drain(name)
    for name in g_kinds:
        g_drain(name)
    for name in y_kinds:
        y_drain(name)
    arrived(act_scr.at[others], y_send.at[len(y_kinds)])
    for i in range(2):
        arrived(n_all.at[pl.ds(0, (ys - 1) * part), :], n_send.at[i])
    pre_copy().wait_send()
    arrived(rs_buf.at[pl.ds(0, chips - 1)], rs_sem.at[0])
    for copy in small_outs:
        copy.wait()

    cut = e_parts[EMBED_FIRST][0]
    skip = core * shift
    half_block = pl.ds(0, chips * own)

    def nearest(k):
        return k + k // 2 * (1 - 2 * lax.rem(k, 2))

    def z_copy(j, r0, n):
        return pltpu.make_async_copy(
            z_scr.at[j, pl.ds(r0, n), :], logits_out.at[pl.ds(r0, n), rows(j, quarter)], z_sem.at[2])

    def block(j, r0, n, pieces):
        r = pl.ds(r0, n)
        z_scr[j, r, :] = lax.dot_general(e_buf[r, :], f_buf[rows(j, quarter), :], NT, preferred_element_type=F32)
        z_copy(j, r0, n).start()
        stats = []
        for q0, m in row_chunks(n, pieces):
            z = z_scr[j, pl.ds(r0 + q0, m), :]
            if shift and (r0 + q0 == 0 or r0 + q0 + m == window):
                index = lax.broadcasted_iota(jnp.int32, z.shape, 0) + (r0 + q0)
                z = jnp.where(jnp.logical_and(index >= skip, index < skip + vocab), z, -jnp.inf)
            top = jnp.max(z, axis=0, keepdims=True)
            stats.append((top, jnp.sum(jnp.exp(z - top), axis=0, keepdims=True)))
        return stats

    def put(j, stats):
        top = functools.reduce(jnp.maximum, [t for t, _ in stats])
        st_scr[0:1, rows(j, quarter)] = top
        st_scr[1:2, rows(j, quarter)] = sum(t * jnp.exp(m - top) for m, t in stats)

    def head(k, carry):
        d = nearest(k)
        j = from_y(d)
        arrived(f_buf.at[half_block, :], f_sem.at[2 + d])
        put(j, block(j, 0, cut, 4))

        @pl.when(k < ys - 2)
        def _():
            collect(nearest(k + 2))
        return carry

    def head_rest(j, carry):
        before = (st_scr[0:1, rows(j, quarter)], st_scr[1:2, rows(j, quarter)])
        put(j, [before] + block(j, cut, window - cut, 1))
        return carry

    for k in range(min(2, ys)):
        collect(nearest(k))
    e_own().wait()
    arrived(e_buf.at[pl.ds(0, cut), most], e_recv.at[0])

    lax.fori_loop(0, ys, head, 0)
    arrived(e_buf.at[pl.ds(cut, window - cut), most], e_recv.at[1])
    lax.fori_loop(0, ys, head_rest, 0)

    for k in range(ys):
        dy = (ys // 2 + k) % ys
        for dx in range(xs):
            if dy + dx > 0:
                pltpu.make_async_remote_copy(
                    src_ref=st_scr, dst_ref=s_buf.at[mine], send_sem=s_sem.at[0], recv_sem=s_sem.at[1],
                    device_id={"yax": lax.rem(y + dy, ys), "xax": lax.rem(x + dx, xs)},
                    device_id_type=pl.DeviceIdType.MESH).start()
    s_buf[mine] = st_scr[...]

    arrived(e_buf.at[:, most], e_send)
    arrived(f_buf.at[pl.ds(0, 2 * (ys * chips - 1) * piece), :], f_sem.at[0])
    arrived(f_buf.at[pl.ds(0, ys * chips * own), :], f_sem.at[1])
    arrived(z_scr, z_sem.at[2])
    everyone = s_buf.at[pl.ds(0, ys * xs - 1)]
    arrived(everyone, s_sem.at[1])
    tops = s_buf[:, 0, :]
    best = jnp.max(tops, axis=0, keepdims=True)
    whole = jnp.sum(s_buf[:, 1, :] * jnp.exp(tops - best), axis=0, keepdims=True)
    norm_scr[...] = best + jnp.log(whole)
    norm_copy = pltpu.make_async_copy(norm_scr, norm_out, z_sem.at[0])
    norm_copy.start()
    arrived(everyone, s_sem.at[0])
    norm_copy.wait()


def finish_kernel(shift, z_hbm, norm_hbm, key, value, out_hbm, k_out, v_out, norm_out,
                  z_buf, o_buf, norm, k_scr, v_scr, in_sem, out_sem):
    count, n, width = o_buf.shape

    def load(i):
        return pltpu.make_async_copy(z_hbm.at[:, pl.ds(i * width, width)], z_buf.at[i], in_sem.at[i])

    def save(i):
        return pltpu.make_async_copy(o_buf.at[i], out_hbm.at[:, pl.ds(i * width, width)], out_sem.at[i])

    small = ((norm_hbm, norm, norm_out), (key, k_scr, k_out), (value, v_scr, v_out))
    small_in = [pltpu.make_async_copy(a, b, in_sem.at[count + i]) for i, (a, b, _) in enumerate(small)]
    small_out = [pltpu.make_async_copy(b, c, out_sem.at[count + i]) for i, (_, b, c) in enumerate(small)]
    small_in[0].start()
    for i in range(count):
        load(i).start()
    for copy in small_in[1:]:
        copy.start()
    small_in[0].wait()
    small_out[0].start()
    odd = lax.rem(lax.axis_index("xax"), 2) == 1
    for i in range(count):
        row = norm[:, pl.ds(i * width, width)]
        load(i).wait()
        if shift:
            @pl.when(odd)
            def _():
                o_buf[i] = z_buf[i, pl.ds(shift, n), :] - row

            @pl.when(jnp.logical_not(odd))
            def _():
                o_buf[i] = z_buf[i, pl.ds(0, n), :] - row
        else:
            o_buf[i] = z_buf[i] - row
        save(i).start()
    for i in (1, 2):
        small_in[i].wait()
        small_out[i].start()
    for copy in small_out:
        copy.wait()
    for i in range(count):
        save(i).wait()


def solution(mesh):
    ys = mesh.shape["yax"]
    xs = mesh.shape["xax"]
    row_spec = P(("dp", "yax", "xax"))

    def local_step(hidden, cache_len, k_cache, v_cache, g_attn, w_query, w_key, w_value,
                   w_gate, w_up, w_out, w_down, g_final, embedding):
        batch, blk = hidden.shape
        own, slots, head_dim = k_cache.shape
        width = blk * xs
        vocab = embedding.shape[0] // xs
        shift = vocab % 8
        window = -(-vocab // 8) * 8
        half = head_dim // 2
        quarter = xs * own
        cols = w_query.shape[1] // xs
        ff = w_gate.shape[1] // xs
        heads = w_query.shape[1] * ys // head_dim
        per = 4
        groups = own // per
        freq_row = (ROPE_BASE ** (-(np.arange(half, dtype=np.float32) * 2.0) / head_dim)).astype(np.float32)
        freq = jnp.asarray(np.tile(freq_row, 4)[None, :])
        any_spec = pl.BlockSpec(memory_space=pl.ANY)
        dma = pltpu.SemaphoreType.DMA
        chips = xs // 2
        scratch = [
            pltpu.VMEM((groups, per, head_dim, slots), BF16),
            pltpu.VMEM((groups, per, head_dim, slots), BF16),
            pltpu.VMEM((quarter, width), BF16),
            pltpu.VMEM((1, width), F32),
            pltpu.VMEM((1, width), F32),
            pltpu.VMEM((w_query.shape[1], blk), BF16),
            pltpu.VMEM((ys, cols, width), BF16),
            pltpu.VMEM((width, 2 * ff), BF16),
            pltpu.VMEM((ys, ff, width), BF16),
            pltpu.VMEM((ys, cols, width), BF16),
            pltpu.VMEM((2 * head_dim, width), BF16),
            pltpu.VMEM((batch, width), BF16),
            pltpu.VMEM((quarter, ys * cols), BF16),
            pltpu.VMEM((xs, own, ys * cols), BF16),
            pltpu.VMEM((own * heads, head_dim), F32),
            pltpu.VMEM((own * heads, 1), F32),
            pltpu.VMEM((own * heads, head_dim), F32),
            pltpu.VMEM((own * heads, head_dim), F32),
            pltpu.VMEM((per * heads, slots), F32),
            pltpu.VMEM((own * heads, head_dim), F32),
            pltpu.VMEM((xs, own, ys * cols), BF16),
            pltpu.VMEM((quarter, ys * cols), BF16),
            pltpu.VMEM((ys, quarter, ff), BF16),
            pltpu.VMEM((quarter, ys * ff), BF16),
            pltpu.VMEM((quarter, width), F32),
            pltpu.VMEM((chips, own, width), F32),
            pltpu.VMEM((2, chips, own, width), F32),
            pltpu.VMEM((chips, own, width), F32),
            pltpu.VMEM((batch, width), BF16),
            pltpu.VMEM((window, width), BF16),
            pltpu.VMEM((ys, window, quarter), F32),
            pltpu.VMEM((2, batch), F32),
            pltpu.VMEM((own, head_dim), BF16),
            pltpu.VMEM((own, head_dim), BF16),
            pltpu.VMEM((1, batch), F32),
            pltpu.VMEM((ys * xs, 2, batch), F32),
            pltpu.SMEM(cache_len.shape, jnp.int32),
            pltpu.VMEM(w_query.shape, BF16),
            pltpu.VMEM((1, 4 * half), F32),
            dma((2, groups)), dma, dma((3,)), dma((7,)), dma((7,)),
            dma((5,)), dma((5, chips)), dma((5,)), dma((4,)), dma((4,)), dma, dma((2,)),
            dma((ys,)), dma((ys,)), dma((2,)), dma((2,)), dma((2,)),
            dma((chips,)), dma((ys,)), dma((ys, chips)), dma((ys, chips)), dma((2 + ys,)), dma((2,)),
        ]
        cfg = (ys, xs, own, vocab, shift)
        key_new, value_new, logits, norm = pl.pallas_call(
            functools.partial(kernel, cfg),
            name="decode_layer",
            out_shape=(
                jax.ShapeDtypeStruct((own, head_dim), BF16),
                jax.ShapeDtypeStruct((own, head_dim), BF16),
                jax.ShapeDtypeStruct((window, batch), F32),
                jax.ShapeDtypeStruct((1, batch), F32)),
            in_specs=[any_spec] * 15,
            out_specs=(any_spec, any_spec, any_spec, any_spec),
            scratch_shapes=scratch,
            compiler_params=pltpu.CompilerParams(
                collective_id=0, has_side_effects=True, vmem_limit_bytes=67043328),
        )(cache_len, hidden, k_cache.transpose(0, 2, 1), v_cache.transpose(0, 2, 1),
          g_attn[None, :], g_final[None, :], w_query, w_key.T, w_value.T, w_gate, w_up, w_out, w_down,
          embedding, freq)
        count = 8
        log_probs, key_new, value_new, norm = pl.pallas_call(
            functools.partial(finish_kernel, shift),
            name="finish",
            out_shape=(
                jax.ShapeDtypeStruct((vocab, batch), F32),
                jax.ShapeDtypeStruct((own, head_dim), BF16),
                jax.ShapeDtypeStruct((own, head_dim), BF16),
                jax.ShapeDtypeStruct((1, batch), F32)),
            in_specs=[any_spec] * 4,
            out_specs=(any_spec,) * 4,
            scratch_shapes=[
                pltpu.VMEM((count, window, batch // count), F32),
                pltpu.VMEM((count, vocab, batch // count), F32),
                pltpu.VMEM((1, batch), F32), pltpu.VMEM((own, head_dim), BF16), pltpu.VMEM((own, head_dim), BF16),
                dma((count + 3,)), dma((count + 3,))],
        )(logits, norm, key_new, value_new)
        return key_new, value_new, log_probs.T, norm[0]

    in_specs = (P("dp", "xax"), P("dp"), row_spec, row_spec, P("xax"), P("xax", "yax"),
                P("xax", None), P("xax", None), P("xax", "yax"), P("xax", "yax"),
                P("yax", "xax"), P("yax", "xax"), P("xax"), P("yax", "xax"))
    out_specs = (row_spec, row_spec, P("dp", ("yax", "xax")), P("dp"))
    return jax.shard_map(local_step, mesh=mesh, in_specs=in_specs, out_specs=out_specs, check_vma=False)
```

```python
import functools

import jax
import jax.numpy as jnp
import numpy as np
from jax import lax
from jax.experimental import pallas as pl
from jax.experimental.pallas import tpu as pltpu
from jax.sharding import PartitionSpec as P

EPS = 1e-6
ROPE_BASE = 10000.0
F32 = jnp.float32
BF16 = jnp.bfloat16
NT = (((1,), (1,)), ((), ()))
EMBED_CHUNKS = 16
EMBED_FIRST = 14


def layer_norm(values_in, gain):
    mean = jnp.mean(values_in, axis=-1, keepdims=True)
    centred = values_in - mean
    var = jnp.mean(centred * centred, axis=-1, keepdims=True)
    return centred * lax.rsqrt(var + EPS) * gain


def row_chunks(total, count):
    cuts = [16 * (total // 16 * i // count) for i in range(count)] + [total]
    return [(cuts[i], cuts[i + 1] - cuts[i]) for i in range(count)]


def kernel(cfg, lens_hbm, hidden, k_hbm, v_hbm, g_attn, g_final, wq_hbm, w_key, w_value, w_gate, w_up,
           w_out, w_down, embed, freq_hbm,
           k_out, v_out, logits_out, norm_out,
           k_buf, v_buf, h_buf, ga_buf, gf_buf, wqt, wq_buf, gu_buf, down_buf, out_buf, kv_buf,
           n_all, q_scr, qx_buf, q2d, snew, krep, vrep, s_scr, od_scr, o_scr, ox_buf, act_scr, act, part_scr,
           pre_buf, rs_scr, rs_buf, f_buf, e_buf, z_scr, st_scr, k_scr, v_scr, norm_scr, s_buf,
           lens, w_query, freq,
           kv_sem, e_own_sem, z_sem, x_send, x_recv, g_send, g_recv, g_last, y_send, y_recv, e_send, e_recv,
           n_recv, n_last, n_send, pre_sem, rs_sem, fxa, fyb, fya, fxb, f_sem, s_sem):
    ys, xs, own, vocab, shift = cfg
    y = lax.axis_index("yax")
    x = lax.axis_index("xax")
    core = lax.rem(x, 2)
    partner = x + 1 - 2 * core
    blk = hidden.shape[1]
    quarter = xs * own
    head_dim = k_hbm.shape[1]
    half = head_dim // 2
    seqs = k_hbm.shape[0]
    slots = k_hbm.shape[2]
    heads = w_query.shape[1] * ys // head_dim
    groups = k_buf.shape[0]
    per = seqs // groups
    window = e_buf.shape[0]

    def lanes(i):
        return pl.ds(pl.multiple_of(i * blk, 128), blk)

    def rows(i, n):
        return pl.ds(pl.multiple_of(i * n, n), n)

    barrier = pltpu.get_barrier_semaphore()

    def signal_row(d, carry):
        pl.semaphore_signal(barrier, inc=1, device_id={"xax": lax.rem(x + d, xs)},
                            device_id_type=pl.DeviceIdType.MESH)
        return carry
    lax.fori_loop(1, xs, signal_row, 0)

    def signal_column(d, carry):
        pl.semaphore_signal(barrier, inc=1, device_id={"yax": lax.rem(y + d, ys)},
                            device_id_type=pl.DeviceIdType.MESH)
        return carry
    lax.fori_loop(1, ys, signal_column, 0)
    small_ins = [pltpu.make_async_copy(a, b, z_sem.at[i])
                 for i, (a, b) in enumerate(((wq_hbm, w_query), (freq_hbm, freq), (lens_hbm, lens)))]
    for copy in small_ins:
        copy.start()
    def cache_copy(g, src, dst, s):
        return pltpu.make_async_copy(src.at[pl.ds(g * per, per)], dst.at[g], kv_sem.at[s, g])

    def start_cache(g, carry):
        cache_copy(g, k_hbm, k_buf, 0).start()
        return carry
    lax.fori_loop(0, groups, start_cache, 0)

    for copy in small_ins:
        copy.wait()
    wqt[...] = w_query[...].astype(F32).T.astype(BF16)

    pl.semaphore_wait(barrier, xs + ys - 2)

    def far(k, n):
        return n // 2 + k // 2 * (2 * lax.rem(k, 2) - 1)

    def arrived(ref, sem):
        pltpu.make_async_copy(ref, ref, sem).wait()

    cols = wqt.shape[0] // xs
    ff = w_gate.shape[1] // xs
    most = pl.ds(0, (xs - 1) * blk)
    x_kinds = {
        "wq": (lambda p: wqt.at[rows(p, cols), :], lambda s: wq_buf.at[y, :, lanes(s)],
               wq_buf.at[y], wq_buf.at[y, :, most]),
        "wo": (lambda p: w_out.at[rows(p, cols), :], lambda s: out_buf.at[y, :, lanes(s)],
               out_buf.at[y], out_buf.at[y, :, most]),
        "down": (lambda p: w_down.at[rows(p, ff), :], lambda s: down_buf.at[y, :, lanes(s)],
                 down_buf.at[y], down_buf.at[y, :, most]),
        "gate": (lambda p: w_gate.at[:, lanes(p)], lambda s: gu_buf.at[rows(s, blk), pl.ds(0, ff)],
                 gu_buf.at[:, pl.ds(0, ff)], gu_buf.at[most, pl.ds(0, ff)]),
        "up": (lambda p: w_up.at[:, lanes(p)], lambda s: gu_buf.at[rows(s, blk), pl.ds(ff, ff)],
               gu_buf.at[:, pl.ds(ff, ff)], gu_buf.at[most, pl.ds(ff, ff)]),
        "q": (lambda p: q_scr.at[rows(p, own), :], lambda s: qx_buf.at[s],
              qx_buf, qx_buf.at[pl.ds(0, xs - 1)]),
        "o": (lambda p: o_scr.at[p], lambda s: ox_buf.at[rows(s, own), :],
              ox_buf, ox_buf.at[pl.ds(0, (xs - 1) * own), :]),
    }
    x_index = {name: i for i, name in enumerate(x_kinds)}

    def x_start(name):
        src, dst = x_kinds[name][:2]
        k = x_index[name]

        def body(k1, carry):
            p = lax.rem(x + far(k1, xs), xs)
            pltpu.make_async_remote_copy(
                src_ref=src(p), dst_ref=dst(x), send_sem=x_send.at[k], recv_sem=x_recv.at[k],
                device_id={"xax": p}, device_id_type=pl.DeviceIdType.MESH).start()
            return carry
        lax.fori_loop(1, xs, body, 0)
        pltpu.make_async_copy(src(x), dst(x), x_recv.at[k]).start()

    def x_wait(name):
        arrived(x_kinds[name][2], x_recv.at[x_index[name]])

    def x_drain(name):
        arrived(x_kinds[name][3], x_send.at[x_index[name]])

    chips = xs // 2
    g_kinds = {
        "hidden": (hidden.at[rows(y, quarter), :], lambda s: h_buf.at[:, lanes(s)], h_buf),
        "ga": (g_attn, lambda s: ga_buf.at[:, lanes(s)], ga_buf),
        "gf": (g_final, lambda s: gf_buf.at[:, lanes(s)], gf_buf),
        "wk": (w_key, lambda s: kv_buf.at[pl.ds(0, head_dim), lanes(s)], kv_buf.at[pl.ds(0, head_dim), :]),
        "wv": (w_value, lambda s: kv_buf.at[pl.ds(head_dim, head_dim), lanes(s)],
               kv_buf.at[pl.ds(head_dim, head_dim), :]),
    }
    g_index = {name: i for i, name in enumerate(g_kinds)}

    def g_copy(name, i, sender):
        src, dst, _ = g_kinds[name]
        k = g_index[name]
        return pltpu.make_async_remote_copy(
            src_ref=src, dst_ref=dst(sender), send_sem=g_send.at[k], recv_sem=g_recv.at[k, i],
            device_id={"xax": lax.rem(x + 2 * i, xs)}, device_id_type=pl.DeviceIdType.MESH)

    def g_pass(name, sender, source):
        k = g_index[name]
        return pltpu.make_async_remote_copy(
            src_ref=source, dst_ref=g_kinds[name][1](sender), send_sem=g_send.at[k], recv_sem=g_last.at[k],
            device_id={"xax": partner}, device_id_type=pl.DeviceIdType.MESH)

    def g_start(name):
        def body(i, carry):
            g_copy(name, far(i, chips), x).start()
            return carry
        lax.fori_loop(1, chips, body, 0)
        src, dst, _ = g_kinds[name]
        g_pass(name, x, src).start()
        pltpu.make_async_copy(src, dst(x), g_last.at[g_index[name]]).start()

    def g_forward(name):
        def body(k1, carry):
            i = k1 + k1 // 2 * (1 - 2 * lax.rem(k1, 2))
            sender = lax.rem(x + xs - 2 * i, xs)
            g_copy(name, i, sender).wait_recv()
            g_pass(name, sender, g_kinds[name][1](sender)).start()
            return carry
        lax.fori_loop(1, chips, body, 0)

    def g_wait(name):
        whole = g_kinds[name][2]
        arrived(whole.at[:, pl.ds(0, (chips + 1) * blk)], g_last.at[g_index[name]])

    def g_drain(name):
        arrived(g_kinds[name][2].at[:, most], g_send.at[g_index[name]])

    y_kinds = {"wq": wq_buf, "wo": out_buf, "down": down_buf}
    y_index = {name: i for i, name in enumerate(y_kinds)}
    others = pl.ds(0, ys - 1)

    def y_start(name):
        buf = y_kinds[name]
        k = y_index[name]

        def body(d, carry):
            pltpu.make_async_remote_copy(
                src_ref=buf.at[y], dst_ref=buf.at[y], send_sem=y_send.at[k], recv_sem=y_recv.at[k],
                device_id={"yax": lax.rem(y + far(d, ys), ys)}, device_id_type=pl.DeviceIdType.MESH).start()
            return carry
        lax.fori_loop(1, ys, body, 0)

    def y_wait(name):
        arrived(y_kinds[name].at[others], y_recv.at[y_index[name]])

    def y_drain(name):
        arrived(y_kinds[name].at[others], y_send.at[y_index[name]])

    e_parts = row_chunks(window, EMBED_CHUNKS)

    def e_first(p):
        return p * vocab - lax.rem(p, 2) * shift

    def e_own():
        return pltpu.make_async_copy(
            embed.at[pl.ds(pl.multiple_of(e_first(x), 8), window), :], e_buf.at[:, lanes(x)], e_own_sem)

    def e_start(c):
        r0, n = e_parts[c]

        def body(d, carry):
            p = lax.rem(x + d, xs)
            pltpu.make_async_remote_copy(
                src_ref=embed.at[pl.ds(pl.multiple_of(e_first(p) + r0, 8), n), :],
                dst_ref=e_buf.at[pl.ds(r0, n), lanes(x)], send_sem=e_send,
                recv_sem=e_recv.at[int(c >= EMBED_FIRST)],
                device_id={"xax": p}, device_id_type=pl.DeviceIdType.MESH).start()
            return carry
        lax.fori_loop(1, xs, body, 0)

    x_start("wq")
    for name in ("hidden", "ga"):
        g_start(name)
    for name in ("wo", "down"):
        x_start(name)
    for name in ("wk", "wv", "gf"):
        g_start(name)
    e_start(0)
    e_own().start()

    def start_cache_v(g, carry):
        cache_copy(g, v_hbm, v_buf, 1).start()
        return carry
    lax.fori_loop(0, groups, start_cache_v, 0)

    x_wait("wq")
    y_start("wq")
    for name in ("hidden", "ga"):
        g_forward(name)
    for name in ("hidden", "ga"):
        g_wait(name)
    my_rows = rows(y, quarter)
    n_all[my_rows, :] = layer_norm(h_buf[...].astype(F32), ga_buf[...]).astype(BF16)

    part = quarter // 2

    def n_rows(j, c):
        return pl.ds(pl.multiple_of(j * quarter + c * part, part), part)

    def n_copy(d, sender):
        r = n_rows(sender, core)
        return pltpu.make_async_remote_copy(
            src_ref=n_all.at[r, :], dst_ref=n_all.at[r, :], send_sem=n_send.at[0],
            recv_sem=n_recv.at[d], device_id={"yax": lax.rem(y + d, ys)},
            device_id_type=pl.DeviceIdType.MESH)

    def n_pass(d, c):
        r = n_rows(lax.rem(y + ys - d, ys), c)
        return pltpu.make_async_remote_copy(
            src_ref=n_all.at[r, :], dst_ref=n_all.at[r, :], send_sem=n_send.at[1],
            recv_sem=n_last.at[d], device_id={"xax": partner},
            device_id_type=pl.DeviceIdType.MESH)

    x_wait("wo")
    y_start("wo")
    y_wait("wq")
    wq_all = wq_buf[...].reshape(ys * cols, xs * blk)
    q_scr[...] = lax.dot_general(n_all[my_rows, :], wq_all, NT, preferred_element_type=F32).astype(BF16)
    x_start("q")
    x_start("gate")
    x_start("up")

    def n_start(d, carry):
        n_copy(far(d, ys), y).start()
        return carry
    lax.fori_loop(1, ys, n_start, 0)
    x_wait("down")
    y_start("down")
    for c in range(1, 7):
        e_start(c)

    row_id = lax.broadcasted_iota(jnp.int32, (own, 4 * half), 0)
    first_row = (y * xs + x) * own
    position = jnp.zeros((own, 4 * half), jnp.int32)
    for b in range(own):
        position = jnp.where(row_id == b, lens[first_row + b], position)
    angle = position.astype(F32) * freq[...]
    cos_a = jnp.cos(angle)
    sin_a = jnp.sin(angle)
    for name in ("wk", "wv", "gf"):
        g_forward(name)
    for name in ("wk", "wv", "gf"):
        g_wait(name)
    mine = y * xs + x
    n_own = n_all[rows(mine, own), :]
    kv = lax.dot_general(n_own, kv_buf[...], NT, preferred_element_type=F32).astype(BF16).astype(F32)
    k1 = kv[:, :half]
    k2 = kv[:, half:head_dim]
    c1 = cos_a[:, :half]
    s1 = sin_a[:, :half]
    key = jnp.concatenate([k1 * c1 - k2 * s1, k2 * c1 + k1 * s1], axis=1).astype(BF16)
    value = kv[:, head_dim:].astype(BF16)
    k_scr[...] = key
    v_scr[...] = value
    small_outs = [pltpu.make_async_copy(k_scr, k_out, z_sem.at[0]),
                  pltpu.make_async_copy(v_scr, v_out, z_sem.at[1])]
    for copy in small_outs:
        copy.start()
    for h in range(heads):
        krep[pl.ds(h, own, stride=heads), :] = key.astype(F32)
        vrep[pl.ds(h, own, stride=heads), :] = value.astype(F32)

    x_wait("q")
    for xc in range(xs // 2):
        qa = qx_buf[2 * xc].astype(F32)
        qb = qx_buf[2 * xc + 1].astype(F32)
        ra = (qa * cos_a - qb * sin_a).astype(BF16).astype(F32)
        rb = (qb * cos_a + qa * sin_a).astype(BF16).astype(F32)
        for yc in range(ys):
            pair = jnp.concatenate([ra[:, yc * half:(yc + 1) * half], rb[:, yc * half:(yc + 1) * half]], axis=1)
            q2d[pl.ds(xc * ys + yc, own, stride=heads), :] = pair
    scale = head_dim ** -0.5
    snew[...] = jnp.sum(q2d[...] * krep[...], axis=1, keepdims=True) * scale

    gr = per * heads
    seg_r = lax.broadcasted_iota(jnp.int32, (gr, per * head_dim), 0) // heads
    seg_c = lax.broadcasted_iota(jnp.int32, (gr, per * head_dim), 1) // head_dim
    diag = (seg_r == seg_c).astype(F32)
    tile = min(512, slots)
    row_g = lax.broadcasted_iota(jnp.int32, (gr, 1), 0) // heads
    lane_g = lax.broadcasted_iota(jnp.int32, (gr, tile), 1)

    def attend(g, carry):
        cache_copy(g, k_hbm, k_buf, 0).wait()
        qg = q2d[rows(g, gr), :]
        qbd = (jnp.concatenate([qg] * per, axis=1) * diag).astype(BF16)
        len_g = jnp.zeros((gr, 1), jnp.int32)
        for s in range(per):
            len_g = jnp.where(row_g == s, lens[first_row + g * per + s], len_g)
        new = snew[rows(g, gr), :]
        top = jnp.full((gr, tile), -jnp.inf, F32)
        kg = k_buf.at[g]
        vg = v_buf.at[g]
        for c in range(slots // tile):
            kc = kg[:, :, pl.ds(c * tile, tile)].reshape(per * head_dim, tile)
            sc = jnp.dot(qbd, kc, preferred_element_type=F32) * scale
            sc = jnp.where(lane_g < len_g - c * tile, sc, -jnp.inf)
            s_scr[:, pl.ds(c * tile, tile)] = sc
            top = jnp.maximum(top, sc)
        row_max = jnp.maximum(jnp.max(top, axis=1, keepdims=True), new)
        total = jnp.zeros((gr, tile), F32)
        for c in range(slots // tile):
            ex = jnp.exp(s_scr[:, pl.ds(c * tile, tile)] - row_max)
            s_scr[:, pl.ds(c * tile, tile)] = ex
            total = total + ex
        w_new = jnp.exp(new - row_max)
        den = jnp.sum(total, axis=1, keepdims=True) + w_new
        inv = 1.0 / den
        cache_copy(g, v_hbm, v_buf, 1).wait()
        mixed = jnp.zeros((gr, per * head_dim), F32)
        for c in range(slots // tile):
            pr = (s_scr[:, pl.ds(c * tile, tile)] * inv).astype(BF16)
            vc = vg[:, :, pl.ds(c * tile, tile)].reshape(per * head_dim, tile)
            mixed = mixed + lax.dot_general(pr, vc, NT, preferred_element_type=F32)
        add = (w_new * inv).astype(BF16).astype(F32) * vrep[rows(g, gr), :]
        for s in range(per):
            od_scr[pl.ds(pl.multiple_of(g * gr + s * heads, heads), heads), :] = (
                mixed[s * heads:(s + 1) * heads, s * head_dim:(s + 1) * head_dim]
                + add[s * heads:(s + 1) * heads, :])
        return carry

    lax.fori_loop(0, groups, attend, 0)
    for xc in range(xs // 2):
        parts = [od_scr[pl.ds(xc * ys + yc, own, stride=heads), :] for yc in range(ys)]
        o_scr[2 * xc] = jnp.concatenate([p[:, :half] for p in parts], axis=1).astype(BF16)
        o_scr[2 * xc + 1] = jnp.concatenate([p[:, half:] for p in parts], axis=1).astype(BF16)
    x_start("o")
    for c in range(7, 12):
        e_start(c)

    def act_copy(dest):
        return pltpu.make_async_remote_copy(
            src_ref=act_scr.at[dest], dst_ref=act.at[:, pl.ds(pl.multiple_of(y * ff, ff), ff)],
            send_sem=y_send.at[len(y_kinds)], recv_sem=y_recv.at[len(y_kinds)],
            device_id={"yax": dest}, device_id_type=pl.DeviceIdType.MESH)

    x_wait("gate")
    x_wait("up")

    def feed(d, carry):
        @pl.when(d < ys - 1)
        def _():
            n_copy(d + 1, lax.rem(y + ys - d - 1, ys)).wait_recv()
            n_pass(d + 1, core).start()
        j = lax.rem(y + ys - d, ys)

        @pl.when(d > 0)
        def _():
            n_pass(d, 1 - core).wait_recv()
        gu = jnp.dot(n_all[rows(j, quarter), :], gu_buf[...], preferred_element_type=F32)
        gu = gu.astype(BF16).astype(F32)
        gate = gu[:, :ff]
        act_scr[j] = (gate * jax.nn.sigmoid(gate) * gu[:, ff:]).astype(BF16)

        @pl.when(d > 0)
        def _():
            act_copy(j).start()
        return carry
    lax.fori_loop(0, ys, feed, 0)
    act[:, pl.ds(pl.multiple_of(y * ff, ff), ff)] = act_scr[y]
    y_wait("wo")
    x_wait("o")
    part_scr[...] = jnp.dot(
        ox_buf[...], out_buf[...].reshape(ys * cols, xs * blk), preferred_element_type=F32)
    y_wait("down")

    arrived(act_scr.at[others], y_recv.at[len(y_kinds)])

    down_all = down_buf[...].reshape(ys * ff, xs * blk)
    part_scr[...] = part_scr[...] + jnp.dot(act[...], down_all, preferred_element_type=F32)

    def branch(c):
        for i in range(chips):
            rs_scr[c, i] = part_scr[pl.ds(pl.multiple_of((2 * i + c) * own, own), own), :]

    def pre_copy():
        return pltpu.make_async_remote_copy(
            src_ref=rs_scr.at[1 - core], dst_ref=pre_buf, send_sem=pre_sem.at[0], recv_sem=pre_sem.at[1],
            device_id={"xax": partner}, device_id_type=pl.DeviceIdType.MESH)

    def rs_copy(dest):
        return pltpu.make_async_remote_copy(
            src_ref=rs_scr.at[core, dest], dst_ref=rs_buf.at[chip], send_sem=rs_sem.at[0],
            recv_sem=rs_sem.at[1], device_id={"xax": 2 * dest + core},
            device_id_type=pl.DeviceIdType.MESH)

    chip = x // 2
    branch(1 - core)
    pre_copy().start()
    branch(core)
    pre_copy().wait_recv()
    rs_scr[core] = rs_scr[core] + pre_buf[...]

    def rs_start(i, carry):
        rs_copy(lax.rem(chip + far(i, chips), chips)).start()
        return carry
    lax.fori_loop(1, chips, rs_start, 0)
    e_start(12)
    arrived(rs_buf.at[pl.ds(0, chips - 1)], rs_sem.at[1])
    rs_buf[chip] = rs_scr[core, chip]
    res = h_buf[rows(x, own), :].astype(F32) + jnp.sum(rs_buf[...], axis=0)
    f_buf[rows(mine, own), :] = layer_norm(res, gf_buf[...]).astype(BF16)

    piece = own // 2

    def f_half(sy, sx, h):
        return f_buf.at[pl.ds(pl.multiple_of((sy * xs + sx) * own + h * piece, piece), piece), :]

    def f_over_x(i, h, sy, sx, sem):
        return pltpu.make_async_remote_copy(
            src_ref=f_half(sy, sx, h), dst_ref=f_half(sy, sx, h), send_sem=f_sem.at[0], recv_sem=sem,
            device_id={"xax": lax.rem(x + 2 * i, xs)}, device_id_type=pl.DeviceIdType.MESH)

    def f_over_y(d, h, sy, sx, sem):
        return pltpu.make_async_remote_copy(
            src_ref=f_half(sy, sx, h), dst_ref=f_half(sy, sx, h), send_sem=f_sem.at[0], recv_sem=sem,
            device_id={"yax": lax.rem(y + d, ys)}, device_id_type=pl.DeviceIdType.MESH)

    def f_pass(d, h, sy, sx):
        pltpu.make_async_remote_copy(
            src_ref=f_half(sy, sx, h), dst_ref=f_half(sy, sx, h), send_sem=f_sem.at[1],
            recv_sem=f_sem.at[2 + d], device_id={"xax": partner},
            device_id_type=pl.DeviceIdType.MESH).start()

    def from_y(d):
        return lax.rem(y + ys - d, ys)

    def from_x(i):
        return lax.rem(x + xs - 2 * i, xs)

    def spread_y(i):
        def body(d, carry):
            f_over_y(far(d, ys), 0, y, from_x(i), fya.at[far(d, ys), i]).start()
            return carry
        lax.fori_loop(1, ys, body, 0)

    def spread_x(d):
        def body(i, carry):
            f_over_x(far(i, chips), 1, from_y(d), x, fxb.at[d, far(i, chips)]).start()
            return carry
        lax.fori_loop(1, chips, body, 0)

    def first_x(i, carry):
        f_over_x(far(i, chips), 0, y, x, fxa.at[far(i, chips)]).start()
        return carry
    lax.fori_loop(1, chips, first_x, 0)

    def first_y(d, carry):
        f_over_y(far(d, ys), 1, y, x, fyb.at[far(d, ys)]).start()
        return carry
    lax.fori_loop(1, ys, first_y, 0)
    spread_y(0)
    spread_x(0)
    f_pass(0, 0, y, x)
    f_pass(0, 1, y, x)
    e_start(13)
    for i in sorted(range(1, max(chips, ys)), key=lambda d: (min(d, max(chips, ys) - d), d)):
        if i < chips:
            f_over_x(i, 0, y, from_x(i), fxa.at[i]).wait_recv()
            spread_y(i)
            f_pass(0, 0, y, from_x(i))
        if i < ys:
            f_over_y(i, 1, from_y(i), x, fyb.at[i]).wait_recv()
            spread_x(i)
            f_pass(i, 1, from_y(i), x)
    for c in range(14, EMBED_CHUNKS):
        e_start(c)

    def collect(d):
        def body(i, carry):
            @pl.when(d > 0)
            def _():
                f_over_y(d, 0, from_y(d), from_x(i), fya.at[d, i]).wait_recv()
                f_pass(d, 0, from_y(d), from_x(i))

            @pl.when(i > 0)
            def _():
                f_over_x(i, 1, from_y(d), from_x(i), fxb.at[d, i]).wait_recv()
                f_pass(d, 1, from_y(d), from_x(i))
            return carry
        lax.fori_loop(0, chips, body, 0)

    for name in x_kinds:
        x_drain(name)
    for name in g_kinds:
        g_drain(name)
    for name in y_kinds:
        y_drain(name)
    arrived(act_scr.at[others], y_send.at[len(y_kinds)])
    for i in range(2):
        arrived(n_all.at[pl.ds(0, (ys - 1) * part), :], n_send.at[i])
    pre_copy().wait_send()
    arrived(rs_buf.at[pl.ds(0, chips - 1)], rs_sem.at[0])
    for copy in small_outs:
        copy.wait()

    cut = e_parts[EMBED_FIRST][0]
    skip = core * shift
    half_block = pl.ds(0, chips * own)

    def nearest(k):
        return k + k // 2 * (1 - 2 * lax.rem(k, 2))

    def z_copy(j, r0, n):
        return pltpu.make_async_copy(
            z_scr.at[j, pl.ds(r0, n), :], logits_out.at[pl.ds(r0, n), rows(j, quarter)], z_sem.at[2])

    def block(j, r0, n, pieces):
        r = pl.ds(r0, n)
        z_scr[j, r, :] = lax.dot_general(e_buf[r, :], f_buf[rows(j, quarter), :], NT, preferred_element_type=F32)
        z_copy(j, r0, n).start()
        stats = []
        for q0, m in row_chunks(n, pieces):
            z = z_scr[j, pl.ds(r0 + q0, m), :]
            if shift and (r0 + q0 == 0 or r0 + q0 + m == window):
                index = lax.broadcasted_iota(jnp.int32, z.shape, 0) + (r0 + q0)
                z = jnp.where(jnp.logical_and(index >= skip, index < skip + vocab), z, -jnp.inf)
            top = jnp.max(z, axis=0, keepdims=True)
            stats.append((top, jnp.sum(jnp.exp(z - top), axis=0, keepdims=True)))
        return stats

    def put(j, stats):
        top = functools.reduce(jnp.maximum, [t for t, _ in stats])
        st_scr[0:1, rows(j, quarter)] = top
        st_scr[1:2, rows(j, quarter)] = sum(t * jnp.exp(m - top) for m, t in stats)

    def head(k, carry):
        d = nearest(k)
        j = from_y(d)
        arrived(f_buf.at[half_block, :], f_sem.at[2 + d])
        put(j, block(j, 0, cut, 4))

        @pl.when(k < ys - 2)
        def _():
            collect(nearest(k + 2))
        return carry

    def head_rest(j, carry):
        before = (st_scr[0:1, rows(j, quarter)], st_scr[1:2, rows(j, quarter)])
        put(j, [before] + block(j, cut, window - cut, 1))
        return carry

    for k in range(min(2, ys)):
        collect(nearest(k))
    e_own().wait()
    arrived(e_buf.at[pl.ds(0, cut), most], e_recv.at[0])

    lax.fori_loop(0, ys, head, 0)
    arrived(e_buf.at[pl.ds(cut, window - cut), most], e_recv.at[1])
    lax.fori_loop(0, ys, head_rest, 0)

    for k in range(ys):
        dy = (ys // 2 + k) % ys
        for dx in range(xs):
            if dy + dx > 0:
                pltpu.make_async_remote_copy(
                    src_ref=st_scr, dst_ref=s_buf.at[mine], send_sem=s_sem.at[0], recv_sem=s_sem.at[1],
                    device_id={"yax": lax.rem(y + dy, ys), "xax": lax.rem(x + dx, xs)},
                    device_id_type=pl.DeviceIdType.MESH).start()
    s_buf[mine] = st_scr[...]

    arrived(e_buf.at[:, most], e_send)
    arrived(f_buf.at[pl.ds(0, 2 * (ys * chips - 1) * piece), :], f_sem.at[0])
    arrived(f_buf.at[pl.ds(0, ys * chips * own), :], f_sem.at[1])
    arrived(z_scr, z_sem.at[2])
    everyone = s_buf.at[pl.ds(0, ys * xs - 1)]
    arrived(everyone, s_sem.at[1])
    tops = s_buf[:, 0, :]
    best = jnp.max(tops, axis=0, keepdims=True)
    whole = jnp.sum(s_buf[:, 1, :] * jnp.exp(tops - best), axis=0, keepdims=True)
    norm_scr[...] = best + jnp.log(whole)
    norm_copy = pltpu.make_async_copy(norm_scr, norm_out, z_sem.at[0])
    norm_copy.start()
    arrived(everyone, s_sem.at[0])
    norm_copy.wait()


def finish_kernel(shift, z_hbm, norm_hbm, key, value, out_hbm, k_out, v_out, norm_out,
                  z_buf, o_buf, norm, k_scr, v_scr, in_sem, out_sem):
    count, n, width = o_buf.shape

    def load(i):
        return pltpu.make_async_copy(z_hbm.at[:, pl.ds(i * width, width)], z_buf.at[i], in_sem.at[i])

    def save(i):
        return pltpu.make_async_copy(o_buf.at[i], out_hbm.at[:, pl.ds(i * width, width)], out_sem.at[i])

    small = ((norm_hbm, norm, norm_out), (key, k_scr, k_out), (value, v_scr, v_out))
    small_in = [pltpu.make_async_copy(a, b, in_sem.at[count + i]) for i, (a, b, _) in enumerate(small)]
    small_out = [pltpu.make_async_copy(b, c, out_sem.at[count + i]) for i, (_, b, c) in enumerate(small)]
    small_in[0].start()
    for i in range(count):
        load(i).start()
    for copy in small_in[1:]:
        copy.start()
    small_in[0].wait()
    small_out[0].start()
    odd = lax.rem(lax.axis_index("xax"), 2) == 1
    for i in range(count):
        row = norm[:, pl.ds(i * width, width)]
        load(i).wait()
        if shift:
            @pl.when(odd)
            def _():
                o_buf[i] = z_buf[i, pl.ds(shift, n), :] - row

            @pl.when(jnp.logical_not(odd))
            def _():
                o_buf[i] = z_buf[i, pl.ds(0, n), :] - row
        else:
            o_buf[i] = z_buf[i] - row
        save(i).start()
    for i in (1, 2):
        small_in[i].wait()
        small_out[i].start()
    for copy in small_out:
        copy.wait()
    for i in range(count):
        save(i).wait()


def solution(mesh):
    ys = mesh.shape["yax"]
    xs = mesh.shape["xax"]
    row_spec = P(("dp", "yax", "xax"))

    def local_step(hidden, cache_len, k_cache, v_cache, g_attn, w_query, w_key, w_value,
                   w_gate, w_up, w_out, w_down, g_final, embedding):
        batch, blk = hidden.shape
        own, slots, head_dim = k_cache.shape
        width = blk * xs
        vocab = embedding.shape[0] // xs
        shift = vocab % 8
        window = -(-vocab // 8) * 8
        half = head_dim // 2
        quarter = xs * own
        cols = w_query.shape[1] // xs
        ff = w_gate.shape[1] // xs
        heads = w_query.shape[1] * ys // head_dim
        per = 4
        groups = own // per
        freq_row = (ROPE_BASE ** (-(np.arange(half, dtype=np.float32) * 2.0) / head_dim)).astype(np.float32)
        freq = jnp.asarray(np.tile(freq_row, 4)[None, :])
        any_spec = pl.BlockSpec(memory_space=pl.ANY)
        dma = pltpu.SemaphoreType.DMA
        chips = xs // 2
        scratch = [
            pltpu.VMEM((groups, per, head_dim, slots), BF16),
            pltpu.VMEM((groups, per, head_dim, slots), BF16),
            pltpu.VMEM((quarter, width), BF16),
            pltpu.VMEM((1, width), F32),
            pltpu.VMEM((1, width), F32),
            pltpu.VMEM((w_query.shape[1], blk), BF16),
            pltpu.VMEM((ys, cols, width), BF16),
            pltpu.VMEM((width, 2 * ff), BF16),
            pltpu.VMEM((ys, ff, width), BF16),
            pltpu.VMEM((ys, cols, width), BF16),
            pltpu.VMEM((2 * head_dim, width), BF16),
            pltpu.VMEM((batch, width), BF16),
            pltpu.VMEM((quarter, ys * cols), BF16),
            pltpu.VMEM((xs, own, ys * cols), BF16),
            pltpu.VMEM((own * heads, head_dim), F32),
            pltpu.VMEM((own * heads, 1), F32),
            pltpu.VMEM((own * heads, head_dim), F32),
            pltpu.VMEM((own * heads, head_dim), F32),
            pltpu.VMEM((per * heads, slots), F32),
            pltpu.VMEM((own * heads, head_dim), F32),
            pltpu.VMEM((xs, own, ys * cols), BF16),
            pltpu.VMEM((quarter, ys * cols), BF16),
            pltpu.VMEM((ys, quarter, ff), BF16),
            pltpu.VMEM((quarter, ys * ff), BF16),
            pltpu.VMEM((quarter, width), F32),
            pltpu.VMEM((chips, own, width), F32),
            pltpu.VMEM((2, chips, own, width), F32),
            pltpu.VMEM((chips, own, width), F32),
            pltpu.VMEM((batch, width), BF16),
            pltpu.VMEM((window, width), BF16),
            pltpu.VMEM((ys, window, quarter), F32),
            pltpu.VMEM((2, batch), F32),
            pltpu.VMEM((own, head_dim), BF16),
            pltpu.VMEM((own, head_dim), BF16),
            pltpu.VMEM((1, batch), F32),
            pltpu.VMEM((ys * xs, 2, batch), F32),
            pltpu.SMEM(cache_len.shape, jnp.int32),
            pltpu.VMEM(w_query.shape, BF16),
            pltpu.VMEM((1, 4 * half), F32),
            dma((2, groups)), dma, dma((3,)), dma((7,)), dma((7,)),
            dma((5,)), dma((5, chips)), dma((5,)), dma((4,)), dma((4,)), dma, dma((2,)),
            dma((ys,)), dma((ys,)), dma((2,)), dma((2,)), dma((2,)),
            dma((chips,)), dma((ys,)), dma((ys, chips)), dma((ys, chips)), dma((2 + ys,)), dma((2,)),
        ]
        cfg = (ys, xs, own, vocab, shift)
        key_new, value_new, logits, norm = pl.pallas_call(
            functools.partial(kernel, cfg),
            name="decode_layer",
            out_shape=(
                jax.ShapeDtypeStruct((own, head_dim), BF16),
                jax.ShapeDtypeStruct((own, head_dim), BF16),
                jax.ShapeDtypeStruct((window, batch), F32),
                jax.ShapeDtypeStruct((1, batch), F32)),
            in_specs=[any_spec] * 15,
            out_specs=(any_spec, any_spec, any_spec, any_spec),
            scratch_shapes=scratch,
            compiler_params=pltpu.CompilerParams(
                collective_id=0, has_side_effects=True, vmem_limit_bytes=67043328),
        )(cache_len, hidden, k_cache.transpose(0, 2, 1), v_cache.transpose(0, 2, 1),
          g_attn[None, :], g_final[None, :], w_query, w_key.T, w_value.T, w_gate, w_up, w_out, w_down,
          embedding, freq)
        count = 8
        log_probs, key_new, value_new, norm = pl.pallas_call(
            functools.partial(finish_kernel, shift),
            name="finish",
            out_shape=(
                jax.ShapeDtypeStruct((vocab, batch), F32),
                jax.ShapeDtypeStruct((own, head_dim), BF16),
                jax.ShapeDtypeStruct((own, head_dim), BF16),
                jax.ShapeDtypeStruct((1, batch), F32)),
            in_specs=[any_spec] * 4,
            out_specs=(any_spec,) * 4,
            scratch_shapes=[
                pltpu.VMEM((count, window, batch // count), F32),
                pltpu.VMEM((count, vocab, batch // count), F32),
                pltpu.VMEM((1, batch), F32), pltpu.VMEM((own, head_dim), BF16), pltpu.VMEM((own, head_dim), BF16),
                dma((count + 3,)), dma((count + 3,))],
        )(logits, norm, key_new, value_new)
        return key_new, value_new, log_probs.T, norm[0]

    in_specs = (P("dp", "xax"), P("dp"), row_spec, row_spec, P("xax"), P("xax", "yax"),
                P("xax", None), P("xax", None), P("xax", "yax"), P("xax", "yax"),
                P("yax", "xax"), P("yax", "xax"), P("xax"), P("yax", "xax"))
    out_specs = (row_spec, row_spec, P("dp", ("yax", "xax")), P("dp"))
    return jax.shard_map(local_step, mesh=mesh, in_specs=in_specs, out_specs=out_specs, check_vma=False)
```
